32 devices in a mesh: fsdp: 8 (over z, y), ctx: 4 (over x, core).
Axes of the slice: x: 2, y: 2, z: 4, core: 2. Of those that a mesh axis runs over, the one named last changes fastest.
Arguments:
- tokens: bfloat16 [32768, 1024], P(('fsdp', 'ctx')), may hold values from -6 to 6
- valid_mask: int32 [32768], P(('fsdp', 'ctx')), may hold values from 0 to 1, as said below
- stretch_start: int32 [128], P(('fsdp', 'ctx')), may hold values from 0 to 1, as said below
- cotangent: bfloat16 [32768, 1024], P(('fsdp', 'ctx')), may hold values from -6 to 6
- norm_gain: float32 [1024], replicated, may hold values from 0.1 to 1.9
- in_weight: bfloat16 [1024, 4384], P(('fsdp', 'ctx')), may hold values from -0.1875 to 0.1875
- conv_weight: float32 [4, 2304], replicated, may hold values from -2 to 2
- conv_bias: float32 [2304], replicated, may hold values from -0.5 to 0.5
- step_bias: float32 [32], replicated, may hold values from -6 to -2
- decay_log: float32 [32], replicated, may hold values from -5 to 1.5
- skip_gain: float32 [32], replicated, may hold values from 0.5 to 1.5
- gate_gain: float32 [2048], replicated, may hold values from 0.1 to 1.9
- out_weight: bfloat16 [2048, 1024], P(('fsdp', 'ctx')), may hold values from -0.125 to 0.125
Outputs:
- output: bfloat16 [32768, 1024], P(('fsdp', 'ctx'))
- input_grad: float32 [32768, 1024], P(('fsdp', 'ctx'))
- in_weight_grad: float32 [1024, 4384], P(('fsdp', 'ctx'))
- out_weight_grad: float32 [2048, 1024], P(('fsdp', 'ctx'))
- norm_gain_grad: float32 [1024], replicated
- conv_weight_grad: float32 [4, 2304], replicated
- conv_bias_grad: float32 [2304], replicated
- step_bias_grad: float32 [32], replicated
- decay_log_grad: float32 [32], replicated
- skip_gain_grad: float32 [32], replicated
- gate_gain_grad: float32 [2048], replicated
The draws below stay inside these ranges and needn't reach their ends.
Inputs may be any that keep to these rules, and one draw needn't show every extreme that they name: `stretch_start`: each group of 4096 tokens holds whole sequences laid end to end, each beginning at a stretch of 256 tokens; a sequence's first stretch lies a multiple of 4 stretches into its group, so the group's first stretch always begins one. A sequence's padding is only the tail of its last stretch; each sequence has 1024 tokens or more. `valid_mask`: 1 exactly for the tokens of sequences as described for stretch_start.
All inputs are finite; a program needn't handle non-finite values.
Results may differ from the reference program's by a relative error of at most 0.0092.
Values may be sent and summed in bfloat16 or wider, within the bound.
A program may use at most 320 MiB of HBM per device.

```python
import jax
import jax.numpy as jnp
from jax import lax

D = 1024
DI = 2048
HEADS = 32
P_SIZE = 64
N = 128
CONVK = 4
Q = 256
MINC = 4
CH = 2304
DPROJ = 4384
GROUP_TOK = 4096
GROUPS = 8
TOKENS = 32768


def sequence_layout(key):
    mixed_key = jax.random.fold_in(key, 11)
    start_key, pad_key = jax.random.split(mixed_key)
    per_group = GROUP_TOK // Q
    column = jnp.arange(per_group)
    candidate = jnp.logical_and(column % MINC == 0, column > 0)
    coin_flips = jax.random.randint(start_key, (GROUPS, per_group), 0, 2)
    starts = jnp.where(column[None, :] == 0, 1, jnp.where(candidate[None, :], coin_flips, 0)).astype(jnp.int32)
    seq_ids = jnp.cumsum(starts, axis=1) - 1
    member = (seq_ids[:, :, None] == column[None, None, :]).astype(jnp.int32)
    lengths = jnp.sum(member, axis=1)
    span_stretches = jnp.sum(member * lengths[:, None, :], axis=2)
    closing = jnp.concatenate([starts[:, 1:], jnp.ones((GROUPS, 1), jnp.int32)], axis=1)
    padding = jax.random.randint(pad_key, (GROUPS, per_group), 0, Q) * (span_stretches > MINC).astype(jnp.int32) * closing
    inside = jnp.arange(Q)
    valid_tokens = (inside[None, None, :] < (Q - padding)[:, :, None]).astype(jnp.int32)
    return (starts.reshape(-1), valid_tokens.reshape(-1))


def draw_stretch_start(key, part):
    return sequence_layout(key)[0]


def draw_valid_mask(key, part):
    return sequence_layout(key)[1]


def spiked(entries, stream_key, source, target, parts, factor):
    owner, partner = [(jnp.arange(entries.shape[axis_at]) // (entries.shape[axis_at] // parts)).reshape([-1 if axis == axis_at else 1 for axis in range(entries.ndim)]) for axis_at in (source, target)]
    chosen = jax.random.permutation(stream_key, parts)[partner]
    strong = (owner == chosen) | (owner == (partner + parts // 2) % parts)
    return jnp.where(strong, factor * entries, entries)


def block_levels(rng, extent, pieces, least, high):
    def one(axis_at, shards_of):
        draws = jax.random.uniform(jax.random.fold_in(jax.random.fold_in(rng, 6), axis_at), (shards_of,), jnp.float32, least / len(pieces), high / len(pieces))
        return jnp.repeat(jnp.exp(draws), extent[axis_at] // shards_of).reshape((-1,) + (1,) * (len(extent) - axis_at - 1))

    level = one(*pieces[0])
    for cut in pieces[1:]:
        level = level * one(*cut)
    return level


def noise(key, extent, spread, bound, cuts=(), kind=jnp.bfloat16):
    level = block_levels(key, extent, cuts, -0.22, 0.18) if cuts else 1.0
    values = jax.random.normal(key, extent, jnp.float32) * spread * level
    return jnp.minimum(jnp.maximum(values, -bound), bound).astype(kind)


def heavy_noise(key, extent, scale, limit, cuts, heavy, held_as=jnp.bfloat16):
    drawn = scale * jax.random.normal(key, extent, jnp.float32)
    if cuts:
        drawn = drawn * block_levels(key, extent, cuts, -0.22, 0.18)
    return jnp.clip(spiked(drawn, jax.random.fold_in(key, 3), *heavy), -limit, limit).astype(held_as)


def setup_inputs(seed: int = 0) -> dict:
    splits = jax.random.split(jax.random.key(seed), 14)
    return {
        "tokens": heavy_noise(splits[0], (TOKENS, D), 1.0, 6.0, ((0, 32),), (0, 1, 32, 2.75)),
        "valid_mask": draw_valid_mask(jax.random.fold_in(splits[13], 71), 0),
        "stretch_start": draw_stretch_start(jax.random.fold_in(splits[13], 71), 0),
        "cotangent": noise(splits[3], (TOKENS, D), 1.0, 6.0, ((0, 32),)),
        "norm_gain": jnp.clip(1.0 + 0.18 * jax.random.normal(splits[4], (D,), jnp.float32), 0.1, 1.9),
        "in_weight": noise(splits[5], (D, DPROJ), D ** -0.5, 0.1875, ((0, 32),)),
        "conv_weight": noise(splits[6], (CONVK, CH), 0.5, 2.0, (), jnp.float32),
        "conv_bias": jnp.clip(jax.random.uniform(splits[7], (CH,), jnp.float32, -0.5, 0.5), -0.5, 0.5),
        "step_bias": jnp.clip(jax.random.uniform(splits[8], (HEADS,), jnp.float32, -6.0, -2.0), -6.0, -2.0),
        "decay_log": jnp.clip(jax.random.uniform(splits[9], (HEADS,), jnp.float32, -5.0, 1.5), -5.0, 1.5),
        "skip_gain": jnp.clip(jax.random.uniform(splits[10], (HEADS,), jnp.float32, 0.5, 1.5), 0.5, 1.5),
        "gate_gain": jnp.clip(1.0 + 0.18 * jax.random.normal(splits[11], (DI,), jnp.float32), 0.1, 1.9),
        "out_weight": noise(splits[12], (DI, D), DI ** -0.5, 0.125, ((0, 32),)),
    }


epsilon = 1e-05
exact_mode = lax.Precision.HIGHEST

@jax.custom_vjp
def low(v):
    return lax.optimization_barrier(v.astype(jnp.bfloat16)).astype(jnp.float32)

@jax.custom_vjp
def low_back(v):
    return v

def low_keep(v):
    return (low(v), None)

def low_pass(kept, grad):
    return (grad,)

def back_keep(v):
    return (v, None)

def back_low(kept, grad):
    return (low(grad),)
low.defvjp(low_keep, low_pass)
low_back.defvjp(back_keep, back_low)

def rms_scale(values_in, gain):
    return values_in * lax.rsqrt(lax.optimization_barrier(jnp.mean(values_in * values_in, axis=-1, keepdims=True)) + epsilon) * gain

def lower_ones(length):
    return (jnp.arange(length)[:, None] >= jnp.arange(length)[None, :]).astype(jnp.float32)

def first_section(blocked, edge_rows, keep_state, valid_blocks, conv_weight, conv_bias, step_bias, decay_log):
    stretches = blocked.shape[0]
    width = blocked.shape[1]
    gate_in = blocked[:, :, :DI]
    conv_in = blocked[:, :, DI:DI + CH]
    step_raw = blocked[:, :, DI + CH:]
    tail_rows = CONVK - 1
    history = jnp.concatenate([edge_rows[None], conv_in[:-1, width - tail_rows:]], axis=0) * keep_state[:, None, None]
    padded = jnp.concatenate([history, conv_in], axis=1)
    convolved = conv_bias + jnp.zeros_like(conv_in)
    for offset in range(CONVK):
        convolved = convolved + conv_weight[offset] * padded[:, offset:offset + width]
    activated = jax.nn.silu(convolved)
    values = activated[:, :, :DI].reshape(stretches, width, HEADS, P_SIZE)
    in_map = activated[:, :, DI:DI + N]
    out_map = activated[:, :, DI + N:]
    step_size = jax.nn.softplus(step_raw + step_bias) * valid_blocks[:, :, None]
    decay_rate = -jnp.exp(decay_log)
    log_decay = jnp.einsum('qs,csh->chq', lower_ones(width), step_size * decay_rate, precision=exact_mode)
    values_low = low(values)
    in_low = low(in_map)
    out_low = low(out_map)
    intersection = low_back(jnp.einsum('cqn,csn->cqs', out_low, in_low, precision=exact_mode))
    causal = lower_ones(width) > 0.5
    log_ratio = log_decay[:, :, :, None] - log_decay[:, :, None, :]
    decay_map = jnp.where(causal, jnp.exp(jnp.where(causal, log_ratio, 0.0)), 0.0)
    step_heads = jnp.swapaxes(step_size, 1, 2)
    mixing = low(intersection[:, None] * decay_map * step_heads[:, :, None, :])
    local_out = jnp.einsum('chqs,cshp->cqhp', mixing, values_low, precision=exact_mode)
    log_total = log_decay[:, :, -1]
    state_weight = jnp.exp(log_total[:, :, None] - log_decay) * step_heads
    weighted = low(values * jnp.swapaxes(state_weight, 1, 2)[:, :, :, None])
    stretch_states = low_back(jnp.einsum('cshp,csn->chpn', weighted, in_low, precision=exact_mode))
    stretch_decay = jnp.exp(log_total)
    return (local_out, values, out_low, log_decay, stretch_states, stretch_decay, gate_in)

def second_section(local_out, values, out_low, log_decay, stretch_states, stretch_decay, gate_in, keep_state, start_state, skip_gain, gate_gain):

    def advance(carried, element):
        state_in, decay_in, keep_in = element
        entering_now = keep_in * carried
        return (decay_in[:, None, None] * entering_now + state_in, entering_now)
    unused, entering = lax.scan(advance, start_state, (stretch_states, stretch_decay, keep_state))
    part = low_back(jnp.einsum('cqn,chpn->cqhp', out_low, low(entering), precision=exact_mode))
    remote_out = part * jnp.swapaxes(jnp.exp(log_decay), 1, 2)[:, :, :, None]
    ssd_out = low_back(local_out + remote_out + skip_gain[:, None] * values)
    row_count = ssd_out.shape[0] * ssd_out.shape[1]
    mixed = ssd_out.reshape(row_count, DI) * jax.nn.silu(gate_in.reshape(row_count, DI))
    return low(rms_scale(mixed, gate_gain))

def layer_forward(inputs, valid_blocks, keep_state, norm_gain, in_weight, conv_weight, conv_bias, step_bias, decay_log, skip_gain, gate_gain, out_weight):
    normed = low(rms_scale(inputs, norm_gain))
    projected = low_back(jnp.dot(normed, in_weight, precision=exact_mode))
    stretches = inputs.shape[0] // Q
    edge_rows = jnp.zeros((CONVK - 1, CH), jnp.float32)
    firsts = first_section(projected.reshape(stretches, Q, DPROJ), edge_rows, keep_state, valid_blocks, conv_weight, conv_bias, step_bias, decay_log)
    start_state = jnp.zeros((HEADS, P_SIZE, N), jnp.float32)
    gated = second_section(*firsts, keep_state, start_state, skip_gain, gate_gain)
    branch = jnp.dot(gated, out_weight, precision=exact_mode)
    return inputs + valid_blocks.reshape(-1)[:, None] * branch

def reference(tokens, valid_mask, stretch_start, cotangent, norm_gain, in_weight, conv_weight, conv_bias, step_bias, decay_log, skip_gain, gate_gain, out_weight):
    groups = tokens.shape[0] // GROUP_TOK
    inputs = tokens.astype(jnp.float32).reshape(groups, GROUP_TOK, D)
    cot_all = cotangent.astype(jnp.float32).reshape(groups, GROUP_TOK, D)
    valid_all = valid_mask.astype(jnp.float32).reshape(groups, GROUP_TOK // Q, Q)
    keep_all = 1.0 - stretch_start.astype(jnp.float32).reshape(groups, GROUP_TOK // Q)
    params = (norm_gain.astype(jnp.float32), in_weight.astype(jnp.float32), conv_weight.astype(jnp.float32), conv_bias.astype(jnp.float32), step_bias.astype(jnp.float32), decay_log.astype(jnp.float32), skip_gain.astype(jnp.float32), gate_gain.astype(jnp.float32), out_weight.astype(jnp.float32))

    def group_step(totals, element):
        group_in, group_valid, group_keep, group_cot = element

        def closed(inputs_here, *weights_here):
            return layer_forward(inputs_here, group_valid, group_keep, *weights_here)
        result, back_fn = jax.vjp(closed, group_in, *params)
        grads = back_fn(group_cot)
        totals = tuple((total + grad for total, grad in zip(totals, grads[1:])))
        return (totals, (result.astype(jnp.bfloat16), grads[0]))
    zero_grads = tuple((jnp.zeros_like(weight_here) for weight_here in params))
    totals, (results, input_grads) = lax.scan(group_step, zero_grads, (inputs, valid_all, keep_all, cot_all))
    output = results.reshape(tokens.shape[0], D)
    input_grad = input_grads.reshape(tokens.shape[0], D)
    return (output, input_grad, totals[1], totals[8], totals[0], totals[2], totals[3], totals[4], totals[5], totals[6], totals[7])
```

```python
import jax
import jax.numpy as jnp
from jax import lax
from jax.experimental import pallas as pl
from jax.experimental.pallas import tpu as pltpu
from jax.sharding import PartitionSpec as P

DI = 2048
HEADS = 32
P_SIZE = 64
N = 128
CONVK = 4
Q = 256
CH = 2304
DPROJ = 4384
UW = CH + 128
GW = 256
GROUPS = DI // GW
HALF = Q // 2

F32 = jnp.float32
BF16 = jnp.bfloat16
LOG2E = 1.4426950408889634
epsilon = 1e-05


def nn(a, b):
    return lax.dot_general(a, b, (((1,), (0,)), ((), ())), preferred_element_type=F32)


def nt(a, b):
    return lax.dot_general(a, b, (((1,), (1,)), ((), ())), preferred_element_type=F32)


def sigmoid(x):
    return 0.5 * jnp.tanh(0.5 * x) + 0.5


def softplus(x):
    e = jnp.exp(-jnp.abs(x))
    w = 1.0 + e
    d = w - 1.0
    return jnp.maximum(x, 0.0) + jnp.where(d == 0.0, e, jnp.log(w) * (e / jnp.where(d == 0.0, 1.0, d)))


def rows_of(shape):
    return lax.broadcasted_iota(jnp.int32, shape, 0)


def lanes_of(shape):
    return lax.broadcasted_iota(jnp.int32, shape, 1)


def split3(x):
    a = x.astype(BF16)
    r = x - a.astype(F32)
    b = r.astype(BF16)
    return a, b, (r - b.astype(F32)).astype(BF16)


def ordered_sum(triangle, x):
    a, b, c = split3(x)
    return nn(triangle, c) + nn(triangle, b) + nn(triangle, a)


def spread(x, out):
    out[0] = x
    for g in range(1, GROUPS):
        out[g] = pltpu.roll(x, 128 - 4 * g, 1)


def spread_rows(x, out):
    for g in range(GROUPS):
        out[g, 0:4] = x[4 * g : 4 * g + 4]


def head_lanes(x, i):
    return jnp.broadcast_to(x[:, i : i + 1], (x.shape[0], 128))


def pick_heads(g):
    shape = (GW, 128)
    return jnp.where(
        lax.shift_right_logical(rows_of(shape), 6) + 4 * g == lanes_of(shape), 1.0, 0.0
    ).astype(BF16)


def forward_kernel(
    u_ref, halo_ref, valid_ref, keep_ref, cw_ref, cb_ref, sb_ref, dl_ref, skip_ref,
    val_ref, vp_ref, conv_ref, bc_ref, ssd_ref, ent_ref, log_ref, step_ref, cum_ref, fin_ref,
    xpad, logs, steps, logt, inter, state,
):
    c = pl.program_id(0)

    @pl.when(c == 0)
    def _():
        xpad[0:8, :] = halo_ref[:, :CH] * keep_ref[0, 0]
        state[...] = jnp.zeros_like(state)
        cum_ref[...] = jnp.zeros_like(cum_ref)

    @pl.when(c > 0)
    def _():
        xpad[0:8, :] = xpad[Q : Q + 8, :]

    xpad[8 : 8 + Q, :] = u_ref[:, :CH]
    raw = u_ref[:, CH:] + sb_ref[...]
    step = softplus(raw) * valid_ref[...]
    step = jnp.where(lanes_of(step.shape) < HEADS, step, 0.0)
    rate = -jnp.exp(dl_ref[...]) * LOG2E
    square = (Q, Q)
    causal = rows_of(square) >= lanes_of(square)
    logd = ordered_sum(jnp.where(causal, 1.0, 0.0).astype(BF16), step * rate)
    log_ref[...] = logd
    step_ref[...] = step
    spread(logd, logs)
    spread(step, steps)
    spread_rows(logd.T, logt)
    half = lanes_of((Q, 128)) < P_SIZE

    def convolved(cols):
        total = cb_ref[:, cols] + cw_ref[0:1, cols] * xpad[5 : 5 + Q, cols]
        for k in range(1, CONVK):
            total = total + cw_ref[k : k + 1, cols] * xpad[5 + k : 5 + k + Q, cols]
        return total

    conv_b = convolved(pl.ds(DI, N))
    conv_c = convolved(pl.ds(DI + N, N))
    conv_ref[:, DI : DI + N] = conv_b.astype(BF16)
    conv_ref[:, DI + N :] = conv_c.astype(BF16)
    act_b = conv_b * sigmoid(conv_b)
    act_c = conv_c * sigmoid(conv_c)
    low_b = act_b.astype(BF16)
    low_c = act_c.astype(BF16)
    bc_ref[:, :N] = low_b
    bc_ref[:, N:] = low_c
    turned_b = act_b.T.astype(BF16)
    inter[...] = jnp.where(causal, nt(low_c, low_b), 0.0)
    ent_ref[0] = state[...].astype(BF16)

    def group(g, unused):
        lg = logs[g]
        sg = steps[g]
        for j in range(2):
            cols = pl.ds(pl.multiple_of(g * GW + 128 * j, 128), 128)
            cv = convolved(cols)
            conv_ref[:, cols] = cv.astype(BF16)
            val = cv * sigmoid(cv)
            val_ref[:, cols] = val.astype(BF16)
            lb = [head_lanes(lg, 2 * j), head_lanes(lg, 2 * j + 1)]
            lp = jnp.where(half, lb[0], lb[1])
            sp = jnp.where(half, head_lanes(sg, 2 * j), head_lanes(sg, 2 * j + 1))
            vp = val * sp
            vp_ref[:, cols] = vp.astype(BF16)
            last = lp[Q - 1 : Q, :]
            weighted = (vp * jnp.exp2(last - lp)).astype(BF16)
            state[:, cols] = jnp.exp2(last) * state[:, cols] + nn(turned_b, weighted)
            cum_ref[c + 1, :, cols] = cum_ref[c, :, cols] + last
            v0 = jnp.where(half, vp, 0.0).astype(BF16)
            v1 = jnp.where(half, 0.0, vp).astype(BF16)
            top = []
            low = []
            for i in range(2):
                row = logt[g, 2 * j + i : 2 * j + i + 1]
                early, late = row[:, :HALF], row[:, HALF:]
                up, down = lb[i][:HALF], lb[i][HALF:]
                top.append((inter[:HALF, :HALF] * jnp.exp2(jnp.minimum(up - early, 0.0))).astype(BF16))
                low.append((inter[HALF:, :HALF] * jnp.exp2(jnp.minimum(down - early, 0.0))).astype(BF16))
                low.append((inter[HALF:, HALF:] * jnp.exp2(jnp.minimum(down - late, 0.0))).astype(BF16))
            skipped = skip_ref[:, cols] * val
            first = nn(jnp.concatenate(top, 1), jnp.concatenate([v0[:HALF], v1[:HALF]], 0))
            second = nn(jnp.concatenate(low, 1), jnp.concatenate([v0, v1], 0))
            ssd_ref[:HALF, cols] = (first + skipped[:HALF]).astype(BF16)
            ssd_ref[HALF:, cols] = (second + skipped[HALF:]).astype(BF16)
        return unused

    lax.fori_loop(0, GROUPS, group, 0)

    @pl.when(c == pl.num_programs(0) - 1)
    def _():
        fin_ref[:N, :] = state[...].astype(BF16)
        a, b, d = split3(cum_ref[c + 1, 0:1, :])
        shape = (16, DI)
        r = rows_of(shape)
        pick = jnp.where(r == 0, jnp.broadcast_to(a.astype(F32), shape), 0.0)
        pick = jnp.where(r == 1, jnp.broadcast_to(b.astype(F32), shape), pick)
        pick = jnp.where(r == 2, jnp.broadcast_to(d.astype(F32), shape), pick)
        pick = jnp.where(r == 3, keep_ref[0, 0], pick)
        fin_ref[N:, :] = pick.astype(BF16)


def decays_and_keeps(tail_ref, count):
    decays = []
    keeps = []
    for k in range(count):
        rows = tail_ref[k].astype(F32)
        decays.append(jnp.exp2(rows[0:1] + rows[1:2] + rows[2:3]))
        keeps.append(rows[3:4])
    return decays, keeps


def gate_kernel(
    pos_ref, keep_ref, all_ref, tail_ref, ssd_in, ent_ref, z_ref, val_ref, bc_ref, log_ref, cum_ref,
    tok_ref, cot_ref, valid_ref, ow_ref, gain_ref,
    out_ref, gated_ref, bg_ref, ds_ref, dz_ref, entt_ref, gnext_ref, gout_ref, dlp_ref, dc_ref, sums_ref,
    start, gstate, logs, ssd_s, mix_s, el_s, pe_s, gg_s, acc,
):
    i = pl.program_id(0)
    c = pl.num_programs(0) - 1 - i

    @pl.when(i == 0)
    def _():
        count = all_ref.shape[0]
        decays, keeps = decays_and_keeps(tail_ref, count)
        pos = pos_ref[0, 0]
        for k in range(count):
            factor = jnp.where(k < pos, keep_ref[0, 0], 0.0) * jnp.ones((1, DI), F32)
            for m in range(k + 1, count):
                factor = factor * jnp.where(m < pos, decays[m] * keeps[m], 1.0)
            term = factor * all_ref[k].astype(F32)
            start[...] = term if k == 0 else start[...] + term
        gstate[...] = jnp.zeros_like(gstate)
        sums_ref[...] = jnp.zeros_like(sums_ref)

    spread(log_ref[...], logs)
    low_c = bc_ref[:, N:]
    turned_c = low_c.astype(F32).T.astype(BF16)
    half = lanes_of((Q, 128)) < P_SIZE
    acc[...] = jnp.zeros_like(acc)

    def enter(g, unused):
        lg = logs[g]
        cols = pl.ds(pl.multiple_of(g * GW, GW), GW)
        entering = (
            ent_ref[0, :, cols].astype(F32) + jnp.exp2(cum_ref[c, 0:1, cols]) * start[:, cols]
        ).astype(BF16)
        entt_ref[0, :, cols] = entering
        part = nn(low_c, entering)
        for j in range(2):
            pc = pl.ds(pl.multiple_of(g * GW + 128 * j, 128), 128)
            el = jnp.exp2(jnp.where(half, head_lanes(lg, 2 * j), head_lanes(lg, 2 * j + 1)))
            pe = el * part[:, 128 * j : 128 * j + 128]
            el_s[:, pc] = el
            pe_s[:, pc] = pe
            ssd = ssd_in[:, pc].astype(F32) + pe
            z = z_ref[:, pc].astype(F32)
            mixed = ssd * (z * sigmoid(z))
            ssd_s[:, pc] = ssd
            mix_s[:, pc] = mixed
            acc[...] += mixed * mixed
        return unused

    lax.fori_loop(0, GROUPS, enter, 0)
    inv = lax.rsqrt(jnp.sum(acc[...], axis=1, keepdims=True) * (1.0 / DI) + epsilon)
    inv = jnp.broadcast_to(inv, (Q, 128))
    valid = valid_ref[...]
    valid8 = jnp.concatenate([valid] * (tok_ref.shape[1] // 128), 1)
    branch_grad = (cot_ref[...].astype(F32) * valid8).astype(BF16)
    bg_ref[...] = branch_grad
    acc[...] = jnp.zeros_like(acc)

    def gate(g, unused):
        cols = pl.ds(pl.multiple_of(g * GW, GW), GW)
        ggrad = nt(branch_grad, ow_ref[cols, :])
        for j in range(2):
            pc = pl.ds(pl.multiple_of(g * GW + 128 * j, 128), 128)
            hat = mix_s[:, pc] * inv
            gain = gain_ref[:, pc]
            mix_s[:, pc] = hat
            gated_ref[:, pc] = (hat * gain).astype(BF16)
            gg = ggrad[:, 128 * j : 128 * j + 128]
            both = gg * hat
            sums_ref[0:1, pc] += jnp.sum(both, axis=0, keepdims=True)
            acc[...] += both * gain
            gg_s[:, pc] = gg * gain
        return unused

    lax.fori_loop(0, GROUPS, gate, 0)
    mean = jnp.sum(acc[...], axis=1, keepdims=True) * (1.0 / DI)
    mean = jnp.broadcast_to(mean, (Q, 128))

    for n in range(tok_ref.shape[1] // 256):
        cols = slice(256 * n, 256 * n + 256)
        branch = nn(gated_ref[...], ow_ref[:, cols])
        out_ref[:, cols] = (tok_ref[:, cols].astype(F32) + valid8[:, :256] * branch).astype(BF16)

    acc[...] = jnp.zeros_like(acc)
    dc_ref[...] = jnp.zeros_like(dc_ref)

    def back(g, unused):
        cols = pl.ds(pl.multiple_of(g * GW, GW), GW)
        dparts = []
        prods = []
        for j in range(2):
            pc = pl.ds(pl.multiple_of(g * GW + 128 * j, 128), 128)
            dmixed = inv * (gg_s[:, pc] - mix_s[:, pc] * mean)
            z = z_ref[:, pc].astype(F32)
            s = sigmoid(z)
            ds = (dmixed * (z * s)).astype(BF16)
            ds_ref[:, pc] = ds
            dz_ref[:, pc] = (dmixed * ssd_s[:, pc] * (s * (1.0 + z * (1.0 - s)))).astype(BF16)
            ds = ds.astype(F32)
            sums_ref[1:2, pc] += jnp.sum(ds * val_ref[:, pc].astype(F32), axis=0, keepdims=True)
            dparts.append((ds * el_s[:, pc]).astype(BF16))
            prods.append((ds * pe_s[:, pc]).astype(BF16))
        dpart = jnp.concatenate(dparts, 1)
        acc[...] += nn(jnp.concatenate(prods, 1), pick_heads(g))
        dc_ref[...] += nt(dpart, entt_ref[0, :, cols])
        gnext_ref[0, :, cols] = gstate[:, cols].astype(BF16)
        total = cum_ref[c + 1, 0:1, cols] - cum_ref[c, 0:1, cols]
        gstate[:, cols] = nn(turned_c, dpart) + jnp.exp2(total) * gstate[:, cols]
        return unused

    lax.fori_loop(0, GROUPS, back, 0)
    dlp_ref[...] = acc[...]

    @pl.when(c == 0)
    def _():
        gout_ref[...] = gstate[...].astype(BF16)


def mixing_kernel(ds_ref, vp_ref, bc_ref, log_ref, dvp_ref, dbc_ref, dlt_ref, logs, logt, inter, dinter, rowsum, turned, colsum):
    logd = log_ref[...]
    spread(logd, logs)
    spread_rows(logd.T, logt)
    low_b = bc_ref[:, :N]
    low_c = bc_ref[:, N:]
    square = (Q, Q)
    causal = rows_of(square) <= lanes_of(square)
    inter[...] = jnp.where(causal, nt(low_b, low_c), 0.0)
    dinter[...] = jnp.zeros_like(dinter)
    half = lanes_of((Q, 128)) < P_SIZE
    lane = lanes_of((HALF, 128))

    def group(g, unused):
        lg = logs[g]
        first_col = jnp.zeros((HALF, 128), F32)
        second_col = jnp.zeros((HALF, 128), F32)
        for j in range(2):
            cols = pl.ds(pl.multiple_of(g * GW + 128 * j, 128), 128)
            vp = vp_ref[:, cols].astype(F32)
            ds = ds_ref[:, cols]
            wide = ds.astype(F32)
            first = []
            second = []
            outs = []
            for i in range(2):
                head = 2 * j + i
                own = half if i == 0 else jnp.logical_not(half)
                vm = jnp.where(own, vp, 0.0).astype(BF16)
                dsm = jnp.where(own, wide, 0.0).astype(BF16)
                outs.append(dsm)
                row = logt[g, head : head + 1]
                early, late = row[:, :HALF], row[:, HALF:]
                lb = head_lanes(lg, head)
                up, down = lb[:HALF], lb[HALF:]
                dup = nt(vm[:HALF], ds)
                ddown = nt(vm[HALF:], ds[HALF:])
                decay = jnp.exp2(jnp.minimum(early - up, 0.0))
                grad = dup[:, :HALF] * decay
                dinter[:HALF, :HALF] += grad
                part = inter[:HALF, :HALF]
                first.append((part * decay).astype(BF16))
                both = grad * part
                row_early = jnp.sum(both, axis=0, keepdims=True)
                col = both
                decay = jnp.exp2(jnp.minimum(late - up, 0.0))
                grad = dup[:, HALF:] * decay
                dinter[:HALF, HALF:] += grad
                part = inter[:HALF, HALF:]
                first.append((part * decay).astype(BF16))
                both = grad * part
                row_late = jnp.sum(both, axis=0, keepdims=True)
                col = jnp.sum(col + both, axis=1, keepdims=True)
                first_col = jnp.where(lane == head, col, first_col)
                decay = jnp.exp2(jnp.minimum(late - down, 0.0))
                grad = ddown * decay
                dinter[HALF:, HALF:] += grad
                part = inter[HALF:, HALF:]
                second.append((part * decay).astype(BF16))
                both = grad * part
                row_late = row_late + jnp.sum(both, axis=0, keepdims=True)
                col = jnp.sum(both, axis=1, keepdims=True)
                second_col = jnp.where(lane == head, col, second_col)
                rowsum[g, head : head + 1, :HALF] = row_early
                rowsum[g, head : head + 1, HALF:] = row_late
            dvp_ref[:HALF, cols] = nn(
                jnp.concatenate(first, 1), jnp.concatenate(outs, 0)
            ).astype(BF16)
            dvp_ref[HALF:, cols] = nn(
                jnp.concatenate(second, 1), jnp.concatenate([outs[0][HALF:], outs[1][HALF:]], 0)
            ).astype(BF16)
        colsum[g, :HALF] = first_col
        colsum[g, HALF:] = second_col
        return unused

    lax.fori_loop(0, GROUPS, group, 0)
    turned[...] = jnp.zeros_like(turned)
    for g in range(GROUPS):
        turned[4 * g : 4 * g + 4] = rowsum[g, 0:4]
    total = turned[...].T
    for g in range(GROUPS):
        total = total - (colsum[g] if g == 0 else pltpu.roll(colsum[g], 4 * g, 1))
    dlt_ref[...] = total
    masked = jnp.where(causal, dinter[...], 0.0)
    dbc_ref[:, :N] = nn(masked.astype(BF16), low_c)
    dbc_ref[:, N:] = nn(masked.T.astype(BF16), low_b)


def back_kernel(
    pos_ref, keep_ref, all_ref, tail_ref, gnext_ref, entt_ref, cum_ref, vp_ref, val_ref, dvp_ref, ds_ref, conv_ref,
    u_ref, halo_ref, bc_ref, log_ref, step_ref, valid_ref, dlp_ref, dlt_ref, dbc_ref, dc_ref,
    cw_ref, sb_ref, dl_ref, skip_ref,
    du_ref, last_ref, edge_ref, sums_ref, small_ref,
    gin, logs, steps, dpad, head, epad, dlw, dst, drow,
):
    i = pl.program_id(0)
    top = pl.num_programs(0)
    c = top - 1 - i

    @pl.when(i == 0)
    def _():
        count = all_ref.shape[0]
        decays, keeps = decays_and_keeps(tail_ref, count)
        pos = pos_ref[0, 0]
        for k in range(count):
            factor = jnp.where(k > pos, keeps[k], 0.0)
            for m in range(k):
                factor = factor * jnp.where(m > pos, decays[m] * keeps[m], 1.0)
            term = factor * all_ref[k].astype(F32)
            gin[...] = term if k == 0 else gin[...] + term
        head[...] = jnp.zeros_like(head)
        sums_ref[...] = jnp.zeros_like(sums_ref)
        small_ref[...] = jnp.zeros_like(small_ref)

    spread(log_ref[...], logs)
    spread(step_ref[...], steps)
    low_b = bc_ref[:, :N]
    half = lanes_of((Q, 128)) < P_SIZE
    dlw[...] = jnp.zeros_like(dlw)
    dst[...] = jnp.zeros_like(dst)
    drow[...] = jnp.zeros_like(drow)

    def conv_back(cols, dact):
        cv = conv_ref[:, cols].astype(F32)
        s = sigmoid(cv)
        dcv = dact * (s * (1.0 + cv * (1.0 - s)))
        dpad[:Q, cols] = dcv
        dpad[Q:, cols] = head[:, cols]
        head[:, cols] = dcv[:8]
        x = u_ref[:, cols]
        sums_ref[4:5, cols] += jnp.sum(dcv, axis=0, keepdims=True)
        total = None
        for j in range(CONVK):
            k = CONVK - 1 - j
            moved = dcv if j == 0 else dpad[j : j + Q, cols]
            sums_ref[k : k + 1, cols] += jnp.sum(moved * x, axis=0, keepdims=True)
            term = cw_ref[k : k + 1, cols] * moved
            total = term if total is None else total + term
        du_ref[:, cols] = total.astype(BF16)

        @pl.when(i == 0)
        def _():
            last_ref[:, cols] = total[Q - 8 :]

    def group(g, db):
        lg = logs[g]
        sg = steps[g]
        cols = pl.ds(pl.multiple_of(g * GW, GW), GW)
        done = cum_ref[c + 1, 0:1, cols]
        after = jnp.exp2(cum_ref[top, 0:1, cols] - done)
        grad = gnext_ref[0, :, cols].astype(F32) + after * gin[:, cols]
        low_g = grad.astype(BF16)
        decay = jnp.exp2(done - cum_ref[c, 0:1, cols])
        row = decay * jnp.sum(grad * entt_ref[0, :, cols].astype(F32), axis=0, keepdims=True)
        coarse = row.astype(BF16).astype(F32)
        r = rows_of((16, GW))
        two = jnp.where(r == 0, jnp.broadcast_to(coarse, (16, GW)), 0.0)
        two = jnp.where(r == 1, jnp.broadcast_to(row - coarse, (16, GW)), two)
        chosen = pick_heads(g)
        drow[...] += nn(two.astype(BF16), chosen)
        dweighted = nn(low_b, low_g)
        weights = []
        moves = []
        stepped = []
        dacts = []
        for j in range(2):
            pc = pl.ds(pl.multiple_of(g * GW + 128 * j, 128), 128)
            lp = jnp.where(half, head_lanes(lg, 2 * j), head_lanes(lg, 2 * j + 1))
            sp = jnp.where(half, head_lanes(sg, 2 * j), head_lanes(sg, 2 * j + 1))
            fade = jnp.exp2(lp[Q - 1 : Q, :] - lp)
            vp = vp_ref[:, pc].astype(F32)
            faded = dweighted[:, 128 * j : 128 * j + 128] * fade
            weights.append((vp * fade).astype(BF16))
            moves.append((faded * vp).astype(BF16))
            both = dvp_ref[:, pc].astype(F32) + faded
            stepped.append((both * val_ref[:, pc].astype(F32)).astype(BF16))
            dacts.append((pc, sp * both + skip_ref[:, pc] * ds_ref[:, pc].astype(F32)))
        dlw[...] += nn(jnp.concatenate(moves, 1), chosen)
        dst[...] += nn(jnp.concatenate(stepped, 1), chosen)
        for pc, dact in dacts:
            conv_back(pc, dact)
        return db + nt(jnp.concatenate(weights, 1), low_g)

    db = lax.fori_loop(0, GROUPS, group, dbc_ref[:, :N])
    conv_back(pl.ds(DI, N), db)
    conv_back(pl.ds(DI + N, N), dbc_ref[:, N:] + dc_ref[...])

    moved = dlw[...]
    at_last = jnp.sum(moved, axis=0, keepdims=True) + drow[0:1] + drow[1:2]
    dlog = dlp_ref[...] + dlt_ref[...] - moved
    dlog = dlog + jnp.where(rows_of(dlog.shape) == Q - 1, at_last, 0.0)
    square = (Q, Q)
    later = jnp.where(rows_of(square) <= lanes_of(square), 1.0, 0.0).astype(BF16)
    dsum = ordered_sum(later, dlog)
    rate = -jnp.exp(dl_ref[...])
    dstep = (dst[...] + dsum * rate) * valid_ref[...]
    raw = u_ref[:, CH:] + sb_ref[...]
    draw = dstep * (1.0 / (1.0 + jnp.exp(-raw)))
    draw = jnp.where(lanes_of(draw.shape) < HEADS, draw, 0.0)
    du_ref[:, CH:] = draw.astype(BF16)
    small_ref[0:1] += jnp.sum(draw, axis=0, keepdims=True)
    small_ref[1:2] += jnp.sum(dsum * step_ref[...], axis=0, keepdims=True) * rate

    @pl.when(c == 0)
    def _():
        epad[0:8, :] = jnp.zeros((8, CH), F32)
        epad[8:16, :] = head[...]
        x = halo_ref[:, :CH] * keep_ref[0, 0]
        total = jnp.zeros((8, CH), F32)
        for j in range(CONVK):
            k = CONVK - 1 - j
            moved = epad[j : j + 8, :]
            sums_ref[k : k + 1, :] += jnp.sum(moved * x, axis=0, keepdims=True)
            total = total + cw_ref[k : k + 1, :] * moved
        edge_ref[...] = total * keep_ref[0, 0]


def spec(block, index):
    return pl.BlockSpec(block, index)


def whole(shape):
    return pl.BlockSpec(shape, lambda *_: (0,) * len(shape))


def scalar():
    return pl.BlockSpec(memory_space=pltpu.SMEM)


def shaped(shape, kind):
    return jax.ShapeDtypeStruct(shape, kind)


def cost(flops, moved):
    return pl.CostEstimate(flops=int(flops), bytes_accessed=int(moved), transcendentals=0)


def params():
    return pltpu.CompilerParams(dimension_semantics=("arbitrary",), vmem_limit_bytes=60 * 1024 * 1024)


LINE = 4


def my_place():
    f = lax.axis_index("fsdp")
    t = lax.axis_index("ctx")
    return f // 2, f % 2, t // 2, t % 2


def device_at(z, y, x, core):
    return {"fsdp": z * 2 + y, "ctx": x * 2 + core}


def order_of(z, y, x, core):
    return (z * 2 + y) * 4 + x * 2 + core


def meet(more=()):
    z, y, x, core = my_place()
    barrier = pltpu.get_barrier_semaphore()
    fixed = [(z, y, x, 1 - core), (z, y, 1 - x, core), (z, 1 - y, x, core)] + list(more)
    for peer in fixed:
        pl.semaphore_signal(
            barrier, inc=1, device_id=device_at(*peer), device_id_type=pl.DeviceIdType.MESH
        )

    @pl.when(z > 0)
    def _():
        pl.semaphore_signal(
            barrier, inc=1, device_id=device_at(z - 1, y, x, core), device_id_type=pl.DeviceIdType.MESH
        )

    @pl.when(z < LINE - 1)
    def _():
        pl.semaphore_signal(
            barrier, inc=1, device_id=device_at(z + 1, y, x, core), device_id_type=pl.DeviceIdType.MESH
        )

    ends = jnp.where(z > 0, 1, 0) + jnp.where(z < LINE - 1, 1, 0)
    pl.semaphore_wait(barrier, len(fixed) + ends)


def send(src, dst, send_sem, recv_sem, peer):
    return pltpu.make_async_remote_copy(
        src_ref=src, dst_ref=dst, send_sem=send_sem, recv_sem=recv_sem,
        device_id=device_at(*peer), device_id_type=pl.DeviceIdType.MESH,
    )


class Gather:
    def __init__(self, own, out, recv, halves, twin, sent, here):
        self.own, self.out, self.rows = own, out, own.shape[0]
        self.recv, self.halves, self.twin, self.sent, self.here = recv, halves, twin, sent, here
        self.place = my_place()

    def block(self, z, y, x, core, half=None):
        size = self.rows if half is None else self.rows // 2
        start = order_of(z, y, x, core) * self.rows + (0 if half is None else half * size)
        return self.out.at[pl.ds(pl.multiple_of(start, 16), size)]

    def copy(self, origin, way, half=None, own=False):
        z, y, x, core = self.place
        oz, oy, ox = origin
        o = oz * 4 + oy * 2 + ox
        dst = self.block(oz, oy, ox, core, half)
        src = self.own if own else dst
        peer = {
            "up": (z + 1, y, x, core), "down": (z - 1, y, x, core), "x": (z, y, 1 - x, core),
            "y": (z, 1 - y, x, core), "twin": (z, y, x, 1 - core),
        }[way]
        sem = self.sent.at[("up", "down", "x", "y", "twin").index(way), o]
        if way == "twin":
            arrival = self.twin.at[o]
        elif half is not None:
            arrival = self.halves.at[half, o]
        else:
            arrival = self.recv.at[o]
        return send(src, dst, sem, arrival, peer)

    def arrived(self, origin, half=None):
        self.copy(origin, "x", half).wait_recv()

    def column(self, r):
        z = self.place[0]
        if r == 0:
            return [(None, z, True, True)]
        return [(z - r >= 0, z - r, True, False), (z + r < LINE, z + r, False, True)]

    def each(self, r, act):
        for valid, oz, below, above in self.column(r):
            if valid is None:
                act(oz, below, above)
            else:
                pl.when(valid)(lambda oz=oz, below=below, above=above: act(oz, below, above))

    def begin(self):
        z, y, x, core = self.place
        pltpu.make_async_copy(self.own, self.block(z, y, x, core), self.here).start()
        self.forward(0)

    def ways(self, oz, below, above, act):
        z = self.place[0]
        if below:
            pl.when(z < LINE - 1)(lambda: act("up"))
        if above:
            pl.when(z > 0)(lambda: act("down"))
        act("x")
        act("y")
        act("twin")

    def forward(self, r):
        z, y, x, core = self.place

        def act(oz, below, above):
            origin = (oz, y, x)
            if r:
                self.arrived(origin)
            self.ways(oz, below, above, lambda way: self.copy(origin, way, own=r == 0).start())

        self.each(r, act)

    def across(self, r):
        z, y, x, core = self.place

        def act(oz, below, above):
            self.arrived((oz, y, 1 - x))
            self.copy((oz, y, 1 - x), "y", 0).start()
            self.copy((oz, y, 1 - x), "twin").start()
            self.arrived((oz, 1 - y, x))
            self.copy((oz, 1 - y, x), "x", 1).start()
            self.copy((oz, 1 - y, x), "twin").start()

        self.each(r, act)

    def corner(self, r):
        z, y, x, core = self.place

        def act(oz, below, above):
            origin = (oz, 1 - y, 1 - x)
            self.arrived(origin, 0)
            self.arrived(origin, 1)
            self.copy(origin, "twin").start()

        self.each(r, act)

    def finish(self):
        z, y, x, core = self.place
        pltpu.make_async_copy(self.own, self.block(z, y, x, core), self.here).wait()
        for r in range(LINE):

            def act(oz, below, above, r=r):
                self.ways(oz, below, above, lambda way: self.copy((oz, y, x), way, own=r == 0).wait_send())
                self.copy((oz, y, 1 - x), "y", 0).wait_send()
                self.copy((oz, 1 - y, x), "x", 1).wait_send()
                for oy, ox in ((y, 1 - x), (1 - y, x), (1 - y, 1 - x)):
                    self.copy((oz, oy, ox), "twin").wait_send()
                for oy, ox in ((y, x), (y, 1 - x), (1 - y, x), (1 - y, 1 - x)):
                    self.copy((oz, oy, ox), "twin").wait_recv()

            self.each(r, act)

    def steps(self):
        return [
            self.begin,
            lambda: self.forward(1),
            lambda: self.across(0),
            lambda: self.forward(2),
            lambda: self.across(1),
            lambda: (self.forward(3), self.corner(0)),
            lambda: self.across(2),
            lambda: self.corner(1),
            lambda: self.across(3),
            lambda: (self.corner(2), self.corner(3)),
            self.finish,
        ]


def gather_scratch():
    dma = pltpu.SemaphoreType.DMA
    return [dma((16,)), dma((2, 16)), dma((16,)), dma((5, 16)), dma(())]


def gather_kernel(count, *refs):
    own, out, sems = refs[:count], refs[count : 2 * count], refs[2 * count :]
    meet()
    lists = [
        Gather(own[k], out[k], *sems[5 * k : 5 * k + 5]).steps() for k in range(count)
    ]
    length = len(lists[0])
    for at in range(length + 2 * (count - 1)):
        for k in range(count):
            if 0 <= at - 2 * k < length:
                lists[k][at - 2 * k]()


def gathered(arrays, number):
    count = len(arrays)
    anywhere = pl.BlockSpec(memory_space=pl.ANY)
    return pl.pallas_call(
        lambda *refs: gather_kernel(count, *refs),
        in_specs=[anywhere] * count,
        out_specs=[anywhere] * count,
        out_shape=[shaped((32 * a.shape[0], a.shape[1]), a.dtype) for a in arrays],
        scratch_shapes=gather_scratch() * count,
        compiler_params=pltpu.CompilerParams(collective_id=number, has_side_effects=True),
        name="gather",
    )(*arrays)


class Scatter:
    def __init__(self, parts, out, twin, got, kept, mixed_y, mixed_x, from_x, from_y, up, down, sems):
        self.parts, self.out = parts, out
        self.got, self.kept = got, kept
        self.mixed = (mixed_y, mixed_x)
        self.sides = (from_x, from_y)
        self.up, self.down = up, down
        self.twin_sent, self.twin_recv, self.sent, self.recv, self.line_sent, self.line_recv = sems
        self.place = my_place()
        self.rows = parts.shape[-2]

    def groups(self):
        z, y, x, core = self.place
        return [(1 - y, 1 - x), (y, 1 - x), (1 - y, x), (y, x)]

    def to_twin(self, k):
        z, y, x, core = self.place
        gy, gx = self.groups()[k]
        return send(
            self.parts.at[:, gy, gx, 1 - core], self.got.at[k], self.twin_sent.at[k], self.twin_recv.at[k],
            (z, y, x, 1 - core),
        )

    def begin(self):
        for k in range(4):
            self.to_twin(k).start()

    def both(self, k):
        z, y, x, core = self.place
        gy, gx = self.groups()[k]
        self.to_twin(k).wait_recv()
        for b in range(LINE):
            total = self.parts[b, gy, gx, core].astype(F32) + self.got[k, b].astype(F32)
            self.kept[k, b] = total.astype(BF16)

    def corner_copy(self, half):
        z, y, x, core = self.place
        size = self.rows // 2
        src = self.kept.at[0, :, pl.ds(half * size, size)]
        peer = (z, 1 - y, x, core) if half == 0 else (z, y, 1 - x, core)
        return send(src, self.mixed[half], self.sent.at[half], self.recv.at[half], peer)

    def side_copy(self, k):
        z, y, x, core = self.place
        peer = (z, y, 1 - x, core) if k == 1 else (z, 1 - y, x, core)
        return send(self.kept.at[k], self.sides[k - 1], self.sent.at[1 + k], self.recv.at[1 + k], peer)

    def corners(self):
        self.both(0)
        self.corner_copy(0).start()
        self.corner_copy(1).start()
        self.both(1)
        self.both(2)
        self.both(3)

    def sides_out(self):
        size = self.rows // 2
        for half, k in ((0, 1), (1, 2)):
            self.corner_copy(half).wait_recv()
            rows = slice(half * size, half * size + size)
            for b in range(LINE):
                total = self.kept[k, b, rows].astype(F32) + self.mixed[half][b].astype(F32)
                self.kept[k, b, rows] = total.astype(BF16)
            self.side_copy(k).start()

    def sides_in(self):
        self.side_copy(1).wait_recv()
        self.side_copy(2).wait_recv()
        for b in range(LINE):
            total = self.kept[3, b].astype(F32) + self.sides[0][b].astype(F32) + self.sides[1][b].astype(F32)
            self.kept[3, b] = total.astype(BF16)

    def line_copy(self, oz, way):
        z, y, x, core = self.place
        buffer = self.up if way == 0 else self.down
        peer = (z + 1, y, x, core) if way == 0 else (z - 1, y, x, core)
        return send(
            self.kept.at[3, oz], buffer.at[oz], self.line_sent.at[way, oz], self.line_recv.at[way, oz], peer
        )

    def line(self, r):
        z = self.place[0]

        def upward():
            oz = z + r

            @pl.when(z > 0)
            def _():
                self.line_copy(oz, 0).wait_recv()
                total = self.kept[3, oz].astype(F32) + self.up[oz].astype(F32)
                self.kept[3, oz] = total.astype(BF16)

            self.line_copy(oz, 0).start()

        def downward():
            oz = z - r

            @pl.when(z < LINE - 1)
            def _():
                self.line_copy(oz, 1).wait_recv()
                total = self.kept[3, oz].astype(F32) + self.down[oz].astype(F32)
                self.kept[3, oz] = total.astype(BF16)

            self.line_copy(oz, 1).start()

        pl.when(z + r < LINE)(upward)
        pl.when(z - r >= 0)(downward)

    def finish(self):
        z = self.place[0]
        self.out[...] = self.kept[3, z].astype(F32)

        @pl.when(z > 0)
        def _():
            self.line_copy(z, 0).wait_recv()
            self.out[...] += self.up[z].astype(F32)

        @pl.when(z < LINE - 1)
        def _():
            self.line_copy(z, 1).wait_recv()
            self.out[...] += self.down[z].astype(F32)

        for k in range(4):
            self.to_twin(k).wait_send()
        for half in range(2):
            self.corner_copy(half).wait_send()
        for k in (1, 2):
            self.side_copy(k).wait_send()
        for r in range(1, LINE):
            pl.when(z + r < LINE)(lambda r=r: self.line_copy(z + r, 0).wait_send())
            pl.when(z - r >= 0)(lambda r=r: self.line_copy(z - r, 1).wait_send())

    def steps(self):
        return [
            self.begin, self.corners, self.sides_out, self.sides_in, lambda: self.line(3), lambda: self.line(2),
            lambda: self.line(1), self.finish,
        ]


def scatter_scratch(rows, columns):
    dma = pltpu.SemaphoreType.DMA
    half = rows // 2
    return [
        pltpu.VMEM((4, LINE, rows, columns), BF16),
        pltpu.VMEM((4, LINE, rows, columns), BF16),
        pltpu.VMEM((LINE, half, columns), BF16),
        pltpu.VMEM((LINE, half, columns), BF16),
        pltpu.VMEM((LINE, rows, columns), BF16),
        pltpu.VMEM((LINE, rows, columns), BF16),
        pltpu.VMEM((LINE, rows, columns), BF16),
        pltpu.VMEM((LINE, rows, columns), BF16),
        dma((4,)), dma((4,)), dma((4,)), dma((4,)), dma((2, LINE)), dma((2, LINE)),
    ]


class Total:
    def __init__(self, own, out, held, got, sent, recv):
        self.own, self.out, self.held, self.got, self.sent, self.recv = own, out, held, got, sent, recv

    def copy(self, k):
        z, y, x, core = my_place()
        near = z + 1 - 2 * (z % 2)
        peer = [
            (z, y, x, 1 - core), (z, y, 1 - x, core), (z, 1 - y, x, core), (near, y, x, core),
            ((z + 2) % LINE, y, x, core),
        ][k]
        return send(self.own if k == 0 else self.held.at[k], self.got.at[k], self.sent.at[k], self.recv.at[k], peer)

    def begin(self):
        self.copy(0).start()

    def turn(self, k):
        self.copy(k).wait_recv()
        mine = self.own[...] if k == 0 else self.held[k]
        total = mine + self.got[k]
        if k < 4:
            self.held[k + 1] = total
            self.copy(k + 1).start()
        else:
            self.out[...] = total

    def finish(self):
        for k in range(5):
            self.copy(k).wait_send()

    def steps(self):
        return [self.begin] + [lambda k=k: self.turn(k) for k in range(5)] + [self.finish]


def scatter_kernel(count, *refs):
    parts, small = refs[:count], refs[count]
    outs, small_out = refs[count + 1 : 2 * count + 1], refs[2 * count + 1]
    scratch = refs[2 * count + 2 :]
    z, y, x, core = my_place()
    meet([((z + 2) % LINE, y, x, core)])
    lists = []
    for k in range(count):
        own = scratch[14 * k : 14 * k + 14]
        lists.append(Scatter(parts[k], outs[k], None, *own[:8], own[8:]).steps())
    lists.append(Total(small, small_out, *scratch[14 * count :]).steps())
    for at in range(max(len(each) for each in lists)):
        for each in lists:
            if at < len(each):
                each[at]()


def scattered(arrays, small, number):
    count = len(arrays)
    shapes = [(a.shape[0] // 32, a.shape[1]) for a in arrays]
    dma = pltpu.SemaphoreType.DMA
    scratch = []
    for shape in shapes:
        scratch += scatter_scratch(*shape)
    scratch += [
        pltpu.VMEM((5,) + small.shape, F32), pltpu.VMEM((5,) + small.shape, F32), dma((5,)), dma((5,)),
    ]
    vmem = pl.BlockSpec(memory_space=pltpu.VMEM)
    return pl.pallas_call(
        lambda *refs: scatter_kernel(count, *refs),
        in_specs=[vmem] * (count + 1),
        out_specs=[vmem] * (count + 1),
        out_shape=[shaped(shape, F32) for shape in shapes] + [shaped(small.shape, F32)],
        scratch_shapes=scratch,
        compiler_params=pltpu.CompilerParams(
            collective_id=number, has_side_effects=True, vmem_limit_bytes=60 * 1024 * 1024
        ),
        name="scatter",
    )(*[a.reshape(LINE, 2, 2, 2, s[0], s[1]) for a, s in zip(arrays, shapes)], small)


def local(
    tokens,
    valid_mask,
    stretch_start,
    cotangent,
    norm_gain,
    in_weight,
    conv_weight,
    conv_bias,
    step_bias,
    decay_log,
    skip_gain,
    gate_gain,
    out_weight,
):
    axes = ("fsdp", "ctx")
    rows, width = tokens.shape
    blocks = rows // Q
    near = lax.axis_size("ctx")
    pos = lax.axis_index("ctx").astype(jnp.int32).reshape(1, 1)
    halo_tokens = lax.ppermute(
        tokens[rows - 8 :], "ctx", [(k, k + 1) for k in range(near - 1)]
    )
    own_u = jnp.pad(in_weight[:, DI:], ((0, 0), (0, UW - (DPROJ - DI))))
    own_z = in_weight[:, :DI]
    boxed = lax.axis_size("fsdp") == 8 and near == 4
    if boxed:
        w_u, w_z, w_o = gathered([own_u, own_z, out_weight], 1)
    else:
        w_u, w_z, w_o = [lax.all_gather(a, axes, axis=0, tiled=True) for a in (own_u, own_z, out_weight)]

    def hats(values):
        wide = values.astype(F32)
        return wide * lax.rsqrt(jnp.mean(wide * wide, axis=-1, keepdims=True) + epsilon)

    normed_more = (hats(jnp.concatenate([tokens, halo_tokens], 0)) * norm_gain).astype(BF16)
    normed = normed_more[:rows]
    valid = jnp.broadcast_to(valid_mask.astype(F32)[:, None], (rows, 128))
    keep = (1.0 - stretch_start[0].astype(F32)).reshape(1, 1)
    taps = conv_weight
    shift = conv_bias.reshape(1, CH)
    bias = jnp.pad(step_bias, (0, 128 - HEADS)).reshape(1, 128)
    logs = jnp.pad(decay_log, (0, 128 - HEADS)).reshape(1, 128)
    skips = jnp.repeat(skip_gain, P_SIZE).reshape(1, DI)
    u = jnp.dot(normed_more, w_u, preferred_element_type=F32)
    halo_block = rows // 8

    same = lambda c: (c, 0)
    same3 = lambda c: (c, 0, 0)
    val, vp, conv, bc, ssd, ent, logd, step, cum, fin = pl.pallas_call(
        forward_kernel,
        grid=(blocks,),
        in_specs=[
            spec((Q, UW), same),
            spec((8, UW), lambda c: (halo_block, 0)),
            spec((Q, 128), same),
            scalar(),
            whole((CONVK, CH)),
            whole((1, CH)),
            whole((1, 128)),
            whole((1, 128)),
            whole((1, DI)),
        ],
        out_specs=[
            spec((Q, DI), same),
            spec((Q, DI), same),
            spec((Q, CH), same),
            spec((Q, 2 * N), same),
            spec((Q, DI), same),
            spec((1, N, DI), same3),
            spec((Q, 128), same),
            spec((Q, 128), same),
            whole((blocks + 1, 8, DI)),
            whole((N + 16, DI)),
        ],
        out_shape=[
            shaped((rows, DI), BF16),
            shaped((rows, DI), BF16),
            shaped((rows, CH), BF16),
            shaped((rows, 2 * N), BF16),
            shaped((rows, DI), BF16),
            shaped((blocks, N, DI), BF16),
            shaped((rows, 128), F32),
            shaped((rows, 128), F32),
            shaped((blocks + 1, 8, DI), F32),
            shaped((N + 16, DI), BF16),
        ],
        scratch_shapes=[
            pltpu.VMEM((Q + 8, CH), F32),
            pltpu.VMEM((GROUPS, Q, 128), F32),
            pltpu.VMEM((GROUPS, Q, 128), F32),
            pltpu.VMEM((GROUPS, 8, Q), F32),
            pltpu.VMEM((Q, Q), F32),
            pltpu.VMEM((N, DI), F32),
        ],
        compiler_params=params(),
        cost_estimate=cost(15e9, 60e6),
        name="forward",
    )(u, u, valid, keep, taps, shift, bias, logs, skips)

    z = jnp.dot(normed, w_z, preferred_element_type=F32).astype(BF16)
    everyone = lax.all_gather(fin, "ctx")
    back = lambda i: (blocks - 1 - i, 0)
    back3 = lambda i: (blocks - 1 - i, 0, 0)
    gains = gate_gain.reshape(1, DI)
    output, gated, branch_grad, ds, dz, entt, gnext, gout, dlp, dc, gate_sums = pl.pallas_call(
        gate_kernel,
        grid=(blocks,),
        in_specs=[
            scalar(),
            scalar(),
            whole((near, N, DI)),
            spec((near, 16, DI), lambda i: (0, N // 16, 0)),
            spec((Q, DI), back),
            spec((1, N, DI), back3),
            spec((Q, DI), back),
            spec((Q, DI), back),
            spec((Q, 2 * N), back),
            spec((Q, 128), back),
            whole((blocks + 1, 8, DI)),
            spec((Q, width), back),
            spec((Q, width), back),
            spec((Q, 128), back),
            whole((DI, width)),
            whole((1, DI)),
        ],
        out_specs=[
            spec((Q, width), back),
            spec((Q, DI), back),
            spec((Q, width), back),
            spec((Q, DI), back),
            spec((Q, DI), back),
            spec((1, N, DI), back3),
            spec((1, N, DI), back3),
            whole((N, DI)),
            spec((Q, 128), back),
            spec((Q, N), back),
            whole((8, DI)),
        ],
        out_shape=[
            shaped((rows, width), BF16),
            shaped((rows, DI), BF16),
            shaped((rows, width), BF16),
            shaped((rows, DI), BF16),
            shaped((rows, DI), BF16),
            shaped((blocks, N, DI), BF16),
            shaped((blocks, N, DI), BF16),
            shaped((N, DI), BF16),
            shaped((rows, 128), F32),
            shaped((rows, N), F32),
            shaped((8, DI), F32),
        ],
        scratch_shapes=[
            pltpu.VMEM((N, DI), F32),
            pltpu.VMEM((N, DI), F32),
            pltpu.VMEM((GROUPS, Q, 128), F32),
            pltpu.VMEM((Q, DI), F32),
            pltpu.VMEM((Q, DI), F32),
            pltpu.VMEM((Q, DI), F32),
            pltpu.VMEM((Q, DI), F32),
            pltpu.VMEM((Q, DI), F32),
            pltpu.VMEM((Q, 128), F32),
        ],
        compiler_params=params(),
        cost_estimate=cost(15e9, 60e6),
        name="gate",
    )(
        pos, keep, everyone, everyone, ssd, ent, z, val, bc, logd, cum, tokens, cotangent, valid, w_o, gains,
    )
    everyone_back = lax.all_gather(gout, "ctx")

    dvp, dbc, dlt = pl.pallas_call(
        mixing_kernel,
        grid=(blocks,),
        in_specs=[
            spec((Q, DI), same),
            spec((Q, DI), same),
            spec((Q, 2 * N), same),
            spec((Q, 128), same),
        ],
        out_specs=[spec((Q, DI), same), spec((Q, 2 * N), same), spec((Q, 128), same)],
        out_shape=[shaped((rows, DI), BF16), shaped((rows, 2 * N), F32), shaped((rows, 128), F32)],
        scratch_shapes=[
            pltpu.VMEM((GROUPS, Q, 128), F32),
            pltpu.VMEM((GROUPS, 8, Q), F32),
            pltpu.VMEM((Q, Q), F32),
            pltpu.VMEM((Q, Q), F32),
            pltpu.VMEM((GROUPS, 8, Q), F32),
            pltpu.VMEM((128, Q), F32),
            pltpu.VMEM((GROUPS, Q, 128), F32),
        ],
        compiler_params=params(),
        cost_estimate=cost(15e9, 60e6),
        name="mixing",
    )(ds, vp, bc, logd)

    def columns_of(left, right):
        return lax.dot_general(
            left, right, (((0,), (0,)), ((), ())), preferred_element_type=F32
        ).astype(BF16)

    out_weight_grad = columns_of(gated, branch_grad)
    gate_columns = columns_of(normed, dz)

    du, last, edge, conv_sums, small = pl.pallas_call(
        back_kernel,
        grid=(blocks,),
        in_specs=[
            scalar(),
            scalar(),
            whole((near, N, DI)),
            spec((near, 16, DI), lambda i: (0, N // 16, 0)),
            spec((1, N, DI), back3),
            spec((1, N, DI), back3),
            whole((blocks + 1, 8, DI)),
            spec((Q, DI), back),
            spec((Q, DI), back),
            spec((Q, DI), back),
            spec((Q, DI), back),
            spec((Q, CH), back),
            spec((Q, UW), back),
            spec((8, UW), lambda i: (halo_block, 0)),
            spec((Q, 2 * N), back),
            spec((Q, 128), back),
            spec((Q, 128), back),
            spec((Q, 128), back),
            spec((Q, 128), back),
            spec((Q, 128), back),
            spec((Q, 2 * N), back),
            spec((Q, N), back),
            whole((CONVK, CH)),
            whole((1, 128)),
            whole((1, 128)),
            whole((1, DI)),
        ],
        out_specs=[
            spec((Q, UW), back),
            whole((8, CH)),
            whole((8, CH)),
            whole((8, CH)),
            whole((8, 128)),
        ],
        out_shape=[
            shaped((rows, UW), BF16),
            shaped((8, CH), F32),
            shaped((8, CH), F32),
            shaped((8, CH), F32),
            shaped((8, 128), F32),
        ],
        scratch_shapes=[
            pltpu.VMEM((N, DI), F32),
            pltpu.VMEM((GROUPS, Q, 128), F32),
            pltpu.VMEM((GROUPS, Q, 128), F32),
            pltpu.VMEM((Q + 8, CH), F32),
            pltpu.VMEM((8, CH), F32),
            pltpu.VMEM((16, CH), F32),
            pltpu.VMEM((Q, 128), F32),
            pltpu.VMEM((Q, 128), F32),
            pltpu.VMEM((16, 128), F32),
        ],
        compiler_params=params(),
        cost_estimate=cost(15e9, 60e6),
        name="back",
    )(
        pos, keep, everyone_back, everyone, gnext, entt, cum, vp, val, dvp, ds, conv, u, u, bc, logd, step, valid,
        dlp, dlt, dbc, dc, taps, bias, logs, skips,
    )
    edge_back = lax.ppermute(edge, "ctx", [(k + 1, k) for k in range(near - 1)])
    du = lax.dynamic_update_slice(du, (last + edge_back).astype(BF16), (rows - 8, 0))
    conv_columns = columns_of(normed, du)
    across = (((1,), (1,)), ((), ()))
    normed_grad = lax.dot_general(dz, w_z, across, preferred_element_type=F32) + lax.dot_general(
        du, w_u, across, preferred_element_type=F32
    )
    inputs = tokens.astype(F32)
    scale = lax.rsqrt(jnp.mean(inputs * inputs, axis=-1, keepdims=True) + epsilon)
    hat = inputs * scale
    inner = normed_grad * norm_gain
    input_grad = cotangent.astype(F32) + scale * (
        inner - hat * jnp.mean(inner * hat, axis=-1, keepdims=True)
    )
    norm_grad = jnp.sum(normed_grad * hat, axis=0)
    packed = jnp.concatenate(
        [
            norm_grad,
            conv_sums[:5].reshape(-1),
            gate_sums[:2].reshape(-1),
            small[:2].reshape(-1),
        ]
    )
    if boxed:
        conv_columns, gate_columns, out_weight_grad, summed = scattered(
            [conv_columns, gate_columns, out_weight_grad], packed.reshape(-1, 128), 2
        )
        summed = summed.reshape(-1)
    else:
        conv_columns, gate_columns, out_weight_grad = [
            lax.psum_scatter(a.astype(F32), axes, scatter_dimension=0, tiled=True)
            for a in (conv_columns, gate_columns, out_weight_grad)
        ]
        summed = lax.psum(packed, axes)
    in_weight_grad = jnp.concatenate([gate_columns, conv_columns[:, : DPROJ - DI]], 1)
    at = width
    conv_weight_grad = summed[at : at + CONVK * CH].reshape(CONVK, CH)
    at += CONVK * CH
    conv_bias_grad = summed[at : at + CH]
    at += CH
    gate_gain_grad = summed[at : at + DI]
    at += DI
    skip_gain_grad = jnp.sum(summed[at : at + DI].reshape(HEADS, P_SIZE), axis=1)
    at += DI
    step_bias_grad = summed[at : at + HEADS]
    decay_log_grad = summed[at + 128 : at + 128 + HEADS]
    return (
        output,
        input_grad,
        in_weight_grad,
        out_weight_grad,
        summed[:width],
        conv_weight_grad,
        conv_bias_grad,
        step_bias_grad,
        decay_log_grad,
        skip_gain_grad,
        gate_gain_grad,
    )


def solution(mesh):
    split = P(("fsdp", "ctx"), None)
    line = P(("fsdp", "ctx"))
    return jax.shard_map(
        local,
        mesh=mesh,
        in_specs=(split, line, line, split, P(), split, P(), P(), P(), P(), P(), P(), split),
        out_specs=(split, split, split, split, P(), P(), P(), P(), P(), P(), P()),
        check_vma=False,
    )
```

```python
import jax
import jax.numpy as jnp
from jax import lax
from jax.experimental import pallas as pl
from jax.experimental.pallas import tpu as pltpu
from jax.sharding import PartitionSpec as P

DI = 2048
HEADS = 32
P_SIZE = 64
N = 128
CONVK = 4
Q = 256
CH = 2304
DPROJ = 4384
UW = CH + 128
GW = 256
GROUPS = DI // GW
HALF = Q // 2

F32 = jnp.float32
BF16 = jnp.bfloat16
LOG2E = 1.4426950408889634
epsilon = 1e-05


def nn(a, b):
    return lax.dot_general(a, b, (((1,), (0,)), ((), ())), preferred_element_type=F32)


def nt(a, b):
    return lax.dot_general(a, b, (((1,), (1,)), ((), ())), preferred_element_type=F32)


def sigmoid(x):
    return 0.5 * jnp.tanh(0.5 * x) + 0.5


def softplus(x):
    e = jnp.exp(-jnp.abs(x))
    w = 1.0 + e
    d = w - 1.0
    return jnp.maximum(x, 0.0) + jnp.where(d == 0.0, e, jnp.log(w) * (e / jnp.where(d == 0.0, 1.0, d)))


def rows_of(shape):
    return lax.broadcasted_iota(jnp.int32, shape, 0)


def lanes_of(shape):
    return lax.broadcasted_iota(jnp.int32, shape, 1)


def split3(x):
    a = x.astype(BF16)
    r = x - a.astype(F32)
    b = r.astype(BF16)
    return a, b, (r - b.astype(F32)).astype(BF16)


def ordered_sum(triangle, x):
    a, b, c = split3(x)
    return nn(triangle, c) + nn(triangle, b) + nn(triangle, a)


def spread(x, out):
    out[0] = x
    for g in range(1, GROUPS):
        out[g] = pltpu.roll(x, 128 - 4 * g, 1)


def spread_rows(x, out):
    for g in range(GROUPS):
        out[g, 0:4] = x[4 * g : 4 * g + 4]


def head_lanes(x, i):
    return jnp.broadcast_to(x[:, i : i + 1], (x.shape[0], 128))


def pick_heads(g):
    shape = (GW, 128)
    return jnp.where(
        lax.shift_right_logical(rows_of(shape), 6) + 4 * g == lanes_of(shape), 1.0, 0.0
    ).astype(BF16)


def quietly(act):
    act()


def when_at(now, plan):
    for place, act in plan:
        pl.when(now == place)(lambda act=act: quietly(act))


def chain_peers():
    pos = lax.axis_index("ctx")
    return [(pos > 0, {"ctx": pos - 1}), (pos < lax.axis_size("ctx") - 1, {"ctx": pos + 1})]


def pass_on(message, arrived, sems, by):
    return pltpu.make_async_remote_copy(
        src_ref=message, dst_ref=arrived, send_sem=sems.at[0], recv_sem=sems.at[1],
        device_id={"ctx": lax.axis_index("ctx") + by}, device_id_type=pl.DeviceIdType.MESH,
    )


def forward_kernel(count, *refs):
    (
        u_ref, halo_ref, valid_ref, keep_ref, cw_ref, cb_ref, sb_ref, dl_ref, skip_ref,
    ) = refs[:9]
    own = refs[9 : 9 + count]
    (
        val_ref, vp_ref, conv_ref, bc_ref, ssd_ref, ent_ref, log_ref, step_ref, cum_ref, start_ref,
    ) = refs[9 + count : 19 + count]
    outs = refs[19 + count : 19 + 2 * count]
    (
        xpad, logs, steps, logt, inter, state, all_vp, all_val, all_bc, all_log, message, arrived, sems,
    ) = refs[19 + 2 * count : 32 + 2 * count]
    gather_sems = refs[32 + 2 * count :]
    i = pl.program_id(0)
    blocks = pl.num_programs(0) // 2
    first = i < blocks
    c = jnp.where(first, i, i - blocks)
    near = lax.axis_size("ctx")
    pos = lax.axis_index("ctx")
    plan = []
    if count:
        lists = [Gather(own[k], outs[k], *gather_sems[5 * k : 5 * k + 5]).steps() for k in range(count)]
        length = len(lists[0])
        for at in range(length + 2 * (count - 1)):
            acts = [lists[k][at - 2 * k] for k in range(count) if 0 <= at - 2 * k < length]
            plan.append((4 * at, lambda acts=acts: [act() for act in acts]))

    @pl.when(i == 0)
    def _():
        meet((box_peers() if count else []) + chain_peers())
        xpad[0:8, :] = halo_ref[:, :CH] * keep_ref[0, 0]
        state[...] = jnp.zeros_like(state)
        cum_ref[...] = jnp.zeros_like(cum_ref)

    half = lanes_of((Q, 128)) < P_SIZE
    square = (Q, Q)
    causal = rows_of(square) >= lanes_of(square)

    @pl.when(first)
    def _():
        @pl.when(i > 0)
        def _():
            xpad[0:8, :] = xpad[Q : Q + 8, :]

        xpad[8 : 8 + Q, :] = u_ref[:, :CH]
        raw = u_ref[:, CH:] + sb_ref[...]
        step = softplus(raw) * valid_ref[...]
        step = jnp.where(lanes_of(step.shape) < HEADS, step, 0.0)
        rate = -jnp.exp(dl_ref[...]) * LOG2E
        logd = ordered_sum(jnp.where(causal, 1.0, 0.0).astype(BF16), step * rate)
        log_ref[...] = logd
        all_log[c] = logd
        step_ref[...] = step
        spread(logd, logs)
        spread(step, steps)

        def convolved(cols):
            total = cb_ref[:, cols] + cw_ref[0:1, cols] * xpad[5 : 5 + Q, cols]
            for k in range(1, CONVK):
                total = total + cw_ref[k : k + 1, cols] * xpad[5 + k : 5 + k + Q, cols]
            return total

        conv_b = convolved(pl.ds(DI, N))
        conv_c = convolved(pl.ds(DI + N, N))
        conv_ref[:, DI : DI + N] = conv_b.astype(BF16)
        conv_ref[:, DI + N :] = conv_c.astype(BF16)
        act_b = conv_b * sigmoid(conv_b)
        act_c = conv_c * sigmoid(conv_c)
        both = jnp.concatenate([act_b.astype(BF16), act_c.astype(BF16)], 1)
        bc_ref[...] = both
        all_bc[c] = both
        turned_b = act_b.T.astype(BF16)
        ent_ref[0] = state[...].astype(BF16)

        def group(g, unused):
            when_at(i * GROUPS + g, plan)
            lg = logs[g]
            sg = steps[g]
            for j in range(2):
                cols = pl.ds(pl.multiple_of(g * GW + 128 * j, 128), 128)
                cv = convolved(cols)
                conv_ref[:, cols] = cv.astype(BF16)
                val = cv * sigmoid(cv)
                low = val.astype(BF16)
                val_ref[:, cols] = low
                all_val[c, :, cols] = low
                lp = jnp.where(half, head_lanes(lg, 2 * j), head_lanes(lg, 2 * j + 1))
                sp = jnp.where(half, head_lanes(sg, 2 * j), head_lanes(sg, 2 * j + 1))
                vp = val * sp
                low = vp.astype(BF16)
                vp_ref[:, cols] = low
                all_vp[c, :, cols] = low
                last = lp[Q - 1 : Q, :]
                weighted = (vp * jnp.exp2(last - lp)).astype(BF16)
                state[:, cols] = jnp.exp2(last) * state[:, cols] + nn(turned_b, weighted)
                cum_ref[c + 1, :, cols] = cum_ref[c, :, cols] + last
            return unused

        lax.fori_loop(0, GROUPS, group, 0)

    for k in range(near):

        @pl.when(jnp.logical_and(i == blocks + k, pos == k))
        def _(k=k):
            if k:
                pass_on(message, arrived, sems, 1).wait_recv()
                entering = keep_ref[0, 0] * arrived[...].astype(F32)
                start_ref[...] = entering.astype(BF16)
            else:
                start_ref[...] = jnp.zeros_like(start_ref)
            if k < near - 1:
                if k:
                    message[...] = (jnp.exp2(cum_ref[blocks, 0:1, :]) * entering + state[...]).astype(BF16)
                else:
                    message[...] = state[...].astype(BF16)
                pass_on(message, arrived, sems, 1).start()

    @pl.when(jnp.logical_not(first))
    def _():
        logd = all_log[c]
        spread(logd, logs)
        spread_rows(logd.T, logt)
        inter[...] = jnp.where(causal, nt(all_bc[c, :, N:], all_bc[c, :, :N]), 0.0)
        left = jnp.where(half[:1], 1.0, 0.0).astype(BF16)
        right = jnp.where(half[:1], 0.0, 1.0).astype(BF16)

        def group(g, unused):
            when_at(i * GROUPS + g, plan)
            lg = logs[g]
            for j in range(2):
                cols = pl.ds(pl.multiple_of(g * GW + 128 * j, 128), 128)
                vp = all_vp[c, :, cols]
                v0 = vp * left
                v1 = vp * right
                top = []
                low = []
                for h in range(2):
                    row = logt[g, 2 * j + h : 2 * j + h + 1]
                    early, late = row[:, :HALF], row[:, HALF:]
                    lb = head_lanes(lg, 2 * j + h)
                    up, down = lb[:HALF], lb[HALF:]
                    top.append((inter[:HALF, :HALF] * jnp.exp2(jnp.minimum(up - early, 0.0))).astype(BF16))
                    low.append((inter[HALF:, :HALF] * jnp.exp2(jnp.minimum(down - early, 0.0))).astype(BF16))
                    low.append((inter[HALF:, HALF:] * jnp.exp2(jnp.minimum(down - late, 0.0))).astype(BF16))
                skipped = skip_ref[:, cols] * all_val[c, :, cols].astype(F32)
                above = nn(jnp.concatenate(top, 1), jnp.concatenate([v0[:HALF], v1[:HALF]], 0))
                below = nn(jnp.concatenate(low, 1), jnp.concatenate([v0, v1], 0))
                ssd_ref[:HALF, cols] = (above + skipped[:HALF]).astype(BF16)
                ssd_ref[HALF:, cols] = (below + skipped[HALF:]).astype(BF16)
            return unused

        lax.fori_loop(0, GROUPS, group, 0)

    @pl.when(jnp.logical_and(i == 2 * blocks - 1, pos < near - 1))
    def _():
        pass_on(message, arrived, sems, 1).wait_send()


def gate_kernel(
    start_ref, ssd_in, ent_ref, z_ref, val_ref, bc_ref, log_ref, cum_ref,
    tok_ref, cot_ref, valid_ref, ow_ref, gain_ref,
    out_ref, gated_ref, bg_ref, ds_ref, dz_ref, entt_ref, gnext_ref, gout_ref, dlp_ref, dc_ref, sums_ref,
    start, gstate, logs, ssd_s, mix_s, el_s, pe_s, gg_s, acc,
):
    i = pl.program_id(0)
    c = pl.num_programs(0) - 1 - i

    @pl.when(i == 0)
    def _():
        start[...] = start_ref[...].astype(F32)
        gstate[...] = jnp.zeros_like(gstate)
        sums_ref[...] = jnp.zeros_like(sums_ref)

    spread(log_ref[...], logs)
    low_c = bc_ref[:, N:]
    turned_c = low_c.astype(F32).T.astype(BF16)
    half = lanes_of((Q, 128)) < P_SIZE
    acc[...] = jnp.zeros_like(acc)

    def enter(g, unused):
        lg = logs[g]
        cols = pl.ds(pl.multiple_of(g * GW, GW), GW)
        entering = (
            ent_ref[0, :, cols].astype(F32) + jnp.exp2(cum_ref[c, 0:1, cols]) * start[:, cols]
        ).astype(BF16)
        entt_ref[0, :, cols] = entering
        part = nn(low_c, entering)
        for j in range(2):
            pc = pl.ds(pl.multiple_of(g * GW + 128 * j, 128), 128)
            el = jnp.exp2(jnp.where(half, head_lanes(lg, 2 * j), head_lanes(lg, 2 * j + 1)))
            pe = el * part[:, 128 * j : 128 * j + 128]
            el_s[:, pc] = el
            pe_s[:, pc] = pe
            ssd = ssd_in[:, pc].astype(F32) + pe
            z = z_ref[:, pc].astype(F32)
            mixed = ssd * (z * sigmoid(z))
            ssd_s[:, pc] = ssd
            mix_s[:, pc] = mixed
            acc[...] += mixed * mixed
        return unused

    lax.fori_loop(0, GROUPS, enter, 0)
    inv = lax.rsqrt(jnp.sum(acc[...], axis=1, keepdims=True) * (1.0 / DI) + epsilon)
    inv = jnp.broadcast_to(inv, (Q, 128))
    valid = valid_ref[...]
    valid8 = jnp.concatenate([valid] * (tok_ref.shape[1] // 128), 1)
    branch_grad = (cot_ref[...].astype(F32) * valid8).astype(BF16)
    bg_ref[...] = branch_grad
    acc[...] = jnp.zeros_like(acc)

    def gate(g, unused):
        cols = pl.ds(pl.multiple_of(g * GW, GW), GW)
        ggrad = nt(branch_grad, ow_ref[cols, :])
        for j in range(2):
            pc = pl.ds(pl.multiple_of(g * GW + 128 * j, 128), 128)
            hat = mix_s[:, pc] * inv
            gain = gain_ref[:, pc]
            mix_s[:, pc] = hat
            gated_ref[:, pc] = (hat * gain).astype(BF16)
            gg = ggrad[:, 128 * j : 128 * j + 128]
            both = gg * hat
            sums_ref[0:1, pc] += jnp.sum(both, axis=0, keepdims=True)
            acc[...] += both * gain
            gg_s[:, pc] = gg * gain
        return unused

    lax.fori_loop(0, GROUPS, gate, 0)
    mean = jnp.sum(acc[...], axis=1, keepdims=True) * (1.0 / DI)
    mean = jnp.broadcast_to(mean, (Q, 128))

    for n in range(tok_ref.shape[1] // 256):
        cols = slice(256 * n, 256 * n + 256)
        branch = nn(gated_ref[...], ow_ref[:, cols])
        out_ref[:, cols] = (tok_ref[:, cols].astype(F32) + valid8[:, :256] * branch).astype(BF16)

    acc[...] = jnp.zeros_like(acc)
    dc_ref[...] = jnp.zeros_like(dc_ref)

    def back(g, unused):
        cols = pl.ds(pl.multiple_of(g * GW, GW), GW)
        dparts = []
        prods = []
        for j in range(2):
            pc = pl.ds(pl.multiple_of(g * GW + 128 * j, 128), 128)
            dmixed = inv * (gg_s[:, pc] - mix_s[:, pc] * mean)
            z = z_ref[:, pc].astype(F32)
            s = sigmoid(z)
            ds = (dmixed * (z * s)).astype(BF16)
            ds_ref[:, pc] = ds
            dz_ref[:, pc] = (dmixed * ssd_s[:, pc] * (s * (1.0 + z * (1.0 - s)))).astype(BF16)
            ds = ds.astype(F32)
            sums_ref[1:2, pc] += jnp.sum(ds * val_ref[:, pc].astype(F32), axis=0, keepdims=True)
            dparts.append((ds * el_s[:, pc]).astype(BF16))
            prods.append((ds * pe_s[:, pc]).astype(BF16))
        dpart = jnp.concatenate(dparts, 1)
        acc[...] += nn(jnp.concatenate(prods, 1), pick_heads(g))
        dc_ref[...] += nt(dpart, entt_ref[0, :, cols])
        gnext_ref[0, :, cols] = gstate[:, cols].astype(BF16)
        total = cum_ref[c + 1, 0:1, cols] - cum_ref[c, 0:1, cols]
        gstate[:, cols] = nn(turned_c, dpart) + jnp.exp2(total) * gstate[:, cols]
        return unused

    lax.fori_loop(0, GROUPS, back, 0)
    dlp_ref[...] = acc[...]

    @pl.when(c == 0)
    def _():
        gout_ref[...] = gstate[...].astype(BF16)


def scatter_plan(count, refs, places):
    parts, outs, scratch = refs
    lists = [
        Scatter(parts[k], outs[k], *scratch[14 * k : 14 * k + 8], scratch[14 * k + 8 : 14 * k + 14]).steps()
        for k in range(count)
    ]
    return [(place, act) for each in lists for place, act in zip(places, each)]


def mixing_kernel(count, *refs):
    ds_ref, vp_ref, bc_ref, log_ref, keep_ref, gout_ref, cum_ref = refs[:7]
    parts = refs[7 : 7 + count]
    dvp_ref, dbc_ref, dlt_ref, gin_ref = refs[7 + count : 11 + count]
    outs = refs[11 + count : 11 + 2 * count]
    (
        logs, logt, inter, dinter, rowsum, turned, colsum, message, arrived, sems,
    ) = refs[11 + 2 * count : 21 + 2 * count]
    i = pl.program_id(0)
    blocks = pl.num_programs(0)
    near = lax.axis_size("ctx")
    pos = lax.axis_index("ctx")
    plan = scatter_plan(count, (parts, outs, refs[21 + 2 * count :]), (0, 10, 15, 20, 23, 26, 29, 31))

    @pl.when(i == 0)
    def _():
        meet((box_peers() if count else []) + chain_peers())

    for k in range(near):

        @pl.when(jnp.logical_and(i == k, pos == near - 1 - k))
        def _(k=k):
            total = gout_ref[...].astype(F32)
            if k:
                pass_on(message, arrived, sems, -1).wait_recv()
                gin_ref[...] = arrived[...]
                total = total + jnp.exp2(cum_ref[blocks, 0:1, :]) * arrived[...].astype(F32)
            else:
                gin_ref[...] = jnp.zeros_like(gin_ref)
            if k < near - 1:
                message[...] = (keep_ref[0, 0] * total).astype(BF16)
                pass_on(message, arrived, sems, -1).start()

    @pl.when(jnp.logical_and(i == blocks - 1, pos > 0))
    def _():
        pass_on(message, arrived, sems, -1).wait_send()

    logd = log_ref[...]
    spread(logd, logs)
    spread_rows(logd.T, logt)
    low_b = bc_ref[:, :N]
    low_c = bc_ref[:, N:]
    square = (Q, Q)
    causal = rows_of(square) <= lanes_of(square)
    inter[...] = jnp.where(causal, nt(low_b, low_c), 0.0)
    dinter[...] = jnp.zeros_like(dinter)
    half = lanes_of((Q, 128)) < P_SIZE
    lane = lanes_of((HALF, 128))

    def group(g, unused):
        when_at(i * GROUPS + g, plan)
        lg = logs[g]
        first_col = jnp.zeros((HALF, 128), F32)
        second_col = jnp.zeros((HALF, 128), F32)
        for j in range(2):
            cols = pl.ds(pl.multiple_of(g * GW + 128 * j, 128), 128)
            vp = vp_ref[:, cols].astype(F32)
            ds = ds_ref[:, cols]
            wide = ds.astype(F32)
            first = []
            second = []
            outs = []
            for h in range(2):
                head = 2 * j + h
                own = half if h == 0 else jnp.logical_not(half)
                vm = jnp.where(own, vp, 0.0).astype(BF16)
                dsm = jnp.where(own, wide, 0.0).astype(BF16)
                outs.append(dsm)
                row = logt[g, head : head + 1]
                early, late = row[:, :HALF], row[:, HALF:]
                lb = head_lanes(lg, head)
                up, down = lb[:HALF], lb[HALF:]
                dup = nt(vm[:HALF], ds)
                ddown = nt(vm[HALF:], ds[HALF:])
                decay = jnp.exp2(jnp.minimum(early - up, 0.0))
                grad = dup[:, :HALF] * decay
                dinter[:HALF, :HALF] += grad
                part = inter[:HALF, :HALF]
                first.append((part * decay).astype(BF16))
                both = grad * part
                row_early = jnp.sum(both, axis=0, keepdims=True)
                col = both
                decay = jnp.exp2(jnp.minimum(late - up, 0.0))
                grad = dup[:, HALF:] * decay
                dinter[:HALF, HALF:] += grad
                part = inter[:HALF, HALF:]
                first.append((part * decay).astype(BF16))
                both = grad * part
                row_late = jnp.sum(both, axis=0, keepdims=True)
                col = jnp.sum(col + both, axis=1, keepdims=True)
                first_col = jnp.where(lane == head, col, first_col)
                decay = jnp.exp2(jnp.minimum(late - down, 0.0))
                grad = ddown * decay
                dinter[HALF:, HALF:] += grad
                part = inter[HALF:, HALF:]
                second.append((part * decay).astype(BF16))
                both = grad * part
                row_late = row_late + jnp.sum(both, axis=0, keepdims=True)
                col = jnp.sum(both, axis=1, keepdims=True)
                second_col = jnp.where(lane == head, col, second_col)
                rowsum[g, head : head + 1, :HALF] = row_early
                rowsum[g, head : head + 1, HALF:] = row_late
            dvp_ref[:HALF, cols] = nn(
                jnp.concatenate(first, 1), jnp.concatenate(outs, 0)
            ).astype(BF16)
            dvp_ref[HALF:, cols] = nn(
                jnp.concatenate(second, 1), jnp.concatenate([outs[0][HALF:], outs[1][HALF:]], 0)
            ).astype(BF16)
        colsum[g, :HALF] = first_col
        colsum[g, HALF:] = second_col
        return unused

    lax.fori_loop(0, GROUPS, group, 0)
    turned[...] = jnp.zeros_like(turned)
    for g in range(GROUPS):
        turned[4 * g : 4 * g + 4] = rowsum[g, 0:4]
    total = turned[...].T
    for g in range(GROUPS):
        total = total - (colsum[g] if g == 0 else pltpu.roll(colsum[g], 4 * g, 1))
    dlt_ref[...] = total
    masked = jnp.where(causal, dinter[...], 0.0)
    dbc_ref[:, :N] = nn(masked.astype(BF16), low_c)
    dbc_ref[:, N:] = nn(masked.T.astype(BF16), low_b)


def back_kernel(count, *refs):
    (
        keep_ref, gin_ref, gnext_ref, entt_ref, cum_ref, vp_ref, val_ref, dvp_ref, ds_ref, conv_ref,
        u_ref, halo_ref, bc_ref, log_ref, step_ref, valid_ref, dlp_ref, dlt_ref, dbc_ref, dc_ref,
        cw_ref, sb_ref, dl_ref, skip_ref,
    ) = refs[:24]
    parts = refs[24 : 24 + count]
    du_ref, last_ref, edge_ref, sums_ref, small_ref = refs[24 + count : 29 + count]
    outs = refs[29 + count : 29 + 2 * count]
    gin, logs, steps, dpad, head, epad, dlw, dst, drow = refs[29 + 2 * count : 38 + 2 * count]
    plan = scatter_plan(count, (parts, outs, refs[38 + 2 * count :]), (0, 6, 11, 16, 20, 23, 26, 30))
    i = pl.program_id(0)
    top = pl.num_programs(0)
    c = top - 1 - i

    @pl.when(i == 0)
    def _():
        if count:
            meet(box_peers())
        gin[...] = gin_ref[...].astype(F32)
        head[...] = jnp.zeros_like(head)
        sums_ref[...] = jnp.zeros_like(sums_ref)
        small_ref[...] = jnp.zeros_like(small_ref)

    spread(log_ref[...], logs)
    spread(step_ref[...], steps)
    low_b = bc_ref[:, :N]
    half = lanes_of((Q, 128)) < P_SIZE
    dlw[...] = jnp.zeros_like(dlw)
    dst[...] = jnp.zeros_like(dst)
    drow[...] = jnp.zeros_like(drow)

    def conv_back(cols, dact):
        cv = conv_ref[:, cols].astype(F32)
        s = sigmoid(cv)
        dcv = dact * (s * (1.0 + cv * (1.0 - s)))
        dpad[:Q, cols] = dcv
        dpad[Q:, cols] = head[:, cols]
        head[:, cols] = dcv[:8]
        x = u_ref[:, cols]
        sums_ref[4:5, cols] += jnp.sum(dcv, axis=0, keepdims=True)
        total = None
        for j in range(CONVK):
            k = CONVK - 1 - j
            moved = dcv if j == 0 else dpad[j : j + Q, cols]
            sums_ref[k : k + 1, cols] += jnp.sum(moved * x, axis=0, keepdims=True)
            term = cw_ref[k : k + 1, cols] * moved
            total = term if total is None else total + term
        du_ref[:, cols] = total.astype(BF16)

        @pl.when(i == 0)
        def _():
            last_ref[:, cols] = total[Q - 8 :]

    def group(g, db):
        when_at(i * GROUPS + g, plan)
        lg = logs[g]
        sg = steps[g]
        cols = pl.ds(pl.multiple_of(g * GW, GW), GW)
        done = cum_ref[c + 1, 0:1, cols]
        after = jnp.exp2(cum_ref[top, 0:1, cols] - done)
        grad = gnext_ref[0, :, cols].astype(F32) + after * gin[:, cols]
        low_g = grad.astype(BF16)
        decay = jnp.exp2(done - cum_ref[c, 0:1, cols])
        row = decay * jnp.sum(grad * entt_ref[0, :, cols].astype(F32), axis=0, keepdims=True)
        coarse = row.astype(BF16).astype(F32)
        r = rows_of((16, GW))
        two = jnp.where(r == 0, jnp.broadcast_to(coarse, (16, GW)), 0.0)
        two = jnp.where(r == 1, jnp.broadcast_to(row - coarse, (16, GW)), two)
        chosen = pick_heads(g)
        drow[...] += nn(two.astype(BF16), chosen)
        dweighted = nn(low_b, low_g)
        weights = []
        moves = []
        stepped = []
        dacts = []
        for j in range(2):
            pc = pl.ds(pl.multiple_of(g * GW + 128 * j, 128), 128)
            lp = jnp.where(half, head_lanes(lg, 2 * j), head_lanes(lg, 2 * j + 1))
            sp = jnp.where(half, head_lanes(sg, 2 * j), head_lanes(sg, 2 * j + 1))
            fade = jnp.exp2(lp[Q - 1 : Q, :] - lp)
            vp = vp_ref[:, pc].astype(F32)
            faded = dweighted[:, 128 * j : 128 * j + 128] * fade
            weights.append((vp * fade).astype(BF16))
            moves.append((faded * vp).astype(BF16))
            both = dvp_ref[:, pc].astype(F32) + faded
            stepped.append((both * val_ref[:, pc].astype(F32)).astype(BF16))
            dacts.append((pc, sp * both + skip_ref[:, pc] * ds_ref[:, pc].astype(F32)))
        dlw[...] += nn(jnp.concatenate(moves, 1), chosen)
        dst[...] += nn(jnp.concatenate(stepped, 1), chosen)
        for pc, dact in dacts:
            conv_back(pc, dact)
        return db + nt(jnp.concatenate(weights, 1), low_g)

    db = lax.fori_loop(0, GROUPS, group, dbc_ref[:, :N])
    conv_back(pl.ds(DI, N), db)
    conv_back(pl.ds(DI + N, N), dbc_ref[:, N:] + dc_ref[...])

    moved = dlw[...]
    at_last = jnp.sum(moved, axis=0, keepdims=True) + drow[0:1] + drow[1:2]
    dlog = dlp_ref[...] + dlt_ref[...] - moved
    dlog = dlog + jnp.where(rows_of(dlog.shape) == Q - 1, at_last, 0.0)
    square = (Q, Q)
    later = jnp.where(rows_of(square) <= lanes_of(square), 1.0, 0.0).astype(BF16)
    dsum = ordered_sum(later, dlog)
    rate = -jnp.exp(dl_ref[...])
    dstep = (dst[...] + dsum * rate) * valid_ref[...]
    raw = u_ref[:, CH:] + sb_ref[...]
    draw = dstep * (1.0 / (1.0 + jnp.exp(-raw)))
    draw = jnp.where(lanes_of(draw.shape) < HEADS, draw, 0.0)
    du_ref[:, CH:] = draw.astype(BF16)
    small_ref[0:1] += jnp.sum(draw, axis=0, keepdims=True)
    small_ref[1:2] += jnp.sum(dsum * step_ref[...], axis=0, keepdims=True) * rate

    @pl.when(c == 0)
    def _():
        epad[0:8, :] = jnp.zeros((8, CH), F32)
        epad[8:16, :] = head[...]
        x = halo_ref[:, :CH] * keep_ref[0, 0]
        total = jnp.zeros((8, CH), F32)
        for j in range(CONVK):
            k = CONVK - 1 - j
            moved = epad[j : j + 8, :]
            sums_ref[k : k + 1, :] += jnp.sum(moved * x, axis=0, keepdims=True)
            total = total + cw_ref[k : k + 1, :] * moved
        edge_ref[...] = total * keep_ref[0, 0]


def spec(block, index):
    return pl.BlockSpec(block, index)


def whole(shape):
    return pl.BlockSpec(shape, lambda *_: (0,) * len(shape))


def scalar():
    return pl.BlockSpec(memory_space=pltpu.SMEM)


def shaped(shape, kind):
    return jax.ShapeDtypeStruct(shape, kind)


def cost(flops, moved):
    return pl.CostEstimate(flops=int(flops), bytes_accessed=int(moved), transcendentals=0)


def params(number=None):
    return pltpu.CompilerParams(
        dimension_semantics=("arbitrary",), vmem_limit_bytes=60 * 1024 * 1024, collective_id=number,
        has_side_effects=number is not None,
    )


LINE = 4


def my_place():
    f = lax.axis_index("fsdp")
    t = lax.axis_index("ctx")
    return f // 2, f % 2, t // 2, t % 2


def device_at(z, y, x, core):
    return {"fsdp": z * 2 + y, "ctx": x * 2 + core}


def order_of(z, y, x, core):
    return (z * 2 + y) * 4 + x * 2 + core


def box_peers():
    z, y, x, core = my_place()
    return [
        (None, device_at(z, y, x, 1 - core)), (None, device_at(z, y, 1 - x, core)),
        (None, device_at(z, 1 - y, x, core)),
        (z > 0, device_at(z - 1, y, x, core)), (z < LINE - 1, device_at(z + 1, y, x, core)),
    ]


def meet(peers):
    barrier = pltpu.get_barrier_semaphore()
    count = 0
    for valid, peer in peers:

        def greet(peer=peer):
            pl.semaphore_signal(barrier, inc=1, device_id=peer, device_id_type=pl.DeviceIdType.MESH)

        if valid is None:
            greet()
            count = count + 1
        else:
            pl.when(valid)(greet)
            count = count + jnp.where(valid, 1, 0)
    pl.semaphore_wait(barrier, count)


def send(src, dst, send_sem, recv_sem, peer):
    return pltpu.make_async_remote_copy(
        src_ref=src, dst_ref=dst, send_sem=send_sem, recv_sem=recv_sem,
        device_id=device_at(*peer), device_id_type=pl.DeviceIdType.MESH,
    )


class Gather:
    def __init__(self, own, out, recv, halves, twin, sent, here):
        self.own, self.out, self.rows = own, out, own.shape[0]
        self.recv, self.halves, self.twin, self.sent, self.here = recv, halves, twin, sent, here
        self.place = my_place()

    def block(self, z, y, x, core, half=None):
        size = self.rows if half is None else self.rows // 2
        start = order_of(z, y, x, core) * self.rows + (0 if half is None else half * size)
        return self.out.at[pl.ds(pl.multiple_of(start, 16), size)]

    def copy(self, origin, way, half=None, own=False):
        z, y, x, core = self.place
        oz, oy, ox = origin
        o = oz * 4 + oy * 2 + ox
        dst = self.block(oz, oy, ox, core, half)
        src = self.own if own else dst
        peer = {
            "up": (z + 1, y, x, core), "down": (z - 1, y, x, core), "x": (z, y, 1 - x, core),
            "y": (z, 1 - y, x, core), "twin": (z, y, x, 1 - core),
        }[way]
        sem = self.sent.at[("up", "down", "x", "y", "twin").index(way), o]
        if way == "twin":
            arrival = self.twin.at[o]
        elif half is not None:
            arrival = self.halves.at[half, o]
        else:
            arrival = self.recv.at[o]
        return send(src, dst, sem, arrival, peer)

    def arrived(self, origin, half=None):
        self.copy(origin, "x", half).wait_recv()

    def column(self, r):
        z = self.place[0]
        if r == 0:
            return [(None, z, True, True)]
        return [(z - r >= 0, z - r, True, False), (z + r < LINE, z + r, False, True)]

    def each(self, r, act):
        for valid, oz, below, above in self.column(r):
            if valid is None:
                act(oz, below, above)
            else:
                pl.when(valid)(lambda oz=oz, below=below, above=above: act(oz, below, above))

    def begin(self):
        z, y, x, core = self.place
        pltpu.make_async_copy(self.own, self.block(z, y, x, core), self.here).start()
        self.forward(0)

    def ways(self, oz, below, above, act):
        z = self.place[0]
        if below:
            pl.when(z < LINE - 1)(lambda: act("up"))
        if above:
            pl.when(z > 0)(lambda: act("down"))
        act("x")
        act("y")
        act("twin")

    def forward(self, r):
        z, y, x, core = self.place

        def act(oz, below, above):
            origin = (oz, y, x)
            if r:
                self.arrived(origin)
            self.ways(oz, below, above, lambda way: self.copy(origin, way, own=r == 0).start())

        self.each(r, act)

    def across(self, r):
        z, y, x, core = self.place

        def act(oz, below, above):
            self.arrived((oz, y, 1 - x))
            self.copy((oz, y, 1 - x), "y", 0).start()
            self.copy((oz, y, 1 - x), "twin").start()
            self.arrived((oz, 1 - y, x))
            self.copy((oz, 1 - y, x), "x", 1).start()
            self.copy((oz, 1 - y, x), "twin").start()

        self.each(r, act)

    def corner(self, r):
        z, y, x, core = self.place

        def act(oz, below, above):
            origin = (oz, 1 - y, 1 - x)
            self.arrived(origin, 0)
            self.arrived(origin, 1)
            self.copy(origin, "twin").start()

        self.each(r, act)

    def finish(self):
        z, y, x, core = self.place
        pltpu.make_async_copy(self.own, self.block(z, y, x, core), self.here).wait()
        for r in range(LINE):

            def act(oz, below, above, r=r):
                self.ways(oz, below, above, lambda way: self.copy((oz, y, x), way, own=r == 0).wait_send())
                self.copy((oz, y, 1 - x), "y", 0).wait_send()
                self.copy((oz, 1 - y, x), "x", 1).wait_send()
                for oy, ox in ((y, 1 - x), (1 - y, x), (1 - y, 1 - x)):
                    self.copy((oz, oy, ox), "twin").wait_send()
                for oy, ox in ((y, x), (y, 1 - x), (1 - y, x), (1 - y, 1 - x)):
                    self.copy((oz, oy, ox), "twin").wait_recv()

            self.each(r, act)

    def steps(self):
        return [
            self.begin,
            lambda: self.forward(1),
            lambda: self.across(0),
            lambda: self.forward(2),
            lambda: self.across(1),
            lambda: (self.forward(3), self.corner(0)),
            lambda: self.across(2),
            lambda: self.corner(1),
            lambda: self.across(3),
            lambda: (self.corner(2), self.corner(3)),
            self.finish,
        ]


def gather_scratch():
    dma = pltpu.SemaphoreType.DMA
    return [dma((16,)), dma((2, 16)), dma((16,)), dma((5, 16)), dma(())]


def gather_kernel(count, *refs):
    own, out, sems = refs[:count], refs[count : 2 * count], refs[2 * count :]
    meet(box_peers())
    lists = [
        Gather(own[k], out[k], *sems[5 * k : 5 * k + 5]).steps() for k in range(count)
    ]
    length = len(lists[0])
    for at in range(length + 2 * (count - 1)):
        for k in range(count):
            if 0 <= at - 2 * k < length:
                lists[k][at - 2 * k]()


def gathered(arrays, number):
    count = len(arrays)
    anywhere = pl.BlockSpec(memory_space=pl.ANY)
    return pl.pallas_call(
        lambda *refs: gather_kernel(count, *refs),
        in_specs=[anywhere] * count,
        out_specs=[anywhere] * count,
        out_shape=[shaped((32 * a.shape[0], a.shape[1]), a.dtype) for a in arrays],
        scratch_shapes=gather_scratch() * count,
        compiler_params=pltpu.CompilerParams(collective_id=number, has_side_effects=True),
        name="gather",
    )(*arrays)


class Scatter:
    def __init__(self, parts, out, got, kept, mixed_y, mixed_x, from_x, from_y, up, down, sems):
        self.parts, self.out = parts, out
        self.got, self.kept = got, kept
        self.mixed = (mixed_y, mixed_x)
        self.sides = (from_x, from_y)
        self.up, self.down = up, down
        self.twin_sent, self.twin_recv, self.sent, self.recv, self.line_sent, self.line_recv = sems
        self.place = my_place()
        self.rows = parts.shape[-2]

    def groups(self):
        z, y, x, core = self.place
        return [(1 - y, 1 - x), (y, 1 - x), (1 - y, x), (y, x)]

    def to_twin(self, k):
        z, y, x, core = self.place
        gy, gx = self.groups()[k]
        return send(
            self.parts.at[:, gy, gx, 1 - core], self.got.at[k], self.twin_sent.at[k], self.twin_recv.at[k],
            (z, y, x, 1 - core),
        )

    def begin(self):
        for k in range(4):
            self.to_twin(k).start()

    def both(self, k):
        z, y, x, core = self.place
        gy, gx = self.groups()[k]
        self.to_twin(k).wait_recv()
        for b in range(LINE):
            total = self.parts[b, gy, gx, core].astype(F32) + self.got[k, b].astype(F32)
            self.kept[k, b] = total.astype(BF16)

    def corner_copy(self, half):
        z, y, x, core = self.place
        size = self.rows // 2
        src = self.kept.at[0, :, pl.ds(half * size, size)]
        peer = (z, 1 - y, x, core) if half == 0 else (z, y, 1 - x, core)
        return send(src, self.mixed[half], self.sent.at[half], self.recv.at[half], peer)

    def side_copy(self, k):
        z, y, x, core = self.place
        peer = (z, y, 1 - x, core) if k == 1 else (z, 1 - y, x, core)
        return send(self.kept.at[k], self.sides[k - 1], self.sent.at[1 + k], self.recv.at[1 + k], peer)

    def corners(self):
        self.both(0)
        self.corner_copy(0).start()
        self.corner_copy(1).start()
        self.both(1)
        self.both(2)
        self.both(3)

    def sides_out(self):
        size = self.rows // 2
        for half, k in ((0, 1), (1, 2)):
            self.corner_copy(half).wait_recv()
            rows = slice(half * size, half * size + size)
            for b in range(LINE):
                total = self.kept[k, b, rows].astype(F32) + self.mixed[half][b].astype(F32)
                self.kept[k, b, rows] = total.astype(BF16)
            self.side_copy(k).start()

    def sides_in(self):
        self.side_copy(1).wait_recv()
        self.side_copy(2).wait_recv()
        for b in range(LINE):
            total = self.kept[3, b].astype(F32) + self.sides[0][b].astype(F32) + self.sides[1][b].astype(F32)
            self.kept[3, b] = total.astype(BF16)

    def line_copy(self, oz, way):
        z, y, x, core = self.place
        buffer = self.up if way == 0 else self.down
        peer = (z + 1, y, x, core) if way == 0 else (z - 1, y, x, core)
        return send(
            self.kept.at[3, oz], buffer.at[oz], self.line_sent.at[way, oz], self.line_recv.at[way, oz], peer
        )

    def line(self, r):
        z = self.place[0]

        def upward():
            oz = z + r

            @pl.when(z > 0)
            def _():
                self.line_copy(oz, 0).wait_recv()
                total = self.kept[3, oz].astype(F32) + self.up[oz].astype(F32)
                self.kept[3, oz] = total.astype(BF16)

            self.line_copy(oz, 0).start()

        def downward():
            oz = z - r

            @pl.when(z < LINE - 1)
            def _():
                self.line_copy(oz, 1).wait_recv()
                total = self.kept[3, oz].astype(F32) + self.down[oz].astype(F32)
                self.kept[3, oz] = total.astype(BF16)

            self.line_copy(oz, 1).start()

        pl.when(z + r < LINE)(upward)
        pl.when(z - r >= 0)(downward)

    def finish(self):
        z = self.place[0]
        self.out[...] = self.kept[3, z].astype(F32)

        @pl.when(z > 0)
        def _():
            self.line_copy(z, 0).wait_recv()
            self.out[...] += self.up[z].astype(F32)

        @pl.when(z < LINE - 1)
        def _():
            self.line_copy(z, 1).wait_recv()
            self.out[...] += self.down[z].astype(F32)

        for k in range(4):
            self.to_twin(k).wait_send()
        for half in range(2):
            self.corner_copy(half).wait_send()
        for k in (1, 2):
            self.side_copy(k).wait_send()
        for r in range(1, LINE):
            pl.when(z + r < LINE)(lambda r=r: self.line_copy(z + r, 0).wait_send())
            pl.when(z - r >= 0)(lambda r=r: self.line_copy(z - r, 1).wait_send())

    def steps(self):
        return [
            self.begin, self.corners, self.sides_out, self.sides_in, lambda: self.line(3), lambda: self.line(2),
            lambda: self.line(1), self.finish,
        ]


def scatter_scratch(rows, columns):
    dma = pltpu.SemaphoreType.DMA
    half = rows // 2
    return [
        pltpu.VMEM((4, LINE, rows, columns), BF16),
        pltpu.VMEM((4, LINE, rows, columns), BF16),
        pltpu.VMEM((LINE, half, columns), BF16),
        pltpu.VMEM((LINE, half, columns), BF16),
        pltpu.VMEM((LINE, rows, columns), BF16),
        pltpu.VMEM((LINE, rows, columns), BF16),
        pltpu.VMEM((LINE, rows, columns), BF16),
        pltpu.VMEM((LINE, rows, columns), BF16),
        dma((4,)), dma((4,)), dma((4,)), dma((4,)), dma((2, LINE)), dma((2, LINE)),
    ]


class Total:
    def __init__(self, own, out, held, got, sent, recv):
        self.own, self.out, self.held, self.got, self.sent, self.recv = own, out, held, got, sent, recv

    def copy(self, k):
        z, y, x, core = my_place()
        near = z + 1 - 2 * (z % 2)
        peer = [
            (z, y, x, 1 - core), (z, y, 1 - x, core), (z, 1 - y, x, core), (near, y, x, core),
            ((z + 2) % LINE, y, x, core),
        ][k]
        return send(self.own if k == 0 else self.held.at[k], self.got.at[k], self.sent.at[k], self.recv.at[k], peer)

    def begin(self):
        self.copy(0).start()

    def turn(self, k):
        self.copy(k).wait_recv()
        mine = self.own[...] if k == 0 else self.held[k]
        total = mine + self.got[k]
        if k < 4:
            self.held[k + 1] = total
            self.copy(k + 1).start()
        else:
            self.out[...] = total

    def finish(self):
        for k in range(5):
            self.copy(k).wait_send()

    def steps(self):
        return [self.begin] + [lambda k=k: self.turn(k) for k in range(5)] + [self.finish]


def scatter_kernel(count, *refs):
    parts, small = refs[:count], refs[count]
    outs, small_out = refs[count + 1 : 2 * count + 1], refs[2 * count + 1]
    scratch = refs[2 * count + 2 :]
    z, y, x, core = my_place()
    meet(box_peers() + [(None, device_at((z + 2) % LINE, y, x, core))])
    lists = []
    for k in range(count):
        own = scratch[14 * k : 14 * k + 14]
        lists.append(Scatter(parts[k], outs[k], *own[:8], own[8:]).steps())
    lists.append(Total(small, small_out, *scratch[14 * count :]).steps())
    for at in range(max(len(each) for each in lists)):
        for each in lists:
            if at < len(each):
                each[at]()


def scattered(arrays, small, number):
    count = len(arrays)
    shapes = [(a.shape[0] // 32, a.shape[1]) for a in arrays]
    dma = pltpu.SemaphoreType.DMA
    scratch = []
    for shape in shapes:
        scratch += scatter_scratch(*shape)
    scratch += [
        pltpu.VMEM((5,) + small.shape, F32), pltpu.VMEM((5,) + small.shape, F32), dma((5,)), dma((5,)),
    ]
    vmem = pl.BlockSpec(memory_space=pltpu.VMEM)
    return pl.pallas_call(
        lambda *refs: scatter_kernel(count, *refs),
        in_specs=[vmem] * (count + 1),
        out_specs=[vmem] * (count + 1),
        out_shape=[shaped(shape, F32) for shape in shapes] + [shaped(small.shape, F32)],
        scratch_shapes=scratch,
        compiler_params=pltpu.CompilerParams(
            collective_id=number, has_side_effects=True, vmem_limit_bytes=60 * 1024 * 1024
        ),
        name="scatter",
    )(*[a.reshape(LINE, 2, 2, 2, s[0], s[1]) for a, s in zip(arrays, shapes)], small)


def local(
    tokens,
    valid_mask,
    stretch_start,
    cotangent,
    norm_gain,
    in_weight,
    conv_weight,
    conv_bias,
    step_bias,
    decay_log,
    skip_gain,
    gate_gain,
    out_weight,
):
    axes = ("fsdp", "ctx")
    rows, width = tokens.shape
    blocks = rows // Q
    near = lax.axis_size("ctx")
    halo_tokens = lax.ppermute(
        tokens[rows - 8 :], "ctx", [(k, k + 1) for k in range(near - 1)]
    )
    own_u = jnp.pad(in_weight[:, DI:], ((0, 0), (0, UW - (DPROJ - DI))))
    own_z = in_weight[:, :DI]
    boxed = lax.axis_size("fsdp") == 8 and near == 4
    if boxed:
        (w_u,) = gathered([own_u], 1)
        later = [own_z, out_weight]
    else:
        w_u, w_z, w_o = [lax.all_gather(a, axes, axis=0, tiled=True) for a in (own_u, own_z, out_weight)]
        later = []
    extra = len(later)
    anywhere = pl.BlockSpec(memory_space=pl.ANY)

    def hats(values):
        wide = values.astype(F32)
        return wide * lax.rsqrt(jnp.mean(wide * wide, axis=-1, keepdims=True) + epsilon)

    normed_more = (hats(jnp.concatenate([tokens, halo_tokens], 0)) * norm_gain).astype(BF16)
    normed = normed_more[:rows]
    valid = jnp.broadcast_to(valid_mask.astype(F32)[:, None], (rows, 128))
    keep = (1.0 - stretch_start[0].astype(F32)).reshape(1, 1)
    taps = conv_weight
    shift = conv_bias.reshape(1, CH)
    bias = jnp.pad(step_bias, (0, 128 - HEADS)).reshape(1, 128)
    logs = jnp.pad(decay_log, (0, 128 - HEADS)).reshape(1, 128)
    skips = jnp.repeat(skip_gain, P_SIZE).reshape(1, DI)
    u = jnp.dot(normed_more, w_u, preferred_element_type=F32)
    halo_block = rows // 8

    same = lambda c: (c, 0)
    same3 = lambda c: (c, 0, 0)
    one = lambda i: (jnp.minimum(i, blocks - 1), 0)
    one3 = lambda i: (jnp.minimum(i, blocks - 1), 0, 0)
    two = lambda i: (jnp.maximum(i - blocks, 0), 0)
    val, vp, conv, bc, ssd, ent, logd, step, cum, start, *filled = pl.pallas_call(
        lambda *refs: forward_kernel(extra, *refs),
        grid=(2 * blocks,),
        in_specs=[
            spec((Q, UW), one),
            spec((8, UW), lambda c: (halo_block, 0)),
            spec((Q, 128), one),
            scalar(),
            whole((CONVK, CH)),
            whole((1, CH)),
            whole((1, 128)),
            whole((1, 128)),
            whole((1, DI)),
        ]
        + [anywhere] * extra,
        out_specs=[
            spec((Q, DI), one),
            spec((Q, DI), one),
            spec((Q, CH), one),
            spec((Q, 2 * N), one),
            spec((Q, DI), two),
            spec((1, N, DI), one3),
            spec((Q, 128), one),
            spec((Q, 128), one),
            whole((blocks + 1, 8, DI)),
            whole((N, DI)),
        ]
        + [anywhere] * extra,
        out_shape=[
            shaped((rows, DI), BF16),
            shaped((rows, DI), BF16),
            shaped((rows, CH), BF16),
            shaped((rows, 2 * N), BF16),
            shaped((rows, DI), BF16),
            shaped((blocks, N, DI), BF16),
            shaped((rows, 128), F32),
            shaped((rows, 128), F32),
            shaped((blocks + 1, 8, DI), F32),
            shaped((N, DI), BF16),
        ]
        + [shaped((32 * a.shape[0], a.shape[1]), a.dtype) for a in later],
        scratch_shapes=[
            pltpu.VMEM((Q + 8, CH), F32),
            pltpu.VMEM((GROUPS, Q, 128), F32),
            pltpu.VMEM((GROUPS, Q, 128), F32),
            pltpu.VMEM((GROUPS, 8, Q), F32),
            pltpu.VMEM((Q, Q), F32),
            pltpu.VMEM((N, DI), F32),
            pltpu.VMEM((blocks, Q, DI), BF16),
            pltpu.VMEM((blocks, Q, DI), BF16),
            pltpu.VMEM((blocks, Q, 2 * N), BF16),
            pltpu.VMEM((blocks, Q, 128), F32),
            pltpu.VMEM((N, DI), BF16),
            pltpu.VMEM((N, DI), BF16),
            pltpu.SemaphoreType.DMA((2,)),
        ]
        + gather_scratch() * extra,
        compiler_params=params(2),
        cost_estimate=cost(15e9, 60e6),
        name="forward",
    )(u, u, valid, keep, taps, shift, bias, logs, skips, *later)
    if later:
        w_z, w_o = filled

    z = jnp.dot(normed, w_z, preferred_element_type=F32).astype(BF16)
    back = lambda i: (blocks - 1 - i, 0)
    back3 = lambda i: (blocks - 1 - i, 0, 0)
    gains = gate_gain.reshape(1, DI)
    output, gated, branch_grad, ds, dz, entt, gnext, gout, dlp, dc, gate_sums = pl.pallas_call(
        gate_kernel,
        grid=(blocks,),
        in_specs=[
            whole((N, DI)),
            spec((Q, DI), back),
            spec((1, N, DI), back3),
            spec((Q, DI), back),
            spec((Q, DI), back),
            spec((Q, 2 * N), back),
            spec((Q, 128), back),
            whole((blocks + 1, 8, DI)),
            spec((Q, width), back),
            spec((Q, width), back),
            spec((Q, 128), back),
            whole((DI, width)),
            whole((1, DI)),
        ],
        out_specs=[
            spec((Q, width), back),
            spec((Q, DI), back),
            spec((Q, width), back),
            spec((Q, DI), back),
            spec((Q, DI), back),
            spec((1, N, DI), back3),
            spec((1, N, DI), back3),
            whole((N, DI)),
            spec((Q, 128), back),
            spec((Q, N), back),
            whole((8, DI)),
        ],
        out_shape=[
            shaped((rows, width), BF16),
            shaped((rows, DI), BF16),
            shaped((rows, width), BF16),
            shaped((rows, DI), BF16),
            shaped((rows, DI), BF16),
            shaped((blocks, N, DI), BF16),
            shaped((blocks, N, DI), BF16),
            shaped((N, DI), BF16),
            shaped((rows, 128), F32),
            shaped((rows, N), F32),
            shaped((8, DI), F32),
        ],
        scratch_shapes=[
            pltpu.VMEM((N, DI), F32),
            pltpu.VMEM((N, DI), F32),
            pltpu.VMEM((GROUPS, Q, 128), F32),
            pltpu.VMEM((Q, DI), F32),
            pltpu.VMEM((Q, DI), F32),
            pltpu.VMEM((Q, DI), F32),
            pltpu.VMEM((Q, DI), F32),
            pltpu.VMEM((Q, DI), F32),
            pltpu.VMEM((Q, 128), F32),
        ],
        compiler_params=params(),
        cost_estimate=cost(15e9, 60e6),
        name="gate",
    )(
        start, ssd, ent, z, val, bc, logd, cum, tokens, cotangent, valid, w_o, gains,
    )

    def columns_of(left, right):
        return lax.dot_general(
            left, right, (((0,), (0,)), ((), ())), preferred_element_type=F32
        ).astype(BF16)

    def in_blocks(a):
        return a.reshape(LINE, 2, 2, 2, a.shape[0] // 32, a.shape[1])

    out_weight_grad = columns_of(gated, branch_grad)
    gate_columns = columns_of(normed, dz)
    mixing_parts = [in_blocks(out_weight_grad)] if boxed else []
    back_parts = [in_blocks(gate_columns)] if boxed else []

    dvp, dbc, dlt, gin, *summed_out = pl.pallas_call(
        lambda *refs: mixing_kernel(len(mixing_parts), *refs),
        grid=(blocks,),
        in_specs=[
            spec((Q, DI), same),
            spec((Q, DI), same),
            spec((Q, 2 * N), same),
            spec((Q, 128), same),
            scalar(),
            whole((N, DI)),
            whole((blocks + 1, 8, DI)),
        ]
        + [pl.BlockSpec(memory_space=pltpu.VMEM) for a in mixing_parts],
        out_specs=[spec((Q, DI), same), spec((Q, 2 * N), same), spec((Q, 128), same), whole((N, DI))]
        + [whole(a.shape[-2:]) for a in mixing_parts],
        out_shape=[
            shaped((rows, DI), BF16), shaped((rows, 2 * N), F32), shaped((rows, 128), F32), shaped((N, DI), BF16),
        ]
        + [shaped(a.shape[-2:], F32) for a in mixing_parts],
        scratch_shapes=[
            pltpu.VMEM((GROUPS, Q, 128), F32),
            pltpu.VMEM((GROUPS, 8, Q), F32),
            pltpu.VMEM((Q, Q), F32),
            pltpu.VMEM((Q, Q), F32),
            pltpu.VMEM((GROUPS, 8, Q), F32),
            pltpu.VMEM((128, Q), F32),
            pltpu.VMEM((GROUPS, Q, 128), F32),
            pltpu.VMEM((N, DI), BF16),
            pltpu.VMEM((N, DI), BF16),
            pltpu.SemaphoreType.DMA((2,)),
        ]
        + [each for a in mixing_parts for each in scatter_scratch(*a.shape[-2:])],
        compiler_params=params(3),
        cost_estimate=cost(15e9, 60e6),
        name="mixing",
    )(ds, vp, bc, logd, keep, gout, cum, *mixing_parts)

    du, last, edge, conv_sums, small, *summed_gate = pl.pallas_call(
        lambda *refs: back_kernel(len(back_parts), *refs),
        grid=(blocks,),
        in_specs=[
            scalar(),
            whole((N, DI)),
            spec((1, N, DI), back3),
            spec((1, N, DI), back3),
            whole((blocks + 1, 8, DI)),
            spec((Q, DI), back),
            spec((Q, DI), back),
            spec((Q, DI), back),
            spec((Q, DI), back),
            spec((Q, CH), back),
            spec((Q, UW), back),
            spec((8, UW), lambda i: (halo_block, 0)),
            spec((Q, 2 * N), back),
            spec((Q, 128), back),
            spec((Q, 128), back),
            spec((Q, 128), back),
            spec((Q, 128), back),
            spec((Q, 128), back),
            spec((Q, 2 * N), back),
            spec((Q, N), back),
            whole((CONVK, CH)),
            whole((1, 128)),
            whole((1, 128)),
            whole((1, DI)),
        ]
        + [pl.BlockSpec(memory_space=pltpu.VMEM) for a in back_parts],
        out_specs=[
            spec((Q, UW), back),
            whole((8, CH)),
            whole((8, CH)),
            whole((8, CH)),
            whole((8, 128)),
        ]
        + [whole(a.shape[-2:]) for a in back_parts],
        out_shape=[
            shaped((rows, UW), BF16),
            shaped((8, CH), F32),
            shaped((8, CH), F32),
            shaped((8, CH), F32),
            shaped((8, 128), F32),
        ]
        + [shaped(a.shape[-2:], F32) for a in back_parts],
        scratch_shapes=[
            pltpu.VMEM((N, DI), F32),
            pltpu.VMEM((GROUPS, Q, 128), F32),
            pltpu.VMEM((GROUPS, Q, 128), F32),
            pltpu.VMEM((Q + 8, CH), F32),
            pltpu.VMEM((8, CH), F32),
            pltpu.VMEM((16, CH), F32),
            pltpu.VMEM((Q, 128), F32),
            pltpu.VMEM((Q, 128), F32),
            pltpu.VMEM((16, 128), F32),
        ]
        + [each for a in back_parts for each in scatter_scratch(*a.shape[-2:])],
        compiler_params=params(4 if back_parts else None),
        cost_estimate=cost(15e9, 60e6),
        name="back",
    )(
        keep, gin, gnext, entt, cum, vp, val, dvp, ds, conv, u, u, bc, logd, step, valid,
        dlp, dlt, dbc, dc, taps, bias, logs, skips, *back_parts,
    )
    edge_back = lax.ppermute(edge, "ctx", [(k + 1, k) for k in range(near - 1)])
    du = lax.dynamic_update_slice(du, (last + edge_back).astype(BF16), (rows - 8, 0))
    conv_columns = columns_of(normed, du)
    across = (((1,), (1,)), ((), ()))
    normed_grad = lax.dot_general(dz, w_z, across, preferred_element_type=F32) + lax.dot_general(
        du, w_u, across, preferred_element_type=F32
    )
    inputs = tokens.astype(F32)
    scale = lax.rsqrt(jnp.mean(inputs * inputs, axis=-1, keepdims=True) + epsilon)
    hat = inputs * scale
    inner = normed_grad * norm_gain
    input_grad = cotangent.astype(F32) + scale * (
        inner - hat * jnp.mean(inner * hat, axis=-1, keepdims=True)
    )
    norm_grad = jnp.sum(normed_grad * hat, axis=0)
    packed = jnp.concatenate(
        [
            norm_grad,
            conv_sums[:5].reshape(-1),
            gate_sums[:2].reshape(-1),
            small[:2].reshape(-1),
        ]
    )
    if boxed:
        (out_weight_grad,) = summed_out
        (gate_columns,) = summed_gate
        conv_columns, summed = scattered([conv_columns], packed.reshape(-1, 128), 5)
        summed = summed.reshape(-1)
    else:
        conv_columns, gate_columns, out_weight_grad = [
            lax.psum_scatter(a.astype(F32), axes, scatter_dimension=0, tiled=True)
            for a in (conv_columns, gate_columns, out_weight_grad)
        ]
        summed = lax.psum(packed, axes)
    in_weight_grad = jnp.concatenate([gate_columns, conv_columns[:, : DPROJ - DI]], 1)
    at = width
    conv_weight_grad = summed[at : at + CONVK * CH].reshape(CONVK, CH)
    at += CONVK * CH
    conv_bias_grad = summed[at : at + CH]
    at += CH
    gate_gain_grad = summed[at : at + DI]
    at += DI
    skip_gain_grad = jnp.sum(summed[at : at + DI].reshape(HEADS, P_SIZE), axis=1)
    at += DI
    step_bias_grad = summed[at : at + HEADS]
    decay_log_grad = summed[at + 128 : at + 128 + HEADS]
    return (
        output,
        input_grad,
        in_weight_grad,
        out_weight_grad,
        summed[:width],
        conv_weight_grad,
        conv_bias_grad,
        step_bias_grad,
        decay_log_grad,
        skip_gain_grad,
        gate_gain_grad,
    )


def solution(mesh):
    split = P(("fsdp", "ctx"), None)
    line = P(("fsdp", "ctx"))
    return jax.shard_map(
        local,
        mesh=mesh,
        in_specs=(split, line, line, split, P(), split, P(), P(), P(), P(), P(), P(), split),
        out_specs=(split, split, split, split, P(), P(), P(), P(), P(), P(), P()),
        check_vma=False,
    )
```

```python
import jax
import jax.numpy as jnp
from jax import lax
from jax.experimental import pallas as pl
from jax.experimental.pallas import tpu as pltpu
from jax.sharding import PartitionSpec as P

DI = 2048
HEADS = 32
P_SIZE = 64
N = 128
CONVK = 4
Q = 256
CH = 2304
DPROJ = 4384
UW = CH + 128
GW = 256
GROUPS = DI // GW
HALF = Q // 2

F32 = jnp.float32
BF16 = jnp.bfloat16
LOG2E = 1.4426950408889634
epsilon = 1e-05


def nn(a, b):
    return lax.dot_general(a, b, (((1,), (0,)), ((), ())), preferred_element_type=F32)


def nt(a, b):
    return lax.dot_general(a, b, (((1,), (1,)), ((), ())), preferred_element_type=F32)


def sigmoid(x):
    return 0.5 * jnp.tanh(0.5 * x) + 0.5


def softplus(x):
    e = jnp.exp(-jnp.abs(x))
    w = 1.0 + e
    d = w - 1.0
    return jnp.maximum(x, 0.0) + jnp.where(d == 0.0, e, jnp.log(w) * (e / jnp.where(d == 0.0, 1.0, d)))


def rows_of(shape):
    return lax.broadcasted_iota(jnp.int32, shape, 0)


def lanes_of(shape):
    return lax.broadcasted_iota(jnp.int32, shape, 1)


def split3(x):
    a = x.astype(BF16)
    r = x - a.astype(F32)
    b = r.astype(BF16)
    return a, b, (r - b.astype(F32)).astype(BF16)


def ordered_sum(triangle, x):
    a, b, c = split3(x)
    return nn(triangle, c) + nn(triangle, b) + nn(triangle, a)


def spread(x, out):
    out[0] = x
    for g in range(1, GROUPS):
        out[g] = pltpu.roll(x, 128 - 4 * g, 1)


def delayed(before, x, by):
    if by == 0:
        return x
    return pltpu.roll(jnp.concatenate([before, x], 0), by, 0)[8:]


def advanced(x, after, by):
    if by == 0:
        return x
    count = x.shape[0]
    return pltpu.roll(jnp.concatenate([x, after], 0), count + 8 - by, 0)[:count]


def fill_picks(out):
    for g in range(GROUPS):
        shape = (128, GW)
        head = lax.shift_right_logical(lanes_of(shape), 6) + 4 * g
        at = rows_of(shape)
        own = jnp.logical_and(jnp.bitwise_and(at, HEADS - 1) == head, at < 3 * HEADS)
        out[:, g * GW : (g + 1) * GW] = jnp.where(own, 1.0, 0.0).astype(BF16)


def in_parts(x):
    lane = lanes_of(x.shape)
    a, b, c = split3(jnp.where(lane < HEADS, x, 0.0))
    wide = a.astype(F32) + pltpu.roll(b.astype(F32), HEADS, 1) + pltpu.roll(c.astype(F32), 2 * HEADS, 1)
    return wide.astype(BF16)


def spread_rows(x, out):
    for g in range(GROUPS):
        out[g, 0:4] = x[4 * g : 4 * g + 4]


def head_lanes(x, i):
    return jnp.broadcast_to(x[:, i : i + 1], (x.shape[0], 128))


def pick_heads(g):
    shape = (GW, 128)
    return jnp.where(
        lax.shift_right_logical(rows_of(shape), 6) + 4 * g == lanes_of(shape), 1.0, 0.0
    ).astype(BF16)


def when_at(now, plan):
    plan = sorted(plan, key=lambda entry: entry[0])
    if len(plan) == 1:
        place, act = plan[0]

        @pl.when(now == place)
        def _():
            act()

    elif plan:
        middle = len(plan) // 2

        def early():
            when_at(now, plan[:middle])

        def late():
            when_at(now, plan[middle:])

        lax.cond(now < plan[middle][0], early, late)


def chain_peers():
    pos = lax.axis_index("ctx")
    return [(pos > 0, {"ctx": pos - 1}), (pos < lax.axis_size("ctx") - 1, {"ctx": pos + 1})]


def pass_on(message, arrived, sems, by):
    return pltpu.make_async_remote_copy(
        src_ref=message, dst_ref=arrived, send_sem=sems.at[0], recv_sem=sems.at[1],
        device_id={"ctx": lax.axis_index("ctx") + by}, device_id_type=pl.DeviceIdType.MESH,
    )


def forward_kernel(count, *refs):
    (
        u_ref, halo_ref, valid_ref, keep_ref, cw_ref, cb_ref, sb_ref, dl_ref, skip_ref,
    ) = refs[:9]
    own = refs[9 : 9 + count]
    (
        val_ref, vp_ref, conv_ref, bc_ref, ssd_ref, ent_ref, log_ref, step_ref, cum_ref, start_ref,
    ) = refs[9 + count : 19 + count]
    outs = refs[19 + count : 19 + 2 * count]
    (
        past, logs, picks, logt, inter, state, all_vp, all_val, all_bc, all_log, message, arrived, sems,
    ) = refs[19 + 2 * count : 32 + 2 * count]
    gather_sems = refs[32 + 2 * count :]
    i = pl.program_id(0)
    blocks = pl.num_programs(0) // 2
    first = i < blocks
    c = jnp.where(first, i, i - blocks)
    near = lax.axis_size("ctx")
    pos = lax.axis_index("ctx")
    plan = []
    if count:
        lists = [Gather(own[k], outs[k], *gather_sems[5 * k : 5 * k + 5]).steps() for k in range(count)]
        length = len(lists[0])
        for at in range(length + 2 * (count - 1)):
            acts = [lists[k][at - 2 * k] for k in range(count) if 0 <= at - 2 * k < length]
            plan.append((FORWARD_PLACES[at], lambda acts=acts: [act() for act in acts]))

    @pl.when(i == 0)
    def _():
        meet((box_peers() if count else []) + chain_peers())
        past[...] = halo_ref[:, :CH] * keep_ref[0, 0]
        fill_picks(picks)
        state[...] = jnp.zeros_like(state)
        cum_ref[...] = jnp.zeros_like(cum_ref)

    half = lanes_of((Q, 128)) < P_SIZE
    square = (Q, Q)
    causal = rows_of(square) >= lanes_of(square)

    @pl.when(first)
    def _():
        raw = u_ref[:, CH:] + sb_ref[...]
        step = softplus(raw) * valid_ref[...]
        step = jnp.where(lanes_of(step.shape) < HEADS, step, 0.0)
        rate = -jnp.exp(dl_ref[...]) * LOG2E
        logd = ordered_sum(jnp.where(causal, 1.0, 0.0).astype(BF16), step * rate)
        log_ref[...] = logd
        all_log[c] = logd
        step_ref[...] = step
        log_parts = in_parts(logd)
        step_parts = in_parts(step)

        def convolved(cols):
            x = u_ref[:, cols]
            before = past[:, cols]
            past[:, cols] = x[Q - 8 :]
            total = cb_ref[:, cols] + cw_ref[CONVK - 1 : CONVK, cols] * x
            for k in range(CONVK - 1):
                total = total + cw_ref[k : k + 1, cols] * delayed(before, x, CONVK - 1 - k)
            return total

        conv_b = convolved(pl.ds(DI, N))
        conv_c = convolved(pl.ds(DI + N, N))
        conv_ref[:, DI : DI + N] = conv_b.astype(BF16)
        conv_ref[:, DI + N :] = conv_c.astype(BF16)
        act_b = conv_b * sigmoid(conv_b)
        act_c = conv_c * sigmoid(conv_c)
        both = jnp.concatenate([act_b.astype(BF16), act_c.astype(BF16)], 1)
        bc_ref[...] = both
        all_bc[c] = both
        turned_b = act_b.T.astype(BF16)
        ent_ref[0] = state[...].astype(BF16)

        def group(g, unused):
            when_at(i * GROUPS + g, plan)
            wide = pl.ds(pl.multiple_of(g * GW, GW), GW)
            log_wide = nn(log_parts, picks[:, wide])
            step_wide = nn(step_parts, picks[:, wide])
            for j in range(2):
                cols = pl.ds(pl.multiple_of(g * GW + 128 * j, 128), 128)
                cv = convolved(cols)
                conv_ref[:, cols] = cv.astype(BF16)
                val = cv * sigmoid(cv)
                low = val.astype(BF16)
                val_ref[:, cols] = low
                all_val[c, :, cols] = low
                lp = log_wide[:, 128 * j : 128 * j + 128]
                vp = val * step_wide[:, 128 * j : 128 * j + 128]
                low = vp.astype(BF16)
                vp_ref[:, cols] = low
                all_vp[c, :, cols] = low
                last = lp[Q - 1 : Q, :]
                weighted = (vp * jnp.exp2(last - lp)).astype(BF16)
                state[:, cols] = jnp.exp2(last) * state[:, cols] + nn(turned_b, weighted)
                cum_ref[c + 1, :, cols] = cum_ref[c, :, cols] + last
            return unused

        lax.fori_loop(0, GROUPS, group, 0)

    for k in range(near):

        @pl.when(jnp.logical_and(i == blocks + k, pos == k))
        def _(k=k):
            if k:
                pass_on(message, arrived, sems, 1).wait_recv()
                entering = keep_ref[0, 0] * arrived[...].astype(F32)
                start_ref[...] = entering.astype(BF16)
            else:
                start_ref[...] = jnp.zeros_like(start_ref)
            if k < near - 1:
                if k:
                    message[...] = (jnp.exp2(cum_ref[blocks, 0:1, :]) * entering + state[...]).astype(BF16)
                else:
                    message[...] = state[...].astype(BF16)
                pass_on(message, arrived, sems, 1).start()

    @pl.when(jnp.logical_not(first))
    def _():
        logd = all_log[c]
        spread(logd, logs)
        spread_rows(logd.T, logt)
        inter[...] = jnp.where(causal, nt(all_bc[c, :, N:], all_bc[c, :, :N]), 0.0)
        left = jnp.where(half[:1], 1.0, 0.0).astype(BF16)
        right = jnp.where(half[:1], 0.0, 1.0).astype(BF16)

        def group(g, unused):
            when_at(i * GROUPS + g, plan)
            lg = logs[g]
            for j in range(2):
                cols = pl.ds(pl.multiple_of(g * GW + 128 * j, 128), 128)
                vp = all_vp[c, :, cols]
                v0 = vp * left
                v1 = vp * right
                top = []
                low = []
                for h in range(2):
                    row = logt[g, 2 * j + h : 2 * j + h + 1]
                    early, late = row[:, :HALF], row[:, HALF:]
                    lb = head_lanes(lg, 2 * j + h)
                    up, down = lb[:HALF], lb[HALF:]
                    top.append((inter[:HALF, :HALF] * jnp.exp2(jnp.minimum(up - early, 0.0))).astype(BF16))
                    low.append((inter[HALF:, :HALF] * jnp.exp2(jnp.minimum(down - early, 0.0))).astype(BF16))
                    low.append((inter[HALF:, HALF:] * jnp.exp2(jnp.minimum(down - late, 0.0))).astype(BF16))
                skipped = skip_ref[:, cols] * all_val[c, :, cols].astype(F32)
                above = nn(jnp.concatenate(top, 1), jnp.concatenate([v0[:HALF], v1[:HALF]], 0))
                below = nn(jnp.concatenate(low, 1), jnp.concatenate([v0, v1], 0))
                ssd_ref[:HALF, cols] = (above + skipped[:HALF]).astype(BF16)
                ssd_ref[HALF:, cols] = (below + skipped[HALF:]).astype(BF16)
            return unused

        lax.fori_loop(0, GROUPS, group, 0)

    @pl.when(jnp.logical_and(i == 2 * blocks - 1, pos < near - 1))
    def _():
        pass_on(message, arrived, sems, 1).wait_send()


def gate_kernel(
    start_ref, ssd_in, ent_ref, z_ref, val_ref, bc_ref, log_ref, cum_ref,
    tok_ref, cot_ref, valid_ref, ow_ref, gain_ref,
    out_ref, gated_ref, bg_ref, ds_ref, dz_ref, entt_ref, gnext_ref, gout_ref, dlp_ref, dc_ref, sums_ref,
    start, gstate, picks, ssd_s, mix_s, el_s, pe_s, gg_s, acc,
):
    i = pl.program_id(0)
    c = pl.num_programs(0) - 1 - i

    @pl.when(i == 0)
    def _():
        start[...] = start_ref[...].astype(F32)
        fill_picks(picks)
        gstate[...] = jnp.zeros_like(gstate)
        sums_ref[...] = jnp.zeros_like(sums_ref)

    log_parts = in_parts(log_ref[...])
    low_c = bc_ref[:, N:]
    turned_c = low_c.astype(F32).T.astype(BF16)
    acc[...] = jnp.zeros_like(acc)

    def enter(g, unused):
        cols = pl.ds(pl.multiple_of(g * GW, GW), GW)
        decay = jnp.exp2(nn(log_parts, picks[:, cols]))
        entering = (
            ent_ref[0, :, cols].astype(F32) + jnp.exp2(cum_ref[c, 0:1, cols]) * start[:, cols]
        ).astype(BF16)
        entt_ref[0, :, cols] = entering
        part = nn(low_c, entering)
        for j in range(2):
            pc = pl.ds(pl.multiple_of(g * GW + 128 * j, 128), 128)
            el = decay[:, 128 * j : 128 * j + 128]
            pe = el * part[:, 128 * j : 128 * j + 128]
            el_s[:, pc] = el
            pe_s[:, pc] = pe
            ssd = ssd_in[:, pc].astype(F32) + pe
            z = z_ref[:, pc].astype(F32)
            mixed = ssd * (z * sigmoid(z))
            ssd_s[:, pc] = ssd
            mix_s[:, pc] = mixed
            acc[...] += mixed * mixed
        return unused

    lax.fori_loop(0, GROUPS, enter, 0)
    inv = lax.rsqrt(jnp.sum(acc[...], axis=1, keepdims=True) * (1.0 / DI) + epsilon)
    inv = jnp.broadcast_to(inv, (Q, 128))
    valid = valid_ref[...]
    valid8 = jnp.concatenate([valid] * (tok_ref.shape[1] // 128), 1)
    branch_grad = (cot_ref[...].astype(F32) * valid8).astype(BF16)
    bg_ref[...] = branch_grad
    acc[...] = jnp.zeros_like(acc)

    def gate(g, unused):
        cols = pl.ds(pl.multiple_of(g * GW, GW), GW)
        ggrad = nt(branch_grad, ow_ref[cols, :])
        for j in range(2):
            pc = pl.ds(pl.multiple_of(g * GW + 128 * j, 128), 128)
            hat = mix_s[:, pc] * inv
            gain = gain_ref[:, pc]
            mix_s[:, pc] = hat
            gated_ref[:, pc] = (hat * gain).astype(BF16)
            gg = ggrad[:, 128 * j : 128 * j + 128]
            both = gg * hat
            sums_ref[0:1, pc] += jnp.sum(both, axis=0, keepdims=True)
            acc[...] += both * gain
            gg_s[:, pc] = gg * gain
        return unused

    lax.fori_loop(0, GROUPS, gate, 0)
    mean = jnp.sum(acc[...], axis=1, keepdims=True) * (1.0 / DI)
    mean = jnp.broadcast_to(mean, (Q, 128))

    for n in range(tok_ref.shape[1] // 256):
        cols = slice(256 * n, 256 * n + 256)
        branch = nn(gated_ref[...], ow_ref[:, cols])
        out_ref[:, cols] = (tok_ref[:, cols].astype(F32) + valid8[:, :256] * branch).astype(BF16)

    acc[...] = jnp.zeros_like(acc)
    dc_ref[...] = jnp.zeros_like(dc_ref)

    def back(g, unused):
        cols = pl.ds(pl.multiple_of(g * GW, GW), GW)
        dparts = []
        prods = []
        for j in range(2):
            pc = pl.ds(pl.multiple_of(g * GW + 128 * j, 128), 128)
            dmixed = inv * (gg_s[:, pc] - mix_s[:, pc] * mean)
            z = z_ref[:, pc].astype(F32)
            s = sigmoid(z)
            ds = (dmixed * (z * s)).astype(BF16)
            ds_ref[:, pc] = ds
            dz_ref[:, pc] = (dmixed * ssd_s[:, pc] * (s * (1.0 + z * (1.0 - s)))).astype(BF16)
            ds = ds.astype(F32)
            sums_ref[1:2, pc] += jnp.sum(ds * val_ref[:, pc].astype(F32), axis=0, keepdims=True)
            dparts.append((ds * el_s[:, pc]).astype(BF16))
            prods.append((ds * pe_s[:, pc]).astype(BF16))
        dpart = jnp.concatenate(dparts, 1)
        acc[...] += nn(jnp.concatenate(prods, 1), pick_heads(g))
        dc_ref[...] += nt(dpart, entt_ref[0, :, cols])
        gnext_ref[0, :, cols] = gstate[:, cols].astype(BF16)
        total = cum_ref[c + 1, 0:1, cols] - cum_ref[c, 0:1, cols]
        gstate[:, cols] = nn(turned_c, dpart) + jnp.exp2(total) * gstate[:, cols]
        return unused

    lax.fori_loop(0, GROUPS, back, 0)
    dlp_ref[...] = acc[...]

    @pl.when(c == 0)
    def _():
        gout_ref[...] = gstate[...].astype(BF16)


FORWARD_PLACES = tuple(5 * k for k in range(13))
MIXING_PLACES = (0, 5, 12, 31)
LINE_PLACES = (1, 4, 8, 12)
BACK_PLACES = (0, 4, 9, 19, 22, 25, 28, 31)


def acting(places, acts):
    joined = {}
    for place, act in zip(places, acts):
        joined.setdefault(place, []).append(act)
    return [(place, lambda acts=acts: [act() for act in acts]) for place, acts in joined.items()]


def plane_scratch(rows, columns):
    dma = pltpu.SemaphoreType.DMA
    return scatter_scratch(rows, columns)[:6] + [dma((4,))] * 4


def line_scratch(rows, columns):
    dma = pltpu.SemaphoreType.DMA
    return [pltpu.VMEM((1, LINE, rows, columns), BF16)] + [pltpu.VMEM((LINE, rows, columns), BF16)] * 2 + [
        dma((2, LINE))
    ] * 2


def mixing_kernel(count, *refs):
    ds_ref, vp_ref, bc_ref, log_ref, keep_ref, gout_ref, cum_ref = refs[:7]
    parts = refs[7 : 7 + count]
    dvp_ref, dbc_ref, dlt_ref, gin_ref = refs[7 + count : 11 + count]
    outs = refs[11 + count : 11 + 2 * count]
    (
        logs, logt, inter, dinter, rowsum, turned, colsum, message, arrived, sems,
    ) = refs[11 + 2 * count : 21 + 2 * count]
    i = pl.program_id(0)
    blocks = pl.num_programs(0)
    near = lax.axis_size("ctx")
    pos = lax.axis_index("ctx")
    plan = []
    if count:
        held = refs[21 + 2 * count :]
        part = Scatter(parts[0], None, *held[:6], None, None, tuple(held[6:10]) + (None, None))
        acts = [part.begin, part.corners, part.sides_out, lambda: part.hand_on(outs[0])]
        plan = acting(MIXING_PLACES, acts)

    @pl.when(i == 0)
    def _():
        meet((box_peers() if count else []) + chain_peers())

    for k in range(near):

        @pl.when(jnp.logical_and(i == k, pos == near - 1 - k))
        def _(k=k):
            total = gout_ref[...].astype(F32)
            if k:
                pass_on(message, arrived, sems, -1).wait_recv()
                gin_ref[...] = arrived[...]
                total = total + jnp.exp2(cum_ref[blocks, 0:1, :]) * arrived[...].astype(F32)
            else:
                gin_ref[...] = jnp.zeros_like(gin_ref)
            if k < near - 1:
                message[...] = (keep_ref[0, 0] * total).astype(BF16)
                pass_on(message, arrived, sems, -1).start()

    @pl.when(jnp.logical_and(i == blocks - 1, pos > 0))
    def _():
        pass_on(message, arrived, sems, -1).wait_send()

    logd = log_ref[...]
    spread(logd, logs)
    spread_rows(logd.T, logt)
    low_b = bc_ref[:, :N]
    low_c = bc_ref[:, N:]
    square = (Q, Q)
    causal = rows_of(square) <= lanes_of(square)
    inter[...] = jnp.where(causal, nt(low_b, low_c), 0.0)
    dinter[...] = jnp.zeros_like(dinter)
    half = lanes_of((Q, 128)) < P_SIZE
    lane = lanes_of((HALF, 128))

    def group(g, unused):
        when_at(i * GROUPS + g, plan)
        lg = logs[g]
        first_col = jnp.zeros((HALF, 128), F32)
        second_col = jnp.zeros((HALF, 128), F32)
        for j in range(2):
            cols = pl.ds(pl.multiple_of(g * GW + 128 * j, 128), 128)
            vp = vp_ref[:, cols].astype(F32)
            ds = ds_ref[:, cols]
            wide = ds.astype(F32)
            first = []
            second = []
            outs = []
            for h in range(2):
                head = 2 * j + h
                own = half if h == 0 else jnp.logical_not(half)
                vm = jnp.where(own, vp, 0.0).astype(BF16)
                dsm = jnp.where(own, wide, 0.0).astype(BF16)
                outs.append(dsm)
                row = logt[g, head : head + 1]
                early, late = row[:, :HALF], row[:, HALF:]
                lb = head_lanes(lg, head)
                up, down = lb[:HALF], lb[HALF:]
                dup = nt(vm[:HALF], ds)
                ddown = nt(vm[HALF:], ds[HALF:])
                decay = jnp.exp2(jnp.minimum(early - up, 0.0))
                grad = dup[:, :HALF] * decay
                dinter[:HALF, :HALF] += grad
                part = inter[:HALF, :HALF]
                first.append((part * decay).astype(BF16))
                both = grad * part
                row_early = jnp.sum(both, axis=0, keepdims=True)
                col = both
                decay = jnp.exp2(jnp.minimum(late - up, 0.0))
                grad = dup[:, HALF:] * decay
                dinter[:HALF, HALF:] += grad
                part = inter[:HALF, HALF:]
                first.append((part * decay).astype(BF16))
                both = grad * part
                row_late = jnp.sum(both, axis=0, keepdims=True)
                col = jnp.sum(col + both, axis=1, keepdims=True)
                first_col = jnp.where(lane == head, col, first_col)
                decay = jnp.exp2(jnp.minimum(late - down, 0.0))
                grad = ddown * decay
                dinter[HALF:, HALF:] += grad
                part = inter[HALF:, HALF:]
                second.append((part * decay).astype(BF16))
                both = grad * part
                row_late = row_late + jnp.sum(both, axis=0, keepdims=True)
                col = jnp.sum(both, axis=1, keepdims=True)
                second_col = jnp.where(lane == head, col, second_col)
                rowsum[g, head : head + 1, :HALF] = row_early
                rowsum[g, head : head + 1, HALF:] = row_late
            dvp_ref[:HALF, cols] = nn(
                jnp.concatenate(first, 1), jnp.concatenate(outs, 0)
            ).astype(BF16)
            dvp_ref[HALF:, cols] = nn(
                jnp.concatenate(second, 1), jnp.concatenate([outs[0][HALF:], outs[1][HALF:]], 0)
            ).astype(BF16)
        colsum[g, :HALF] = first_col
        colsum[g, HALF:] = second_col
        return unused

    lax.fori_loop(0, GROUPS, group, 0)
    turned[...] = jnp.zeros_like(turned)
    for g in range(GROUPS):
        turned[4 * g : 4 * g + 4] = rowsum[g, 0:4]
    total = turned[...].T
    for g in range(GROUPS):
        total = total - (colsum[g] if g == 0 else pltpu.roll(colsum[g], 4 * g, 1))
    dlt_ref[...] = total
    masked = jnp.where(causal, dinter[...], 0.0)
    dbc_ref[:, :N] = nn(masked.astype(BF16), low_c)
    dbc_ref[:, N:] = nn(masked.T.astype(BF16), low_b)


def back_kernel(count, *refs):
    (
        keep_ref, gin_ref, gnext_ref, entt_ref, cum_ref, vp_ref, val_ref, dvp_ref, ds_ref, conv_ref,
        u_ref, halo_ref, bc_ref, log_ref, step_ref, valid_ref, dlp_ref, dlt_ref, dbc_ref, dc_ref,
        cw_ref, sb_ref, dl_ref, skip_ref,
    ) = refs[:24]
    parts = refs[24 : 24 + count]
    du_ref, last_ref, edge_ref, sums_ref, small_ref = refs[24 + count : 29 + count]
    outs = refs[29 + count : 29 + 2 * count]
    gin, picks, head, epad, dlw, dst, drow = refs[29 + 2 * count : 36 + 2 * count]
    plan = []
    if count:
        held = refs[36 + 2 * count :]
        full = Scatter(parts[1], outs[1], *held[:8], held[8:14])
        line = Scatter(None, outs[0], None, held[14], None, None, None, None, *held[15:17], (None,) * 4 + tuple(held[17:19]))
        acts = [lambda: line.line(3), lambda: line.line(2), lambda: line.line(1), line.line_done]
        plan = acting(BACK_PLACES + LINE_PLACES, full.steps() + acts)
    i = pl.program_id(0)
    top = pl.num_programs(0)
    c = top - 1 - i

    @pl.when(i == 0)
    def _():
        if count:
            meet(box_peers())
            line.kept[0] = parts[0][...]
        gin[...] = gin_ref[...].astype(F32)
        fill_picks(picks)
        head[...] = jnp.zeros_like(head)
        sums_ref[...] = jnp.zeros_like(sums_ref)
        small_ref[...] = jnp.zeros_like(small_ref)

    log_parts = in_parts(log_ref[...])
    step_parts = in_parts(step_ref[...])
    low_b = bc_ref[:, :N]
    dlw[...] = jnp.zeros_like(dlw)
    dst[...] = jnp.zeros_like(dst)
    drow[...] = jnp.zeros_like(drow)

    def conv_back(cols, dact):
        cv = conv_ref[:, cols].astype(F32)
        s = sigmoid(cv)
        dcv = dact * (s * (1.0 + cv * (1.0 - s)))
        after = head[:, cols]
        head[:, cols] = dcv[:8]
        x = u_ref[:, cols]
        sums_ref[4:5, cols] += jnp.sum(dcv, axis=0, keepdims=True)
        total = None
        for j in range(CONVK):
            k = CONVK - 1 - j
            moved = advanced(dcv, after, j)
            sums_ref[k : k + 1, cols] += jnp.sum(moved * x, axis=0, keepdims=True)
            term = cw_ref[k : k + 1, cols] * moved
            total = term if total is None else total + term
        du_ref[:, cols] = total.astype(BF16)

        @pl.when(i == 0)
        def _():
            last_ref[:, cols] = total[Q - 8 :]

    def group(g, db):
        when_at(i * GROUPS + g, plan)
        cols = pl.ds(pl.multiple_of(g * GW, GW), GW)
        log_wide = nn(log_parts, picks[:, cols])
        step_wide = nn(step_parts, picks[:, cols])
        done = cum_ref[c + 1, 0:1, cols]
        after = jnp.exp2(cum_ref[top, 0:1, cols] - done)
        grad = gnext_ref[0, :, cols].astype(F32) + after * gin[:, cols]
        low_g = grad.astype(BF16)
        decay = jnp.exp2(done - cum_ref[c, 0:1, cols])
        row = decay * jnp.sum(grad * entt_ref[0, :, cols].astype(F32), axis=0, keepdims=True)
        coarse = row.astype(BF16).astype(F32)
        r = rows_of((16, GW))
        two = jnp.where(r == 0, jnp.broadcast_to(coarse, (16, GW)), 0.0)
        two = jnp.where(r == 1, jnp.broadcast_to(row - coarse, (16, GW)), two)
        chosen = pick_heads(g)
        drow[...] += nn(two.astype(BF16), chosen)
        dweighted = nn(low_b, low_g)
        weights = []
        moves = []
        stepped = []
        dacts = []
        for j in range(2):
            pc = pl.ds(pl.multiple_of(g * GW + 128 * j, 128), 128)
            lp = log_wide[:, 128 * j : 128 * j + 128]
            sp = step_wide[:, 128 * j : 128 * j + 128]
            fade = jnp.exp2(lp[Q - 1 : Q, :] - lp)
            vp = vp_ref[:, pc].astype(F32)
            faded = dweighted[:, 128 * j : 128 * j + 128] * fade
            weights.append((vp * fade).astype(BF16))
            moves.append((faded * vp).astype(BF16))
            both = dvp_ref[:, pc].astype(F32) + faded
            stepped.append((both * val_ref[:, pc].astype(F32)).astype(BF16))
            dacts.append((pc, sp * both + skip_ref[:, pc] * ds_ref[:, pc].astype(F32)))
        dlw[...] += nn(jnp.concatenate(moves, 1), chosen)
        dst[...] += nn(jnp.concatenate(stepped, 1), chosen)
        for pc, dact in dacts:
            conv_back(pc, dact)
        return db + nt(jnp.concatenate(weights, 1), low_g)

    db = lax.fori_loop(0, GROUPS, group, dbc_ref[:, :N])
    conv_back(pl.ds(DI, N), db)
    conv_back(pl.ds(DI + N, N), dbc_ref[:, N:] + dc_ref[...])

    moved = dlw[...]
    at_last = jnp.sum(moved, axis=0, keepdims=True) + drow[0:1] + drow[1:2]
    dlog = dlp_ref[...] + dlt_ref[...] - moved
    dlog = dlog + jnp.where(rows_of(dlog.shape) == Q - 1, at_last, 0.0)
    square = (Q, Q)
    later = jnp.where(rows_of(square) <= lanes_of(square), 1.0, 0.0).astype(BF16)
    dsum = ordered_sum(later, dlog)
    rate = -jnp.exp(dl_ref[...])
    dstep = (dst[...] + dsum * rate) * valid_ref[...]
    raw = u_ref[:, CH:] + sb_ref[...]
    draw = dstep * (1.0 / (1.0 + jnp.exp(-raw)))
    draw = jnp.where(lanes_of(draw.shape) < HEADS, draw, 0.0)
    du_ref[:, CH:] = draw.astype(BF16)
    small_ref[0:1] += jnp.sum(draw, axis=0, keepdims=True)
    small_ref[1:2] += jnp.sum(dsum * step_ref[...], axis=0, keepdims=True) * rate

    @pl.when(c == 0)
    def _():
        epad[0:8, :] = jnp.zeros((8, CH), F32)
        epad[8:16, :] = head[...]
        x = halo_ref[:, :CH] * keep_ref[0, 0]
        total = jnp.zeros((8, CH), F32)
        for j in range(CONVK):
            k = CONVK - 1 - j
            moved = epad[j : j + 8, :]
            sums_ref[k : k + 1, :] += jnp.sum(moved * x, axis=0, keepdims=True)
            total = total + cw_ref[k : k + 1, :] * moved
        edge_ref[...] = total * keep_ref[0, 0]


def spec(block, index):
    return pl.BlockSpec(block, index)


def whole(shape):
    return pl.BlockSpec(shape, lambda *_: (0,) * len(shape))


def scalar():
    return pl.BlockSpec(memory_space=pltpu.SMEM)


def shaped(shape, kind):
    return jax.ShapeDtypeStruct(shape, kind)


def cost(flops, moved):
    return pl.CostEstimate(flops=int(flops), bytes_accessed=int(moved), transcendentals=0)


def params(number=None):
    return pltpu.CompilerParams(
        dimension_semantics=("arbitrary",), vmem_limit_bytes=60 * 1024 * 1024, collective_id=number,
        has_side_effects=number is not None,
    )


LINE = 4


def my_place():
    f = lax.axis_index("fsdp")
    t = lax.axis_index("ctx")
    return f // 2, f % 2, t // 2, t % 2


def device_at(z, y, x, core):
    return {"fsdp": z * 2 + y, "ctx": x * 2 + core}


def order_of(z, y, x, core):
    return (z * 2 + y) * 4 + x * 2 + core


def box_peers():
    z, y, x, core = my_place()
    return [
        (None, device_at(z, y, x, 1 - core)), (None, device_at(z, y, 1 - x, core)),
        (None, device_at(z, 1 - y, x, core)),
        (z > 0, device_at(z - 1, y, x, core)), (z < LINE - 1, device_at(z + 1, y, x, core)),
    ]


def meet(peers):
    barrier = pltpu.get_barrier_semaphore()
    count = 0
    for valid, peer in peers:

        def greet(peer=peer):
            pl.semaphore_signal(barrier, inc=1, device_id=peer, device_id_type=pl.DeviceIdType.MESH)

        if valid is None:
            greet()
            count = count + 1
        else:
            pl.when(valid)(greet)
            count = count + jnp.where(valid, 1, 0)
    pl.semaphore_wait(barrier, count)


def send(src, dst, send_sem, recv_sem, peer):
    return pltpu.make_async_remote_copy(
        src_ref=src, dst_ref=dst, send_sem=send_sem, recv_sem=recv_sem,
        device_id=device_at(*peer), device_id_type=pl.DeviceIdType.MESH,
    )


class Gather:
    def __init__(self, own, out, recv, halves, twin, sent, here):
        self.own, self.out, self.rows = own, out, own.shape[0]
        self.recv, self.halves, self.twin, self.sent, self.here = recv, halves, twin, sent, here
        self.place = my_place()

    def block(self, z, y, x, core, half=None):
        size = self.rows if half is None else self.rows // 2
        start = order_of(z, y, x, core) * self.rows + (0 if half is None else half * size)
        return self.out.at[pl.ds(pl.multiple_of(start, 16), size)]

    def copy(self, origin, way, half=None, own=False):
        z, y, x, core = self.place
        oz, oy, ox = origin
        o = oz * 4 + oy * 2 + ox
        dst = self.block(oz, oy, ox, core, half)
        src = self.own if own else dst
        peer = {
            "up": (z + 1, y, x, core), "down": (z - 1, y, x, core), "x": (z, y, 1 - x, core),
            "y": (z, 1 - y, x, core), "twin": (z, y, x, 1 - core),
        }[way]
        sem = self.sent.at[("up", "down", "x", "y", "twin").index(way), o]
        if way == "twin":
            arrival = self.twin.at[o]
        elif half is not None:
            arrival = self.halves.at[half, o]
        else:
            arrival = self.recv.at[o]
        return send(src, dst, sem, arrival, peer)

    def arrived(self, origin, half=None):
        self.copy(origin, "x", half).wait_recv()

    def column(self, r):
        z = self.place[0]
        if r == 0:
            return [(None, z, True, True)]
        return [(z - r >= 0, z - r, True, False), (z + r < LINE, z + r, False, True)]

    def each(self, r, act):
        for valid, oz, below, above in self.column(r):
            if valid is None:
                act(oz, below, above)
            else:
                pl.when(valid)(lambda oz=oz, below=below, above=above: act(oz, below, above))

    def begin(self):
        z, y, x, core = self.place
        pltpu.make_async_copy(self.own, self.block(z, y, x, core), self.here).start()
        self.forward(0)

    def ways(self, oz, below, above, act):
        z = self.place[0]
        if below:
            pl.when(z < LINE - 1)(lambda: act("up"))
        if above:
            pl.when(z > 0)(lambda: act("down"))
        act("x")
        act("y")
        act("twin")

    def forward(self, r):
        z, y, x, core = self.place

        def act(oz, below, above):
            origin = (oz, y, x)
            if r:
                self.arrived(origin)
            self.ways(oz, below, above, lambda way: self.copy(origin, way, own=r == 0).start())

        self.each(r, act)

    def across(self, r):
        z, y, x, core = self.place

        def act(oz, below, above):
            self.arrived((oz, y, 1 - x))
            self.copy((oz, y, 1 - x), "y", 0).start()
            self.copy((oz, y, 1 - x), "twin").start()
            self.arrived((oz, 1 - y, x))
            self.copy((oz, 1 - y, x), "x", 1).start()
            self.copy((oz, 1 - y, x), "twin").start()

        self.each(r, act)

    def corner(self, r):
        z, y, x, core = self.place

        def act(oz, below, above):
            origin = (oz, 1 - y, 1 - x)
            self.arrived(origin, 0)
            self.arrived(origin, 1)
            self.copy(origin, "twin").start()

        self.each(r, act)

    def finish(self):
        z, y, x, core = self.place
        pltpu.make_async_copy(self.own, self.block(z, y, x, core), self.here).wait()
        for r in range(LINE):

            def act(oz, below, above, r=r):
                self.ways(oz, below, above, lambda way: self.copy((oz, y, x), way, own=r == 0).wait_send())
                self.copy((oz, y, 1 - x), "y", 0).wait_send()
                self.copy((oz, 1 - y, x), "x", 1).wait_send()
                for oy, ox in ((y, 1 - x), (1 - y, x), (1 - y, 1 - x)):
                    self.copy((oz, oy, ox), "twin").wait_send()
                for oy, ox in ((y, x), (y, 1 - x), (1 - y, x), (1 - y, 1 - x)):
                    self.copy((oz, oy, ox), "twin").wait_recv()

            self.each(r, act)

    def steps(self):
        return [
            self.begin,
            lambda: self.forward(1),
            lambda: self.across(0),
            lambda: self.forward(2),
            lambda: self.across(1),
            lambda: (self.forward(3), self.corner(0)),
            lambda: self.across(2),
            lambda: self.corner(1),
            lambda: self.across(3),
            lambda: (self.corner(2), self.corner(3)),
            self.finish,
        ]


def gather_scratch():
    dma = pltpu.SemaphoreType.DMA
    return [dma((16,)), dma((2, 16)), dma((16,)), dma((5, 16)), dma(())]


def gather_kernel(count, *refs):
    own, out, sems = refs[:count], refs[count : 2 * count], refs[2 * count :]
    meet(box_peers())
    lists = [
        Gather(own[k], out[k], *sems[5 * k : 5 * k + 5]).steps() for k in range(count)
    ]
    length = len(lists[0])
    for at in range(length + 2 * (count - 1)):
        for k in range(count):
            if 0 <= at - 2 * k < length:
                lists[k][at - 2 * k]()


def gathered(arrays, number):
    count = len(arrays)
    anywhere = pl.BlockSpec(memory_space=pl.ANY)
    return pl.pallas_call(
        lambda *refs: gather_kernel(count, *refs),
        in_specs=[anywhere] * count,
        out_specs=[anywhere] * count,
        out_shape=[shaped((32 * a.shape[0], a.shape[1]), a.dtype) for a in arrays],
        scratch_shapes=gather_scratch() * count,
        compiler_params=pltpu.CompilerParams(collective_id=number, has_side_effects=True),
        name="gather",
    )(*arrays)


class Scatter:
    def __init__(self, parts, out, got, kept, mixed_y, mixed_x, from_x, from_y, up, down, sems):
        self.parts, self.out = parts, out
        self.got, self.kept = got, kept
        self.mixed = (mixed_y, mixed_x)
        self.sides = (from_x, from_y)
        self.up, self.down = up, down
        self.twin_sent, self.twin_recv, self.sent, self.recv, self.line_sent, self.line_recv = sems
        self.place = my_place()
        self.rows = kept.shape[-2]
        self.last = kept.shape[0] - 1

    def groups(self):
        z, y, x, core = self.place
        return [(1 - y, 1 - x), (y, 1 - x), (1 - y, x), (y, x)]

    def to_twin(self, k):
        z, y, x, core = self.place
        gy, gx = self.groups()[k]
        return send(
            self.parts.at[:, gy * 4 + gx * 2 + 1 - core], self.got.at[k], self.twin_sent.at[k], self.twin_recv.at[k],
            (z, y, x, 1 - core),
        )

    def begin(self):
        for k in range(4):
            self.to_twin(k).start()

    def add(self, k, sources, first=0, rows=None):
        rows = self.rows if rows is None else rows
        pieces = rows // 16

        def piece(n, unused):
            b = n // pieces
            at = (n - b * pieces) * 16
            here = pl.ds(pl.multiple_of(first + at, 16), 16)
            total = None
            for source in sources:
                term = source(b, pl.multiple_of(at, 16), here).astype(F32)
                total = term if total is None else total + term
            self.kept[k, b, here] = total.astype(BF16)
            return unused

        lax.fori_loop(0, LINE * pieces, piece, 0)

    def own(self, k):
        return lambda b, at, here: self.kept[k, b, here]

    def both(self, k):
        z, y, x, core = self.place
        gy, gx = self.groups()[k]
        self.to_twin(k).wait_recv()
        self.add(
            k, [lambda b, at, here: self.parts[b, gy * 4 + gx * 2 + core, here], lambda b, at, here: self.got[k, b, here]]
        )

    def corner_copy(self, half):
        z, y, x, core = self.place
        size = self.rows // 2
        src = self.kept.at[0, :, pl.ds(half * size, size)]
        peer = (z, 1 - y, x, core) if half == 0 else (z, y, 1 - x, core)
        return send(src, self.mixed[half], self.sent.at[half], self.recv.at[half], peer)

    def side_copy(self, k):
        z, y, x, core = self.place
        peer = (z, y, 1 - x, core) if k == 1 else (z, 1 - y, x, core)
        return send(self.kept.at[k], self.sides[k - 1], self.sent.at[1 + k], self.recv.at[1 + k], peer)

    def corners(self):
        self.both(0)
        self.corner_copy(0).start()
        self.corner_copy(1).start()
        self.both(1)
        self.both(2)
        self.both(3)

    def sides_out(self):
        size = self.rows // 2
        for half, k in ((0, 1), (1, 2)):
            self.corner_copy(half).wait_recv()
            self.add(
                k, [self.own(k), lambda b, at, here, half=half: self.mixed[half][b, pl.ds(at, 16)]],
                half * size, size,
            )
            self.side_copy(k).start()

    def sides_in(self):
        self.side_copy(1).wait_recv()
        self.side_copy(2).wait_recv()
        self.add(
            3,
            [
                self.own(3), lambda b, at, here: self.sides[0][b, here], lambda b, at, here: self.sides[1][b, here],
            ],
        )

    def line_copy(self, oz, way):
        z, y, x, core = self.place
        buffer = self.up if way == 0 else self.down
        peer = (z + 1, y, x, core) if way == 0 else (z - 1, y, x, core)
        return send(
            self.kept.at[self.last, oz], buffer.at[oz], self.line_sent.at[way, oz], self.line_recv.at[way, oz], peer
        )

    def add_line(self, oz, buffer):
        def piece(n, unused):
            here = pl.ds(pl.multiple_of(n * 16, 16), 16)
            total = self.kept[self.last, oz, here].astype(F32) + buffer[oz, here].astype(F32)
            self.kept[self.last, oz, here] = total.astype(BF16)
            return unused

        lax.fori_loop(0, self.rows // 16, piece, 0)

    def line(self, r):
        z = self.place[0]

        def upward():
            oz = z + r

            @pl.when(z > 0)
            def _():
                self.line_copy(oz, 0).wait_recv()
                self.add_line(oz, self.up)

            self.line_copy(oz, 0).start()

        def downward():
            oz = z - r

            @pl.when(z < LINE - 1)
            def _():
                self.line_copy(oz, 1).wait_recv()
                self.add_line(oz, self.down)

            self.line_copy(oz, 1).start()

        pl.when(z + r < LINE)(upward)
        pl.when(z - r >= 0)(downward)

    def plane_sent(self):
        for k in range(4):
            self.to_twin(k).wait_send()
        for half in range(2):
            self.corner_copy(half).wait_send()
        for k in (1, 2):
            self.side_copy(k).wait_send()

    def hand_on(self, out):
        self.sides_in()
        out[...] = self.kept[self.last]
        self.plane_sent()

    def line_done(self):
        z = self.place[0]
        self.out[...] = self.kept[self.last, z].astype(F32)

        @pl.when(z > 0)
        def _():
            self.line_copy(z, 0).wait_recv()
            self.out[...] += self.up[z].astype(F32)

        @pl.when(z < LINE - 1)
        def _():
            self.line_copy(z, 1).wait_recv()
            self.out[...] += self.down[z].astype(F32)

        for r in range(1, LINE):
            pl.when(z + r < LINE)(lambda r=r: self.line_copy(z + r, 0).wait_send())
            pl.when(z - r >= 0)(lambda r=r: self.line_copy(z - r, 1).wait_send())

    def finish(self):
        self.line_done()
        self.plane_sent()

    def steps(self):
        return [
            self.begin, self.corners, self.sides_out, self.sides_in, lambda: self.line(3), lambda: self.line(2),
            lambda: self.line(1), self.finish,
        ]


def scatter_scratch(rows, columns):
    dma = pltpu.SemaphoreType.DMA
    half = rows // 2
    return [
        pltpu.VMEM((4, LINE, rows, columns), BF16),
        pltpu.VMEM((4, LINE, rows, columns), BF16),
        pltpu.VMEM((LINE, half, columns), BF16),
        pltpu.VMEM((LINE, half, columns), BF16),
        pltpu.VMEM((LINE, rows, columns), BF16),
        pltpu.VMEM((LINE, rows, columns), BF16),
        pltpu.VMEM((LINE, rows, columns), BF16),
        pltpu.VMEM((LINE, rows, columns), BF16),
        dma((4,)), dma((4,)), dma((4,)), dma((4,)), dma((2, LINE)), dma((2, LINE)),
    ]


class Total:
    def __init__(self, own, out, held, got, sent, recv):
        self.own, self.out, self.held, self.got, self.sent, self.recv = own, out, held, got, sent, recv

    def copy(self, k):
        z, y, x, core = my_place()
        near = z + 1 - 2 * (z % 2)
        peer = [
            (z, y, x, 1 - core), (z, y, 1 - x, core), (z, 1 - y, x, core), (near, y, x, core),
            ((z + 2) % LINE, y, x, core),
        ][k]
        return send(self.own if k == 0 else self.held.at[k], self.got.at[k], self.sent.at[k], self.recv.at[k], peer)

    def begin(self):
        self.copy(0).start()

    def turn(self, k):
        self.copy(k).wait_recv()
        mine = self.own[...] if k == 0 else self.held[k]
        total = mine + self.got[k]
        if k < 4:
            self.held[k + 1] = total
            self.copy(k + 1).start()
        else:
            self.out[...] = total

    def finish(self):
        for k in range(5):
            self.copy(k).wait_send()

    def steps(self):
        return [self.begin] + [lambda k=k: self.turn(k) for k in range(5)] + [self.finish]


WIDE = 256
SPLIT = 1280


def final_kernel(*refs):
    (
        turned_ref, du_cols, dz_ref, du_ref, tok_ref, cot_ref, gain_ref, wz_any, wu_any, gate_ref, conv_ref, gsum_ref,
        small_ref,
    ) = refs[:13]
    grad_ref, inw_ref, sums_ref = refs[13:16]
    (
        wz, wu, sems, parts_a, parts_b, out_a, out_b, packed, normed_grad, held, got, sent, recv,
    ) = refs[16:29]
    i = pl.program_id(0)
    steps = pl.num_programs(0) - tok_blocks(turned_ref)
    z, y, x, core = my_place()
    scr_a, scr_b = refs[29:43], refs[43:57]
    sum_a = Scatter(parts_a, out_a, *scr_a[:8], scr_a[8:])
    sum_b = Scatter(parts_b, out_b, *scr_b[:8], scr_b[8:])
    small = Total(packed, sums_ref, held, got, sent, recv)
    load_z = pltpu.make_async_copy(wz_any, wz, sems.at[0])
    load_u = pltpu.make_async_copy(wu_any, wu, sems.at[1])

    @pl.when(i == 0)
    def _():
        load_z.start()
        load_u.start()
        meet(box_peers() + [(None, device_at((z + 2) % LINE, y, x, core))])
        packed[...] = jnp.zeros_like(packed)
        packed[0:5, :] = conv_ref[0:5, :]
        packed[5:6, :DI] = gsum_ref[0:1, :]
        packed[5:6, DI : DI + 128] = small_ref[0:1, :]
        packed[5:6, DI + 128 :] = small_ref[1:2, :]
        packed[6:7, :DI] = gsum_ref[1:2, :]
        inw_ref[:, :DI] = gate_ref[...]

    plan = [
        (20, sum_a.begin), (32, sum_a.corners), (40, sum_b.begin), (42, sum_a.sides_out), (47, sum_b.corners),
        (52, sum_a.sides_in), (53, lambda: sum_a.line(3)), (54, sum_b.sides_out),
    ]

    @pl.when(i < steps)
    def _():
        when_at(4 * i, plan[:2])
        result = nn(turned_ref[...], du_cols[...]).astype(BF16)
        rows = parts_a.shape[2]

        def keep(parts, cols, width):
            for b in range(LINE):
                for q in range(8):
                    first = (b * 8 + q) * rows
                    parts[b, q, :, cols] = result[first : first + rows, :width]

        edge = SPLIT // WIDE

        @pl.when(i < edge)
        def _():
            keep(parts_a, pl.ds(pl.multiple_of(i * WIDE, WIDE), WIDE), WIDE)

        @pl.when(jnp.logical_and(i >= edge, i < steps - 1))
        def _():
            keep(parts_b, pl.ds(pl.multiple_of((i - edge) * WIDE, WIDE), WIDE), WIDE)

        @pl.when(i == steps - 1)
        def _():
            keep(parts_b, slice((steps - 1 - edge) * WIDE, UW - SPLIT), UW - SPLIT - (steps - 1 - edge) * WIDE)

    @pl.when(i == steps)
    def _():
        load_z.wait()
        load_u.wait()

    @pl.when(i >= steps)
    def _():
        width = tok_ref.shape[1]
        chunk = width // 4

        def part(n, unused):
            when_at(4 * i + n, plan[2:])
            feats = pl.ds(pl.multiple_of(n * chunk, chunk), chunk)
            normed_grad[:, feats] = nt(dz_ref[...], wz[feats, :]) + nt(du_ref[...], wu[feats, :])
            return unused

        lax.fori_loop(0, 4, part, 0)
        values = tok_ref[...].astype(F32)
        scale = lax.rsqrt(jnp.sum(values * values, axis=1, keepdims=True) * (1.0 / width) + epsilon)
        hat = values * scale
        grad = normed_grad[...]
        packed[7:8, :width] += jnp.sum(grad * hat, axis=0, keepdims=True)
        inner = grad * gain_ref[...]
        mean = jnp.sum(inner * hat, axis=1, keepdims=True) * (1.0 / width)
        grad_ref[...] = cot_ref[...].astype(F32) + scale * (inner - hat * mean)

    @pl.when(i == pl.num_programs(0) - 1)
    def _():
        small.begin()
        sum_a.line(2)
        small.turn(0)
        sum_a.line(1)
        small.turn(1)
        sum_b.sides_in()
        sum_b.line(3)
        sum_a.finish()
        small.turn(2)
        sum_b.line(2)
        small.turn(3)
        sum_b.line(1)
        small.turn(4)
        sum_b.finish()
        small.finish()
        inw_ref[:, DI : DI + SPLIT] = out_a[...]
        inw_ref[:, DI + SPLIT :] = out_b[:, : DPROJ - DI - SPLIT]


def tok_blocks(turned_ref):
    return turned_ref.shape[1] // Q


def final(turned, du, dz, tokens, cotangent, gain, w_z, w_u, gate_columns, conv_sums, gate_sums, small, number):
    width, rows = turned.shape
    steps = -(-UW // WIDE)
    blocks = rows // Q
    dma = pltpu.SemaphoreType.DMA
    own = width // 32
    anywhere = pl.BlockSpec(memory_space=pl.ANY)
    later = lambda i: (jnp.maximum(i - steps, 0), 0)
    sums = (8, CH)
    return pl.pallas_call(
        final_kernel,
        grid=(steps + blocks,),
        in_specs=[
            whole((width, rows)),
            spec((rows, WIDE), lambda i: (0, jnp.minimum(i, steps - 1))),
            spec((Q, DI), later),
            spec((Q, UW), later),
            spec((Q, width), later),
            spec((Q, width), later),
            whole((1, width)),
            anywhere,
            anywhere,
            whole((own, DI)),
            whole(sums),
            whole((8, DI)),
            whole((8, 128)),
        ],
        out_specs=[spec((Q, width), later), whole((own, DPROJ)), whole(sums)],
        out_shape=[shaped((rows, width), F32), shaped((own, DPROJ), F32), shaped(sums, F32)],
        scratch_shapes=[
            pltpu.VMEM((width, DI), BF16),
            pltpu.VMEM((width, UW), BF16),
            dma((2,)),
            pltpu.VMEM((LINE, 8, own, SPLIT), BF16),
            pltpu.VMEM((LINE, 8, own, UW - SPLIT), BF16),
            pltpu.VMEM((own, SPLIT), F32),
            pltpu.VMEM((own, UW - SPLIT), F32),
            pltpu.VMEM(sums, F32),
            pltpu.VMEM((Q, width), F32),
            pltpu.VMEM((5,) + sums, F32),
            pltpu.VMEM((5,) + sums, F32),
            dma((5,)),
            dma((5,)),
        ]
        + scatter_scratch(own, SPLIT)
        + scatter_scratch(own, UW - SPLIT),
        compiler_params=params(number),
        cost_estimate=cost(20e9, 60e6),
        name="final",
    )(turned, du, dz, du, tokens, cotangent, gain, w_z, w_u, gate_columns, conv_sums, gate_sums, small)


def local(
    tokens,
    valid_mask,
    stretch_start,
    cotangent,
    norm_gain,
    in_weight,
    conv_weight,
    conv_bias,
    step_bias,
    decay_log,
    skip_gain,
    gate_gain,
    out_weight,
):
    axes = ("fsdp", "ctx")
    rows, width = tokens.shape
    blocks = rows // Q
    near = lax.axis_size("ctx")
    halo_tokens = lax.ppermute(
        tokens[rows - 8 :], "ctx", [(k, k + 1) for k in range(near - 1)]
    )
    own_u = jnp.pad(in_weight[:, DI:], ((0, 0), (0, UW - (DPROJ - DI))))
    own_z = in_weight[:, :DI]
    boxed = lax.axis_size("fsdp") == 8 and near == 4
    if boxed:
        (w_u,) = gathered([own_u], 1)
        later = [own_z, out_weight]
    else:
        w_u, w_z, w_o = [lax.all_gather(a, axes, axis=0, tiled=True) for a in (own_u, own_z, out_weight)]
        later = []
    extra = len(later)
    anywhere = pl.BlockSpec(memory_space=pl.ANY)

    def hats(values):
        wide = values.astype(F32)
        return wide * lax.rsqrt(jnp.mean(wide * wide, axis=-1, keepdims=True) + epsilon)

    normed_more = (hats(jnp.concatenate([tokens, halo_tokens], 0)) * norm_gain).astype(BF16)
    normed = normed_more[:rows]
    valid = jnp.broadcast_to(valid_mask.astype(F32)[:, None], (rows, 128))
    keep = (1.0 - stretch_start[0].astype(F32)).reshape(1, 1)
    taps = conv_weight
    shift = conv_bias.reshape(1, CH)
    bias = jnp.pad(step_bias, (0, 128 - HEADS)).reshape(1, 128)
    logs = jnp.pad(decay_log, (0, 128 - HEADS)).reshape(1, 128)
    skips = jnp.repeat(skip_gain, P_SIZE).reshape(1, DI)
    u = jnp.dot(normed_more, w_u, preferred_element_type=F32)
    halo_block = rows // 8

    same = lambda c: (c, 0)
    same3 = lambda c: (c, 0, 0)
    one = lambda i: (jnp.minimum(i, blocks - 1), 0)
    one3 = lambda i: (jnp.minimum(i, blocks - 1), 0, 0)
    two = lambda i: (jnp.maximum(i - blocks, 0), 0)
    val, vp, conv, bc, ssd, ent, logd, step, cum, start, *filled = pl.pallas_call(
        lambda *refs: forward_kernel(extra, *refs),
        grid=(2 * blocks,),
        in_specs=[
            spec((Q, UW), one),
            spec((8, UW), lambda c: (halo_block, 0)),
            spec((Q, 128), one),
            scalar(),
            whole((CONVK, CH)),
            whole((1, CH)),
            whole((1, 128)),
            whole((1, 128)),
            whole((1, DI)),
        ]
        + [anywhere] * extra,
        out_specs=[
            spec((Q, DI), one),
            spec((Q, DI), one),
            spec((Q, CH), one),
            spec((Q, 2 * N), one),
            spec((Q, DI), two),
            spec((1, N, DI), one3),
            spec((Q, 128), one),
            spec((Q, 128), one),
            whole((blocks + 1, 8, DI)),
            whole((N, DI)),
        ]
        + [anywhere] * extra,
        out_shape=[
            shaped((rows, DI), BF16),
            shaped((rows, DI), BF16),
            shaped((rows, CH), BF16),
            shaped((rows, 2 * N), BF16),
            shaped((rows, DI), BF16),
            shaped((blocks, N, DI), BF16),
            shaped((rows, 128), F32),
            shaped((rows, 128), F32),
            shaped((blocks + 1, 8, DI), F32),
            shaped((N, DI), BF16),
        ]
        + [shaped((32 * a.shape[0], a.shape[1]), a.dtype) for a in later],
        scratch_shapes=[
            pltpu.VMEM((8, CH), F32),
            pltpu.VMEM((GROUPS, Q, 128), F32),
            pltpu.VMEM((128, DI), BF16),
            pltpu.VMEM((GROUPS, 8, Q), F32),
            pltpu.VMEM((Q, Q), F32),
            pltpu.VMEM((N, DI), F32),
            pltpu.VMEM((blocks, Q, DI), BF16),
            pltpu.VMEM((blocks, Q, DI), BF16),
            pltpu.VMEM((blocks, Q, 2 * N), BF16),
            pltpu.VMEM((blocks, Q, 128), F32),
            pltpu.VMEM((N, DI), BF16),
            pltpu.VMEM((N, DI), BF16),
            pltpu.SemaphoreType.DMA((2,)),
        ]
        + gather_scratch() * extra,
        compiler_params=params(2),
        cost_estimate=cost(15e9, 60e6),
        name="forward",
    )(u, u, valid, keep, taps, shift, bias, logs, skips, *later)
    if later:
        w_z, w_o = filled

    z = jnp.dot(normed, w_z, preferred_element_type=F32).astype(BF16)
    back = lambda i: (blocks - 1 - i, 0)
    back3 = lambda i: (blocks - 1 - i, 0, 0)
    gains = gate_gain.reshape(1, DI)
    output, gated, branch_grad, ds, dz, entt, gnext, gout, dlp, dc, gate_sums = pl.pallas_call(
        gate_kernel,
        grid=(blocks,),
        in_specs=[
            whole((N, DI)),
            spec((Q, DI), back),
            spec((1, N, DI), back3),
            spec((Q, DI), back),
            spec((Q, DI), back),
            spec((Q, 2 * N), back),
            spec((Q, 128), back),
            whole((blocks + 1, 8, DI)),
            spec((Q, width), back),
            spec((Q, width), back),
            spec((Q, 128), back),
            whole((DI, width)),
            whole((1, DI)),
        ],
        out_specs=[
            spec((Q, width), back),
            spec((Q, DI), back),
            spec((Q, width), back),
            spec((Q, DI), back),
            spec((Q, DI), back),
            spec((1, N, DI), back3),
            spec((1, N, DI), back3),
            whole((N, DI)),
            spec((Q, 128), back),
            spec((Q, N), back),
            whole((8, DI)),
        ],
        out_shape=[
            shaped((rows, width), BF16),
            shaped((rows, DI), BF16),
            shaped((rows, width), BF16),
            shaped((rows, DI), BF16),
            shaped((rows, DI), BF16),
            shaped((blocks, N, DI), BF16),
            shaped((blocks, N, DI), BF16),
            shaped((N, DI), BF16),
            shaped((rows, 128), F32),
            shaped((rows, N), F32),
            shaped((8, DI), F32),
        ],
        scratch_shapes=[
            pltpu.VMEM((N, DI), F32),
            pltpu.VMEM((N, DI), F32),
            pltpu.VMEM((128, DI), BF16),
            pltpu.VMEM((Q, DI), F32),
            pltpu.VMEM((Q, DI), F32),
            pltpu.VMEM((Q, DI), F32),
            pltpu.VMEM((Q, DI), F32),
            pltpu.VMEM((Q, DI), F32),
            pltpu.VMEM((Q, 128), F32),
        ],
        compiler_params=params(),
        cost_estimate=cost(15e9, 60e6),
        name="gate",
    )(
        start, ssd, ent, z, val, bc, logd, cum, tokens, cotangent, valid, w_o, gains,
    )

    def columns_of(left, right):
        return lax.dot_general(
            left, right, (((0,), (0,)), ((), ())), preferred_element_type=F32
        ).astype(BF16)

    def in_blocks(a):
        return a.reshape(LINE, 8, a.shape[0] // 32, a.shape[1])

    out_weight_grad = columns_of(gated, branch_grad)
    gate_columns = columns_of(normed, dz)
    mixing_parts = [in_blocks(out_weight_grad)] if boxed else []

    dvp, dbc, dlt, gin, *summed_out = pl.pallas_call(
        lambda *refs: mixing_kernel(len(mixing_parts), *refs),
        grid=(blocks,),
        in_specs=[
            spec((Q, DI), same),
            spec((Q, DI), same),
            spec((Q, 2 * N), same),
            spec((Q, 128), same),
            scalar(),
            whole((N, DI)),
            whole((blocks + 1, 8, DI)),
        ]
        + [pl.BlockSpec(memory_space=pltpu.VMEM) for a in mixing_parts],
        out_specs=[spec((Q, DI), same), spec((Q, 2 * N), same), spec((Q, 128), same), whole((N, DI))]
        + [whole((LINE,) + a.shape[-2:]) for a in mixing_parts],
        out_shape=[
            shaped((rows, DI), BF16), shaped((rows, 2 * N), F32), shaped((rows, 128), F32), shaped((N, DI), BF16),
        ]
        + [shaped((LINE,) + a.shape[-2:], BF16) for a in mixing_parts],
        scratch_shapes=[
            pltpu.VMEM((GROUPS, Q, 128), F32),
            pltpu.VMEM((GROUPS, 8, Q), F32),
            pltpu.VMEM((Q, Q), F32),
            pltpu.VMEM((Q, Q), F32),
            pltpu.VMEM((GROUPS, 8, Q), F32),
            pltpu.VMEM((128, Q), F32),
            pltpu.VMEM((GROUPS, Q, 128), F32),
            pltpu.VMEM((N, DI), BF16),
            pltpu.VMEM((N, DI), BF16),
            pltpu.SemaphoreType.DMA((2,)),
        ]
        + [each for a in mixing_parts for each in plane_scratch(*a.shape[-2:])],
        compiler_params=params(3),
        cost_estimate=cost(15e9, 60e6),
        name="mixing",
    )(ds, vp, bc, logd, keep, gout, cum, *mixing_parts)

    back_parts = summed_out + [in_blocks(gate_columns)] if boxed else []
    du, last, edge, conv_sums, small, *summed_gate = pl.pallas_call(
        lambda *refs: back_kernel(len(back_parts), *refs),
        grid=(blocks,),
        in_specs=[
            scalar(),
            whole((N, DI)),
            spec((1, N, DI), back3),
            spec((1, N, DI), back3),
            whole((blocks + 1, 8, DI)),
            spec((Q, DI), back),
            spec((Q, DI), back),
            spec((Q, DI), back),
            spec((Q, DI), back),
            spec((Q, CH), back),
            spec((Q, UW), back),
            spec((8, UW), lambda i: (halo_block, 0)),
            spec((Q, 2 * N), back),
            spec((Q, 128), back),
            spec((Q, 128), back),
            spec((Q, 128), back),
            spec((Q, 128), back),
            spec((Q, 128), back),
            spec((Q, 2 * N), back),
            spec((Q, N), back),
            whole((CONVK, CH)),
            whole((1, 128)),
            whole((1, 128)),
            whole((1, DI)),
        ]
        + [pl.BlockSpec(memory_space=pltpu.VMEM) for a in back_parts],
        out_specs=[
            spec((Q, UW), back),
            whole((8, CH)),
            whole((8, CH)),
            whole((8, CH)),
            whole((8, 128)),
        ]
        + [whole(a.shape[-2:]) for a in back_parts],
        out_shape=[
            shaped((rows, UW), BF16),
            shaped((8, CH), F32),
            shaped((8, CH), F32),
            shaped((8, CH), F32),
            shaped((8, 128), F32),
        ]
        + [shaped(a.shape[-2:], F32) for a in back_parts],
        scratch_shapes=[
            pltpu.VMEM((N, DI), F32),
            pltpu.VMEM((128, DI), BF16),
            pltpu.VMEM((8, CH), F32),
            pltpu.VMEM((16, CH), F32),
            pltpu.VMEM((Q, 128), F32),
            pltpu.VMEM((Q, 128), F32),
            pltpu.VMEM((16, 128), F32),
        ]
        + (
            scatter_scratch(*back_parts[1].shape[-2:]) + line_scratch(*back_parts[0].shape[-2:])
            if back_parts
            else []
        ),
        compiler_params=params(4 if back_parts else None),
        cost_estimate=cost(15e9, 60e6),
        name="back",
    )(
        keep, gin, gnext, entt, cum, vp, val, dvp, ds, conv, u, u, bc, logd, step, valid,
        dlp, dlt, dbc, dc, taps, bias, logs, skips, *back_parts,
    )
    edge_back = lax.ppermute(edge, "ctx", [(k + 1, k) for k in range(near - 1)])
    du = lax.dynamic_update_slice(du, (last + edge_back).astype(BF16), (rows - 8, 0))
    if boxed:
        out_weight_grad, gate_columns = summed_gate
        input_grad, in_weight_grad, sums = final(
            normed.T, du, dz, tokens, cotangent, norm_gain.reshape(1, width), w_z, w_u, gate_columns, conv_sums,
            gate_sums, small, 5,
        )
        return (
            output,
            input_grad,
            in_weight_grad,
            out_weight_grad,
            sums[7, :width],
            sums[:CONVK],
            sums[CONVK],
            sums[5, DI : DI + HEADS],
            sums[5, DI + 128 : DI + 128 + HEADS],
            jnp.sum(sums[6, :DI].reshape(HEADS, P_SIZE), axis=1),
            sums[5, :DI],
        )
    conv_columns = columns_of(normed, du)
    across = (((1,), (1,)), ((), ()))
    normed_grad = lax.dot_general(dz, w_z, across, preferred_element_type=F32) + lax.dot_general(
        du, w_u, across, preferred_element_type=F32
    )
    inputs = tokens.astype(F32)
    scale = lax.rsqrt(jnp.mean(inputs * inputs, axis=-1, keepdims=True) + epsilon)
    hat = inputs * scale
    inner = normed_grad * norm_gain
    input_grad = cotangent.astype(F32) + scale * (
        inner - hat * jnp.mean(inner * hat, axis=-1, keepdims=True)
    )
    norm_grad = jnp.sum(normed_grad * hat, axis=0)
    packed = jnp.concatenate(
        [
            norm_grad,
            conv_sums[:5].reshape(-1),
            gate_sums[:2].reshape(-1),
            small[:2].reshape(-1),
        ]
    )
    conv_columns, gate_columns, out_weight_grad = [
        lax.psum_scatter(a.astype(F32), axes, scatter_dimension=0, tiled=True)
        for a in (conv_columns, gate_columns, out_weight_grad)
    ]
    summed = lax.psum(packed, axes)
    in_weight_grad = jnp.concatenate([gate_columns, conv_columns[:, : DPROJ - DI]], 1)
    at = width
    conv_weight_grad = summed[at : at + CONVK * CH].reshape(CONVK, CH)
    at += CONVK * CH
    conv_bias_grad = summed[at : at + CH]
    at += CH
    gate_gain_grad = summed[at : at + DI]
    at += DI
    skip_gain_grad = jnp.sum(summed[at : at + DI].reshape(HEADS, P_SIZE), axis=1)
    at += DI
    step_bias_grad = summed[at : at + HEADS]
    decay_log_grad = summed[at + 128 : at + 128 + HEADS]
    return (
        output,
        input_grad,
        in_weight_grad,
        out_weight_grad,
        summed[:width],
        conv_weight_grad,
        conv_bias_grad,
        step_bias_grad,
        decay_log_grad,
        skip_gain_grad,
        gate_gain_grad,
    )


def solution(mesh):
    split = P(("fsdp", "ctx"), None)
    line = P(("fsdp", "ctx"))
    return jax.shard_map(
        local,
        mesh=mesh,
        in_specs=(split, line, line, split, P(), split, P(), P(), P(), P(), P(), P(), split),
        out_specs=(split, split, split, split, P(), P(), P(), P(), P(), P(), P()),
        check_vma=False,
    )
```

```python
import jax
import jax.numpy as jnp
from jax import lax
from jax.experimental import pallas as pl
from jax.experimental.pallas import tpu as pltpu
from jax.sharding import PartitionSpec as P

DI = 2048
HEADS = 32
P_SIZE = 64
N = 128
CONVK = 4
Q = 256
CH = 2304
DPROJ = 4384
UW = CH + 128
GW = 256
GROUPS = DI // GW
HALF = Q // 2
HALO = 16

F32 = jnp.float32
BF16 = jnp.bfloat16
LOG2E = 1.4426950408889634
epsilon = 1e-05


def nn(a, b):
    return lax.dot_general(a, b, (((1,), (0,)), ((), ())), preferred_element_type=F32)


def nt(a, b):
    return lax.dot_general(a, b, (((1,), (1,)), ((), ())), preferred_element_type=F32)


def sigmoid(x):
    return 0.5 * jnp.tanh(0.5 * x) + 0.5


def softplus(x):
    e = jnp.exp(-jnp.abs(x))
    w = 1.0 + e
    d = w - 1.0
    return jnp.maximum(x, 0.0) + jnp.where(d == 0.0, e, jnp.log(w) * (e / jnp.where(d == 0.0, 1.0, d)))


def rows_of(shape):
    return lax.broadcasted_iota(jnp.int32, shape, 0)


def lanes_of(shape):
    return lax.broadcasted_iota(jnp.int32, shape, 1)


def split3(x):
    a = x.astype(BF16)
    r = x - a.astype(F32)
    b = r.astype(BF16)
    return a, b, (r - b.astype(F32)).astype(BF16)


def ordered_sum(triangle, x):
    a, b, c = split3(x)
    return nn(triangle, c) + nn(triangle, b) + nn(triangle, a)


def spread(x, out):
    out[0] = x
    for g in range(1, GROUPS):
        out[g] = pltpu.roll(x, 128 - 4 * g, 1)


def delayed(before, x, by):
    if by == 0:
        return x
    return pltpu.roll(jnp.concatenate([before, x], 0), by, 0)[8:]


def advanced(x, after, by):
    if by == 0:
        return x
    count = x.shape[0]
    return pltpu.roll(jnp.concatenate([x, after], 0), count + 8 - by, 0)[:count]


def fill_picks(out):
    for g in range(GROUPS):
        shape = (128, GW)
        head = lax.shift_right_logical(lanes_of(shape), 6) + 4 * g
        at = rows_of(shape)
        own = jnp.logical_and(jnp.bitwise_and(at, HEADS - 1) == head, at < 3 * HEADS)
        out[:, g * GW : (g + 1) * GW] = jnp.where(own, 1.0, 0.0).astype(BF16)


def in_parts(x):
    lane = lanes_of(x.shape)
    a, b, c = split3(jnp.where(lane < HEADS, x, 0.0))
    wide = a.astype(F32) + pltpu.roll(b.astype(F32), HEADS, 1) + pltpu.roll(c.astype(F32), 2 * HEADS, 1)
    return wide.astype(BF16)


def spread_rows(x, out):
    for g in range(GROUPS):
        out[g, 0:4] = x[4 * g : 4 * g + 4]


def head_lanes(x, i):
    return jnp.broadcast_to(x[:, i : i + 1], (x.shape[0], 128))


def pick_heads(g):
    shape = (GW, 128)
    return jnp.where(
        lax.shift_right_logical(rows_of(shape), 6) + 4 * g == lanes_of(shape), 1.0, 0.0
    ).astype(BF16)


def when_at(now, plan):
    plan = sorted(plan, key=lambda entry: entry[0])
    if len(plan) == 1:
        place, act = plan[0]

        @pl.when(now == place)
        def _():
            act()

    elif plan:
        middle = len(plan) // 2

        def early():
            when_at(now, plan[:middle])

        def late():
            when_at(now, plan[middle:])

        lax.cond(now < plan[middle][0], early, late)


def chain_peers():
    pos = lax.axis_index("ctx")
    return [(pos > 0, {"ctx": pos - 1}), (pos < lax.axis_size("ctx") - 1, {"ctx": pos + 1})]


def pass_on(message, arrived, sems, by):
    return pltpu.make_async_remote_copy(
        src_ref=message, dst_ref=arrived, send_sem=sems.at[0], recv_sem=sems.at[1],
        device_id={"ctx": lax.axis_index("ctx") + by}, device_id_type=pl.DeviceIdType.MESH,
    )


def forward_kernel(count, *refs):
    (
        normed_ref, halo_ref, wu_any, valid_ref, keep_ref, cw_ref, cb_ref, sb_ref, dl_ref, skip_ref,
    ) = refs[:10]
    own = refs[10 : 10 + count]
    (
        val_ref, vp_ref, conv_ref, bc_ref, ssd_ref, ent_ref, log_ref, step_ref, cum_ref, start_ref, u_ref, ahead_ref,
    ) = refs[10 + count : 22 + count]
    outs = refs[22 + count : 22 + 2 * count]
    (
        past, logs, picks, logt, inter, state, all_vp, all_val, all_bc, all_log, message, arrived, sems, wu, load, log_wide, step_wide,
    ) = refs[22 + 2 * count : 39 + 2 * count]
    gather_sems = refs[39 + 2 * count :]
    i = pl.program_id(0)
    blocks = pl.num_programs(0) // 2
    first = i < blocks
    c = jnp.where(first, i, i - blocks)
    near = lax.axis_size("ctx")
    pos = lax.axis_index("ctx")
    plan = []
    if count:
        lists = [Gather(own[k], outs[k], (0, outs[k].shape[1], 0), *gather_sems[5 * k : 5 * k + 5]).steps() for k in range(count)]
        length = len(lists[0])
        for at in range(length + 2 * (count - 1)):
            acts = [lists[k][at - 2 * k] for k in range(count) if 0 <= at - 2 * k < length]
            plan.append((FORWARD_PLACES[at], lambda acts=acts: [act() for act in acts]))

    @pl.when(i == 0)
    def _():
        fetch = pltpu.make_async_copy(wu_any, wu, load)
        fetch.start()
        fill_picks(picks)
        meet((box_peers() if count else []) + chain_peers())
        fetch.wait()
        before = nn(halo_ref[...], wu[...])[8:]
        ahead_ref[...] = before
        past[...] = before[:, :CH] * keep_ref[0, 0]
        state[...] = jnp.zeros_like(state)
        cum_ref[...] = jnp.zeros_like(cum_ref)

    half = lanes_of((Q, 128)) < P_SIZE
    square = (Q, Q)
    causal = rows_of(square) >= lanes_of(square)

    @pl.when(first)
    def _():
        tail = nn(normed_ref[...], wu[:, DI:])
        u_ref[:, DI:] = tail
        raw = tail[:, 2 * N :] + sb_ref[...]
        step = softplus(raw) * valid_ref[...]
        step = jnp.where(lanes_of(step.shape) < HEADS, step, 0.0)
        rate = -jnp.exp(dl_ref[...]) * LOG2E
        logd = ordered_sum(jnp.where(causal, 1.0, 0.0).astype(BF16), step * rate)
        log_ref[...] = logd
        all_log[c] = logd
        step_ref[...] = step
        log_parts = in_parts(logd)
        step_parts = in_parts(step)

        def convolved(cols, x):
            before = past[:, cols]
            past[:, cols] = x[Q - 8 :]
            total = cb_ref[:, cols] + cw_ref[CONVK - 1 : CONVK, cols] * x
            for k in range(CONVK - 1):
                total = total + cw_ref[k : k + 1, cols] * delayed(before, x, CONVK - 1 - k)
            return total

        conv_b = convolved(pl.ds(DI, N), tail[:, :N])
        conv_c = convolved(pl.ds(DI + N, N), tail[:, N : 2 * N])
        conv_ref[:, DI : DI + N] = conv_b.astype(BF16)
        conv_ref[:, DI + N :] = conv_c.astype(BF16)
        act_b = conv_b * sigmoid(conv_b)
        act_c = conv_c * sigmoid(conv_c)
        both = jnp.concatenate([act_b.astype(BF16), act_c.astype(BF16)], 1)
        bc_ref[...] = both
        all_bc[c] = both
        turned_b = act_b.T.astype(BF16)
        ent_ref[0] = state[...].astype(BF16)

        def ahead(g):
            cols = pl.ds(pl.multiple_of(g * GW, GW), GW)
            slot = g % 2
            u_ref[:, cols] = nn(normed_ref[...], wu[:, cols])
            log_wide[slot] = nn(log_parts, picks[:, cols])
            step_wide[slot] = nn(step_parts, picks[:, cols])

        ahead(0)

        def group(g, unused):
            when_at(i * GROUPS + g, plan)
            slot = g % 2
            for j in range(2):
                cols = pl.ds(pl.multiple_of(g * GW + 128 * j, 128), 128)
                cv = convolved(cols, u_ref[:, cols])
                conv_ref[:, cols] = cv.astype(BF16)
                val = cv * sigmoid(cv)
                low = val.astype(BF16)
                val_ref[:, cols] = low
                all_val[c, :, cols] = low
                lp = log_wide[slot, :, 128 * j : 128 * j + 128]
                vp = val * step_wide[slot, :, 128 * j : 128 * j + 128]
                low = vp.astype(BF16)
                vp_ref[:, cols] = low
                all_vp[c, :, cols] = low
                last = lp[Q - 1 : Q, :]
                weighted = (vp * jnp.exp2(last - lp)).astype(BF16)
                state[:, cols] = jnp.exp2(last) * state[:, cols] + nn(turned_b, weighted)
                cum_ref[c + 1, :, cols] = cum_ref[c, :, cols] + last
            ahead(lax.rem(g + 1, GROUPS))
            return unused

        lax.fori_loop(0, GROUPS, group, 0)

    def hop(k):
        @pl.when(pos == k)
        def _():
            if k:
                pass_on(message, arrived, sems, 1).wait_recv()
                entering = keep_ref[0, 0] * arrived[...].astype(F32)
                start_ref[...] = entering.astype(BF16)
            else:
                start_ref[...] = jnp.zeros_like(start_ref)
            if k < near - 1:
                if k:
                    message[...] = (jnp.exp2(cum_ref[blocks, 0:1, :]) * entering + state[...]).astype(BF16)
                else:
                    message[...] = state[...].astype(BF16)
                pass_on(message, arrived, sems, 1).start()

    hops = [(blocks * GROUPS + FORWARD_HOPS[k], lambda k=k: hop(k)) for k in range(near)]

    @pl.when(jnp.logical_not(first))
    def _():
        logd = all_log[c]
        spread(logd, logs)
        spread_rows(logd.T, logt)
        inter[...] = jnp.where(causal, nt(all_bc[c, :, N:], all_bc[c, :, :N]), 0.0)
        left = jnp.where(half[:1], 1.0, 0.0).astype(BF16)
        right = jnp.where(half[:1], 0.0, 1.0).astype(BF16)

        def group(g, unused):
            when_at(i * GROUPS + g, plan)
            when_at(i * GROUPS + g, hops)
            lg = logs[g]
            for j in range(2):
                cols = pl.ds(pl.multiple_of(g * GW + 128 * j, 128), 128)
                vp = all_vp[c, :, cols]
                v0 = vp * left
                v1 = vp * right
                top = []
                low = []
                for h in range(2):
                    row = logt[g, 2 * j + h : 2 * j + h + 1]
                    early, late = row[:, :HALF], row[:, HALF:]
                    lb = head_lanes(lg, 2 * j + h)
                    up, down = lb[:HALF], lb[HALF:]
                    top.append((inter[:HALF, :HALF] * jnp.exp2(jnp.minimum(up - early, 0.0))).astype(BF16))
                    low.append((inter[HALF:, :HALF] * jnp.exp2(jnp.minimum(down - early, 0.0))).astype(BF16))
                    low.append((inter[HALF:, HALF:] * jnp.exp2(jnp.minimum(down - late, 0.0))).astype(BF16))
                skipped = skip_ref[:, cols] * all_val[c, :, cols].astype(F32)
                above = nn(jnp.concatenate(top, 1), jnp.concatenate([v0[:HALF], v1[:HALF]], 0))
                below = nn(jnp.concatenate(low, 1), jnp.concatenate([v0, v1], 0))
                ssd_ref[:HALF, cols] = (above + skipped[:HALF]).astype(BF16)
                ssd_ref[HALF:, cols] = (below + skipped[HALF:]).astype(BF16)
            return unused

        lax.fori_loop(0, GROUPS, group, 0)

    @pl.when(jnp.logical_and(i == 2 * blocks - 1, pos < near - 1))
    def _():
        pass_on(message, arrived, sems, 1).wait_send()


def gate_kernel(
    start_ref, ssd_in, ent_ref, z_ref, val_ref, bc_ref, log_ref, cum_ref,
    tok_ref, cot_ref, valid_ref, ow_ref, gain_ref,
    out_ref, gated_ref, bg_ref, ds_ref, dz_ref, entt_ref, gnext_ref, gout_ref, dlp_ref, dc_ref, sums_ref,
    start, gstate, picks, ssd_s, mix_s, el_s, pe_s, gg_s, acc,
):
    i = pl.program_id(0)
    c = pl.num_programs(0) - 1 - i

    @pl.when(i == 0)
    def _():
        start[...] = start_ref[...].astype(F32)
        fill_picks(picks)
        gstate[...] = jnp.zeros_like(gstate)
        sums_ref[...] = jnp.zeros_like(sums_ref)

    log_parts = in_parts(log_ref[...])
    low_c = bc_ref[:, N:]
    turned_c = low_c.astype(F32).T.astype(BF16)
    acc[...] = jnp.zeros_like(acc)

    def enter(g, unused):
        cols = pl.ds(pl.multiple_of(g * GW, GW), GW)
        decay = jnp.exp2(nn(log_parts, picks[:, cols]))
        entering = (
            ent_ref[0, :, cols].astype(F32) + jnp.exp2(cum_ref[c, 0:1, cols]) * start[:, cols]
        ).astype(BF16)
        entt_ref[0, :, cols] = entering
        part = nn(low_c, entering)
        for j in range(2):
            pc = pl.ds(pl.multiple_of(g * GW + 128 * j, 128), 128)
            el = decay[:, 128 * j : 128 * j + 128]
            pe = el * part[:, 128 * j : 128 * j + 128]
            el_s[:, pc] = el
            pe_s[:, pc] = pe
            ssd = ssd_in[:, pc].astype(F32) + pe
            z = z_ref[:, pc].astype(F32)
            mixed = ssd * (z * sigmoid(z))
            ssd_s[:, pc] = ssd
            mix_s[:, pc] = mixed
            acc[...] += mixed * mixed
        return unused

    lax.fori_loop(0, GROUPS, enter, 0)
    inv = lax.rsqrt(jnp.sum(acc[...], axis=1, keepdims=True) * (1.0 / DI) + epsilon)
    inv = jnp.broadcast_to(inv, (Q, 128))
    valid = valid_ref[...]
    valid8 = jnp.concatenate([valid] * (tok_ref.shape[1] // 128), 1)
    branch_grad = (cot_ref[...].astype(F32) * valid8).astype(BF16)
    bg_ref[...] = branch_grad
    acc[...] = jnp.zeros_like(acc)

    def gate(g, unused):
        cols = pl.ds(pl.multiple_of(g * GW, GW), GW)
        ggrad = nt(branch_grad, ow_ref[cols, :])
        for j in range(2):
            pc = pl.ds(pl.multiple_of(g * GW + 128 * j, 128), 128)
            hat = mix_s[:, pc] * inv
            gain = gain_ref[:, pc]
            mix_s[:, pc] = hat
            gated_ref[:, pc] = (hat * gain).astype(BF16)
            gg = ggrad[:, 128 * j : 128 * j + 128]
            both = gg * hat
            sums_ref[0:1, pc] += jnp.sum(both, axis=0, keepdims=True)
            acc[...] += both * gain
            gg_s[:, pc] = gg * gain
        return unused

    lax.fori_loop(0, GROUPS, gate, 0)
    mean = jnp.sum(acc[...], axis=1, keepdims=True) * (1.0 / DI)
    mean = jnp.broadcast_to(mean, (Q, 128))

    for n in range(tok_ref.shape[1] // 256):
        cols = slice(256 * n, 256 * n + 256)
        branch = nn(gated_ref[...], ow_ref[:, cols])
        out_ref[:, cols] = (tok_ref[:, cols].astype(F32) + valid8[:, :256] * branch).astype(BF16)

    acc[...] = jnp.zeros_like(acc)
    dc_ref[...] = jnp.zeros_like(dc_ref)

    def back(g, unused):
        cols = pl.ds(pl.multiple_of(g * GW, GW), GW)
        dparts = []
        prods = []
        for j in range(2):
            pc = pl.ds(pl.multiple_of(g * GW + 128 * j, 128), 128)
            dmixed = inv * (gg_s[:, pc] - mix_s[:, pc] * mean)
            z = z_ref[:, pc].astype(F32)
            s = sigmoid(z)
            ds = (dmixed * (z * s)).astype(BF16)
            ds_ref[:, pc] = ds
            dz_ref[:, pc] = (dmixed * ssd_s[:, pc] * (s * (1.0 + z * (1.0 - s)))).astype(BF16)
            ds = ds.astype(F32)
            sums_ref[1:2, pc] += jnp.sum(ds * val_ref[:, pc].astype(F32), axis=0, keepdims=True)
            dparts.append((ds * el_s[:, pc]).astype(BF16))
            prods.append((ds * pe_s[:, pc]).astype(BF16))
        dpart = jnp.concatenate(dparts, 1)
        acc[...] += nn(jnp.concatenate(prods, 1), pick_heads(g))
        dc_ref[...] += nt(dpart, entt_ref[0, :, cols])
        gnext_ref[0, :, cols] = gstate[:, cols].astype(BF16)
        total = cum_ref[c + 1, 0:1, cols] - cum_ref[c, 0:1, cols]
        gstate[:, cols] = nn(turned_c, dpart) + jnp.exp2(total) * gstate[:, cols]
        return unused

    lax.fori_loop(0, GROUPS, back, 0)
    dlp_ref[...] = acc[...]

    @pl.when(c == 0)
    def _():
        gout_ref[...] = gstate[...].astype(BF16)


FORWARD_PLACES = tuple(5 * k for k in range(13))
FORWARD_HOPS = (0, 8, 20, 30)
MIXING_HOPS = (0, 8, 20, 30)
MIXING_PLACES = (0, 5, 12, 31)
LINE_PLACES = (1, 4, 8, 12)
BACK_PLACES = (0, 4, 9, 19, 22, 25, 28, 31)


def acting(places, acts):
    joined = {}
    for place, act in zip(places, acts):
        joined.setdefault(place, []).append(act)
    return [(place, lambda acts=acts: [act() for act in acts]) for place, acts in joined.items()]


def plane_scratch(rows, columns):
    dma = pltpu.SemaphoreType.DMA
    return scatter_scratch(rows, columns)[:6] + [dma((4,))] * 4


def line_scratch(rows, columns):
    dma = pltpu.SemaphoreType.DMA
    return [pltpu.VMEM((1, LINE, rows, columns), BF16)] + [pltpu.VMEM((LINE, rows, columns), BF16)] * 2 + [
        dma((2, LINE))
    ] * 2


def mixing_kernel(count, *refs):
    ds_ref, vp_ref, bc_ref, log_ref, keep_ref, gout_ref, cum_ref = refs[:7]
    parts = refs[7 : 7 + count]
    dvp_ref, dbc_ref, dlt_ref, gin_ref = refs[7 + count : 11 + count]
    outs = refs[11 + count : 11 + 2 * count]
    (
        logs, logt, inter, dinter, rowsum, turned, colsum, message, arrived, sems,
    ) = refs[11 + 2 * count : 21 + 2 * count]
    i = pl.program_id(0)
    blocks = pl.num_programs(0)
    near = lax.axis_size("ctx")
    pos = lax.axis_index("ctx")
    plan = []
    if count:
        held = refs[21 + 2 * count :]
        part = Scatter(parts[0], None, *held[:6], None, None, tuple(held[6:10]) + (None, None))
        acts = [part.begin, part.corners, part.sides_out, lambda: part.hand_on(outs[0])]
        plan = acting(MIXING_PLACES, acts)

    @pl.when(i == 0)
    def _():
        meet((box_peers() if count else []) + chain_peers())

    def hop(k):
        @pl.when(pos == near - 1 - k)
        def _():
            total = gout_ref[...].astype(F32)
            if k:
                pass_on(message, arrived, sems, -1).wait_recv()
                gin_ref[...] = arrived[...]
                total = total + jnp.exp2(cum_ref[blocks, 0:1, :]) * arrived[...].astype(F32)
            else:
                gin_ref[...] = jnp.zeros_like(gin_ref)
            if k < near - 1:
                message[...] = (keep_ref[0, 0] * total).astype(BF16)
                pass_on(message, arrived, sems, -1).start()

    hops = [(MIXING_HOPS[k], lambda k=k: hop(k)) for k in range(near)]

    logd = log_ref[...]
    spread(logd, logs)
    spread_rows(logd.T, logt)
    low_b = bc_ref[:, :N]
    low_c = bc_ref[:, N:]
    square = (Q, Q)
    causal = rows_of(square) <= lanes_of(square)
    inter[...] = jnp.where(causal, nt(low_b, low_c), 0.0)
    dinter[...] = jnp.zeros_like(dinter)
    half = lanes_of((Q, 128)) < P_SIZE
    lane = lanes_of((HALF, 128))

    def group(g, unused):
        when_at(i * GROUPS + g, plan)
        when_at(i * GROUPS + g, hops)
        lg = logs[g]
        first_col = jnp.zeros((HALF, 128), F32)
        second_col = jnp.zeros((HALF, 128), F32)
        for j in range(2):
            cols = pl.ds(pl.multiple_of(g * GW + 128 * j, 128), 128)
            vp = vp_ref[:, cols].astype(F32)
            ds = ds_ref[:, cols]
            wide = ds.astype(F32)
            first = []
            second = []
            outs = []
            for h in range(2):
                head = 2 * j + h
                own = half if h == 0 else jnp.logical_not(half)
                vm = jnp.where(own, vp, 0.0).astype(BF16)
                dsm = jnp.where(own, wide, 0.0).astype(BF16)
                outs.append(dsm)
                row = logt[g, head : head + 1]
                early, late = row[:, :HALF], row[:, HALF:]
                lb = head_lanes(lg, head)
                up, down = lb[:HALF], lb[HALF:]
                dup = nt(vm[:HALF], ds)
                ddown = nt(vm[HALF:], ds[HALF:])
                decay = jnp.exp2(jnp.minimum(early - up, 0.0))
                grad = dup[:, :HALF] * decay
                dinter[:HALF, :HALF] += grad
                part = inter[:HALF, :HALF]
                first.append((part * decay).astype(BF16))
                both = grad * part
                row_early = jnp.sum(both, axis=0, keepdims=True)
                col = both
                decay = jnp.exp2(jnp.minimum(late - up, 0.0))
                grad = dup[:, HALF:] * decay
                dinter[:HALF, HALF:] += grad
                part = inter[:HALF, HALF:]
                first.append((part * decay).astype(BF16))
                both = grad * part
                row_late = jnp.sum(both, axis=0, keepdims=True)
                col = jnp.sum(col + both, axis=1, keepdims=True)
                first_col = jnp.where(lane == head, col, first_col)
                decay = jnp.exp2(jnp.minimum(late - down, 0.0))
                grad = ddown * decay
                dinter[HALF:, HALF:] += grad
                part = inter[HALF:, HALF:]
                second.append((part * decay).astype(BF16))
                both = grad * part
                row_late = row_late + jnp.sum(both, axis=0, keepdims=True)
                col = jnp.sum(both, axis=1, keepdims=True)
                second_col = jnp.where(lane == head, col, second_col)
                rowsum[g, head : head + 1, :HALF] = row_early
                rowsum[g, head : head + 1, HALF:] = row_late
            dvp_ref[:HALF, cols] = nn(
                jnp.concatenate(first, 1), jnp.concatenate(outs, 0)
            ).astype(BF16)
            dvp_ref[HALF:, cols] = nn(
                jnp.concatenate(second, 1), jnp.concatenate([outs[0][HALF:], outs[1][HALF:]], 0)
            ).astype(BF16)
        colsum[g, :HALF] = first_col
        colsum[g, HALF:] = second_col
        return unused

    lax.fori_loop(0, GROUPS, group, 0)
    turned[...] = jnp.zeros_like(turned)
    for g in range(GROUPS):
        turned[4 * g : 4 * g + 4] = rowsum[g, 0:4]
    total = turned[...].T
    for g in range(GROUPS):
        total = total - (colsum[g] if g == 0 else pltpu.roll(colsum[g], 4 * g, 1))
    dlt_ref[...] = total
    masked = jnp.where(causal, dinter[...], 0.0)
    dbc_ref[:, :N] = nn(masked.astype(BF16), low_c)
    dbc_ref[:, N:] = nn(masked.T.astype(BF16), low_b)

    @pl.when(jnp.logical_and(i == blocks - 1, pos > 0))
    def _():
        pass_on(message, arrived, sems, -1).wait_send()


def back_kernel(count, *refs):
    (
        keep_ref, gin_ref, gnext_ref, entt_ref, cum_ref, vp_ref, val_ref, dvp_ref, ds_ref, conv_ref,
        u_ref, halo_ref, bc_ref, log_ref, step_ref, valid_ref, dlp_ref, dlt_ref, dbc_ref, dc_ref,
        cw_ref, sb_ref, dl_ref, skip_ref,
    ) = refs[:24]
    parts = refs[24 : 24 + count]
    du_ref, last_ref, edge_ref, sums_ref, small_ref = refs[24 + count : 29 + count]
    outs = refs[29 + count : 29 + 2 * count]
    gin, picks, head, epad, dlw, dst, drow = refs[29 + 2 * count : 36 + 2 * count]
    plan = []
    if count:
        held = refs[36 + 2 * count :]
        full = Scatter(parts[1], outs[1], *held[:8], held[8:14])
        line = Scatter(None, outs[0], None, held[14], None, None, None, None, *held[15:17], (None,) * 4 + tuple(held[17:19]))
        acts = [lambda: line.line(3), lambda: line.line(2), lambda: line.line(1), line.line_done]
        plan = acting(BACK_PLACES + LINE_PLACES, full.steps() + acts)
    i = pl.program_id(0)
    top = pl.num_programs(0)
    c = top - 1 - i

    @pl.when(i == 0)
    def _():
        if count:
            meet(box_peers())
            line.kept[0] = parts[0][...]
        gin[...] = gin_ref[...].astype(F32)
        fill_picks(picks)
        head[...] = jnp.zeros_like(head)
        sums_ref[...] = jnp.zeros_like(sums_ref)
        small_ref[...] = jnp.zeros_like(small_ref)

    log_parts = in_parts(log_ref[...])
    step_parts = in_parts(step_ref[...])
    low_b = bc_ref[:, :N]
    dlw[...] = jnp.zeros_like(dlw)
    dst[...] = jnp.zeros_like(dst)
    drow[...] = jnp.zeros_like(drow)

    def conv_back(cols, dact):
        cv = conv_ref[:, cols].astype(F32)
        s = sigmoid(cv)
        dcv = dact * (s * (1.0 + cv * (1.0 - s)))
        after = head[:, cols]
        head[:, cols] = dcv[:8]
        x = u_ref[:, cols]
        sums_ref[4:5, cols] += jnp.sum(dcv, axis=0, keepdims=True)
        total = None
        for j in range(CONVK):
            k = CONVK - 1 - j
            moved = advanced(dcv, after, j)
            sums_ref[k : k + 1, cols] += jnp.sum(moved * x, axis=0, keepdims=True)
            term = cw_ref[k : k + 1, cols] * moved
            total = term if total is None else total + term
        du_ref[:, cols] = total.astype(BF16)

        @pl.when(i == 0)
        def _():
            last_ref[:, cols] = total[Q - 8 :]

    def group(g, db):
        when_at(i * GROUPS + g, plan)
        cols = pl.ds(pl.multiple_of(g * GW, GW), GW)
        log_wide = nn(log_parts, picks[:, cols])
        step_wide = nn(step_parts, picks[:, cols])
        done = cum_ref[c + 1, 0:1, cols]
        after = jnp.exp2(cum_ref[top, 0:1, cols] - done)
        grad = gnext_ref[0, :, cols].astype(F32) + after * gin[:, cols]
        low_g = grad.astype(BF16)
        decay = jnp.exp2(done - cum_ref[c, 0:1, cols])
        row = decay * jnp.sum(grad * entt_ref[0, :, cols].astype(F32), axis=0, keepdims=True)
        coarse = row.astype(BF16).astype(F32)
        r = rows_of((16, GW))
        two = jnp.where(r == 0, jnp.broadcast_to(coarse, (16, GW)), 0.0)
        two = jnp.where(r == 1, jnp.broadcast_to(row - coarse, (16, GW)), two)
        chosen = pick_heads(g)
        drow[...] += nn(two.astype(BF16), chosen)
        dweighted = nn(low_b, low_g)
        weights = []
        moves = []
        stepped = []
        dacts = []
        for j in range(2):
            pc = pl.ds(pl.multiple_of(g * GW + 128 * j, 128), 128)
            lp = log_wide[:, 128 * j : 128 * j + 128]
            sp = step_wide[:, 128 * j : 128 * j + 128]
            fade = jnp.exp2(lp[Q - 1 : Q, :] - lp)
            vp = vp_ref[:, pc].astype(F32)
            faded = dweighted[:, 128 * j : 128 * j + 128] * fade
            weights.append((vp * fade).astype(BF16))
            moves.append((faded * vp).astype(BF16))
            both = dvp_ref[:, pc].astype(F32) + faded
            stepped.append((both * val_ref[:, pc].astype(F32)).astype(BF16))
            dacts.append((pc, sp * both + skip_ref[:, pc] * ds_ref[:, pc].astype(F32)))
        dlw[...] += nn(jnp.concatenate(moves, 1), chosen)
        dst[...] += nn(jnp.concatenate(stepped, 1), chosen)
        for pc, dact in dacts:
            conv_back(pc, dact)
        return db + nt(jnp.concatenate(weights, 1), low_g)

    db = lax.fori_loop(0, GROUPS, group, dbc_ref[:, :N])
    conv_back(pl.ds(DI, N), db)
    conv_back(pl.ds(DI + N, N), dbc_ref[:, N:] + dc_ref[...])

    moved = dlw[...]
    at_last = jnp.sum(moved, axis=0, keepdims=True) + drow[0:1] + drow[1:2]
    dlog = dlp_ref[...] + dlt_ref[...] - moved
    dlog = dlog + jnp.where(rows_of(dlog.shape) == Q - 1, at_last, 0.0)
    square = (Q, Q)
    later = jnp.where(rows_of(square) <= lanes_of(square), 1.0, 0.0).astype(BF16)
    dsum = ordered_sum(later, dlog)
    rate = -jnp.exp(dl_ref[...])
    dstep = (dst[...] + dsum * rate) * valid_ref[...]
    raw = u_ref[:, CH:] + sb_ref[...]
    draw = dstep * (1.0 / (1.0 + jnp.exp(-raw)))
    draw = jnp.where(lanes_of(draw.shape) < HEADS, draw, 0.0)
    du_ref[:, CH:] = draw.astype(BF16)
    small_ref[0:1] += jnp.sum(draw, axis=0, keepdims=True)
    small_ref[1:2] += jnp.sum(dsum * step_ref[...], axis=0, keepdims=True) * rate

    @pl.when(c == 0)
    def _():
        epad[0:8, :] = jnp.zeros((8, CH), F32)
        epad[8:16, :] = head[...]
        x = halo_ref[:, :CH] * keep_ref[0, 0]
        total = jnp.zeros((8, CH), F32)
        for j in range(CONVK):
            k = CONVK - 1 - j
            moved = epad[j : j + 8, :]
            sums_ref[k : k + 1, :] += jnp.sum(moved * x, axis=0, keepdims=True)
            total = total + cw_ref[k : k + 1, :] * moved
        edge_ref[...] = total * keep_ref[0, 0]


def spec(block, index):
    return pl.BlockSpec(block, index)


def whole(shape):
    return pl.BlockSpec(shape, lambda *_: (0,) * len(shape))


def scalar():
    return pl.BlockSpec(memory_space=pltpu.SMEM)


def shaped(shape, kind):
    return jax.ShapeDtypeStruct(shape, kind)


def cost(flops, moved):
    return pl.CostEstimate(flops=int(flops), bytes_accessed=int(moved), transcendentals=0)


def params(number=None):
    return pltpu.CompilerParams(
        dimension_semantics=("arbitrary",), vmem_limit_bytes=60 * 1024 * 1024, collective_id=number,
        has_side_effects=number is not None,
    )


LINE = 4


def my_place():
    f = lax.axis_index("fsdp")
    t = lax.axis_index("ctx")
    return f // 2, f % 2, t // 2, t % 2


def device_at(z, y, x, core):
    return {"fsdp": z * 2 + y, "ctx": x * 2 + core}


def order_of(z, y, x, core):
    return (z * 2 + y) * 4 + x * 2 + core


def box_peers():
    z, y, x, core = my_place()
    return [
        (None, device_at(z, y, x, 1 - core)), (None, device_at(z, y, 1 - x, core)),
        (None, device_at(z, 1 - y, x, core)),
        (z > 0, device_at(z - 1, y, x, core)), (z < LINE - 1, device_at(z + 1, y, x, core)),
    ]


def meet(peers):
    barrier = pltpu.get_barrier_semaphore()
    count = 0
    for valid, peer in peers:

        def greet(peer=peer):
            pl.semaphore_signal(barrier, inc=1, device_id=peer, device_id_type=pl.DeviceIdType.MESH)

        if valid is None:
            greet()
            count = count + 1
        else:
            pl.when(valid)(greet)
            count = count + jnp.where(valid, 1, 0)
    pl.semaphore_wait(barrier, count)


def send(src, dst, send_sem, recv_sem, peer):
    return pltpu.make_async_remote_copy(
        src_ref=src, dst_ref=dst, send_sem=send_sem, recv_sem=recv_sem,
        device_id=device_at(*peer), device_id_type=pl.DeviceIdType.MESH,
    )


class Gather:
    def __init__(self, own, out, window, recv, halves, twin, sent, here):
        first, self.width, self.at = window
        self.own, self.out, self.rows = own.at[:, pl.ds(first, self.width)], out, own.shape[0]
        self.recv, self.halves, self.twin, self.sent, self.here = recv, halves, twin, sent, here
        self.place = my_place()

    def block(self, z, y, x, core, half=None):
        size = self.rows if half is None else self.rows // 2
        start = order_of(z, y, x, core) * self.rows + (0 if half is None else half * size)
        return self.out.at[pl.ds(pl.multiple_of(start, 16), size), pl.ds(self.at, self.width)]

    def copy(self, origin, way, half=None, own=False):
        z, y, x, core = self.place
        oz, oy, ox = origin
        o = oz * 4 + oy * 2 + ox
        dst = self.block(oz, oy, ox, core, half)
        src = self.own if own else dst
        peer = {
            "up": (z + 1, y, x, core), "down": (z - 1, y, x, core), "x": (z, y, 1 - x, core),
            "y": (z, 1 - y, x, core), "twin": (z, y, x, 1 - core),
        }[way]
        sem = self.sent.at[("up", "down", "x", "y", "twin").index(way), o]
        if way == "twin":
            arrival = self.twin.at[o]
        elif half is not None:
            arrival = self.halves.at[half, o]
        else:
            arrival = self.recv.at[o]
        return send(src, dst, sem, arrival, peer)

    def arrived(self, origin, half=None):
        self.copy(origin, "x", half).wait_recv()

    def column(self, r):
        z = self.place[0]
        if r == 0:
            return [(None, z, True, True)]
        return [(z - r >= 0, z - r, True, False), (z + r < LINE, z + r, False, True)]

    def each(self, r, act):
        for valid, oz, below, above in self.column(r):
            if valid is None:
                act(oz, below, above)
            else:
                pl.when(valid)(lambda oz=oz, below=below, above=above: act(oz, below, above))

    def begin(self):
        z, y, x, core = self.place
        pltpu.make_async_copy(self.own, self.block(z, y, x, core), self.here).start()
        self.forward(0)

    def ways(self, oz, below, above, act):
        z = self.place[0]
        if below:
            pl.when(z < LINE - 1)(lambda: act("up"))
        if above:
            pl.when(z > 0)(lambda: act("down"))
        act("x")
        act("y")
        act("twin")

    def forward(self, r):
        z, y, x, core = self.place

        def act(oz, below, above):
            origin = (oz, y, x)
            if r:
                self.arrived(origin)
            self.ways(oz, below, above, lambda way: self.copy(origin, way, own=r == 0).start())

        self.each(r, act)

    def across(self, r):
        z, y, x, core = self.place

        def act(oz, below, above):
            self.arrived((oz, y, 1 - x))
            self.copy((oz, y, 1 - x), "y", 0).start()
            self.copy((oz, y, 1 - x), "twin").start()
            self.arrived((oz, 1 - y, x))
            self.copy((oz, 1 - y, x), "x", 1).start()
            self.copy((oz, 1 - y, x), "twin").start()

        self.each(r, act)

    def corner(self, r):
        z, y, x, core = self.place

        def act(oz, below, above):
            origin = (oz, 1 - y, 1 - x)
            self.arrived(origin, 0)
            self.arrived(origin, 1)
            self.copy(origin, "twin").start()

        self.each(r, act)

    def finish(self):
        z, y, x, core = self.place
        pltpu.make_async_copy(self.own, self.block(z, y, x, core), self.here).wait()
        for r in range(LINE):

            def act(oz, below, above, r=r):
                self.ways(oz, below, above, lambda way: self.copy((oz, y, x), way, own=r == 0).wait_send())
                self.copy((oz, y, 1 - x), "y", 0).wait_send()
                self.copy((oz, 1 - y, x), "x", 1).wait_send()
                for oy, ox in ((y, 1 - x), (1 - y, x), (1 - y, 1 - x)):
                    self.copy((oz, oy, ox), "twin").wait_send()
                for oy, ox in ((y, x), (y, 1 - x), (1 - y, x), (1 - y, 1 - x)):
                    self.copy((oz, oy, ox), "twin").wait_recv()

            self.each(r, act)

    def steps(self):
        return [
            self.begin,
            lambda: self.forward(1),
            lambda: self.across(0),
            lambda: self.forward(2),
            lambda: self.across(1),
            lambda: (self.forward(3), self.corner(0)),
            lambda: self.across(2),
            lambda: self.corner(1),
            lambda: self.across(3),
            lambda: (self.corner(2), self.corner(3)),
            self.finish,
        ]


def gather_scratch():
    dma = pltpu.SemaphoreType.DMA
    return [dma((16,)), dma((2, 16)), dma((16,)), dma((5, 16)), dma(())]


U_WINDOWS = ((DI, 1280, 0), (DI + 1280, UW - 1280, 1280))


def gather_kernel(own, tok_ref, gain_ref, out, normed_ref, turned_ref, near_rows, sems, *gather_sems):
    rows, width = tok_ref.shape
    meet(box_peers() + chain_peers())
    pos = lax.axis_index("ctx")
    last = pos == lax.axis_size("ctx") - 1
    lists = [Gather(own, out, window, *gather_sems[5 * k : 5 * k + 5]).steps() for k, window in enumerate(U_WINDOWS)]
    for each in lists:
        each[0]()
    halo = pass_on(tok_ref.at[pl.ds(rows - HALO, HALO)], near_rows, sems, 1)

    @pl.when(jnp.logical_not(last))
    def _():
        halo.start()

    def normed(values):
        wide = values.astype(F32)
        scale = lax.rsqrt(jnp.sum(wide * wide, axis=1, keepdims=True) * (1.0 / width) + epsilon)
        return wide * scale * gain_ref[...]

    def block(r, unused):
        here = pl.ds(pl.multiple_of(r * 128, 128), 128)
        values = normed(tok_ref[here, :])
        normed_ref[here, :] = values.astype(BF16)
        turned_ref[:, here] = values.T.astype(BF16)
        return unused

    def hops(at):
        for k, each in enumerate(lists):
            if 1 <= at - k < len(each):
                each[at - k]()

    parts = 4
    for at in range(parts):
        lax.fori_loop(at * rows // 128 // parts, (at + 1) * rows // 128 // parts, block, 0)
        hops(at + 1)

    @pl.when(pos > 0)
    def _():
        halo.wait_recv()

    @pl.when(pos == 0)
    def _():
        near_rows[...] = jnp.zeros_like(near_rows)

    normed_ref[rows:, :] = normed(near_rows[...]).astype(BF16)

    @pl.when(jnp.logical_not(last))
    def _():
        halo.wait_send()

    for at in range(parts + 1, len(lists[0]) + 1):
        hops(at)


def gathered(own, tokens, gain, number):
    rows, width = tokens.shape
    anywhere = pl.BlockSpec(memory_space=pl.ANY)
    vmem = pl.BlockSpec(memory_space=pltpu.VMEM)
    return pl.pallas_call(
        gather_kernel,
        in_specs=[anywhere, vmem, vmem],
        out_specs=[anywhere, vmem, vmem],
        out_shape=[
            shaped((32 * own.shape[0], UW), BF16), shaped((rows + HALO, width), BF16), shaped((width, rows), BF16),
        ],
        scratch_shapes=[pltpu.VMEM((HALO, width), BF16), pltpu.SemaphoreType.DMA((2,))] + gather_scratch() * 2,
        compiler_params=pltpu.CompilerParams(
            collective_id=number, has_side_effects=True, vmem_limit_bytes=60 * 1024 * 1024
        ),
        name="gather",
    )(own, tokens, gain)


class Scatter:
    def __init__(self, parts, out, got, kept, mixed_y, mixed_x, from_x, from_y, up, down, sems):
        self.parts, self.out = parts, out
        self.got, self.kept = got, kept
        self.mixed = (mixed_y, mixed_x)
        self.sides = (from_x, from_y)
        self.up, self.down = up, down
        self.twin_sent, self.twin_recv, self.sent, self.recv, self.line_sent, self.line_recv = sems
        self.place = my_place()
        self.rows = kept.shape[-2]
        self.last = kept.shape[0] - 1

    def groups(self):
        z, y, x, core = self.place
        return [(1 - y, 1 - x), (y, 1 - x), (1 - y, x), (y, x)]

    def to_twin(self, k):
        z, y, x, core = self.place
        gy, gx = self.groups()[k]
        return send(
            self.parts.at[:, gy * 4 + gx * 2 + 1 - core], self.got.at[k], self.twin_sent.at[k], self.twin_recv.at[k],
            (z, y, x, 1 - core),
        )

    def begin(self):
        for k in range(4):
            self.to_twin(k).start()

    def add(self, k, sources, first=0, rows=None):
        rows = self.rows if rows is None else rows
        pieces = rows // 16

        def piece(n, unused):
            b = n // pieces
            at = (n - b * pieces) * 16
            here = pl.ds(pl.multiple_of(first + at, 16), 16)
            total = None
            for source in sources:
                term = source(b, pl.multiple_of(at, 16), here).astype(F32)
                total = term if total is None else total + term
            self.kept[k, b, here] = total.astype(BF16)
            return unused

        lax.fori_loop(0, LINE * pieces, piece, 0)

    def own(self, k):
        return lambda b, at, here: self.kept[k, b, here]

    def both(self, k):
        z, y, x, core = self.place
        gy, gx = self.groups()[k]
        self.to_twin(k).wait_recv()
        self.add(
            k, [lambda b, at, here: self.parts[b, gy * 4 + gx * 2 + core, here], lambda b, at, here: self.got[k, b, here]]
        )

    def corner_copy(self, half):
        z, y, x, core = self.place
        size = self.rows // 2
        src = self.kept.at[0, :, pl.ds(half * size, size)]
        peer = (z, 1 - y, x, core) if half == 0 else (z, y, 1 - x, core)
        return send(src, self.mixed[half], self.sent.at[half], self.recv.at[half], peer)

    def side_copy(self, k):
        z, y, x, core = self.place
        peer = (z, y, 1 - x, core) if k == 1 else (z, 1 - y, x, core)
        return send(self.kept.at[k], self.sides[k - 1], self.sent.at[1 + k], self.recv.at[1 + k], peer)

    def corners(self):
        self.both(0)
        self.corner_copy(0).start()
        self.corner_copy(1).start()
        self.both(1)
        self.both(2)
        self.both(3)

    def sides_out(self):
        size = self.rows // 2
        for half, k in ((0, 1), (1, 2)):
            self.corner_copy(half).wait_recv()
            self.add(
                k, [self.own(k), lambda b, at, here, half=half: self.mixed[half][b, pl.ds(at, 16)]],
                half * size, size,
            )
            self.side_copy(k).start()

    def sides_in(self):
        self.side_copy(1).wait_recv()
        self.side_copy(2).wait_recv()
        self.add(
            3,
            [
                self.own(3), lambda b, at, here: self.sides[0][b, here], lambda b, at, here: self.sides[1][b, here],
            ],
        )

    def line_copy(self, oz, way):
        z, y, x, core = self.place
        buffer = self.up if way == 0 else self.down
        peer = (z + 1, y, x, core) if way == 0 else (z - 1, y, x, core)
        return send(
            self.kept.at[self.last, oz], buffer.at[oz], self.line_sent.at[way, oz], self.line_recv.at[way, oz], peer
        )

    def add_line(self, oz, buffer):
        def piece(n, unused):
            here = pl.ds(pl.multiple_of(n * 16, 16), 16)
            total = self.kept[self.last, oz, here].astype(F32) + buffer[oz, here].astype(F32)
            self.kept[self.last, oz, here] = total.astype(BF16)
            return unused

        lax.fori_loop(0, self.rows // 16, piece, 0)

    def line(self, r):
        z = self.place[0]

        def upward():
            oz = z + r

            @pl.when(z > 0)
            def _():
                self.line_copy(oz, 0).wait_recv()
                self.add_line(oz, self.up)

            self.line_copy(oz, 0).start()

        def downward():
            oz = z - r

            @pl.when(z < LINE - 1)
            def _():
                self.line_copy(oz, 1).wait_recv()
                self.add_line(oz, self.down)

            self.line_copy(oz, 1).start()

        pl.when(z + r < LINE)(upward)
        pl.when(z - r >= 0)(downward)

    def plane_sent(self):
        for k in range(4):
            self.to_twin(k).wait_send()
        for half in range(2):
            self.corner_copy(half).wait_send()
        for k in (1, 2):
            self.side_copy(k).wait_send()

    def hand_on(self, out):
        self.sides_in()
        out[...] = self.kept[self.last]
        self.plane_sent()

    def line_done(self):
        z = self.place[0]
        self.out[...] = self.kept[self.last, z].astype(F32)

        @pl.when(z > 0)
        def _():
            self.line_copy(z, 0).wait_recv()
            self.out[...] += self.up[z].astype(F32)

        @pl.when(z < LINE - 1)
        def _():
            self.line_copy(z, 1).wait_recv()
            self.out[...] += self.down[z].astype(F32)

        for r in range(1, LINE):
            pl.when(z + r < LINE)(lambda r=r: self.line_copy(z + r, 0).wait_send())
            pl.when(z - r >= 0)(lambda r=r: self.line_copy(z - r, 1).wait_send())

    def finish(self):
        self.line_done()
        self.plane_sent()

    def steps(self):
        return [
            self.begin, self.corners, self.sides_out, self.sides_in, lambda: self.line(3), lambda: self.line(2),
            lambda: self.line(1), self.finish,
        ]


def scatter_scratch(rows, columns):
    dma = pltpu.SemaphoreType.DMA
    half = rows // 2
    return [
        pltpu.VMEM((4, LINE, rows, columns), BF16),
        pltpu.VMEM((4, LINE, rows, columns), BF16),
        pltpu.VMEM((LINE, half, columns), BF16),
        pltpu.VMEM((LINE, half, columns), BF16),
        pltpu.VMEM((LINE, rows, columns), BF16),
        pltpu.VMEM((LINE, rows, columns), BF16),
        pltpu.VMEM((LINE, rows, columns), BF16),
        pltpu.VMEM((LINE, rows, columns), BF16),
        dma((4,)), dma((4,)), dma((4,)), dma((4,)), dma((2, LINE)), dma((2, LINE)),
    ]


class Total:
    def __init__(self, own, out, held, got, sent, recv):
        self.own, self.out, self.held, self.got, self.sent, self.recv = own, out, held, got, sent, recv

    def copy(self, k):
        z, y, x, core = my_place()
        near = z + 1 - 2 * (z % 2)
        peer = [
            (z, y, x, 1 - core), (z, y, 1 - x, core), (z, 1 - y, x, core), (near, y, x, core),
            ((z + 2) % LINE, y, x, core),
        ][k]
        return send(self.own if k == 0 else self.held.at[k], self.got.at[k], self.sent.at[k], self.recv.at[k], peer)

    def begin(self):
        self.copy(0).start()

    def turn(self, k):
        self.copy(k).wait_recv()
        mine = self.own[...] if k == 0 else self.held[k]
        total = mine + self.got[k]
        if k < 4:
            self.held[k + 1] = total
            self.copy(k + 1).start()
        else:
            self.out[...] = total

    def finish(self):
        for k in range(5):
            self.copy(k).wait_send()

    def steps(self):
        return [self.begin] + [lambda k=k: self.turn(k) for k in range(5)] + [self.finish]


WIDE = 256
SPLIT = 1280


def final_kernel(*refs):
    (
        turned_ref, du_cols, dz_ref, du_ref, tok_ref, gain_ref, wz_any, wu_any, gate_ref, conv_ref, gsum_ref,
        small_ref,
    ) = refs[:12]
    grad_ref, inw_ref, sums_ref, norm_ref = refs[12:16]
    (
        wz, wu, sems, parts_a, parts_b, out_a, out_b, packed, normed_grad, held, got, sent, recv, gains,
        gains_held, gains_got, gains_sent, gains_recv,
    ) = refs[16:34]
    i = pl.program_id(0)
    steps = pl.num_programs(0) - tok_blocks(turned_ref)
    z, y, x, core = my_place()
    scr_a, scr_b = refs[34:48], refs[48:62]
    sum_a = Scatter(parts_a, out_a, *scr_a[:8], scr_a[8:])
    sum_b = Scatter(parts_b, out_b, *scr_b[:8], scr_b[8:])
    small = Total(packed, sums_ref, held, got, sent, recv)
    norm = Total(gains, norm_ref, gains_held, gains_got, gains_sent, gains_recv)
    load_z = pltpu.make_async_copy(wz_any, wz, sems.at[0])
    load_u = pltpu.make_async_copy(wu_any, wu, sems.at[1])

    @pl.when(i == 0)
    def _():
        load_z.start()
        load_u.start()
        meet(box_peers() + [(None, device_at((z + 2) % LINE, y, x, core))])
        packed[...] = jnp.zeros_like(packed)
        packed[0:5, :] = conv_ref[0:5, :]
        packed[5:6, :DI] = gsum_ref[0:1, :]
        packed[5:6, DI : DI + 128] = small_ref[0:1, :]
        packed[5:6, DI + 128 :] = small_ref[1:2, :]
        packed[6:7, :DI] = gsum_ref[1:2, :]
        gains[...] = jnp.zeros_like(gains)
        small.begin()
        inw_ref[:, :DI] = gate_ref[...]

    first = [
        (8, lambda: small.turn(0)), (20, lambda: (sum_a.begin(), small.turn(1))), (28, sum_a.corners),
        (36, lambda: (sum_a.sides_out(), small.turn(2))),
    ]
    second = [
        (40, sum_b.begin), (43, sum_b.corners), (45, lambda: small.turn(3)),
        (47, lambda: (sum_a.sides_in(), sum_a.line(3))), (49, sum_b.sides_out), (51, lambda: sum_a.line(2)),
        (53, lambda: small.turn(4)), (55, lambda: sum_a.line(1)),
    ]

    @pl.when(i < steps)
    def _():
        when_at(4 * i, first)
        result = nn(turned_ref[...], du_cols[...]).astype(BF16)
        rows = parts_a.shape[2]

        def keep(parts, cols, width):
            for b in range(LINE):
                for q in range(8):
                    first = (b * 8 + q) * rows
                    parts[b, q, :, cols] = result[first : first + rows, :width]

        edge = SPLIT // WIDE

        @pl.when(i < edge)
        def _():
            keep(parts_a, pl.ds(pl.multiple_of(i * WIDE, WIDE), WIDE), WIDE)

        @pl.when(jnp.logical_and(i >= edge, i < steps - 1))
        def _():
            keep(parts_b, pl.ds(pl.multiple_of((i - edge) * WIDE, WIDE), WIDE), WIDE)

        @pl.when(i == steps - 1)
        def _():
            keep(parts_b, slice((steps - 1 - edge) * WIDE, UW - SPLIT), UW - SPLIT - (steps - 1 - edge) * WIDE)

    @pl.when(i == steps)
    def _():
        load_z.wait()
        load_u.wait()

    @pl.when(i >= steps)
    def _():
        width = tok_ref.shape[1]
        chunk = width // 4

        def part(n, unused):
            when_at(4 * i + n, second)
            feats = pl.ds(pl.multiple_of(n * chunk, chunk), chunk)
            normed_grad[:, feats] = nt(dz_ref[...], wz[feats, :]) + nt(du_ref[...], wu[feats, :])
            return unused

        lax.fori_loop(0, 4, part, 0)
        values = tok_ref[...].astype(F32)
        scale = lax.rsqrt(jnp.sum(values * values, axis=1, keepdims=True) * (1.0 / width) + epsilon)
        hat = values * scale
        grad = normed_grad[...]
        gains[...] += jnp.sum(grad * hat, axis=0, keepdims=True)
        inner = grad * gain_ref[...]
        mean = jnp.sum(inner * hat, axis=1, keepdims=True) * (1.0 / width)
        grad_ref[...] = (scale * (inner - hat * mean)).astype(BF16)

    @pl.when(i == pl.num_programs(0) - 1)
    def _():
        norm.begin()
        sum_b.sides_in()
        sum_b.line(3)
        norm.turn(0)
        norm.turn(1)
        sum_b.line(2)
        norm.turn(2)
        sum_a.finish()
        sum_b.line(1)
        norm.turn(3)
        norm.turn(4)
        sum_b.finish()
        small.finish()
        norm.finish()
        inw_ref[:, DI : DI + SPLIT] = out_a[...]
        inw_ref[:, DI + SPLIT :] = out_b[:, : DPROJ - DI - SPLIT]


def tok_blocks(turned_ref):
    return turned_ref.shape[1] // Q


def final(turned, du, dz, tokens, gain, w_z, w_u, gate_columns, conv_sums, gate_sums, small, number):
    width, rows = turned.shape
    steps = -(-UW // WIDE)
    blocks = rows // Q
    dma = pltpu.SemaphoreType.DMA
    own = width // 32
    anywhere = pl.BlockSpec(memory_space=pl.ANY)
    later = lambda i: (jnp.maximum(i - steps, 0), 0)
    sums = (8, CH)
    return pl.pallas_call(
        final_kernel,
        grid=(steps + blocks,),
        in_specs=[
            whole((width, rows)),
            spec((rows, WIDE), lambda i: (0, jnp.minimum(i, steps - 1))),
            spec((Q, DI), later),
            spec((Q, UW), later),
            spec((Q, width), later),
            whole((1, width)),
            anywhere,
            anywhere,
            whole((own, DI)),
            whole(sums),
            whole((8, DI)),
            whole((8, 128)),
        ],
        out_specs=[spec((Q, width), later), whole((own, DPROJ)), whole(sums), whole((1, width))],
        out_shape=[
            shaped((rows, width), BF16), shaped((own, DPROJ), F32), shaped(sums, F32), shaped((1, width), F32),
        ],
        scratch_shapes=[
            pltpu.VMEM((width, DI), BF16),
            pltpu.VMEM((width, UW), BF16),
            dma((2,)),
            pltpu.VMEM((LINE, 8, own, SPLIT), BF16),
            pltpu.VMEM((LINE, 8, own, UW - SPLIT), BF16),
            pltpu.VMEM((own, SPLIT), F32),
            pltpu.VMEM((own, UW - SPLIT), F32),
            pltpu.VMEM(sums, F32),
            pltpu.VMEM((Q, width), F32),
            pltpu.VMEM((5,) + sums, F32),
            pltpu.VMEM((5,) + sums, F32),
            dma((5,)),
            dma((5,)),
            pltpu.VMEM((1, width), F32),
            pltpu.VMEM((5, 1, width), F32),
            pltpu.VMEM((5, 1, width), F32),
            dma((5,)),
            dma((5,)),
        ]
        + scatter_scratch(own, SPLIT)
        + scatter_scratch(own, UW - SPLIT),
        compiler_params=params(number),
        cost_estimate=cost(20e9, 60e6),
        name="final",
    )(turned, du, dz, du, tokens, gain, w_z, w_u, gate_columns, conv_sums, gate_sums, small)


def close_kernel(
    part_ref, cot_ref, inw_in, outw_in, sums_ref, norm_in, back_in,
    grad_ref, inw_ref, outw_ref, norm_ref, taps_ref, shift_ref, bias_ref, decay_ref, skip_ref, gate_ref,
):
    grad_ref[...] = cot_ref[...].astype(F32) + part_ref[...].astype(F32)

    @pl.when(pl.program_id(0) == 0)
    def _():
        inw_ref[...] = inw_in[...]
        outw_ref[...] = outw_in[...]
        norm_ref[...] = norm_in[0]
        taps_ref[...] = sums_ref[:CONVK]
        shift_ref[...] = sums_ref[CONVK]
        bias_ref[...] = sums_ref[5, DI : DI + 128]
        decay_ref[...] = sums_ref[5, DI + 128 :]
        gate_ref[...] = sums_ref[5, :DI]
        lane = lanes_of((1, 128))
        total = jnp.zeros((1, 128), F32)
        for h in range(HEADS):
            here = jnp.sum(back_in[6:7, h * P_SIZE : (h + 1) * P_SIZE], axis=1, keepdims=True)
            total = jnp.where(lane == h, here, total)
        skip_ref[...] = total[0]


def close(part, cotangent, inw, outw, sums, norm):
    rows, width = part.shape
    at = lambda i: (i, 0)
    line = lambda n: pl.BlockSpec((n,), lambda i: (0,))
    return pl.pallas_call(
        close_kernel,
        grid=(rows // Q,),
        in_specs=[
            spec((Q, width), at), spec((Q, width), at), whole(inw.shape), whole(outw.shape), whole(sums.shape),
            whole(norm.shape), whole(sums.shape),
        ],
        out_specs=[
            spec((Q, width), at), whole(inw.shape), whole(outw.shape), line(width), whole((CONVK, CH)), line(CH),
            line(128), line(128), line(128), line(DI),
        ],
        out_shape=[
            shaped((rows, width), F32), shaped(inw.shape, F32), shaped(outw.shape, F32), shaped((width,), F32),
            shaped((CONVK, CH), F32), shaped((CH,), F32), shaped((128,), F32), shaped((128,), F32),
            shaped((128,), F32), shaped((DI,), F32),
        ],
        compiler_params=params(),
        name="close",
    )(part, cotangent, inw, outw, sums, norm, sums)


def local(
    tokens,
    valid_mask,
    stretch_start,
    cotangent,
    norm_gain,
    in_weight,
    conv_weight,
    conv_bias,
    step_bias,
    decay_log,
    skip_gain,
    gate_gain,
    out_weight,
):
    axes = ("fsdp", "ctx")
    rows, width = tokens.shape
    blocks = rows // Q
    near = lax.axis_size("ctx")
    boxed = lax.axis_size("fsdp") == 8 and near == 4
    if boxed:
        own = jnp.pad(in_weight, ((0, 0), (0, UW + DI - DPROJ)))
        w_u, normed_more, turned = gathered(own, tokens, norm_gain.reshape(1, width), 1)
        later = [own, out_weight]
        later_widths = [DI, width]
    else:
        own_u = jnp.pad(in_weight[:, DI:], ((0, 0), (0, UW - (DPROJ - DI))))
        w_u, w_z, w_o = [
            lax.all_gather(a, axes, axis=0, tiled=True) for a in (own_u, in_weight[:, :DI], out_weight)
        ]
        later = []
        later_widths = []
        halo_tokens = lax.ppermute(tokens[rows - HALO :], "ctx", [(k, k + 1) for k in range(near - 1)])
        wide = jnp.concatenate([tokens, halo_tokens], 0).astype(F32)
        scale = lax.rsqrt(jnp.mean(wide * wide, axis=-1, keepdims=True) + epsilon)
        normed_more = (wide * scale * norm_gain).astype(BF16)
    extra = len(later)
    anywhere = pl.BlockSpec(memory_space=pl.ANY)

    normed = normed_more[:rows]
    valid = jnp.broadcast_to(valid_mask.astype(F32)[:, None], (rows, 128))
    keep = (1.0 - stretch_start[0].astype(F32)).reshape(1, 1)
    taps = conv_weight
    shift = conv_bias.reshape(1, CH)
    bias = jnp.pad(step_bias, (0, 128 - HEADS)).reshape(1, 128)
    logs = jnp.pad(decay_log, (0, 128 - HEADS)).reshape(1, 128)
    skips = jnp.repeat(skip_gain, P_SIZE).reshape(1, DI)

    same = lambda c: (c, 0)
    same3 = lambda c: (c, 0, 0)
    one = lambda i: (jnp.minimum(i, blocks - 1), 0)
    one3 = lambda i: (jnp.minimum(i, blocks - 1), 0, 0)
    two = lambda i: (jnp.maximum(i - blocks, 0), 0)
    val, vp, conv, bc, ssd, ent, logd, step, cum, start, u, ahead, *filled = pl.pallas_call(
        lambda *refs: forward_kernel(extra, *refs),
        grid=(2 * blocks,),
        in_specs=[
            spec((Q, width), one),
            spec((HALO, width), lambda c: (rows // HALO, 0)),
            anywhere,
            spec((Q, 128), one),
            scalar(),
            whole((CONVK, CH)),
            whole((1, CH)),
            whole((1, 128)),
            whole((1, 128)),
            whole((1, DI)),
        ]
        + [anywhere] * extra,
        out_specs=[
            spec((Q, DI), one),
            spec((Q, DI), one),
            spec((Q, CH), one),
            spec((Q, 2 * N), one),
            spec((Q, DI), two),
            spec((1, N, DI), one3),
            spec((Q, 128), one),
            spec((Q, 128), one),
            whole((blocks + 1, 8, DI)),
            whole((N, DI)),
            spec((Q, UW), one),
            whole((8, UW)),
        ]
        + [anywhere] * extra,
        out_shape=[
            shaped((rows, DI), BF16),
            shaped((rows, DI), BF16),
            shaped((rows, CH), BF16),
            shaped((rows, 2 * N), BF16),
            shaped((rows, DI), BF16),
            shaped((blocks, N, DI), BF16),
            shaped((rows, 128), F32),
            shaped((rows, 128), F32),
            shaped((blocks + 1, 8, DI), F32),
            shaped((N, DI), BF16),
            shaped((rows, UW), F32),
            shaped((8, UW), F32),
        ]
        + [shaped((32 * a.shape[0], n), a.dtype) for a, n in zip(later, later_widths)],
        scratch_shapes=[
            pltpu.VMEM((8, CH), F32),
            pltpu.VMEM((GROUPS, Q, 128), F32),
            pltpu.VMEM((128, DI), BF16),
            pltpu.VMEM((GROUPS, 8, Q), F32),
            pltpu.VMEM((Q, Q), F32),
            pltpu.VMEM((N, DI), F32),
            pltpu.VMEM((blocks, Q, DI), BF16),
            pltpu.VMEM((blocks, Q, DI), BF16),
            pltpu.VMEM((blocks, Q, 2 * N), BF16),
            pltpu.VMEM((blocks, Q, 128), F32),
            pltpu.VMEM((N, DI), BF16),
            pltpu.VMEM((N, DI), BF16),
            pltpu.SemaphoreType.DMA((2,)),
            pltpu.VMEM((w_u.shape[0], UW), BF16),
            pltpu.SemaphoreType.DMA(()),
            pltpu.VMEM((2, Q, GW), F32),
            pltpu.VMEM((2, Q, GW), F32),
        ]
        + gather_scratch() * extra,
        compiler_params=params(2),
        cost_estimate=cost(15e9, 60e6),
        name="forward",
    )(normed_more, normed_more, w_u, valid, keep, taps, shift, bias, logs, skips, *later)
    if later:
        w_z, w_o = filled

    z = jnp.dot(normed, w_z, preferred_element_type=F32).astype(BF16)
    back = lambda i: (blocks - 1 - i, 0)
    back3 = lambda i: (blocks - 1 - i, 0, 0)
    gains = gate_gain.reshape(1, DI)
    output, gated, branch_grad, ds, dz, entt, gnext, gout, dlp, dc, gate_sums = pl.pallas_call(
        gate_kernel,
        grid=(blocks,),
        in_specs=[
            whole((N, DI)),
            spec((Q, DI), back),
            spec((1, N, DI), back3),
            spec((Q, DI), back),
            spec((Q, DI), back),
            spec((Q, 2 * N), back),
            spec((Q, 128), back),
            whole((blocks + 1, 8, DI)),
            spec((Q, width), back),
            spec((Q, width), back),
            spec((Q, 128), back),
            whole((DI, width)),
            whole((1, DI)),
        ],
        out_specs=[
            spec((Q, width), back),
            spec((Q, DI), back),
            spec((Q, width), back),
            spec((Q, DI), back),
            spec((Q, DI), back),
            spec((1, N, DI), back3),
            spec((1, N, DI), back3),
            whole((N, DI)),
            spec((Q, 128), back),
            spec((Q, N), back),
            whole((8, DI)),
        ],
        out_shape=[
            shaped((rows, width), BF16),
            shaped((rows, DI), BF16),
            shaped((rows, width), BF16),
            shaped((rows, DI), BF16),
            shaped((rows, DI), BF16),
            shaped((blocks, N, DI), BF16),
            shaped((blocks, N, DI), BF16),
            shaped((N, DI), BF16),
            shaped((rows, 128), F32),
            shaped((rows, N), F32),
            shaped((8, DI), F32),
        ],
        scratch_shapes=[
            pltpu.VMEM((N, DI), F32),
            pltpu.VMEM((N, DI), F32),
            pltpu.VMEM((128, DI), BF16),
            pltpu.VMEM((Q, DI), F32),
            pltpu.VMEM((Q, DI), F32),
            pltpu.VMEM((Q, DI), F32),
            pltpu.VMEM((Q, DI), F32),
            pltpu.VMEM((Q, DI), F32),
            pltpu.VMEM((Q, 128), F32),
        ],
        compiler_params=params(),
        cost_estimate=cost(15e9, 60e6),
        name="gate",
    )(
        start, ssd, ent, z, val, bc, logd, cum, tokens, cotangent, valid, w_o, gains,
    )

    def columns_of(left, right):
        return lax.dot_general(
            left, right, (((0,), (0,)), ((), ())), preferred_element_type=F32
        ).astype(BF16)

    def in_blocks(a):
        return a.reshape(LINE, 8, a.shape[0] // 32, a.shape[1])

    out_weight_grad = columns_of(gated, branch_grad)
    gate_columns = columns_of(normed, dz)
    mixing_parts = [in_blocks(out_weight_grad)] if boxed else []

    dvp, dbc, dlt, gin, *summed_out = pl.pallas_call(
        lambda *refs: mixing_kernel(len(mixing_parts), *refs),
        grid=(blocks,),
        in_specs=[
            spec((Q, DI), same),
            spec((Q, DI), same),
            spec((Q, 2 * N), same),
            spec((Q, 128), same),
            scalar(),
            whole((N, DI)),
            whole((blocks + 1, 8, DI)),
        ]
        + [pl.BlockSpec(memory_space=pltpu.VMEM) for a in mixing_parts],
        out_specs=[spec((Q, DI), same), spec((Q, 2 * N), same), spec((Q, 128), same), whole((N, DI))]
        + [whole((LINE,) + a.shape[-2:]) for a in mixing_parts],
        out_shape=[
            shaped((rows, DI), BF16), shaped((rows, 2 * N), F32), shaped((rows, 128), F32), shaped((N, DI), BF16),
        ]
        + [shaped((LINE,) + a.shape[-2:], BF16) for a in mixing_parts],
        scratch_shapes=[
            pltpu.VMEM((GROUPS, Q, 128), F32),
            pltpu.VMEM((GROUPS, 8, Q), F32),
            pltpu.VMEM((Q, Q), F32),
            pltpu.VMEM((Q, Q), F32),
            pltpu.VMEM((GROUPS, 8, Q), F32),
            pltpu.VMEM((128, Q), F32),
            pltpu.VMEM((GROUPS, Q, 128), F32),
            pltpu.VMEM((N, DI), BF16),
            pltpu.VMEM((N, DI), BF16),
            pltpu.SemaphoreType.DMA((2,)),
        ]
        + [each for a in mixing_parts for each in plane_scratch(*a.shape[-2:])],
        compiler_params=params(3),
        cost_estimate=cost(15e9, 60e6),
        name="mixing",
    )(ds, vp, bc, logd, keep, gout, cum, *mixing_parts)

    back_parts = summed_out + [in_blocks(gate_columns)] if boxed else []
    du, last, edge, conv_sums, small, *summed_gate = pl.pallas_call(
        lambda *refs: back_kernel(len(back_parts), *refs),
        grid=(blocks,),
        in_specs=[
            scalar(),
            whole((N, DI)),
            spec((1, N, DI), back3),
            spec((1, N, DI), back3),
            whole((blocks + 1, 8, DI)),
            spec((Q, DI), back),
            spec((Q, DI), back),
            spec((Q, DI), back),
            spec((Q, DI), back),
            spec((Q, CH), back),
            spec((Q, UW), back),
            whole((8, UW)),
            spec((Q, 2 * N), back),
            spec((Q, 128), back),
            spec((Q, 128), back),
            spec((Q, 128), back),
            spec((Q, 128), back),
            spec((Q, 128), back),
            spec((Q, 2 * N), back),
            spec((Q, N), back),
            whole((CONVK, CH)),
            whole((1, 128)),
            whole((1, 128)),
            whole((1, DI)),
        ]
        + [pl.BlockSpec(memory_space=pltpu.VMEM) for a in back_parts],
        out_specs=[
            spec((Q, UW), back),
            whole((8, CH)),
            whole((8, CH)),
            whole((8, CH)),
            whole((8, 128)),
        ]
        + [whole(a.shape[-2:]) for a in back_parts],
        out_shape=[
            shaped((rows, UW), BF16),
            shaped((8, CH), F32),
            shaped((8, CH), F32),
            shaped((8, CH), F32),
            shaped((8, 128), F32),
        ]
        + [shaped(a.shape[-2:], F32) for a in back_parts],
        scratch_shapes=[
            pltpu.VMEM((N, DI), F32),
            pltpu.VMEM((128, DI), BF16),
            pltpu.VMEM((8, CH), F32),
            pltpu.VMEM((16, CH), F32),
            pltpu.VMEM((Q, 128), F32),
            pltpu.VMEM((Q, 128), F32),
            pltpu.VMEM((16, 128), F32),
        ]
        + (
            scatter_scratch(*back_parts[1].shape[-2:]) + line_scratch(*back_parts[0].shape[-2:])
            if back_parts
            else []
        ),
        compiler_params=params(4 if back_parts else None),
        cost_estimate=cost(15e9, 60e6),
        name="back",
    )(
        keep, gin, gnext, entt, cum, vp, val, dvp, ds, conv, u, ahead, bc, logd, step, valid,
        dlp, dlt, dbc, dc, taps, bias, logs, skips, *back_parts,
    )
    edge_back = lax.ppermute(edge, "ctx", [(k + 1, k) for k in range(near - 1)])
    du = lax.dynamic_update_slice(du, (last + edge_back).astype(BF16), (rows - 8, 0))
    if boxed:
        out_weight_grad, gate_columns = summed_gate
        part, in_weight_grad, sums, norm_sum = final(
            turned, du, dz, tokens, norm_gain.reshape(1, width), w_z, w_u, gate_columns, conv_sums,
            gate_sums, small, 5,
        )
        results = close(part, cotangent, in_weight_grad, out_weight_grad, sums, norm_sum)
        input_grad, in_weight_grad, out_weight_grad, norm_sum, taps_sum, shift_sum = results[:6]
        bias_sum, decay_sum, skip_sum, gate_sum = results[6:]
        return (
            output,
            input_grad,
            in_weight_grad,
            out_weight_grad,
            norm_sum,
            taps_sum,
            shift_sum,
            bias_sum[:HEADS],
            decay_sum[:HEADS],
            skip_sum[:HEADS],
            gate_sum,
        )
    conv_columns = columns_of(normed, du)
    across = (((1,), (1,)), ((), ()))
    normed_grad = lax.dot_general(dz, w_z, across, preferred_element_type=F32) + lax.dot_general(
        du, w_u, across, preferred_element_type=F32
    )
    inputs = tokens.astype(F32)
    scale = lax.rsqrt(jnp.mean(inputs * inputs, axis=-1, keepdims=True) + epsilon)
    hat = inputs * scale
    inner = normed_grad * norm_gain
    input_grad = cotangent.astype(F32) + scale * (
        inner - hat * jnp.mean(inner * hat, axis=-1, keepdims=True)
    )
    norm_grad = jnp.sum(normed_grad * hat, axis=0)
    packed = jnp.concatenate(
        [
            norm_grad,
            conv_sums[:5].reshape(-1),
            gate_sums[:2].reshape(-1),
            small[:2].reshape(-1),
        ]
    )
    conv_columns, gate_columns, out_weight_grad = [
        lax.psum_scatter(a.astype(F32), axes, scatter_dimension=0, tiled=True)
        for a in (conv_columns, gate_columns, out_weight_grad)
    ]
    summed = lax.psum(packed, axes)
    in_weight_grad = jnp.concatenate([gate_columns, conv_columns[:, : DPROJ - DI]], 1)
    at = width
    conv_weight_grad = summed[at : at + CONVK * CH].reshape(CONVK, CH)
    at += CONVK * CH
    conv_bias_grad = summed[at : at + CH]
    at += CH
    gate_gain_grad = summed[at : at + DI]
    at += DI
    skip_gain_grad = jnp.sum(summed[at : at + DI].reshape(HEADS, P_SIZE), axis=1)
    at += DI
    step_bias_grad = summed[at : at + HEADS]
    decay_log_grad = summed[at + 128 : at + 128 + HEADS]
    return (
        output,
        input_grad,
        in_weight_grad,
        out_weight_grad,
        summed[:width],
        conv_weight_grad,
        conv_bias_grad,
        step_bias_grad,
        decay_log_grad,
        skip_gain_grad,
        gate_gain_grad,
    )


def solution(mesh):
    split = P(("fsdp", "ctx"), None)
    line = P(("fsdp", "ctx"))
    return jax.shard_map(
        local,
        mesh=mesh,
        in_specs=(split, line, line, split, P(), split, P(), P(), P(), P(), P(), P(), split),
        out_specs=(split, split, split, split, P(), P(), P(), P(), P(), P(), P()),
        check_vma=False,
    )
```

```python
import jax
import jax.numpy as jnp
from jax import lax
from jax.experimental import pallas as pl
from jax.experimental.pallas import tpu as pltpu
from jax.sharding import PartitionSpec as P

DI = 2048
HEADS = 32
P_SIZE = 64
N = 128
CONVK = 4
Q = 256
CH = 2304
DPROJ = 4384
UW = CH + 128
GW = 256
GROUPS = DI // GW
HALF = Q // 2
HALO = 16

F32 = jnp.float32
BF16 = jnp.bfloat16
LOG2E = 1.4426950408889634
epsilon = 1e-05


def nn(a, b):
    return lax.dot_general(a, b, (((1,), (0,)), ((), ())), preferred_element_type=F32)


def nt(a, b):
    return lax.dot_general(a, b, (((1,), (1,)), ((), ())), preferred_element_type=F32)


def sigmoid(x):
    return 0.5 * jnp.tanh(0.5 * x) + 0.5


def softplus(x):
    e = jnp.exp(-jnp.abs(x))
    w = 1.0 + e
    d = w - 1.0
    return jnp.maximum(x, 0.0) + jnp.where(d == 0.0, e, jnp.log(w) * (e / jnp.where(d == 0.0, 1.0, d)))


def rows_of(shape):
    return lax.broadcasted_iota(jnp.int32, shape, 0)


def lanes_of(shape):
    return lax.broadcasted_iota(jnp.int32, shape, 1)


def split3(x):
    a = x.astype(BF16)
    r = x - a.astype(F32)
    b = r.astype(BF16)
    return a, b, (r - b.astype(F32)).astype(BF16)


def ordered_sum(triangle, x):
    a, b, c = split3(x)
    return nn(triangle, c) + nn(triangle, b) + nn(triangle, a)


def spread(x, out):
    out[0] = x
    for g in range(1, GROUPS):
        out[g] = pltpu.roll(x, 128 - 4 * g, 1)


def delayed(before, x, by):
    if by == 0:
        return x
    return pltpu.roll(jnp.concatenate([before, x], 0), by, 0)[8:]


def advanced(x, after, by):
    if by == 0:
        return x
    count = x.shape[0]
    return pltpu.roll(jnp.concatenate([x, after], 0), count + 8 - by, 0)[:count]


def fill_picks(out):
    for g in range(GROUPS):
        shape = (128, GW)
        head = lax.shift_right_logical(lanes_of(shape), 6) + 4 * g
        at = rows_of(shape)
        own = jnp.logical_and(jnp.bitwise_and(at, HEADS - 1) == head, at < 3 * HEADS)
        out[:, g * GW : (g + 1) * GW] = jnp.where(own, 1.0, 0.0).astype(BF16)


def in_parts(x):
    lane = lanes_of(x.shape)
    a, b, c = split3(jnp.where(lane < HEADS, x, 0.0))
    wide = a.astype(F32) + pltpu.roll(b.astype(F32), HEADS, 1) + pltpu.roll(c.astype(F32), 2 * HEADS, 1)
    return wide.astype(BF16)


def spread_rows(x, out):
    for g in range(GROUPS):
        out[g, 0:4] = x[4 * g : 4 * g + 4]


def head_lanes(x, i):
    return jnp.broadcast_to(x[:, i : i + 1], (x.shape[0], 128))


def pick_heads(g):
    shape = (GW, 128)
    return jnp.where(
        lax.shift_right_logical(rows_of(shape), 6) + 4 * g == lanes_of(shape), 1.0, 0.0
    ).astype(BF16)


def when_at(now, plan):
    plan = sorted(plan, key=lambda entry: entry[0])
    if len(plan) == 1:
        place, act = plan[0]

        @pl.when(now == place)
        def _():
            act()

    elif plan:
        middle = len(plan) // 2

        def early():
            when_at(now, plan[:middle])

        def late():
            when_at(now, plan[middle:])

        lax.cond(now < plan[middle][0], early, late)


def chain_peers():
    pos = lax.axis_index("ctx")
    return [(pos > 0, {"ctx": pos - 1}), (pos < lax.axis_size("ctx") - 1, {"ctx": pos + 1})]


def pass_on(message, arrived, sems, by):
    return pltpu.make_async_remote_copy(
        src_ref=message, dst_ref=arrived, send_sem=sems.at[0], recv_sem=sems.at[1],
        device_id={"ctx": lax.axis_index("ctx") + by}, device_id_type=pl.DeviceIdType.MESH,
    )


def lay_heads(out, line):
    out[...] = jnp.zeros_like(out)
    out[0, :HEADS] = line[...]


def lay_out(out, line, picks):
    shape = (8, 128)
    heads = jnp.zeros((1, 128), F32)
    for h in range(HEADS):
        heads = jnp.where(lanes_of((1, 128)) == h, line[h], heads)
    out[...] = nn(in_parts(jnp.broadcast_to(heads, shape)), picks[...])[0:1]


def forward_kernel(count, *refs):
    (
        normed_ref, halo_ref, wu_any, valid_ref, keep_ref, cw_ref, cb_line, sb_line, dl_line, skip_line,
    ) = refs[:10]
    own = refs[10 : 10 + count]
    (
        val_ref, vp_ref, conv_ref, bc_ref, ssd_ref, ent_ref, log_ref, step_ref, cum_ref, start_ref, u_ref, ahead_ref,
    ) = refs[10 + count : 22 + count]
    outs = refs[22 + count : 22 + 2 * count]
    (
        past, logs, picks, logt, inter, state, all_vp, all_val, all_bc, all_log, message, arrived, sems, wu, load, log_wide, step_wide, cb_ref, sb_ref, dl_ref, skip_ref,
    ) = refs[22 + 2 * count : 43 + 2 * count]
    gather_sems = refs[43 + 2 * count :]
    i = pl.program_id(0)
    blocks = pl.num_programs(0) // 2
    first = i < blocks
    c = jnp.where(first, i, i - blocks)
    near = lax.axis_size("ctx")
    pos = lax.axis_index("ctx")
    plan = []
    if count:
        lists = [Gather(own[k], outs[k], (0, outs[k].shape[1], 0), *gather_sems[5 * k : 5 * k + 5]).steps() for k in range(count)]
        length = len(lists[0])
        for at in range(length + 2 * (count - 1)):
            acts = [lists[k][at - 2 * k] for k in range(count) if 0 <= at - 2 * k < length]
            plan.append((FORWARD_PLACES[at], lambda acts=acts: [act() for act in acts]))

    @pl.when(i == 0)
    def _():
        fetch = pltpu.make_async_copy(wu_any, wu, load)
        fetch.start()
        fill_picks(picks)
        cb_ref[0] = cb_line[...]
        lay_heads(sb_ref, sb_line)
        lay_heads(dl_ref, dl_line)
        lay_out(skip_ref, skip_line, picks)
        meet((box_peers() if count else []) + chain_peers())
        fetch.wait()
        before = nn(halo_ref[...], wu[...])[8:]
        ahead_ref[...] = before
        past[...] = before[:, :CH] * keep_ref[0, 0]
        state[...] = jnp.zeros_like(state)
        cum_ref[...] = jnp.zeros_like(cum_ref)

    half = lanes_of((Q, 128)) < P_SIZE
    square = (Q, Q)
    causal = rows_of(square) >= lanes_of(square)

    @pl.when(first)
    def _():
        tail = nn(normed_ref[...], wu[:, DI:])
        u_ref[:, DI:] = tail
        raw = tail[:, 2 * N :] + sb_ref[...]
        step = softplus(raw) * valid_ref[...]
        step = jnp.where(lanes_of(step.shape) < HEADS, step, 0.0)
        rate = -jnp.exp(dl_ref[...]) * LOG2E
        logd = ordered_sum(jnp.where(causal, 1.0, 0.0).astype(BF16), step * rate)
        log_ref[...] = logd
        all_log[c] = logd
        step_ref[...] = step
        log_parts = in_parts(logd)
        step_parts = in_parts(step)

        def convolved(cols, x):
            before = past[:, cols]
            past[:, cols] = x[Q - 8 :]
            total = cb_ref[:, cols] + cw_ref[CONVK - 1 : CONVK, cols] * x
            for k in range(CONVK - 1):
                total = total + cw_ref[k : k + 1, cols] * delayed(before, x, CONVK - 1 - k)
            return total

        conv_b = convolved(pl.ds(DI, N), tail[:, :N])
        conv_c = convolved(pl.ds(DI + N, N), tail[:, N : 2 * N])
        conv_ref[:, DI : DI + N] = conv_b.astype(BF16)
        conv_ref[:, DI + N :] = conv_c.astype(BF16)
        act_b = conv_b * sigmoid(conv_b)
        act_c = conv_c * sigmoid(conv_c)
        both = jnp.concatenate([act_b.astype(BF16), act_c.astype(BF16)], 1)
        bc_ref[...] = both
        all_bc[c] = both
        turned_b = act_b.T.astype(BF16)
        ent_ref[0] = state[...].astype(BF16)

        def ahead(g):
            cols = pl.ds(pl.multiple_of(g * GW, GW), GW)
            slot = g % 2
            u_ref[:, cols] = nn(normed_ref[...], wu[:, cols])
            log_wide[slot] = nn(log_parts, picks[:, cols])
            step_wide[slot] = nn(step_parts, picks[:, cols])

        ahead(0)

        def group(g, unused):
            when_at(i * GROUPS + g, plan)
            slot = g % 2
            for j in range(2):
                cols = pl.ds(pl.multiple_of(g * GW + 128 * j, 128), 128)
                cv = convolved(cols, u_ref[:, cols])
                conv_ref[:, cols] = cv.astype(BF16)
                val = cv * sigmoid(cv)
                low = val.astype(BF16)
                val_ref[:, cols] = low
                all_val[c, :, cols] = low
                lp = log_wide[slot, :, 128 * j : 128 * j + 128]
                vp = val * step_wide[slot, :, 128 * j : 128 * j + 128]
                low = vp.astype(BF16)
                vp_ref[:, cols] = low
                all_vp[c, :, cols] = low
                last = lp[Q - 1 : Q, :]
                weighted = (vp * jnp.exp2(last - lp)).astype(BF16)
                state[:, cols] = jnp.exp2(last) * state[:, cols] + nn(turned_b, weighted)
                cum_ref[c + 1, :, cols] = cum_ref[c, :, cols] + last
            ahead(lax.rem(g + 1, GROUPS))
            return unused

        lax.fori_loop(0, GROUPS, group, 0)

    def hop(k):
        @pl.when(pos == k)
        def _():
            if k:
                pass_on(message, arrived, sems, 1).wait_recv()
                entering = keep_ref[0, 0] * arrived[...].astype(F32)
                start_ref[...] = entering.astype(BF16)
            else:
                start_ref[...] = jnp.zeros_like(start_ref)
            if k < near - 1:
                if k:
                    message[...] = (jnp.exp2(cum_ref[blocks, 0:1, :]) * entering + state[...]).astype(BF16)
                else:
                    message[...] = state[...].astype(BF16)
                pass_on(message, arrived, sems, 1).start()

    hops = [(blocks * GROUPS + FORWARD_HOPS[k], lambda k=k: hop(k)) for k in range(near)]

    @pl.when(jnp.logical_not(first))
    def _():
        logd = all_log[c]
        spread(logd, logs)
        spread_rows(logd.T, logt)
        inter[...] = jnp.where(causal, nt(all_bc[c, :, N:], all_bc[c, :, :N]), 0.0)
        left = jnp.where(half[:1], 1.0, 0.0).astype(BF16)
        right = jnp.where(half[:1], 0.0, 1.0).astype(BF16)

        def group(g, unused):
            when_at(i * GROUPS + g, plan)
            when_at(i * GROUPS + g, hops)
            lg = logs[g]
            for j in range(2):
                cols = pl.ds(pl.multiple_of(g * GW + 128 * j, 128), 128)
                vp = all_vp[c, :, cols]
                v0 = vp * left
                v1 = vp * right
                top = []
                low = []
                for h in range(2):
                    row = logt[g, 2 * j + h : 2 * j + h + 1]
                    early, late = row[:, :HALF], row[:, HALF:]
                    lb = head_lanes(lg, 2 * j + h)
                    up, down = lb[:HALF], lb[HALF:]
                    top.append((inter[:HALF, :HALF] * jnp.exp2(jnp.minimum(up - early, 0.0))).astype(BF16))
                    low.append((inter[HALF:, :HALF] * jnp.exp2(jnp.minimum(down - early, 0.0))).astype(BF16))
                    low.append((inter[HALF:, HALF:] * jnp.exp2(jnp.minimum(down - late, 0.0))).astype(BF16))
                skipped = skip_ref[:, cols] * all_val[c, :, cols].astype(F32)
                above = nn(jnp.concatenate(top, 1), jnp.concatenate([v0[:HALF], v1[:HALF]], 0))
                below = nn(jnp.concatenate(low, 1), jnp.concatenate([v0, v1], 0))
                ssd_ref[:HALF, cols] = (above + skipped[:HALF]).astype(BF16)
                ssd_ref[HALF:, cols] = (below + skipped[HALF:]).astype(BF16)
            return unused

        lax.fori_loop(0, GROUPS, group, 0)

    @pl.when(jnp.logical_and(i == 2 * blocks - 1, pos < near - 1))
    def _():
        pass_on(message, arrived, sems, 1).wait_send()


def gate_kernel(
    start_ref, ssd_in, ent_ref, z_ref, val_ref, bc_ref, log_ref, cum_ref,
    tok_ref, cot_ref, valid_ref, ow_ref, gain_line,
    out_ref, gated_ref, bg_ref, ds_ref, dz_ref, entt_ref, gnext_ref, gout_ref, dlp_ref, dc_ref, sums_ref,
    start, gstate, picks, ssd_s, mix_s, el_s, pe_s, gg_s, acc, gain_ref,
):
    i = pl.program_id(0)
    c = pl.num_programs(0) - 1 - i

    @pl.when(i == 0)
    def _():
        start[...] = start_ref[...].astype(F32)
        fill_picks(picks)
        gain_ref[0] = gain_line[...]
        gstate[...] = jnp.zeros_like(gstate)
        sums_ref[...] = jnp.zeros_like(sums_ref)

    log_parts = in_parts(log_ref[...])
    low_c = bc_ref[:, N:]
    turned_c = low_c.astype(F32).T.astype(BF16)
    acc[...] = jnp.zeros_like(acc)

    def enter(g, unused):
        cols = pl.ds(pl.multiple_of(g * GW, GW), GW)
        decay = jnp.exp2(nn(log_parts, picks[:, cols]))
        entering = (
            ent_ref[0, :, cols].astype(F32) + jnp.exp2(cum_ref[c, 0:1, cols]) * start[:, cols]
        ).astype(BF16)
        entt_ref[0, :, cols] = entering
        part = nn(low_c, entering)
        for j in range(2):
            pc = pl.ds(pl.multiple_of(g * GW + 128 * j, 128), 128)
            el = decay[:, 128 * j : 128 * j + 128]
            pe = el * part[:, 128 * j : 128 * j + 128]
            el_s[:, pc] = el
            pe_s[:, pc] = pe
            ssd = ssd_in[:, pc].astype(F32) + pe
            z = z_ref[:, pc].astype(F32)
            mixed = ssd * (z * sigmoid(z))
            ssd_s[:, pc] = ssd
            mix_s[:, pc] = mixed
            acc[...] += mixed * mixed
        return unused

    lax.fori_loop(0, GROUPS, enter, 0)
    inv = lax.rsqrt(jnp.sum(acc[...], axis=1, keepdims=True) * (1.0 / DI) + epsilon)
    inv = jnp.broadcast_to(inv, (Q, 128))
    valid = valid_ref[...]
    valid8 = jnp.concatenate([valid] * (tok_ref.shape[1] // 128), 1)
    branch_grad = (cot_ref[...].astype(F32) * valid8).astype(BF16)
    bg_ref[...] = branch_grad
    acc[...] = jnp.zeros_like(acc)

    def gate(g, unused):
        cols = pl.ds(pl.multiple_of(g * GW, GW), GW)
        ggrad = nt(branch_grad, ow_ref[cols, :])
        for j in range(2):
            pc = pl.ds(pl.multiple_of(g * GW + 128 * j, 128), 128)
            hat = mix_s[:, pc] * inv
            gain = gain_ref[:, pc]
            mix_s[:, pc] = hat
            gated_ref[:, pc] = (hat * gain).astype(BF16)
            gg = ggrad[:, 128 * j : 128 * j + 128]
            both = gg * hat
            sums_ref[0:1, pc] += jnp.sum(both, axis=0, keepdims=True)
            acc[...] += both * gain
            gg_s[:, pc] = gg * gain
        return unused

    lax.fori_loop(0, GROUPS, gate, 0)
    mean = jnp.sum(acc[...], axis=1, keepdims=True) * (1.0 / DI)
    mean = jnp.broadcast_to(mean, (Q, 128))

    for n in range(tok_ref.shape[1] // 256):
        cols = slice(256 * n, 256 * n + 256)
        branch = nn(gated_ref[...], ow_ref[:, cols])
        out_ref[:, cols] = (tok_ref[:, cols].astype(F32) + valid8[:, :256] * branch).astype(BF16)

    acc[...] = jnp.zeros_like(acc)
    dc_ref[...] = jnp.zeros_like(dc_ref)

    def back(g, unused):
        cols = pl.ds(pl.multiple_of(g * GW, GW), GW)
        dparts = []
        prods = []
        for j in range(2):
            pc = pl.ds(pl.multiple_of(g * GW + 128 * j, 128), 128)
            dmixed = inv * (gg_s[:, pc] - mix_s[:, pc] * mean)
            z = z_ref[:, pc].astype(F32)
            s = sigmoid(z)
            ds = (dmixed * (z * s)).astype(BF16)
            ds_ref[:, pc] = ds
            dz_ref[:, pc] = (dmixed * ssd_s[:, pc] * (s * (1.0 + z * (1.0 - s)))).astype(BF16)
            ds = ds.astype(F32)
            sums_ref[1:2, pc] += jnp.sum(ds * val_ref[:, pc].astype(F32), axis=0, keepdims=True)
            dparts.append((ds * el_s[:, pc]).astype(BF16))
            prods.append((ds * pe_s[:, pc]).astype(BF16))
        dpart = jnp.concatenate(dparts, 1)
        acc[...] += nn(jnp.concatenate(prods, 1), pick_heads(g))
        dc_ref[...] += nt(dpart, entt_ref[0, :, cols])
        gnext_ref[0, :, cols] = gstate[:, cols].astype(BF16)
        total = cum_ref[c + 1, 0:1, cols] - cum_ref[c, 0:1, cols]
        gstate[:, cols] = nn(turned_c, dpart) + jnp.exp2(total) * gstate[:, cols]
        return unused

    lax.fori_loop(0, GROUPS, back, 0)
    dlp_ref[...] = acc[...]

    @pl.when(c == 0)
    def _():
        gout_ref[...] = gstate[...].astype(BF16)


FORWARD_PLACES = tuple(5 * k for k in range(13))
FORWARD_HOPS = (0, 8, 20, 30)
MIXING_HOPS = (0, 8, 20, 30)
MIXING_PLACES = (0, 5, 12, 31)
LINE_PLACES = (1, 12)
BACK_PLACES = (0, 4, 9, 20, 31)


def acting(places, acts):
    joined = {}
    for place, act in zip(places, acts):
        joined.setdefault(place, []).append(act)
    return [(place, lambda acts=acts: [act() for act in acts]) for place, acts in joined.items()]


def plane_scratch(rows, columns):
    dma = pltpu.SemaphoreType.DMA
    return scatter_scratch(rows, columns)[:6] + [dma((4,))] * 5


def line_scratch(rows, columns):
    dma = pltpu.SemaphoreType.DMA
    return [
        pltpu.VMEM((1, LINE, rows, columns), BF16), pltpu.VMEM((LINE, rows, columns), BF16), dma((LINE,)), dma((LINE,)),
    ]


def mixing_kernel(count, *refs):
    ds_ref, vp_ref, bc_ref, log_ref, keep_ref, gout_ref, cum_ref = refs[:7]
    parts = refs[7 : 7 + count]
    dvp_ref, dbc_ref, dlt_ref, gin_ref = refs[7 + count : 11 + count]
    outs = refs[11 + count : 11 + 2 * count]
    (
        logs, logt, inter, dinter, rowsum, turned, colsum, message, arrived, sems,
    ) = refs[11 + 2 * count : 21 + 2 * count]
    i = pl.program_id(0)
    blocks = pl.num_programs(0)
    near = lax.axis_size("ctx")
    pos = lax.axis_index("ctx")
    plan = []
    if count:
        held = refs[21 + 2 * count :]
        part = Scatter(parts[0], None, *held[:6], None, tuple(held[6:10]) + (None, None), held[10])
        acts = [part.begin, part.corners, part.sides_out, lambda: part.hand_on(outs[0])]
        plan = acting(MIXING_PLACES, acts)

    @pl.when(i == 0)
    def _():
        meet((box_peers() if count else []) + chain_peers())

    def hop(k):
        @pl.when(pos == near - 1 - k)
        def _():
            total = gout_ref[...].astype(F32)
            if k:
                pass_on(message, arrived, sems, -1).wait_recv()
                gin_ref[...] = arrived[...]
                total = total + jnp.exp2(cum_ref[blocks, 0:1, :]) * arrived[...].astype(F32)
            else:
                gin_ref[...] = jnp.zeros_like(gin_ref)
            if k < near - 1:
                message[...] = (keep_ref[0, 0] * total).astype(BF16)
                pass_on(message, arrived, sems, -1).start()

    hops = [(MIXING_HOPS[k], lambda k=k: hop(k)) for k in range(near)]

    logd = log_ref[...]
    spread(logd, logs)
    spread_rows(logd.T, logt)
    low_b = bc_ref[:, :N]
    low_c = bc_ref[:, N:]
    square = (Q, Q)
    causal = rows_of(square) <= lanes_of(square)
    inter[...] = jnp.where(causal, nt(low_b, low_c), 0.0)
    dinter[...] = jnp.zeros_like(dinter)
    half = lanes_of((Q, 128)) < P_SIZE
    lane = lanes_of((HALF, 128))

    def group(g, unused):
        when_at(i * GROUPS + g, plan)
        when_at(i * GROUPS + g, hops)
        lg = logs[g]
        first_col = jnp.zeros((HALF, 128), F32)
        second_col = jnp.zeros((HALF, 128), F32)
        for j in range(2):
            cols = pl.ds(pl.multiple_of(g * GW + 128 * j, 128), 128)
            vp = vp_ref[:, cols].astype(F32)
            ds = ds_ref[:, cols]
            wide = ds.astype(F32)
            first = []
            second = []
            outs = []
            for h in range(2):
                head = 2 * j + h
                own = half if h == 0 else jnp.logical_not(half)
                vm = jnp.where(own, vp, 0.0).astype(BF16)
                dsm = jnp.where(own, wide, 0.0).astype(BF16)
                outs.append(dsm)
                row = logt[g, head : head + 1]
                early, late = row[:, :HALF], row[:, HALF:]
                lb = head_lanes(lg, head)
                up, down = lb[:HALF], lb[HALF:]
                dup = nt(vm[:HALF], ds)
                ddown = nt(vm[HALF:], ds[HALF:])
                decay = jnp.exp2(jnp.minimum(early - up, 0.0))
                grad = dup[:, :HALF] * decay
                dinter[:HALF, :HALF] += grad
                part = inter[:HALF, :HALF]
                first.append((part * decay).astype(BF16))
                both = grad * part
                row_early = jnp.sum(both, axis=0, keepdims=True)
                col = both
                decay = jnp.exp2(jnp.minimum(late - up, 0.0))
                grad = dup[:, HALF:] * decay
                dinter[:HALF, HALF:] += grad
                part = inter[:HALF, HALF:]
                first.append((part * decay).astype(BF16))
                both = grad * part
                row_late = jnp.sum(both, axis=0, keepdims=True)
                col = jnp.sum(col + both, axis=1, keepdims=True)
                first_col = jnp.where(lane == head, col, first_col)
                decay = jnp.exp2(jnp.minimum(late - down, 0.0))
                grad = ddown * decay
                dinter[HALF:, HALF:] += grad
                part = inter[HALF:, HALF:]
                second.append((part * decay).astype(BF16))
                both = grad * part
                row_late = row_late + jnp.sum(both, axis=0, keepdims=True)
                col = jnp.sum(both, axis=1, keepdims=True)
                second_col = jnp.where(lane == head, col, second_col)
                rowsum[g, head : head + 1, :HALF] = row_early
                rowsum[g, head : head + 1, HALF:] = row_late
            dvp_ref[:HALF, cols] = nn(
                jnp.concatenate(first, 1), jnp.concatenate(outs, 0)
            ).astype(BF16)
            dvp_ref[HALF:, cols] = nn(
                jnp.concatenate(second, 1), jnp.concatenate([outs[0][HALF:], outs[1][HALF:]], 0)
            ).astype(BF16)
        colsum[g, :HALF] = first_col
        colsum[g, HALF:] = second_col
        return unused

    lax.fori_loop(0, GROUPS, group, 0)
    turned[...] = jnp.zeros_like(turned)
    for g in range(GROUPS):
        turned[4 * g : 4 * g + 4] = rowsum[g, 0:4]
    total = turned[...].T
    for g in range(GROUPS):
        total = total - (colsum[g] if g == 0 else pltpu.roll(colsum[g], 4 * g, 1))
    dlt_ref[...] = total
    masked = jnp.where(causal, dinter[...], 0.0)
    dbc_ref[:, :N] = nn(masked.astype(BF16), low_c)
    dbc_ref[:, N:] = nn(masked.T.astype(BF16), low_b)

    @pl.when(jnp.logical_and(i == blocks - 1, pos > 0))
    def _():
        pass_on(message, arrived, sems, -1).wait_send()


def back_kernel(count, *refs):
    (
        keep_ref, gin_ref, gnext_ref, entt_ref, cum_ref, vp_ref, val_ref, dvp_ref, ds_ref, conv_ref,
        u_ref, halo_ref, bc_ref, log_ref, step_ref, valid_ref, dlp_ref, dlt_ref, dbc_ref, dc_ref,
        cw_ref, sb_line, dl_line, skip_line,
    ) = refs[:24]
    parts = refs[24 : 24 + count]
    du_ref, last_ref, edge_ref, sums_ref, small_ref = refs[24 + count : 29 + count]
    outs = refs[29 + count : 29 + 2 * count]
    gin, picks, head, epad, dlw, dst, drow, sb_ref, dl_ref, skip_ref = refs[29 + 2 * count : 39 + 2 * count]
    plan = []
    if count:
        held = refs[39 + 2 * count :]
        full = Scatter(parts[1], outs[1], *held[:7], held[7:13], held[17])
        line = Scatter(None, outs[0], None, held[13], None, None, None, None, held[14], (None,) * 4 + tuple(held[15:17]))
        acts = [line.line, line.line_done]
        plan = acting(BACK_PLACES + LINE_PLACES, full.steps() + acts)
    i = pl.program_id(0)
    top = pl.num_programs(0)
    c = top - 1 - i

    @pl.when(i == 0)
    def _():
        if count:
            meet(box_peers()[:3] + line_peers())
            line.kept[0] = parts[0][...]
        gin[...] = gin_ref[...].astype(F32)
        fill_picks(picks)
        lay_heads(sb_ref, sb_line)
        lay_heads(dl_ref, dl_line)
        lay_out(skip_ref, skip_line, picks)
        head[...] = jnp.zeros_like(head)
        sums_ref[...] = jnp.zeros_like(sums_ref)
        small_ref[...] = jnp.zeros_like(small_ref)

    log_parts = in_parts(log_ref[...])
    step_parts = in_parts(step_ref[...])
    low_b = bc_ref[:, :N]
    dlw[...] = jnp.zeros_like(dlw)
    dst[...] = jnp.zeros_like(dst)
    drow[...] = jnp.zeros_like(drow)

    def conv_back(cols, dact):
        cv = conv_ref[:, cols].astype(F32)
        s = sigmoid(cv)
        dcv = dact * (s * (1.0 + cv * (1.0 - s)))
        after = head[:, cols]
        head[:, cols] = dcv[:8]
        x = u_ref[:, cols]
        sums_ref[4:5, cols] += jnp.sum(dcv, axis=0, keepdims=True)
        total = None
        for j in range(CONVK):
            k = CONVK - 1 - j
            moved = advanced(dcv, after, j)
            sums_ref[k : k + 1, cols] += jnp.sum(moved * x, axis=0, keepdims=True)
            term = cw_ref[k : k + 1, cols] * moved
            total = term if total is None else total + term
        du_ref[:, cols] = total.astype(BF16)

        @pl.when(i == 0)
        def _():
            last_ref[:, cols] = total[Q - 8 :]

    def group(g, db):
        when_at(i * GROUPS + g, plan)
        cols = pl.ds(pl.multiple_of(g * GW, GW), GW)
        log_wide = nn(log_parts, picks[:, cols])
        step_wide = nn(step_parts, picks[:, cols])
        done = cum_ref[c + 1, 0:1, cols]
        after = jnp.exp2(cum_ref[top, 0:1, cols] - done)
        grad = gnext_ref[0, :, cols].astype(F32) + after * gin[:, cols]
        low_g = grad.astype(BF16)
        decay = jnp.exp2(done - cum_ref[c, 0:1, cols])
        row = decay * jnp.sum(grad * entt_ref[0, :, cols].astype(F32), axis=0, keepdims=True)
        coarse = row.astype(BF16).astype(F32)
        r = rows_of((16, GW))
        two = jnp.where(r == 0, jnp.broadcast_to(coarse, (16, GW)), 0.0)
        two = jnp.where(r == 1, jnp.broadcast_to(row - coarse, (16, GW)), two)
        chosen = pick_heads(g)
        drow[...] += nn(two.astype(BF16), chosen)
        dweighted = nn(low_b, low_g)
        weights = []
        moves = []
        stepped = []
        dacts = []
        for j in range(2):
            pc = pl.ds(pl.multiple_of(g * GW + 128 * j, 128), 128)
            lp = log_wide[:, 128 * j : 128 * j + 128]
            sp = step_wide[:, 128 * j : 128 * j + 128]
            fade = jnp.exp2(lp[Q - 1 : Q, :] - lp)
            vp = vp_ref[:, pc].astype(F32)
            faded = dweighted[:, 128 * j : 128 * j + 128] * fade
            weights.append((vp * fade).astype(BF16))
            moves.append((faded * vp).astype(BF16))
            both = dvp_ref[:, pc].astype(F32) + faded
            stepped.append((both * val_ref[:, pc].astype(F32)).astype(BF16))
            dacts.append((pc, sp * both + skip_ref[:, pc] * ds_ref[:, pc].astype(F32)))
        dlw[...] += nn(jnp.concatenate(moves, 1), chosen)
        dst[...] += nn(jnp.concatenate(stepped, 1), chosen)
        for pc, dact in dacts:
            conv_back(pc, dact)
        return db + nt(jnp.concatenate(weights, 1), low_g)

    db = lax.fori_loop(0, GROUPS, group, dbc_ref[:, :N])
    conv_back(pl.ds(DI, N), db)
    conv_back(pl.ds(DI + N, N), dbc_ref[:, N:] + dc_ref[...])

    moved = dlw[...]
    at_last = jnp.sum(moved, axis=0, keepdims=True) + drow[0:1] + drow[1:2]
    dlog = dlp_ref[...] + dlt_ref[...] - moved
    dlog = dlog + jnp.where(rows_of(dlog.shape) == Q - 1, at_last, 0.0)
    square = (Q, Q)
    later = jnp.where(rows_of(square) <= lanes_of(square), 1.0, 0.0).astype(BF16)
    dsum = ordered_sum(later, dlog)
    rate = -jnp.exp(dl_ref[...])
    dstep = (dst[...] + dsum * rate) * valid_ref[...]
    raw = u_ref[:, CH:] + sb_ref[...]
    draw = dstep * (1.0 / (1.0 + jnp.exp(-raw)))
    draw = jnp.where(lanes_of(draw.shape) < HEADS, draw, 0.0)
    du_ref[:, CH:] = draw.astype(BF16)
    small_ref[0:1] += jnp.sum(draw, axis=0, keepdims=True)
    small_ref[1:2] += jnp.sum(dsum * step_ref[...], axis=0, keepdims=True) * rate

    @pl.when(c == 0)
    def _():
        epad[0:8, :] = jnp.zeros((8, CH), F32)
        epad[8:16, :] = head[...]
        x = halo_ref[:, :CH] * keep_ref[0, 0]
        total = jnp.zeros((8, CH), F32)
        for j in range(CONVK):
            k = CONVK - 1 - j
            moved = epad[j : j + 8, :]
            sums_ref[k : k + 1, :] += jnp.sum(moved * x, axis=0, keepdims=True)
            total = total + cw_ref[k : k + 1, :] * moved
        edge_ref[...] = total * keep_ref[0, 0]


def spec(block, index):
    return pl.BlockSpec(block, index)


def whole(shape):
    return pl.BlockSpec(shape, lambda *_: (0,) * len(shape))


def scalar():
    return pl.BlockSpec(memory_space=pltpu.SMEM)


def shaped(shape, kind):
    return jax.ShapeDtypeStruct(shape, kind)


def cost(flops, moved):
    return pl.CostEstimate(flops=int(flops), bytes_accessed=int(moved), transcendentals=0)


def params(number=None):
    return pltpu.CompilerParams(
        dimension_semantics=("arbitrary",), vmem_limit_bytes=60 * 1024 * 1024, collective_id=number,
        has_side_effects=number is not None,
    )


LINE = 4


def my_place():
    f = lax.axis_index("fsdp")
    t = lax.axis_index("ctx")
    return f // 2, f % 2, t // 2, t % 2


def device_at(z, y, x, core):
    return {"fsdp": z * 2 + y, "ctx": x * 2 + core}


def order_of(z, y, x, core):
    return (z * 2 + y) * 4 + x * 2 + core


def box_peers():
    z, y, x, core = my_place()
    return [
        (None, device_at(z, y, x, 1 - core)), (None, device_at(z, y, 1 - x, core)),
        (None, device_at(z, 1 - y, x, core)),
        (z > 0, device_at(z - 1, y, x, core)), (z < LINE - 1, device_at(z + 1, y, x, core)),
    ]


def plane_peers():
    z, y, x, core = my_place()
    turns = [(a, b, c) for a in range(2) for b in range(2) for c in range(2) if a + b + c]
    return [(None, device_at(z, (y + a) % 2, (x + b) % 2, (core + c) % 2)) for a, b, c in turns]


def line_peers():
    z, y, x, core = my_place()
    ups = [(z + r < LINE, device_at(z + r, y, x, core)) for r in range(1, LINE)]
    return ups + [(z - r >= 0, device_at(z - r, y, x, core)) for r in range(1, LINE)]


def meet(peers):
    barrier = pltpu.get_barrier_semaphore()
    count = 0
    for valid, peer in peers:

        def greet(peer=peer):
            pl.semaphore_signal(barrier, inc=1, device_id=peer, device_id_type=pl.DeviceIdType.MESH)

        if valid is None:
            greet()
            count = count + 1
        else:
            pl.when(valid)(greet)
            count = count + jnp.where(valid, 1, 0)
    pl.semaphore_wait(barrier, count)


def send(src, dst, send_sem, recv_sem, peer):
    return pltpu.make_async_remote_copy(
        src_ref=src, dst_ref=dst, send_sem=send_sem, recv_sem=recv_sem,
        device_id=device_at(*peer), device_id_type=pl.DeviceIdType.MESH,
    )


class Gather:
    def __init__(self, own, out, window, recv, halves, twin, sent, here):
        first, self.width, self.at = window
        self.own, self.out, self.rows = own.at[:, pl.ds(first, self.width)], out, own.shape[0]
        self.recv, self.halves, self.twin, self.sent, self.here = recv, halves, twin, sent, here
        self.place = my_place()

    def block(self, z, y, x, core, half=None):
        size = self.rows if half is None else self.rows // 2
        start = order_of(z, y, x, core) * self.rows + (0 if half is None else half * size)
        return self.out.at[pl.ds(pl.multiple_of(start, 16), size), pl.ds(self.at, self.width)]

    def copy(self, origin, way, half=None, own=False):
        z, y, x, core = self.place
        oz, oy, ox = origin
        o = oz * 4 + oy * 2 + ox
        dst = self.block(oz, oy, ox, core, half)
        src = self.own if own else dst
        peer = {
            "up": (z + 1, y, x, core), "down": (z - 1, y, x, core), "x": (z, y, 1 - x, core),
            "y": (z, 1 - y, x, core), "twin": (z, y, x, 1 - core),
        }[way]
        sem = self.sent.at[("up", "down", "x", "y", "twin").index(way), o]
        if way == "twin":
            arrival = self.twin.at[o]
        elif half is not None:
            arrival = self.halves.at[half, o]
        else:
            arrival = self.recv.at[o]
        return send(src, dst, sem, arrival, peer)

    def arrived(self, origin, half=None):
        self.copy(origin, "x", half).wait_recv()

    def column(self, r):
        z = self.place[0]
        if r == 0:
            return [(None, z, True, True)]
        return [(z - r >= 0, z - r, True, False), (z + r < LINE, z + r, False, True)]

    def each(self, r, act):
        for valid, oz, below, above in self.column(r):
            if valid is None:
                act(oz, below, above)
            else:
                pl.when(valid)(lambda oz=oz, below=below, above=above: act(oz, below, above))

    def begin(self):
        z, y, x, core = self.place
        pltpu.make_async_copy(self.own, self.block(z, y, x, core), self.here).start()
        self.forward(0)

    def ways(self, oz, below, above, act):
        z = self.place[0]
        if below:
            pl.when(z < LINE - 1)(lambda: act("up"))
        if above:
            pl.when(z > 0)(lambda: act("down"))
        act("x")
        act("y")
        act("twin")

    def forward(self, r):
        z, y, x, core = self.place

        def act(oz, below, above):
            origin = (oz, y, x)
            if r:
                self.arrived(origin)
            self.ways(oz, below, above, lambda way: self.copy(origin, way, own=r == 0).start())

        self.each(r, act)

    def across(self, r):
        z, y, x, core = self.place

        def act(oz, below, above):
            self.arrived((oz, y, 1 - x))
            self.copy((oz, y, 1 - x), "y", 0).start()
            self.copy((oz, y, 1 - x), "twin").start()
            self.arrived((oz, 1 - y, x))
            self.copy((oz, 1 - y, x), "x", 1).start()
            self.copy((oz, 1 - y, x), "twin").start()

        self.each(r, act)

    def corner(self, r):
        z, y, x, core = self.place

        def act(oz, below, above):
            origin = (oz, 1 - y, 1 - x)
            self.arrived(origin, 0)
            self.arrived(origin, 1)
            self.copy(origin, "twin").start()

        self.each(r, act)

    def finish(self):
        z, y, x, core = self.place
        pltpu.make_async_copy(self.own, self.block(z, y, x, core), self.here).wait()
        for r in range(LINE):

            def act(oz, below, above, r=r):
                self.ways(oz, below, above, lambda way: self.copy((oz, y, x), way, own=r == 0).wait_send())
                self.copy((oz, y, 1 - x), "y", 0).wait_send()
                self.copy((oz, 1 - y, x), "x", 1).wait_send()
                for oy, ox in ((y, 1 - x), (1 - y, x), (1 - y, 1 - x)):
                    self.copy((oz, oy, ox), "twin").wait_send()
                for oy, ox in ((y, x), (y, 1 - x), (1 - y, x), (1 - y, 1 - x)):
                    self.copy((oz, oy, ox), "twin").wait_recv()

            self.each(r, act)

    def steps(self):
        return [
            self.begin,
            lambda: self.forward(1),
            lambda: self.across(0),
            lambda: self.forward(2),
            lambda: self.across(1),
            lambda: (self.forward(3), self.corner(0)),
            lambda: self.across(2),
            lambda: self.corner(1),
            lambda: self.across(3),
            lambda: (self.corner(2), self.corner(3)),
            self.finish,
        ]


def gather_scratch():
    dma = pltpu.SemaphoreType.DMA
    return [dma((16,)), dma((2, 16)), dma((16,)), dma((5, 16)), dma(())]


U_WINDOWS = ((DI, 1280, 0), (DI + 1280, UW - 1280, 1280))


def gather_kernel(own, tok_ref, gain_ref, out, normed_ref, turned_ref, near_rows, sems, *gather_sems):
    rows, width = tok_ref.shape
    meet(box_peers() + chain_peers())
    pos = lax.axis_index("ctx")
    last = pos == lax.axis_size("ctx") - 1
    lists = [Gather(own, out, window, *gather_sems[5 * k : 5 * k + 5]).steps() for k, window in enumerate(U_WINDOWS)]
    for each in lists:
        each[0]()
    halo = pass_on(tok_ref.at[pl.ds(rows - HALO, HALO)], near_rows, sems, 1)

    @pl.when(jnp.logical_not(last))
    def _():
        halo.start()

    def normed(values):
        wide = values.astype(F32)
        scale = lax.rsqrt(jnp.sum(wide * wide, axis=1, keepdims=True) * (1.0 / width) + epsilon)
        return wide * scale * gain_ref[...]

    def block(r, unused):
        here = pl.ds(pl.multiple_of(r * 128, 128), 128)
        values = normed(tok_ref[here, :])
        normed_ref[here, :] = values.astype(BF16)
        turned_ref[:, here] = values.T.astype(BF16)
        return unused

    def hops(at):
        for k, each in enumerate(lists):
            if 1 <= at - k < len(each):
                each[at - k]()

    parts = 4
    for at in range(parts):
        lax.fori_loop(at * rows // 128 // parts, (at + 1) * rows // 128 // parts, block, 0)
        hops(at + 1)

    @pl.when(pos > 0)
    def _():
        halo.wait_recv()

    @pl.when(pos == 0)
    def _():
        near_rows[...] = jnp.zeros_like(near_rows)

    normed_ref[rows:, :] = normed(near_rows[...]).astype(BF16)

    @pl.when(jnp.logical_not(last))
    def _():
        halo.wait_send()

    for at in range(parts + 1, len(lists[0]) + len(lists) - 1):
        hops(at)


def gathered(own, tokens, gain, number):
    rows, width = tokens.shape
    anywhere = pl.BlockSpec(memory_space=pl.ANY)
    vmem = pl.BlockSpec(memory_space=pltpu.VMEM)
    return pl.pallas_call(
        gather_kernel,
        in_specs=[anywhere, vmem, vmem],
        out_specs=[anywhere, vmem, vmem],
        out_shape=[
            shaped((32 * own.shape[0], UW), BF16), shaped((rows + HALO, width), BF16), shaped((width, rows), BF16),
        ],
        scratch_shapes=[pltpu.VMEM((HALO, width), BF16), pltpu.SemaphoreType.DMA((2,))] + gather_scratch() * 2,
        compiler_params=pltpu.CompilerParams(
            collective_id=number, has_side_effects=True, vmem_limit_bytes=60 * 1024 * 1024
        ),
        name="gather",
    )(own, tokens, gain)


class Scatter:
    def __init__(self, parts, out, got, kept, mixed_y, mixed_x, from_x, from_y, along, sems, fetched=None):
        self.parts, self.out = parts, out
        self.got, self.kept = got, kept
        self.mixed = (mixed_y, mixed_x)
        self.sides = (from_x, from_y)
        self.along = along
        self.twin_sent, self.twin_recv, self.sent, self.recv, self.line_sent, self.line_recv = sems
        self.place = my_place()
        self.rows = kept.shape[-2]
        self.last = kept.shape[0] - 1
        self.fetched = fetched

    def groups(self):
        z, y, x, core = self.place
        return [(1 - y, 1 - x), (y, 1 - x), (1 - y, x), (y, x)]

    def to_twin(self, k):
        z, y, x, core = self.place
        gy, gx = self.groups()[k]
        return send(
            self.parts.at[:, gy * 4 + gx * 2 + 1 - core], self.got.at[k], self.twin_sent.at[k], self.twin_recv.at[k],
            (z, y, x, 1 - core),
        )

    def fetch(self, k):
        z, y, x, core = self.place
        gy, gx = self.groups()[k]
        return pltpu.make_async_copy(
            self.parts.at[:, gy * 4 + gx * 2 + core], self.kept.at[k], self.fetched.at[k]
        )

    def begin(self):
        for k in range(4):
            self.to_twin(k).start()
        if self.fetched is not None:
            for k in range(4):
                self.fetch(k).start()

    def add(self, k, sources, first=0, rows=None):
        rows = self.rows if rows is None else rows
        pieces = rows // 16

        def piece(n, unused):
            b = n // pieces
            at = (n - b * pieces) * 16
            here = pl.ds(pl.multiple_of(first + at, 16), 16)
            total = None
            for source in sources:
                term = source(b, pl.multiple_of(at, 16), here).astype(F32)
                total = term if total is None else total + term
            self.kept[k, b, here] = total.astype(BF16)
            return unused

        lax.fori_loop(0, LINE * pieces, piece, 0)

    def own(self, k):
        return lambda b, at, here: self.kept[k, b, here]

    def both(self, k):
        z, y, x, core = self.place
        gy, gx = self.groups()[k]
        self.to_twin(k).wait_recv()
        mine = lambda b, at, here: self.parts[b, gy * 4 + gx * 2 + core, here]
        if self.fetched is not None:
            self.fetch(k).wait()
            mine = self.own(k)
        self.add(k, [mine, lambda b, at, here: self.got[k, b, here]])

    def corner_copy(self, half):
        z, y, x, core = self.place
        size = self.rows // 2
        src = self.kept.at[0, :, pl.ds(half * size, size)]
        peer = (z, 1 - y, x, core) if half == 0 else (z, y, 1 - x, core)
        return send(src, self.mixed[half], self.sent.at[half], self.recv.at[half], peer)

    def side_copy(self, k):
        z, y, x, core = self.place
        peer = (z, y, 1 - x, core) if k == 1 else (z, 1 - y, x, core)
        return send(self.kept.at[k], self.sides[k - 1], self.sent.at[1 + k], self.recv.at[1 + k], peer)

    def corners(self):
        self.both(0)
        self.corner_copy(0).start()
        self.corner_copy(1).start()
        self.both(1)
        self.both(2)
        self.both(3)

    def sides_out(self):
        size = self.rows // 2
        for half, k in ((0, 1), (1, 2)):
            self.corner_copy(half).wait_recv()
            self.add(
                k, [self.own(k), lambda b, at, here, half=half: self.mixed[half][b, pl.ds(at, 16)]],
                half * size, size,
            )
            self.side_copy(k).start()

    def sides_in(self):
        self.side_copy(1).wait_recv()
        self.side_copy(2).wait_recv()
        self.add(
            3,
            [
                self.own(3), lambda b, at, here: self.sides[0][b, here], lambda b, at, here: self.sides[1][b, here],
            ],
        )

    def line_copy(self, origin, target):
        z, y, x, core = self.place
        return send(
            self.kept.at[self.last, target], self.along.at[origin], self.line_sent.at[target],
            self.line_recv.at[origin], (target, y, x, core),
        )

    def others(self, act):
        z = self.place[0]
        for r in range(1, LINE):
            pl.when(z + r < LINE)(lambda r=r: act(z + r))
            pl.when(z - r >= 0)(lambda r=r: act(z - r))

    def line(self):
        z = self.place[0]
        self.others(lambda target: self.line_copy(z, target).start())

    def plane_sent(self):
        for k in range(4):
            self.to_twin(k).wait_send()
        for half in range(2):
            self.corner_copy(half).wait_send()
        for k in (1, 2):
            self.side_copy(k).wait_send()

    def hand_on(self, out):
        self.sides_in()
        out[...] = self.kept[self.last]
        self.plane_sent()

    def line_done(self):
        z = self.place[0]
        self.out[...] = self.kept[self.last, z].astype(F32)

        def arrive(origin):
            self.line_copy(origin, z).wait_recv()
            self.out[...] += self.along[origin].astype(F32)

        self.others(arrive)
        self.others(lambda target: self.line_copy(z, target).wait_send())

    def finish(self):
        self.line_done()
        self.plane_sent()

    def steps(self):
        return [
            self.begin, self.corners, self.sides_out, lambda: (self.sides_in(), self.line()), self.finish,
        ]


def scatter_scratch(rows, columns):
    dma = pltpu.SemaphoreType.DMA
    half = rows // 2
    return [
        pltpu.VMEM((4, LINE, rows, columns), BF16),
        pltpu.VMEM((4, LINE, rows, columns), BF16),
        pltpu.VMEM((LINE, half, columns), BF16),
        pltpu.VMEM((LINE, half, columns), BF16),
        pltpu.VMEM((LINE, rows, columns), BF16),
        pltpu.VMEM((LINE, rows, columns), BF16),
        pltpu.VMEM((LINE, rows, columns), BF16),
        dma((4,)), dma((4,)), dma((4,)), dma((4,)), dma((LINE,)), dma((LINE,)),
    ]


class Quick:
    def __init__(self, own, out, plane, line, sems):
        self.own, self.out, self.plane, self.along = own, out, plane, line
        self.sent, self.recv, self.line_sent, self.line_recv = sems
        self.place = my_place()

    def peers(self):
        z, y, x, core = self.place
        turns = [(a, b, c) for a in range(2) for b in range(2) for c in range(2) if a + b + c]
        return [((y + a) % 2, (x + b) % 2, (core + c) % 2) for a, b, c in turns]

    def copy(self, origin, target):
        z = self.place[0]
        number = lambda where: where[0] * 4 + where[1] * 2 + where[2]
        return send(
            self.own, self.plane.at[number(origin)], self.sent.at[number(target)], self.recv.at[number(origin)],
            (z,) + tuple(target),
        )

    def begin(self):
        here = self.place[1:]
        self.plane[here[0] * 4 + here[1] * 2 + here[2]] = self.own[...]
        for peer in self.peers():
            self.copy(here, peer).start()

    def line_copy(self, origin, target):
        z, y, x, core = self.place
        return send(
            self.along.at[z], self.along.at[origin], self.line_sent.at[target], self.line_recv.at[origin],
            (target, y, x, core),
        )

    def others(self, act):
        z = self.place[0]
        for r in range(1, LINE):
            pl.when(z + r < LINE)(lambda r=r: act(z + r))
            pl.when(z - r >= 0)(lambda r=r: act(z - r))

    def turn(self):
        z, here = self.place[0], self.place[1:]
        for peer in self.peers():
            self.copy(peer, here).wait_recv()
        total = self.plane[0]
        for k in range(1, 8):
            total = total + self.plane[k]
        self.along[z] = total
        self.others(lambda target: self.line_copy(z, target).start())

    def finish(self):
        z, here = self.place[0], self.place[1:]
        self.others(lambda origin: self.line_copy(origin, z).wait_recv())
        total = self.along[0]
        for k in range(1, LINE):
            total = total + self.along[k]
        self.out[...] = total
        for peer in self.peers():
            self.copy(here, peer).wait_send()
        self.others(lambda target: self.line_copy(z, target).wait_send())


class Total:
    def __init__(self, own, out, held, got, sent, recv):
        self.own, self.out, self.held, self.got, self.sent, self.recv = own, out, held, got, sent, recv

    def copy(self, k):
        z, y, x, core = my_place()
        near = z + 1 - 2 * (z % 2)
        peer = [
            (z, y, x, 1 - core), (z, y, 1 - x, core), (z, 1 - y, x, core), (near, y, x, core),
            ((z + 2) % LINE, y, x, core),
        ][k]
        return send(self.own if k == 0 else self.held.at[k], self.got.at[k], self.sent.at[k], self.recv.at[k], peer)

    def begin(self):
        self.copy(0).start()

    def turn(self, k):
        self.copy(k).wait_recv()
        mine = self.own[...] if k == 0 else self.held[k]
        total = mine + self.got[k]
        if k < 4:
            self.held[k + 1] = total
            self.copy(k + 1).start()
        else:
            self.out[...] = total

    def finish(self):
        for k in range(5):
            self.copy(k).wait_send()

    def steps(self):
        return [self.begin] + [lambda k=k: self.turn(k) for k in range(5)] + [self.finish]


WIDE = 512
SPLIT = 1536


def patched(values, fixed, first):
    count = values.shape[0]
    end = values[count - 16 :].astype(F32)
    own = jnp.logical_and(rows_of(end.shape) >= 8, lanes_of(end.shape) + first < CH)
    chosen = jnp.where(own, fixed, end)
    return jnp.concatenate([values[: count - 16], chosen.astype(BF16)], 0)


def final_kernel(*refs):
    (
        turned_ref, du_cols, dz_ref, du_ref, tok_ref, gain_ref, wz_any, wu_any, gate_ref, conv_ref, gsum_ref,
        small_ref, last_ref, edge_ref,
    ) = refs[:14]
    grad_ref, inw_ref, sums_ref, norm_ref = refs[14:18]
    (
        wz, wu, sems, parts_a, parts_b, out_a, out_b, packed, normed_grad, held, got, sent, recv, gains,
        gains_plane, gains_line, gains_sent, gains_recv, gains_out, gains_in, fixed, edge_got, edge_sems, du_block,
    ) = refs[18:42]
    i = pl.program_id(0)
    steps = pl.num_programs(0) - tok_blocks(turned_ref)
    z, y, x, core = my_place()
    scr_a, scr_b = refs[42:55], refs[55:68]
    sum_a = Scatter(parts_a, out_a, *scr_a[:7], scr_a[7:])
    sum_b = Scatter(parts_b, out_b, *scr_b[:7], scr_b[7:])
    small = Total(packed, sums_ref, held, got, sent, recv)
    norm = Quick(gains, norm_ref, gains_plane, gains_line, (gains_sent, gains_recv, gains_out, gains_in))
    load_z = pltpu.make_async_copy(wz_any, wz, sems.at[0])
    load_u = pltpu.make_async_copy(wu_any, wu, sems.at[1])

    @pl.when(i == 0)
    def _():
        load_z.start()
        load_u.start()
        meet(plane_peers() + line_peers() + chain_peers())
        packed[...] = jnp.zeros_like(packed)
        packed[0:5, :] = conv_ref[0:5, :]
        packed[5:6, :DI] = gsum_ref[0:1, :]
        packed[5:6, DI : DI + 128] = small_ref[0:1, :]
        packed[5:6, DI + 128 :] = small_ref[1:2, :]
        packed[6:7, :DI] = gsum_ref[1:2, :]
        pos = lax.axis_index("ctx")
        back_edge = pass_on(edge_ref, edge_got, edge_sems, -1)

        @pl.when(pos > 0)
        def _():
            back_edge.start()

        gains[...] = jnp.zeros_like(gains)
        small.begin()
        inw_ref[:, :DI] = gate_ref[...]
        fixed[...] = jnp.zeros_like(fixed)
        fixed[8:16, :CH] = last_ref[...]

        @pl.when(pos < lax.axis_size("ctx") - 1)
        def _():
            back_edge.wait_recv()
            fixed[8:16, :CH] += edge_got[...]

        @pl.when(pos > 0)
        def _():
            back_edge.wait_send()

    first = [
        (4, lambda: small.turn(0)), (8, lambda: small.turn(1)), (12, lambda: (sum_a.begin(), small.turn(2))),
        (16, lambda: (sum_a.corners(), small.turn(3))),
    ]
    second = [
        (20, lambda: (sum_b.begin(), sum_a.sides_out())), (23, sum_b.corners), (25, lambda: small.turn(4)),
        (29, lambda: (sum_a.sides_in(), sum_a.line())), (30, sum_b.sides_out),
    ]

    @pl.when(i < steps)
    def _():
        when_at(4 * i, first)
        at = pl.ds(pl.multiple_of(i * WIDE, WIDE), WIDE)
        result = nn(turned_ref[...], patched(du_cols[...], fixed[:, at], i * WIDE)).astype(BF16)
        rows = parts_a.shape[2]

        def keep(parts, cols, width):
            for b in range(LINE):
                for q in range(8):
                    first = (b * 8 + q) * rows
                    parts[b, q, :, cols] = result[first : first + rows, :width]

        edge = SPLIT // WIDE

        @pl.when(i < edge)
        def _():
            keep(parts_a, pl.ds(pl.multiple_of(i * WIDE, WIDE), WIDE), WIDE)

        @pl.when(jnp.logical_and(i >= edge, i < steps - 1))
        def _():
            keep(parts_b, pl.ds(pl.multiple_of((i - edge) * WIDE, WIDE), WIDE), WIDE)

        @pl.when(i == steps - 1)
        def _():
            keep(parts_b, slice((steps - 1 - edge) * WIDE, UW - SPLIT), UW - SPLIT - (steps - 1 - edge) * WIDE)

    @pl.when(i == steps)
    def _():
        load_z.wait()
        load_u.wait()

    @pl.when(i >= steps)
    def _():
        width = tok_ref.shape[1]
        chunk = width // 4
        at_end = i == pl.num_programs(0) - 1
        du_block[:, :CH] = patched(du_ref[:, :CH], fixed[:, :CH], jnp.where(at_end, 0, CH))
        du_block[:, CH:] = du_ref[:, CH:]

        def part(n, unused):
            when_at(4 * i + n, second)
            feats = pl.ds(pl.multiple_of(n * chunk, chunk), chunk)
            normed_grad[:, feats] = nt(dz_ref[...], wz[feats, :]) + nt(du_block[...], wu[feats, :])
            return unused

        lax.fori_loop(0, 4, part, 0)
        values = tok_ref[...].astype(F32)
        scale = lax.rsqrt(jnp.sum(values * values, axis=1, keepdims=True) * (1.0 / width) + epsilon)
        hat = values * scale
        grad = normed_grad[...]
        gains[...] += jnp.sum(grad * hat, axis=0, keepdims=True)
        inner = grad * gain_ref[...]
        mean = jnp.sum(inner * hat, axis=1, keepdims=True) * (1.0 / width)
        grad_ref[...] = (scale * (inner - hat * mean)).astype(BF16)

    @pl.when(i == pl.num_programs(0) - 1)
    def _():
        norm.begin()
        sum_b.sides_in()
        sum_b.line()
        norm.turn()
        sum_a.finish()
        norm.finish()
        sum_b.finish()
        small.finish()
        inw_ref[:, DI : DI + SPLIT] = out_a[...]
        inw_ref[:, DI + SPLIT :] = out_b[:, : DPROJ - DI - SPLIT]


def tok_blocks(turned_ref):
    return turned_ref.shape[1] // Q


def final(turned, du, dz, tokens, gain, w_z, w_u, gate_columns, conv_sums, gate_sums, small, last, edge, number):
    width, rows = turned.shape
    steps = -(-UW // WIDE)
    blocks = rows // Q
    dma = pltpu.SemaphoreType.DMA
    own = width // 32
    anywhere = pl.BlockSpec(memory_space=pl.ANY)
    later = lambda i: (jnp.maximum(i - steps, 0), 0)
    sums = (8, CH)
    return pl.pallas_call(
        final_kernel,
        grid=(steps + blocks,),
        in_specs=[
            whole((width, rows)),
            spec((rows, WIDE), lambda i: (0, jnp.minimum(i, steps - 1))),
            spec((Q, DI), later),
            spec((Q, UW), later),
            spec((Q, width), later),
            whole((1, width)),
            anywhere,
            anywhere,
            whole((own, DI)),
            whole(sums),
            whole((8, DI)),
            whole((8, 128)),
            whole((8, CH)),
            whole((8, CH)),
        ],
        out_specs=[spec((Q, width), later), whole((own, DPROJ)), whole(sums), whole((1, width))],
        out_shape=[
            shaped((rows, width), BF16), shaped((own, DPROJ), F32), shaped(sums, F32), shaped((1, width), F32),
        ],
        scratch_shapes=[
            pltpu.VMEM((width, DI), BF16),
            pltpu.VMEM((width, UW), BF16),
            dma((2,)),
            pltpu.VMEM((LINE, 8, own, SPLIT), BF16),
            pltpu.VMEM((LINE, 8, own, UW - SPLIT), BF16),
            pltpu.VMEM((own, SPLIT), F32),
            pltpu.VMEM((own, UW - SPLIT), F32),
            pltpu.VMEM(sums, F32),
            pltpu.VMEM((Q, width), F32),
            pltpu.VMEM((5,) + sums, F32),
            pltpu.VMEM((5,) + sums, F32),
            dma((5,)),
            dma((5,)),
            pltpu.VMEM((1, width), F32),
            pltpu.VMEM((8, 1, width), F32),
            pltpu.VMEM((LINE, 1, width), F32),
            dma((8,)),
            dma((8,)),
            dma((LINE,)),
            dma((LINE,)),
            pltpu.VMEM((16, -(-UW // WIDE) * WIDE), F32),
            pltpu.VMEM((8, CH), F32),
            dma((2,)),
            pltpu.VMEM((Q, UW), BF16),
        ]
        + scatter_scratch(own, SPLIT)
        + scatter_scratch(own, UW - SPLIT),
        compiler_params=params(number),
        cost_estimate=cost(20e9, 60e6),
        name="final",
    )(turned, du, dz, du, tokens, gain, w_z, w_u, gate_columns, conv_sums, gate_sums, small, last, edge)


def close_kernel(
    part_ref, cot_ref, inw_in, outw_in, sums_ref, norm_in, back_in,
    grad_ref, inw_ref, outw_ref, norm_ref, taps_ref, shift_ref, bias_ref, decay_ref, skip_ref, gate_ref,
):
    grad_ref[...] = cot_ref[...].astype(F32) + part_ref[...].astype(F32)

    @pl.when(pl.program_id(0) == 0)
    def _():
        inw_ref[...] = inw_in[...]
        outw_ref[...] = outw_in[...]
        norm_ref[...] = norm_in[0]
        taps_ref[...] = sums_ref[:CONVK]
        shift_ref[...] = sums_ref[CONVK]
        bias_ref[...] = sums_ref[5, DI : DI + 128]
        decay_ref[...] = sums_ref[5, DI + 128 :]
        gate_ref[...] = sums_ref[5, :DI]
        lane = lanes_of((1, 128))
        total = jnp.zeros((1, 128), F32)
        for h in range(HEADS):
            here = jnp.sum(back_in[6:7, h * P_SIZE : (h + 1) * P_SIZE], axis=1, keepdims=True)
            total = jnp.where(lane == h, here, total)
        skip_ref[...] = total[0]


def close(part, cotangent, inw, outw, sums, norm):
    rows, width = part.shape
    at = lambda i: (i, 0)
    line = lambda n: pl.BlockSpec((n,), lambda i: (0,))
    return pl.pallas_call(
        close_kernel,
        grid=(rows // Q,),
        in_specs=[
            spec((Q, width), at), spec((Q, width), at), whole(inw.shape), whole(outw.shape), whole(sums.shape),
            whole(norm.shape), whole(sums.shape),
        ],
        out_specs=[
            spec((Q, width), at), whole(inw.shape), whole(outw.shape), line(width), whole((CONVK, CH)), line(CH),
            line(128), line(128), line(128), line(DI),
        ],
        out_shape=[
            shaped((rows, width), F32), shaped(inw.shape, F32), shaped(outw.shape, F32), shaped((width,), F32),
            shaped((CONVK, CH), F32), shaped((CH,), F32), shaped((128,), F32), shaped((128,), F32),
            shaped((128,), F32), shaped((DI,), F32),
        ],
        compiler_params=params(),
        name="close",
    )(part, cotangent, inw, outw, sums, norm, sums)


def local(
    tokens,
    valid_mask,
    stretch_start,
    cotangent,
    norm_gain,
    in_weight,
    conv_weight,
    conv_bias,
    step_bias,
    decay_log,
    skip_gain,
    gate_gain,
    out_weight,
):
    axes = ("fsdp", "ctx")
    rows, width = tokens.shape
    blocks = rows // Q
    near = lax.axis_size("ctx")
    boxed = lax.axis_size("fsdp") == 8 and near == 4
    if boxed:
        own = jnp.pad(in_weight, ((0, 0), (0, UW + DI - DPROJ)))
        w_u, normed_more, turned = gathered(own, tokens, norm_gain.reshape(1, width), 1)
        later = [own, out_weight]
        later_widths = [DI, width]
    else:
        own_u = jnp.pad(in_weight[:, DI:], ((0, 0), (0, UW - (DPROJ - DI))))
        w_u, w_z, w_o = [
            lax.all_gather(a, axes, axis=0, tiled=True) for a in (own_u, in_weight[:, :DI], out_weight)
        ]
        later = []
        later_widths = []
        halo_tokens = lax.ppermute(tokens[rows - HALO :], "ctx", [(k, k + 1) for k in range(near - 1)])
        wide = jnp.concatenate([tokens, halo_tokens], 0).astype(F32)
        scale = lax.rsqrt(jnp.mean(wide * wide, axis=-1, keepdims=True) + epsilon)
        normed_more = (wide * scale * norm_gain).astype(BF16)
    extra = len(later)
    anywhere = pl.BlockSpec(memory_space=pl.ANY)

    normed = normed_more[:rows]
    valid = jnp.broadcast_to(valid_mask.astype(F32)[:, None], (rows, 128))
    keep = (1.0 - stretch_start[0].astype(F32)).reshape(1, 1)
    taps = conv_weight

    same = lambda c: (c, 0)
    same3 = lambda c: (c, 0, 0)
    one = lambda i: (jnp.minimum(i, blocks - 1), 0)
    one3 = lambda i: (jnp.minimum(i, blocks - 1), 0, 0)
    two = lambda i: (jnp.maximum(i - blocks, 0), 0)
    val, vp, conv, bc, ssd, ent, logd, step, cum, start, u, ahead, *filled = pl.pallas_call(
        lambda *refs: forward_kernel(extra, *refs),
        grid=(2 * blocks,),
        in_specs=[
            spec((Q, width), one),
            spec((HALO, width), lambda c: (rows // HALO, 0)),
            anywhere,
            spec((Q, 128), one),
            scalar(),
            whole((CONVK, CH)),
            whole((CH,)),
            whole((HEADS,)),
            whole((HEADS,)),
            scalar(),
        ]
        + [anywhere] * extra,
        out_specs=[
            spec((Q, DI), one),
            spec((Q, DI), one),
            spec((Q, CH), one),
            spec((Q, 2 * N), one),
            spec((Q, DI), two),
            spec((1, N, DI), one3),
            spec((Q, 128), one),
            spec((Q, 128), one),
            whole((blocks + 1, 8, DI)),
            whole((N, DI)),
            spec((Q, UW), one),
            whole((8, UW)),
        ]
        + [anywhere] * extra,
        out_shape=[
            shaped((rows, DI), BF16),
            shaped((rows, DI), BF16),
            shaped((rows, CH), BF16),
            shaped((rows, 2 * N), BF16),
            shaped((rows, DI), BF16),
            shaped((blocks, N, DI), BF16),
            shaped((rows, 128), F32),
            shaped((rows, 128), F32),
            shaped((blocks + 1, 8, DI), F32),
            shaped((N, DI), BF16),
            shaped((rows, UW), F32),
            shaped((8, UW), F32),
        ]
        + [shaped((32 * a.shape[0], n), a.dtype) for a, n in zip(later, later_widths)],
        scratch_shapes=[
            pltpu.VMEM((8, CH), F32),
            pltpu.VMEM((GROUPS, Q, 128), F32),
            pltpu.VMEM((128, DI), BF16),
            pltpu.VMEM((GROUPS, 8, Q), F32),
            pltpu.VMEM((Q, Q), F32),
            pltpu.VMEM((N, DI), F32),
            pltpu.VMEM((blocks, Q, DI), BF16),
            pltpu.VMEM((blocks, Q, DI), BF16),
            pltpu.VMEM((blocks, Q, 2 * N), BF16),
            pltpu.VMEM((blocks, Q, 128), F32),
            pltpu.VMEM((N, DI), BF16),
            pltpu.VMEM((N, DI), BF16),
            pltpu.SemaphoreType.DMA((2,)),
            pltpu.VMEM((w_u.shape[0], UW), BF16),
            pltpu.SemaphoreType.DMA(()),
            pltpu.VMEM((2, Q, GW), F32),
            pltpu.VMEM((2, Q, GW), F32),
            pltpu.VMEM((1, CH), F32),
            pltpu.VMEM((1, 128), F32),
            pltpu.VMEM((1, 128), F32),
            pltpu.VMEM((1, DI), F32),
        ]
        + gather_scratch() * extra,
        compiler_params=params(2),
        cost_estimate=cost(15e9, 60e6),
        name="forward",
    )(normed_more, normed_more, w_u, valid, keep, taps, conv_bias, step_bias, decay_log, skip_gain, *later)
    if later:
        w_z, w_o = filled

    z = jnp.dot(normed, w_z, preferred_element_type=F32).astype(BF16)
    back = lambda i: (blocks - 1 - i, 0)
    back3 = lambda i: (blocks - 1 - i, 0, 0)
    output, gated, branch_grad, ds, dz, entt, gnext, gout, dlp, dc, gate_sums = pl.pallas_call(
        gate_kernel,
        grid=(blocks,),
        in_specs=[
            whole((N, DI)),
            spec((Q, DI), back),
            spec((1, N, DI), back3),
            spec((Q, DI), back),
            spec((Q, DI), back),
            spec((Q, 2 * N), back),
            spec((Q, 128), back),
            whole((blocks + 1, 8, DI)),
            spec((Q, width), back),
            spec((Q, width), back),
            spec((Q, 128), back),
            whole((DI, width)),
            whole((DI,)),
        ],
        out_specs=[
            spec((Q, width), back),
            spec((Q, DI), back),
            spec((Q, width), back),
            spec((Q, DI), back),
            spec((Q, DI), back),
            spec((1, N, DI), back3),
            spec((1, N, DI), back3),
            whole((N, DI)),
            spec((Q, 128), back),
            spec((Q, N), back),
            whole((8, DI)),
        ],
        out_shape=[
            shaped((rows, width), BF16),
            shaped((rows, DI), BF16),
            shaped((rows, width), BF16),
            shaped((rows, DI), BF16),
            shaped((rows, DI), BF16),
            shaped((blocks, N, DI), BF16),
            shaped((blocks, N, DI), BF16),
            shaped((N, DI), BF16),
            shaped((rows, 128), F32),
            shaped((rows, N), F32),
            shaped((8, DI), F32),
        ],
        scratch_shapes=[
            pltpu.VMEM((N, DI), F32),
            pltpu.VMEM((N, DI), F32),
            pltpu.VMEM((128, DI), BF16),
            pltpu.VMEM((Q, DI), F32),
            pltpu.VMEM((Q, DI), F32),
            pltpu.VMEM((Q, DI), F32),
            pltpu.VMEM((Q, DI), F32),
            pltpu.VMEM((Q, DI), F32),
            pltpu.VMEM((Q, 128), F32),
            pltpu.VMEM((1, DI), F32),
        ],
        compiler_params=params(),
        cost_estimate=cost(15e9, 60e6),
        name="gate",
    )(
        start, ssd, ent, z, val, bc, logd, cum, tokens, cotangent, valid, w_o, gate_gain,
    )

    def columns_of(left, right):
        return lax.dot_general(
            left, right, (((0,), (0,)), ((), ())), preferred_element_type=F32
        ).astype(BF16)

    def in_blocks(a):
        return a.reshape(LINE, 8, a.shape[0] // 32, a.shape[1])

    out_weight_grad = columns_of(gated, branch_grad)
    gate_columns = columns_of(normed, dz)
    mixing_parts = [in_blocks(out_weight_grad)] if boxed else []

    dvp, dbc, dlt, gin, *summed_out = pl.pallas_call(
        lambda *refs: mixing_kernel(len(mixing_parts), *refs),
        grid=(blocks,),
        in_specs=[
            spec((Q, DI), same),
            spec((Q, DI), same),
            spec((Q, 2 * N), same),
            spec((Q, 128), same),
            scalar(),
            whole((N, DI)),
            whole((blocks + 1, 8, DI)),
        ]
        + [anywhere for a in mixing_parts],
        out_specs=[spec((Q, DI), same), spec((Q, 2 * N), same), spec((Q, 128), same), whole((N, DI))]
        + [whole((LINE,) + a.shape[-2:]) for a in mixing_parts],
        out_shape=[
            shaped((rows, DI), BF16), shaped((rows, 2 * N), F32), shaped((rows, 128), F32), shaped((N, DI), BF16),
        ]
        + [shaped((LINE,) + a.shape[-2:], BF16) for a in mixing_parts],
        scratch_shapes=[
            pltpu.VMEM((GROUPS, Q, 128), F32),
            pltpu.VMEM((GROUPS, 8, Q), F32),
            pltpu.VMEM((Q, Q), F32),
            pltpu.VMEM((Q, Q), F32),
            pltpu.VMEM((GROUPS, 8, Q), F32),
            pltpu.VMEM((128, Q), F32),
            pltpu.VMEM((GROUPS, Q, 128), F32),
            pltpu.VMEM((N, DI), BF16),
            pltpu.VMEM((N, DI), BF16),
            pltpu.SemaphoreType.DMA((2,)),
        ]
        + [each for a in mixing_parts for each in plane_scratch(*a.shape[-2:])],
        compiler_params=params(3),
        cost_estimate=cost(15e9, 60e6),
        name="mixing",
    )(ds, vp, bc, logd, keep, gout, cum, *mixing_parts)

    back_parts = summed_out + [in_blocks(gate_columns)] if boxed else []
    du, last, edge, conv_sums, small, *summed_gate = pl.pallas_call(
        lambda *refs: back_kernel(len(back_parts), *refs),
        grid=(blocks,),
        in_specs=[
            scalar(),
            whole((N, DI)),
            spec((1, N, DI), back3),
            spec((1, N, DI), back3),
            whole((blocks + 1, 8, DI)),
            spec((Q, DI), back),
            spec((Q, DI), back),
            spec((Q, DI), back),
            spec((Q, DI), back),
            spec((Q, CH), back),
            spec((Q, UW), back),
            whole((8, UW)),
            spec((Q, 2 * N), back),
            spec((Q, 128), back),
            spec((Q, 128), back),
            spec((Q, 128), back),
            spec((Q, 128), back),
            spec((Q, 128), back),
            spec((Q, 2 * N), back),
            spec((Q, N), back),
            whole((CONVK, CH)),
            whole((HEADS,)),
            whole((HEADS,)),
            scalar(),
        ]
        + [pl.BlockSpec(memory_space=pltpu.VMEM), anywhere][: len(back_parts)],
        out_specs=[
            spec((Q, UW), back),
            whole((8, CH)),
            whole((8, CH)),
            whole((8, CH)),
            whole((8, 128)),
        ]
        + [whole(a.shape[-2:]) for a in back_parts],
        out_shape=[
            shaped((rows, UW), BF16),
            shaped((8, CH), F32),
            shaped((8, CH), F32),
            shaped((8, CH), F32),
            shaped((8, 128), F32),
        ]
        + [shaped(a.shape[-2:], F32) for a in back_parts],
        scratch_shapes=[
            pltpu.VMEM((N, DI), F32),
            pltpu.VMEM((128, DI), BF16),
            pltpu.VMEM((8, CH), F32),
            pltpu.VMEM((16, CH), F32),
            pltpu.VMEM((Q, 128), F32),
            pltpu.VMEM((Q, 128), F32),
            pltpu.VMEM((16, 128), F32),
            pltpu.VMEM((1, 128), F32),
            pltpu.VMEM((1, 128), F32),
            pltpu.VMEM((1, DI), F32),
        ]
        + (
            scatter_scratch(*back_parts[1].shape[-2:])
            + line_scratch(*back_parts[0].shape[-2:])
            + [pltpu.SemaphoreType.DMA((4,))]
            if back_parts
            else []
        ),
        compiler_params=params(4 if back_parts else None),
        cost_estimate=cost(15e9, 60e6),
        name="back",
    )(
        keep, gin, gnext, entt, cum, vp, val, dvp, ds, conv, u, ahead, bc, logd, step, valid,
        dlp, dlt, dbc, dc, taps, step_bias, decay_log, skip_gain, *back_parts,
    )
    if boxed:
        out_weight_grad, gate_columns = summed_gate
        part, in_weight_grad, sums, norm_sum = final(
            turned, du, dz, tokens, norm_gain.reshape(1, width), w_z, w_u, gate_columns, conv_sums,
            gate_sums, small, last, edge, 5,
        )
        results = close(part, cotangent, in_weight_grad, out_weight_grad, sums, norm_sum)
        input_grad, in_weight_grad, out_weight_grad, norm_sum, taps_sum, shift_sum = results[:6]
        bias_sum, decay_sum, skip_sum, gate_sum = results[6:]
        return (
            output,
            input_grad,
            in_weight_grad,
            out_weight_grad,
            norm_sum,
            taps_sum,
            shift_sum,
            bias_sum[:HEADS],
            decay_sum[:HEADS],
            skip_sum[:HEADS],
            gate_sum,
        )
    edge_back = lax.ppermute(edge, "ctx", [(k + 1, k) for k in range(near - 1)])
    du = lax.dynamic_update_slice(du, (last + edge_back).astype(BF16), (rows - 8, 0))
    conv_columns = columns_of(normed, du)
    across = (((1,), (1,)), ((), ()))
    normed_grad = lax.dot_general(dz, w_z, across, preferred_element_type=F32) + lax.dot_general(
        du, w_u, across, preferred_element_type=F32
    )
    inputs = tokens.astype(F32)
    scale = lax.rsqrt(jnp.mean(inputs * inputs, axis=-1, keepdims=True) + epsilon)
    hat = inputs * scale
    inner = normed_grad * norm_gain
    input_grad = cotangent.astype(F32) + scale * (
        inner - hat * jnp.mean(inner * hat, axis=-1, keepdims=True)
    )
    norm_grad = jnp.sum(normed_grad * hat, axis=0)
    packed = jnp.concatenate(
        [
            norm_grad,
            conv_sums[:5].reshape(-1),
            gate_sums[:2].reshape(-1),
            small[:2].reshape(-1),
        ]
    )
    conv_columns, gate_columns, out_weight_grad = [
        lax.psum_scatter(a.astype(F32), axes, scatter_dimension=0, tiled=True)
        for a in (conv_columns, gate_columns, out_weight_grad)
    ]
    summed = lax.psum(packed, axes)
    in_weight_grad = jnp.concatenate([gate_columns, conv_columns[:, : DPROJ - DI]], 1)
    at = width
    conv_weight_grad = summed[at : at + CONVK * CH].reshape(CONVK, CH)
    at += CONVK * CH
    conv_bias_grad = summed[at : at + CH]
    at += CH
    gate_gain_grad = summed[at : at + DI]
    at += DI
    skip_gain_grad = jnp.sum(summed[at : at + DI].reshape(HEADS, P_SIZE), axis=1)
    at += DI
    step_bias_grad = summed[at : at + HEADS]
    decay_log_grad = summed[at + 128 : at + 128 + HEADS]
    return (
        output,
        input_grad,
        in_weight_grad,
        out_weight_grad,
        summed[:width],
        conv_weight_grad,
        conv_bias_grad,
        step_bias_grad,
        decay_log_grad,
        skip_gain_grad,
        gate_gain_grad,
    )


def solution(mesh):
    split = P(("fsdp", "ctx"), None)
    line = P(("fsdp", "ctx"))
    return jax.shard_map(
        local,
        mesh=mesh,
        in_specs=(split, line, line, split, P(), split, P(), P(), P(), P(), P(), P(), split),
        out_specs=(split, split, split, split, P(), P(), P(), P(), P(), P(), P()),
        check_vma=False,
    )
```

```python
import jax
import jax.numpy as jnp
from jax import lax
from jax.experimental import pallas as pl
from jax.experimental.pallas import tpu as pltpu
from jax.sharding import PartitionSpec as P

DI = 2048
HEADS = 32
P_SIZE = 64
N = 128
CONVK = 4
Q = 256
CH = 2304
DPROJ = 4384
UW = CH + 128
GW = 256
GROUPS = DI // GW
HALF = Q // 2
HALO = 16

F32 = jnp.float32
BF16 = jnp.bfloat16
LOG2E = 1.4426950408889634
epsilon = 1e-05


def nn(a, b):
    return lax.dot_general(a, b, (((1,), (0,)), ((), ())), preferred_element_type=F32)


def nt(a, b):
    return lax.dot_general(a, b, (((1,), (1,)), ((), ())), preferred_element_type=F32)


def sigmoid(x):
    return 0.5 * jnp.tanh(0.5 * x) + 0.5


def softplus(x):
    e = jnp.exp(-jnp.abs(x))
    w = 1.0 + e
    d = w - 1.0
    return jnp.maximum(x, 0.0) + jnp.where(d == 0.0, e, jnp.log(w) * (e / jnp.where(d == 0.0, 1.0, d)))


def rows_of(shape):
    return lax.broadcasted_iota(jnp.int32, shape, 0)


def lanes_of(shape):
    return lax.broadcasted_iota(jnp.int32, shape, 1)


def split3(x):
    a = x.astype(BF16)
    r = x - a.astype(F32)
    b = r.astype(BF16)
    return a, b, (r - b.astype(F32)).astype(BF16)


def ordered_sum(triangle, x):
    a, b, c = split3(x)
    return nn(triangle, c) + nn(triangle, b) + nn(triangle, a)


def spread(x, out):
    out[0] = x
    for g in range(1, GROUPS):
        out[g] = pltpu.roll(x, 128 - 4 * g, 1)


def delayed(before, x, by):
    if by == 0:
        return x
    return pltpu.roll(jnp.concatenate([before, x], 0), by, 0)[8:]


def advanced(x, after, by):
    if by == 0:
        return x
    count = x.shape[0]
    return pltpu.roll(jnp.concatenate([x, after], 0), count + 8 - by, 0)[:count]


def fill_picks(out):
    for g in range(GROUPS):
        shape = (128, GW)
        head = lax.shift_right_logical(lanes_of(shape), 6) + 4 * g
        at = rows_of(shape)
        own = jnp.logical_and(jnp.bitwise_and(at, HEADS - 1) == head, at < 3 * HEADS)
        out[:, g * GW : (g + 1) * GW] = jnp.where(own, 1.0, 0.0).astype(BF16)


def in_parts(x):
    lane = lanes_of(x.shape)
    a, b, c = split3(jnp.where(lane < HEADS, x, 0.0))
    wide = a.astype(F32) + pltpu.roll(b.astype(F32), HEADS, 1) + pltpu.roll(c.astype(F32), 2 * HEADS, 1)
    return wide.astype(BF16)


def spread_rows(x, out):
    for g in range(GROUPS):
        out[g, 0:4] = x[4 * g : 4 * g + 4]


def head_lanes(x, i):
    return jnp.broadcast_to(x[:, i : i + 1], (x.shape[0], 128))


def pick_heads(g):
    shape = (GW, 128)
    return jnp.where(
        lax.shift_right_logical(rows_of(shape), 6) + 4 * g == lanes_of(shape), 1.0, 0.0
    ).astype(BF16)


def when_at(now, plan):
    plan = sorted(plan, key=lambda entry: entry[0])
    if len(plan) == 1:
        place, act = plan[0]

        @pl.when(now == place)
        def _():
            act()

    elif plan:
        middle = len(plan) // 2

        def early():
            when_at(now, plan[:middle])

        def late():
            when_at(now, plan[middle:])

        lax.cond(now < plan[middle][0], early, late)


def chain_peers():
    pos = lax.axis_index("ctx")
    return [(pos > 0, {"ctx": pos - 1}), (pos < lax.axis_size("ctx") - 1, {"ctx": pos + 1})]


def pass_on(message, arrived, sems, by):
    return pltpu.make_async_remote_copy(
        src_ref=message, dst_ref=arrived, send_sem=sems.at[0], recv_sem=sems.at[1],
        device_id={"ctx": lax.axis_index("ctx") + by}, device_id_type=pl.DeviceIdType.MESH,
    )


def lay_heads(out, line):
    out[...] = jnp.zeros_like(out)
    out[0, :HEADS] = line[...]


def lay_out(out, line, picks):
    shape = (8, 128)
    heads = jnp.zeros((1, 128), F32)
    for h in range(HEADS):
        heads = jnp.where(lanes_of((1, 128)) == h, line[h], heads)
    out[...] = nn(in_parts(jnp.broadcast_to(heads, shape)), picks[...])[0:1]


def forward_kernel(count, *refs):
    (
        normed_ref, halo_ref, wu_any, valid_ref, keep_ref, cw_ref, cb_line, sb_line, dl_line, skip_line,
    ) = refs[:10]
    own = refs[10 : 10 + count]
    (
        val_ref, vp_ref, conv_ref, bc_ref, ssd_ref, ent_ref, log_ref, step_ref, cum_ref, start_ref, u_ref, ahead_ref,
    ) = refs[10 + count : 22 + count]
    outs = refs[22 + count : 22 + 2 * count]
    (
        past, logs, picks, logt, inter, state, all_vp, all_val, all_bc, all_log, message, arrived, sems, wu, load, log_wide, step_wide, cb_ref, sb_ref, dl_ref, skip_ref,
    ) = refs[22 + 2 * count : 43 + 2 * count]
    gather_sems = refs[43 + 2 * count :]
    i = pl.program_id(0)
    blocks = pl.num_programs(0) // 2
    first = i < blocks
    c = jnp.where(first, i, i - blocks)
    near = lax.axis_size("ctx")
    pos = lax.axis_index("ctx")
    plan = []
    if count:
        lists = [Gather(own[k], outs[k], (0, outs[k].shape[1], 0), *gather_sems[5 * k : 5 * k + 5]).steps() for k in range(count)]
        length = len(lists[0])
        for at in range(length + 2 * (count - 1)):
            acts = [lists[k][at - 2 * k] for k in range(count) if 0 <= at - 2 * k < length]
            plan.append((FORWARD_PLACES[at], lambda acts=acts: [act() for act in acts]))

    @pl.when(i == 0)
    def _():
        fetch = pltpu.make_async_copy(wu_any, wu, load)
        fetch.start()
        fill_picks(picks)
        cb_ref[0] = cb_line[...]
        lay_heads(sb_ref, sb_line)
        lay_heads(dl_ref, dl_line)
        lay_out(skip_ref, skip_line, picks)
        meet((box_peers() if count else []) + chain_peers())
        fetch.wait()
        before = nn(halo_ref[...], wu[...])[8:]
        ahead_ref[...] = before
        past[...] = before[:, :CH] * keep_ref[0, 0]
        state[...] = jnp.zeros_like(state)
        cum_ref[...] = jnp.zeros_like(cum_ref)

    half = lanes_of((Q, 128)) < P_SIZE
    square = (Q, Q)
    causal = rows_of(square) >= lanes_of(square)

    @pl.when(first)
    def _():
        tail = nn(normed_ref[...], wu[:, DI:])
        u_ref[:, DI:] = tail
        raw = tail[:, 2 * N :] + sb_ref[...]
        step = softplus(raw) * valid_ref[...]
        step = jnp.where(lanes_of(step.shape) < HEADS, step, 0.0)
        rate = -jnp.exp(dl_ref[...]) * LOG2E
        logd = ordered_sum(jnp.where(causal, 1.0, 0.0).astype(BF16), step * rate)
        log_ref[...] = logd
        all_log[c] = logd
        step_ref[...] = step
        log_parts = in_parts(logd)
        step_parts = in_parts(step)

        def convolved(cols, x):
            before = past[:, cols]
            past[:, cols] = x[Q - 8 :]
            total = cb_ref[:, cols] + cw_ref[CONVK - 1 : CONVK, cols] * x
            for k in range(CONVK - 1):
                total = total + cw_ref[k : k + 1, cols] * delayed(before, x, CONVK - 1 - k)
            return total

        conv_b = convolved(pl.ds(DI, N), tail[:, :N])
        conv_c = convolved(pl.ds(DI + N, N), tail[:, N : 2 * N])
        conv_ref[:, DI : DI + N] = conv_b.astype(BF16)
        conv_ref[:, DI + N :] = conv_c.astype(BF16)
        act_b = conv_b * sigmoid(conv_b)
        act_c = conv_c * sigmoid(conv_c)
        both = jnp.concatenate([act_b.astype(BF16), act_c.astype(BF16)], 1)
        bc_ref[...] = both
        all_bc[c] = both
        turned_b = act_b.T.astype(BF16)
        ent_ref[0] = state[...].astype(BF16)

        def ahead(g):
            cols = pl.ds(pl.multiple_of(g * GW, GW), GW)
            slot = g % 2
            u_ref[:, cols] = nn(normed_ref[...], wu[:, cols])
            log_wide[slot] = nn(log_parts, picks[:, cols])
            step_wide[slot] = nn(step_parts, picks[:, cols])

        ahead(0)

        def group(g, unused):
            when_at(i * GROUPS + g, plan)
            slot = g % 2
            for j in range(2):
                cols = pl.ds(pl.multiple_of(g * GW + 128 * j, 128), 128)
                cv = convolved(cols, u_ref[:, cols])
                conv_ref[:, cols] = cv.astype(BF16)
                val = cv * sigmoid(cv)
                low = val.astype(BF16)
                val_ref[:, cols] = low
                all_val[c, :, cols] = low
                lp = log_wide[slot, :, 128 * j : 128 * j + 128]
                vp = val * step_wide[slot, :, 128 * j : 128 * j + 128]
                low = vp.astype(BF16)
                vp_ref[:, cols] = low
                all_vp[c, :, cols] = low
                last = lp[Q - 1 : Q, :]
                weighted = (vp * jnp.exp2(last - lp)).astype(BF16)
                state[:, cols] = jnp.exp2(last) * state[:, cols] + nn(turned_b, weighted)
                cum_ref[c + 1, :, cols] = cum_ref[c, :, cols] + last
            ahead(lax.rem(g + 1, GROUPS))
            return unused

        lax.fori_loop(0, GROUPS, group, 0)

    def hop(k):
        @pl.when(pos == k)
        def _():
            if k:
                pass_on(message, arrived, sems, 1).wait_recv()
                entering = keep_ref[0, 0] * arrived[...].astype(F32)
                start_ref[...] = entering.astype(BF16)
            else:
                start_ref[...] = jnp.zeros_like(start_ref)
            if k < near - 1:
                if k:
                    message[...] = (jnp.exp2(cum_ref[blocks, 0:1, :]) * entering + state[...]).astype(BF16)
                else:
                    message[...] = state[...].astype(BF16)
                pass_on(message, arrived, sems, 1).start()

    hops = [(blocks * GROUPS + FORWARD_HOPS[k], lambda k=k: hop(k)) for k in range(near)]

    @pl.when(jnp.logical_not(first))
    def _():
        logd = all_log[c]
        spread(logd, logs)
        spread_rows(logd.T, logt)
        inter[...] = jnp.where(causal, nt(all_bc[c, :, N:], all_bc[c, :, :N]), 0.0)
        left = jnp.where(half[:1], 1.0, 0.0).astype(BF16)
        right = jnp.where(half[:1], 0.0, 1.0).astype(BF16)

        def group(g, unused):
            when_at(i * GROUPS + g, plan)
            when_at(i * GROUPS + g, hops)
            lg = logs[g]
            for j in range(2):
                cols = pl.ds(pl.multiple_of(g * GW + 128 * j, 128), 128)
                vp = all_vp[c, :, cols]
                v0 = vp * left
                v1 = vp * right
                top = []
                low = []
                for h in range(2):
                    row = logt[g, 2 * j + h : 2 * j + h + 1]
                    early, late = row[:, :HALF], row[:, HALF:]
                    lb = head_lanes(lg, 2 * j + h)
                    up, down = lb[:HALF], lb[HALF:]
                    top.append((inter[:HALF, :HALF] * jnp.exp2(jnp.minimum(up - early, 0.0))).astype(BF16))
                    low.append((inter[HALF:, :HALF] * jnp.exp2(jnp.minimum(down - early, 0.0))).astype(BF16))
                    low.append((inter[HALF:, HALF:] * jnp.exp2(jnp.minimum(down - late, 0.0))).astype(BF16))
                skipped = skip_ref[:, cols] * all_val[c, :, cols].astype(F32)
                above = nn(jnp.concatenate(top, 1), jnp.concatenate([v0[:HALF], v1[:HALF]], 0))
                below = nn(jnp.concatenate(low, 1), jnp.concatenate([v0, v1], 0))
                ssd_ref[:HALF, cols] = (above + skipped[:HALF]).astype(BF16)
                ssd_ref[HALF:, cols] = (below + skipped[HALF:]).astype(BF16)
            return unused

        lax.fori_loop(0, GROUPS, group, 0)

    @pl.when(jnp.logical_and(i == 2 * blocks - 1, pos < near - 1))
    def _():
        pass_on(message, arrived, sems, 1).wait_send()


def gate_kernel(
    start_ref, ssd_in, ent_ref, z_ref, val_ref, bc_ref, log_ref, cum_ref,
    tok_ref, cot_ref, valid_ref, ow_any, gain_line,
    out_ref, gated_ref, bg_ref, ds_ref, dz_ref, entt_ref, gnext_ref, gout_ref, dlp_ref, dc_ref, sums_ref,
    start, gstate, picks, ssd_s, mix_s, el_s, pe_s, gg_s, acc, gain_ref, ow_ref, load,
):
    i = pl.program_id(0)
    c = pl.num_programs(0) - 1 - i

    @pl.when(i == 0)
    def _():
        pltpu.make_async_copy(ow_any, ow_ref, load).start()
        start[...] = start_ref[...].astype(F32)
        fill_picks(picks)
        gain_ref[0] = gain_line[...]
        gstate[...] = jnp.zeros_like(gstate)
        sums_ref[...] = jnp.zeros_like(sums_ref)

    log_parts = in_parts(log_ref[...])
    low_c = bc_ref[:, N:]
    turned_c = low_c.astype(F32).T.astype(BF16)
    acc[...] = jnp.zeros_like(acc)

    def enter(g, unused):
        cols = pl.ds(pl.multiple_of(g * GW, GW), GW)
        decay = jnp.exp2(nn(log_parts, picks[:, cols]))
        entering = (
            ent_ref[0, :, cols].astype(F32) + jnp.exp2(cum_ref[c, 0:1, cols]) * start[:, cols]
        ).astype(BF16)
        entt_ref[0, :, cols] = entering
        part = nn(low_c, entering)
        for j in range(2):
            pc = pl.ds(pl.multiple_of(g * GW + 128 * j, 128), 128)
            el = decay[:, 128 * j : 128 * j + 128]
            pe = el * part[:, 128 * j : 128 * j + 128]
            el_s[:, pc] = el
            pe_s[:, pc] = pe
            ssd = ssd_in[:, pc].astype(F32) + pe
            z = z_ref[:, pc].astype(F32)
            mixed = ssd * (z * sigmoid(z))
            ssd_s[:, pc] = ssd
            mix_s[:, pc] = mixed
            acc[...] += mixed * mixed
        return unused

    lax.fori_loop(0, GROUPS, enter, 0)

    @pl.when(i == 0)
    def _():
        pltpu.make_async_copy(ow_any, ow_ref, load).wait()

    inv = lax.rsqrt(jnp.sum(acc[...], axis=1, keepdims=True) * (1.0 / DI) + epsilon)
    inv = jnp.broadcast_to(inv, (Q, 128))
    valid = valid_ref[...]
    valid8 = jnp.concatenate([valid] * (tok_ref.shape[1] // 128), 1)
    branch_grad = (cot_ref[...].astype(F32) * valid8).astype(BF16)
    bg_ref[...] = branch_grad
    acc[...] = jnp.zeros_like(acc)

    def gate(g, unused):
        cols = pl.ds(pl.multiple_of(g * GW, GW), GW)
        ggrad = nt(branch_grad, ow_ref[cols, :])
        for j in range(2):
            pc = pl.ds(pl.multiple_of(g * GW + 128 * j, 128), 128)
            hat = mix_s[:, pc] * inv
            gain = gain_ref[:, pc]
            mix_s[:, pc] = hat
            gated_ref[:, pc] = (hat * gain).astype(BF16)
            gg = ggrad[:, 128 * j : 128 * j + 128]
            both = gg * hat
            sums_ref[0:1, pc] += jnp.sum(both, axis=0, keepdims=True)
            acc[...] += both * gain
            gg_s[:, pc] = gg * gain
        return unused

    lax.fori_loop(0, GROUPS, gate, 0)
    mean = jnp.sum(acc[...], axis=1, keepdims=True) * (1.0 / DI)
    mean = jnp.broadcast_to(mean, (Q, 128))

    for n in range(tok_ref.shape[1] // 256):
        cols = slice(256 * n, 256 * n + 256)
        branch = nn(gated_ref[...], ow_ref[:, cols])
        out_ref[:, cols] = (tok_ref[:, cols].astype(F32) + valid8[:, :256] * branch).astype(BF16)

    acc[...] = jnp.zeros_like(acc)
    dc_ref[...] = jnp.zeros_like(dc_ref)

    def back(g, unused):
        cols = pl.ds(pl.multiple_of(g * GW, GW), GW)
        dparts = []
        prods = []
        for j in range(2):
            pc = pl.ds(pl.multiple_of(g * GW + 128 * j, 128), 128)
            dmixed = inv * (gg_s[:, pc] - mix_s[:, pc] * mean)
            z = z_ref[:, pc].astype(F32)
            s = sigmoid(z)
            ds = (dmixed * (z * s)).astype(BF16)
            ds_ref[:, pc] = ds
            dz_ref[:, pc] = (dmixed * ssd_s[:, pc] * (s * (1.0 + z * (1.0 - s)))).astype(BF16)
            ds = ds.astype(F32)
            sums_ref[1:2, pc] += jnp.sum(ds * val_ref[:, pc].astype(F32), axis=0, keepdims=True)
            dparts.append((ds * el_s[:, pc]).astype(BF16))
            prods.append((ds * pe_s[:, pc]).astype(BF16))
        dpart = jnp.concatenate(dparts, 1)
        acc[...] += nn(jnp.concatenate(prods, 1), pick_heads(g))
        dc_ref[...] += nt(dpart, entt_ref[0, :, cols])
        gnext_ref[0, :, cols] = gstate[:, cols].astype(BF16)
        total = cum_ref[c + 1, 0:1, cols] - cum_ref[c, 0:1, cols]
        gstate[:, cols] = nn(turned_c, dpart) + jnp.exp2(total) * gstate[:, cols]
        return unused

    lax.fori_loop(0, GROUPS, back, 0)
    dlp_ref[...] = acc[...]

    @pl.when(c == 0)
    def _():
        gout_ref[...] = gstate[...].astype(BF16)


FORWARD_PLACES = tuple(5 * k for k in range(13))
FORWARD_HOPS = (0, 8, 20, 30)
MIXING_HOPS = (0, 8, 20, 30)
MIXING_PLACES = (0, 5, 12, 31)
LINE_PLACES = (1, 12)
BACK_PLACES = (0, 4, 9, 20, 31)


def acting(places, acts):
    joined = {}
    for place, act in zip(places, acts):
        joined.setdefault(place, []).append(act)
    return [(place, lambda acts=acts: [act() for act in acts]) for place, acts in joined.items()]


def plane_scratch(rows, columns):
    dma = pltpu.SemaphoreType.DMA
    return scatter_scratch(rows, columns)[:6] + [dma((4,))] * 5


def line_scratch(rows, columns):
    dma = pltpu.SemaphoreType.DMA
    return [
        pltpu.VMEM((1, LINE, rows, columns), BF16), pltpu.VMEM((LINE, rows, columns), BF16), dma((LINE,)), dma((LINE,)),
    ]


def mixing_kernel(count, *refs):
    ds_ref, vp_ref, bc_ref, log_ref, keep_ref, gout_ref, cum_ref = refs[:7]
    parts = refs[7 : 7 + count]
    dvp_ref, dbc_ref, dlt_ref, gin_ref = refs[7 + count : 11 + count]
    outs = refs[11 + count : 11 + 2 * count]
    (
        logs, logt, inter, dinter, rowsum, turned, colsum, message, arrived, sems,
    ) = refs[11 + 2 * count : 21 + 2 * count]
    i = pl.program_id(0)
    blocks = pl.num_programs(0)
    near = lax.axis_size("ctx")
    pos = lax.axis_index("ctx")
    plan = []
    if count:
        held = refs[21 + 2 * count :]
        part = Scatter(parts[0], None, *held[:6], None, tuple(held[6:10]) + (None, None), held[10])
        acts = [part.begin, part.corners, part.sides_out, lambda: part.hand_on(outs[0])]
        plan = acting(MIXING_PLACES, acts)

    @pl.when(i == 0)
    def _():
        meet((box_peers() if count else []) + chain_peers())

    def hop(k):
        @pl.when(pos == near - 1 - k)
        def _():
            total = gout_ref[...].astype(F32)
            if k:
                pass_on(message, arrived, sems, -1).wait_recv()
                gin_ref[...] = arrived[...]
                total = total + jnp.exp2(cum_ref[blocks, 0:1, :]) * arrived[...].astype(F32)
            else:
                gin_ref[...] = jnp.zeros_like(gin_ref)
            if k < near - 1:
                message[...] = (keep_ref[0, 0] * total).astype(BF16)
                pass_on(message, arrived, sems, -1).start()

    hops = [(MIXING_HOPS[k], lambda k=k: hop(k)) for k in range(near)]

    logd = log_ref[...]
    spread(logd, logs)
    spread_rows(logd.T, logt)
    low_b = bc_ref[:, :N]
    low_c = bc_ref[:, N:]
    square = (Q, Q)
    causal = rows_of(square) <= lanes_of(square)
    inter[...] = jnp.where(causal, nt(low_b, low_c), 0.0)
    dinter[...] = jnp.zeros_like(dinter)
    half = lanes_of((Q, 128)) < P_SIZE
    lane = lanes_of((HALF, 128))

    def group(g, unused):
        when_at(i * GROUPS + g, plan)
        when_at(i * GROUPS + g, hops)
        lg = logs[g]
        first_col = jnp.zeros((HALF, 128), F32)
        second_col = jnp.zeros((HALF, 128), F32)
        for j in range(2):
            cols = pl.ds(pl.multiple_of(g * GW + 128 * j, 128), 128)
            vp = vp_ref[:, cols].astype(F32)
            ds = ds_ref[:, cols]
            wide = ds.astype(F32)
            first = []
            second = []
            outs = []
            for h in range(2):
                head = 2 * j + h
                own = half if h == 0 else jnp.logical_not(half)
                vm = jnp.where(own, vp, 0.0).astype(BF16)
                dsm = jnp.where(own, wide, 0.0).astype(BF16)
                outs.append(dsm)
                row = logt[g, head : head + 1]
                early, late = row[:, :HALF], row[:, HALF:]
                lb = head_lanes(lg, head)
                up, down = lb[:HALF], lb[HALF:]
                dup = nt(vm[:HALF], ds)
                ddown = nt(vm[HALF:], ds[HALF:])
                decay = jnp.exp2(jnp.minimum(early - up, 0.0))
                grad = dup[:, :HALF] * decay
                dinter[:HALF, :HALF] += grad
                part = inter[:HALF, :HALF]
                first.append((part * decay).astype(BF16))
                both = grad * part
                row_early = jnp.sum(both, axis=0, keepdims=True)
                col = both
                decay = jnp.exp2(jnp.minimum(late - up, 0.0))
                grad = dup[:, HALF:] * decay
                dinter[:HALF, HALF:] += grad
                part = inter[:HALF, HALF:]
                first.append((part * decay).astype(BF16))
                both = grad * part
                row_late = jnp.sum(both, axis=0, keepdims=True)
                col = jnp.sum(col + both, axis=1, keepdims=True)
                first_col = jnp.where(lane == head, col, first_col)
                decay = jnp.exp2(jnp.minimum(late - down, 0.0))
                grad = ddown * decay
                dinter[HALF:, HALF:] += grad
                part = inter[HALF:, HALF:]
                second.append((part * decay).astype(BF16))
                both = grad * part
                row_late = row_late + jnp.sum(both, axis=0, keepdims=True)
                col = jnp.sum(both, axis=1, keepdims=True)
                second_col = jnp.where(lane == head, col, second_col)
                rowsum[g, head : head + 1, :HALF] = row_early
                rowsum[g, head : head + 1, HALF:] = row_late
            dvp_ref[:HALF, cols] = nn(
                jnp.concatenate(first, 1), jnp.concatenate(outs, 0)
            ).astype(BF16)
            dvp_ref[HALF:, cols] = nn(
                jnp.concatenate(second, 1), jnp.concatenate([outs[0][HALF:], outs[1][HALF:]], 0)
            ).astype(BF16)
        colsum[g, :HALF] = first_col
        colsum[g, HALF:] = second_col
        return unused

    lax.fori_loop(0, GROUPS, group, 0)
    turned[...] = jnp.zeros_like(turned)
    for g in range(GROUPS):
        turned[4 * g : 4 * g + 4] = rowsum[g, 0:4]
    total = turned[...].T
    for g in range(GROUPS):
        total = total - (colsum[g] if g == 0 else pltpu.roll(colsum[g], 4 * g, 1))
    dlt_ref[...] = total
    masked = jnp.where(causal, dinter[...], 0.0)
    dbc_ref[:, :N] = nn(masked.astype(BF16), low_c)
    dbc_ref[:, N:] = nn(masked.T.astype(BF16), low_b)

    @pl.when(jnp.logical_and(i == blocks - 1, pos > 0))
    def _():
        pass_on(message, arrived, sems, -1).wait_send()


def back_kernel(count, *refs):
    (
        keep_ref, gin_ref, gnext_ref, entt_ref, cum_ref, vp_ref, val_ref, dvp_ref, ds_ref, conv_ref,
        u_ref, halo_ref, bc_ref, log_ref, step_ref, valid_ref, dlp_ref, dlt_ref, dbc_ref, dc_ref,
        cw_ref, sb_line, dl_line, skip_line,
    ) = refs[:24]
    parts = refs[24 : 24 + count]
    du_ref, last_ref, edge_ref, sums_ref, small_ref = refs[24 + count : 29 + count]
    outs = refs[29 + count : 29 + 2 * count]
    gin, picks, head, epad, dlw, dst, drow, sb_ref, dl_ref, skip_ref = refs[29 + 2 * count : 39 + 2 * count]
    plan = []
    if count:
        held = refs[39 + 2 * count :]
        full = Scatter(parts[1], outs[1], *held[:7], held[7:13], held[17])
        line = Scatter(None, outs[0], None, held[13], None, None, None, None, held[14], (None,) * 4 + tuple(held[15:17]))
        acts = [line.line, line.line_done]
        plan = acting(BACK_PLACES + LINE_PLACES, full.steps() + acts)
    i = pl.program_id(0)
    top = pl.num_programs(0)
    c = top - 1 - i

    @pl.when(i == 0)
    def _():
        if count:
            meet(box_peers()[:3] + line_peers())
            line.kept[0] = parts[0][...]
        gin[...] = gin_ref[...].astype(F32)
        fill_picks(picks)
        lay_heads(sb_ref, sb_line)
        lay_heads(dl_ref, dl_line)
        lay_out(skip_ref, skip_line, picks)
        head[...] = jnp.zeros_like(head)
        sums_ref[...] = jnp.zeros_like(sums_ref)
        small_ref[...] = jnp.zeros_like(small_ref)

    log_parts = in_parts(log_ref[...])
    step_parts = in_parts(step_ref[...])
    low_b = bc_ref[:, :N]
    dlw[...] = jnp.zeros_like(dlw)
    dst[...] = jnp.zeros_like(dst)
    drow[...] = jnp.zeros_like(drow)

    def conv_back(cols, dact):
        cv = conv_ref[:, cols].astype(F32)
        s = sigmoid(cv)
        dcv = dact * (s * (1.0 + cv * (1.0 - s)))
        after = head[:, cols]
        head[:, cols] = dcv[:8]
        x = u_ref[:, cols]
        sums_ref[4:5, cols] += jnp.sum(dcv, axis=0, keepdims=True)
        total = None
        for j in range(CONVK):
            k = CONVK - 1 - j
            moved = advanced(dcv, after, j)
            sums_ref[k : k + 1, cols] += jnp.sum(moved * x, axis=0, keepdims=True)
            term = cw_ref[k : k + 1, cols] * moved
            total = term if total is None else total + term
        du_ref[:, cols] = total.astype(BF16)

        @pl.when(i == 0)
        def _():
            last_ref[:, cols] = total[Q - 8 :]

    def group(g, db):
        when_at(i * GROUPS + g, plan)
        cols = pl.ds(pl.multiple_of(g * GW, GW), GW)
        log_wide = nn(log_parts, picks[:, cols])
        step_wide = nn(step_parts, picks[:, cols])
        done = cum_ref[c + 1, 0:1, cols]
        after = jnp.exp2(cum_ref[top, 0:1, cols] - done)
        grad = gnext_ref[0, :, cols].astype(F32) + after * gin[:, cols]
        low_g = grad.astype(BF16)
        decay = jnp.exp2(done - cum_ref[c, 0:1, cols])
        row = decay * jnp.sum(grad * entt_ref[0, :, cols].astype(F32), axis=0, keepdims=True)
        coarse = row.astype(BF16).astype(F32)
        r = rows_of((16, GW))
        two = jnp.where(r == 0, jnp.broadcast_to(coarse, (16, GW)), 0.0)
        two = jnp.where(r == 1, jnp.broadcast_to(row - coarse, (16, GW)), two)
        chosen = pick_heads(g)
        drow[...] += nn(two.astype(BF16), chosen)
        dweighted = nn(low_b, low_g)
        weights = []
        moves = []
        stepped = []
        dacts = []
        for j in range(2):
            pc = pl.ds(pl.multiple_of(g * GW + 128 * j, 128), 128)
            lp = log_wide[:, 128 * j : 128 * j + 128]
            sp = step_wide[:, 128 * j : 128 * j + 128]
            fade = jnp.exp2(lp[Q - 1 : Q, :] - lp)
            vp = vp_ref[:, pc].astype(F32)
            faded = dweighted[:, 128 * j : 128 * j + 128] * fade
            weights.append((vp * fade).astype(BF16))
            moves.append((faded * vp).astype(BF16))
            both = dvp_ref[:, pc].astype(F32) + faded
            stepped.append((both * val_ref[:, pc].astype(F32)).astype(BF16))
            dacts.append((pc, sp * both + skip_ref[:, pc] * ds_ref[:, pc].astype(F32)))
        dlw[...] += nn(jnp.concatenate(moves, 1), chosen)
        dst[...] += nn(jnp.concatenate(stepped, 1), chosen)
        for pc, dact in dacts:
            conv_back(pc, dact)
        return db + nt(jnp.concatenate(weights, 1), low_g)

    db = lax.fori_loop(0, GROUPS, group, dbc_ref[:, :N])
    conv_back(pl.ds(DI, N), db)
    conv_back(pl.ds(DI + N, N), dbc_ref[:, N:] + dc_ref[...])

    moved = dlw[...]
    at_last = jnp.sum(moved, axis=0, keepdims=True) + drow[0:1] + drow[1:2]
    dlog = dlp_ref[...] + dlt_ref[...] - moved
    dlog = dlog + jnp.where(rows_of(dlog.shape) == Q - 1, at_last, 0.0)
    square = (Q, Q)
    later = jnp.where(rows_of(square) <= lanes_of(square), 1.0, 0.0).astype(BF16)
    dsum = ordered_sum(later, dlog)
    rate = -jnp.exp(dl_ref[...])
    dstep = (dst[...] + dsum * rate) * valid_ref[...]
    raw = u_ref[:, CH:] + sb_ref[...]
    draw = dstep * (1.0 / (1.0 + jnp.exp(-raw)))
    draw = jnp.where(lanes_of(draw.shape) < HEADS, draw, 0.0)
    du_ref[:, CH:] = draw.astype(BF16)
    small_ref[0:1] += jnp.sum(draw, axis=0, keepdims=True)
    small_ref[1:2] += jnp.sum(dsum * step_ref[...], axis=0, keepdims=True) * rate

    @pl.when(c == 0)
    def _():
        epad[0:8, :] = jnp.zeros((8, CH), F32)
        epad[8:16, :] = head[...]
        x = halo_ref[:, :CH] * keep_ref[0, 0]
        total = jnp.zeros((8, CH), F32)
        for j in range(CONVK):
            k = CONVK - 1 - j
            moved = epad[j : j + 8, :]
            sums_ref[k : k + 1, :] += jnp.sum(moved * x, axis=0, keepdims=True)
            total = total + cw_ref[k : k + 1, :] * moved
        edge_ref[...] = total * keep_ref[0, 0]


def spec(block, index):
    return pl.BlockSpec(block, index)


def whole(shape):
    return pl.BlockSpec(shape, lambda *_: (0,) * len(shape))


def scalar():
    return pl.BlockSpec(memory_space=pltpu.SMEM)


def shaped(shape, kind):
    return jax.ShapeDtypeStruct(shape, kind)


def cost(flops, moved):
    return pl.CostEstimate(flops=int(flops), bytes_accessed=int(moved), transcendentals=0)


def params(number=None):
    return pltpu.CompilerParams(
        dimension_semantics=("arbitrary",), vmem_limit_bytes=60 * 1024 * 1024, collective_id=number,
        has_side_effects=number is not None,
    )


LINE = 4


def my_place():
    f = lax.axis_index("fsdp")
    t = lax.axis_index("ctx")
    return f // 2, f % 2, t // 2, t % 2


def device_at(z, y, x, core):
    return {"fsdp": z * 2 + y, "ctx": x * 2 + core}


def order_of(z, y, x, core):
    return (z * 2 + y) * 4 + x * 2 + core


def box_peers():
    z, y, x, core = my_place()
    return [
        (None, device_at(z, y, x, 1 - core)), (None, device_at(z, y, 1 - x, core)),
        (None, device_at(z, 1 - y, x, core)),
        (z > 0, device_at(z - 1, y, x, core)), (z < LINE - 1, device_at(z + 1, y, x, core)),
    ]


def plane_peers():
    z, y, x, core = my_place()
    turns = [(a, b, c) for a in range(2) for b in range(2) for c in range(2) if a + b + c]
    return [(None, device_at(z, (y + a) % 2, (x + b) % 2, (core + c) % 2)) for a, b, c in turns]


def line_peers():
    z, y, x, core = my_place()
    ups = [(z + r < LINE, device_at(z + r, y, x, core)) for r in range(1, LINE)]
    return ups + [(z - r >= 0, device_at(z - r, y, x, core)) for r in range(1, LINE)]


def meet(peers):
    barrier = pltpu.get_barrier_semaphore()
    count = 0
    for valid, peer in peers:

        def greet(peer=peer):
            pl.semaphore_signal(barrier, inc=1, device_id=peer, device_id_type=pl.DeviceIdType.MESH)

        if valid is None:
            greet()
            count = count + 1
        else:
            pl.when(valid)(greet)
            count = count + jnp.where(valid, 1, 0)
    pl.semaphore_wait(barrier, count)


def send(src, dst, send_sem, recv_sem, peer):
    return pltpu.make_async_remote_copy(
        src_ref=src, dst_ref=dst, send_sem=send_sem, recv_sem=recv_sem,
        device_id=device_at(*peer), device_id_type=pl.DeviceIdType.MESH,
    )


class Gather:
    def __init__(self, own, out, window, recv, halves, twin, sent, here):
        first, self.width, self.at = window
        self.own, self.out, self.rows = own.at[:, pl.ds(first, self.width)], out, own.shape[0]
        self.recv, self.halves, self.twin, self.sent, self.here = recv, halves, twin, sent, here
        self.place = my_place()

    def block(self, z, y, x, core, half=None):
        size = self.rows if half is None else self.rows // 2
        start = order_of(z, y, x, core) * self.rows + (0 if half is None else half * size)
        return self.out.at[pl.ds(pl.multiple_of(start, 16), size), pl.ds(self.at, self.width)]

    def copy(self, origin, way, half=None, own=False):
        z, y, x, core = self.place
        oz, oy, ox = origin
        o = oz * 4 + oy * 2 + ox
        dst = self.block(oz, oy, ox, core, half)
        src = self.own if own else dst
        peer = {
            "up": (z + 1, y, x, core), "down": (z - 1, y, x, core), "x": (z, y, 1 - x, core),
            "y": (z, 1 - y, x, core), "twin": (z, y, x, 1 - core),
        }[way]
        sem = self.sent.at[("up", "down", "x", "y", "twin").index(way), o]
        if way == "twin":
            arrival = self.twin.at[o]
        elif half is not None:
            arrival = self.halves.at[half, o]
        else:
            arrival = self.recv.at[o]
        return send(src, dst, sem, arrival, peer)

    def arrived(self, origin, half=None):
        self.copy(origin, "x", half).wait_recv()

    def column(self, r):
        z = self.place[0]
        if r == 0:
            return [(None, z, True, True)]
        return [(z - r >= 0, z - r, True, False), (z + r < LINE, z + r, False, True)]

    def each(self, r, act):
        for valid, oz, below, above in self.column(r):
            if valid is None:
                act(oz, below, above)
            else:
                pl.when(valid)(lambda oz=oz, below=below, above=above: act(oz, below, above))

    def begin(self):
        z, y, x, core = self.place
        pltpu.make_async_copy(self.own, self.block(z, y, x, core), self.here).start()
        self.forward(0)

    def ways(self, oz, below, above, act):
        z = self.place[0]
        if below:
            pl.when(z < LINE - 1)(lambda: act("up"))
        if above:
            pl.when(z > 0)(lambda: act("down"))
        act("x")
        act("y")
        act("twin")

    def forward(self, r):
        z, y, x, core = self.place

        def act(oz, below, above):
            origin = (oz, y, x)
            if r:
                self.arrived(origin)
            self.ways(oz, below, above, lambda way: self.copy(origin, way, own=r == 0).start())

        self.each(r, act)

    def across(self, r):
        z, y, x, core = self.place

        def act(oz, below, above):
            self.arrived((oz, y, 1 - x))
            self.copy((oz, y, 1 - x), "y", 0).start()
            self.copy((oz, y, 1 - x), "twin").start()
            self.arrived((oz, 1 - y, x))
            self.copy((oz, 1 - y, x), "x", 1).start()
            self.copy((oz, 1 - y, x), "twin").start()

        self.each(r, act)

    def corner(self, r):
        z, y, x, core = self.place

        def act(oz, below, above):
            origin = (oz, 1 - y, 1 - x)
            self.arrived(origin, 0)
            self.arrived(origin, 1)
            self.copy(origin, "twin").start()

        self.each(r, act)

    def finish(self):
        z, y, x, core = self.place
        pltpu.make_async_copy(self.own, self.block(z, y, x, core), self.here).wait()
        for r in range(LINE):

            def act(oz, below, above, r=r):
                self.ways(oz, below, above, lambda way: self.copy((oz, y, x), way, own=r == 0).wait_send())
                self.copy((oz, y, 1 - x), "y", 0).wait_send()
                self.copy((oz, 1 - y, x), "x", 1).wait_send()
                for oy, ox in ((y, 1 - x), (1 - y, x), (1 - y, 1 - x)):
                    self.copy((oz, oy, ox), "twin").wait_send()
                for oy, ox in ((y, x), (y, 1 - x), (1 - y, x), (1 - y, 1 - x)):
                    self.copy((oz, oy, ox), "twin").wait_recv()

            self.each(r, act)

    def steps(self):
        return [
            self.begin,
            lambda: self.forward(1),
            lambda: self.across(0),
            lambda: self.forward(2),
            lambda: self.across(1),
            lambda: (self.forward(3), self.corner(0)),
            lambda: self.across(2),
            lambda: self.corner(1),
            lambda: self.across(3),
            lambda: (self.corner(2), self.corner(3)),
            self.finish,
        ]


def gather_scratch():
    dma = pltpu.SemaphoreType.DMA
    return [dma((16,)), dma((2, 16)), dma((16,)), dma((5, 16)), dma(())]


U_WINDOWS = ((DI, 1280, 0), (DI + 1280, UW - 1280, 1280))


def gather_kernel(own, tok_ref, gain_ref, out, normed_ref, turned_ref, near_rows, sems, *gather_sems):
    rows, width = tok_ref.shape
    meet(box_peers() + chain_peers())
    pos = lax.axis_index("ctx")
    last = pos == lax.axis_size("ctx") - 1
    lists = [Gather(own, out, window, *gather_sems[5 * k : 5 * k + 5]).steps() for k, window in enumerate(U_WINDOWS)]
    for each in lists:
        each[0]()
    halo = pass_on(tok_ref.at[pl.ds(rows - HALO, HALO)], near_rows, sems, 1)

    @pl.when(jnp.logical_not(last))
    def _():
        halo.start()

    def normed(values):
        wide = values.astype(F32)
        scale = lax.rsqrt(jnp.sum(wide * wide, axis=1, keepdims=True) * (1.0 / width) + epsilon)
        return wide * scale * gain_ref[...]

    def block(r, unused):
        here = pl.ds(pl.multiple_of(r * 128, 128), 128)
        values = normed(tok_ref[here, :])
        normed_ref[here, :] = values.astype(BF16)
        turned_ref[:, here] = values.T.astype(BF16)
        return unused

    def hops(at):
        for k, each in enumerate(lists):
            if 1 <= at - k < len(each):
                each[at - k]()

    parts = 4
    for at in range(parts):
        lax.fori_loop(at * rows // 128 // parts, (at + 1) * rows // 128 // parts, block, 0)
        hops(at + 1)

    @pl.when(pos > 0)
    def _():
        halo.wait_recv()

    @pl.when(pos == 0)
    def _():
        near_rows[...] = jnp.zeros_like(near_rows)

    normed_ref[rows:, :] = normed(near_rows[...]).astype(BF16)

    @pl.when(jnp.logical_not(last))
    def _():
        halo.wait_send()

    for at in range(parts + 1, len(lists[0]) + len(lists) - 1):
        hops(at)


def gathered(own, tokens, gain, number):
    rows, width = tokens.shape
    anywhere = pl.BlockSpec(memory_space=pl.ANY)
    vmem = pl.BlockSpec(memory_space=pltpu.VMEM)
    return pl.pallas_call(
        gather_kernel,
        in_specs=[anywhere, vmem, vmem],
        out_specs=[anywhere, vmem, vmem],
        out_shape=[
            shaped((32 * own.shape[0], UW), BF16), shaped((rows + HALO, width), BF16), shaped((width, rows), BF16),
        ],
        scratch_shapes=[pltpu.VMEM((HALO, width), BF16), pltpu.SemaphoreType.DMA((2,))] + gather_scratch() * 2,
        compiler_params=pltpu.CompilerParams(
            collective_id=number, has_side_effects=True, vmem_limit_bytes=60 * 1024 * 1024
        ),
        name="gather",
    )(own, tokens, gain)


class Scatter:
    def __init__(self, parts, out, got, kept, mixed_y, mixed_x, from_x, from_y, along, sems, fetched=None):
        self.parts, self.out = parts, out
        self.got, self.kept = got, kept
        self.mixed = (mixed_y, mixed_x)
        self.sides = (from_x, from_y)
        self.along = along
        self.twin_sent, self.twin_recv, self.sent, self.recv, self.line_sent, self.line_recv = sems
        self.place = my_place()
        self.rows = kept.shape[-2]
        self.last = kept.shape[0] - 1
        self.fetched = fetched

    def groups(self):
        z, y, x, core = self.place
        return [(1 - y, 1 - x), (y, 1 - x), (1 - y, x), (y, x)]

    def to_twin(self, k):
        z, y, x, core = self.place
        gy, gx = self.groups()[k]
        return send(
            self.parts.at[:, gy * 4 + gx * 2 + 1 - core], self.got.at[k], self.twin_sent.at[k], self.twin_recv.at[k],
            (z, y, x, 1 - core),
        )

    def fetch(self, k):
        z, y, x, core = self.place
        gy, gx = self.groups()[k]
        return pltpu.make_async_copy(
            self.parts.at[:, gy * 4 + gx * 2 + core], self.kept.at[k], self.fetched.at[k]
        )

    def begin(self):
        for k in range(4):
            self.to_twin(k).start()
        if self.fetched is not None:
            for k in range(4):
                self.fetch(k).start()

    def add(self, k, sources, first=0, rows=None):
        rows = self.rows if rows is None else rows
        pieces = rows // 16

        def piece(n, unused):
            b = n // pieces
            at = (n - b * pieces) * 16
            here = pl.ds(pl.multiple_of(first + at, 16), 16)
            total = None
            for source in sources:
                term = source(b, pl.multiple_of(at, 16), here).astype(F32)
                total = term if total is None else total + term
            self.kept[k, b, here] = total.astype(BF16)
            return unused

        lax.fori_loop(0, LINE * pieces, piece, 0)

    def own(self, k):
        return lambda b, at, here: self.kept[k, b, here]

    def both(self, k):
        z, y, x, core = self.place
        gy, gx = self.groups()[k]
        self.to_twin(k).wait_recv()
        mine = lambda b, at, here: self.parts[b, gy * 4 + gx * 2 + core, here]
        if self.fetched is not None:
            self.fetch(k).wait()
            mine = self.own(k)
        self.add(k, [mine, lambda b, at, here: self.got[k, b, here]])

    def corner_copy(self, half):
        z, y, x, core = self.place
        size = self.rows // 2
        src = self.kept.at[0, :, pl.ds(half * size, size)]
        peer = (z, 1 - y, x, core) if half == 0 else (z, y, 1 - x, core)
        return send(src, self.mixed[half], self.sent.at[half], self.recv.at[half], peer)

    def side_copy(self, k):
        z, y, x, core = self.place
        peer = (z, y, 1 - x, core) if k == 1 else (z, 1 - y, x, core)
        return send(self.kept.at[k], self.sides[k - 1], self.sent.at[1 + k], self.recv.at[1 + k], peer)

    def corners(self):
        self.both(0)
        self.corner_copy(0).start()
        self.corner_copy(1).start()
        self.both(1)
        self.both(2)
        self.both(3)

    def sides_out(self):
        size = self.rows // 2
        for half, k in ((0, 1), (1, 2)):
            self.corner_copy(half).wait_recv()
            self.add(
                k, [self.own(k), lambda b, at, here, half=half: self.mixed[half][b, pl.ds(at, 16)]],
                half * size, size,
            )
            self.side_copy(k).start()

    def sides_in(self):
        self.side_copy(1).wait_recv()
        self.side_copy(2).wait_recv()
        self.add(
            3,
            [
                self.own(3), lambda b, at, here: self.sides[0][b, here], lambda b, at, here: self.sides[1][b, here],
            ],
        )

    def line_copy(self, origin, target):
        z, y, x, core = self.place
        return send(
            self.kept.at[self.last, target], self.along.at[origin], self.line_sent.at[target],
            self.line_recv.at[origin], (target, y, x, core),
        )

    def others(self, act):
        z = self.place[0]
        for r in range(1, LINE):
            pl.when(z + r < LINE)(lambda r=r: act(z + r))
            pl.when(z - r >= 0)(lambda r=r: act(z - r))

    def line(self):
        z = self.place[0]
        self.others(lambda target: self.line_copy(z, target).start())

    def plane_sent(self):
        for k in range(4):
            self.to_twin(k).wait_send()
        for half in range(2):
            self.corner_copy(half).wait_send()
        for k in (1, 2):
            self.side_copy(k).wait_send()

    def hand_on(self, out):
        self.sides_in()
        out[...] = self.kept[self.last]
        self.plane_sent()

    def line_done(self):
        z = self.place[0]
        self.out[...] = self.kept[self.last, z].astype(F32)

        def arrive(origin):
            self.line_copy(origin, z).wait_recv()
            self.out[...] += self.along[origin].astype(F32)

        self.others(arrive)
        self.others(lambda target: self.line_copy(z, target).wait_send())

    def finish(self):
        self.line_done()
        self.plane_sent()

    def steps(self):
        return [
            self.begin, self.corners, self.sides_out, lambda: (self.sides_in(), self.line()), self.finish,
        ]


def scatter_scratch(rows, columns):
    dma = pltpu.SemaphoreType.DMA
    half = rows // 2
    return [
        pltpu.VMEM((4, LINE, rows, columns), BF16),
        pltpu.VMEM((4, LINE, rows, columns), BF16),
        pltpu.VMEM((LINE, half, columns), BF16),
        pltpu.VMEM((LINE, half, columns), BF16),
        pltpu.VMEM((LINE, rows, columns), BF16),
        pltpu.VMEM((LINE, rows, columns), BF16),
        pltpu.VMEM((LINE, rows, columns), BF16),
        dma((4,)), dma((4,)), dma((4,)), dma((4,)), dma((LINE,)), dma((LINE,)),
    ]


class Quick:
    def __init__(self, own, out, plane, line, sems):
        self.own, self.out, self.plane, self.along = own, out, plane, line
        self.sent, self.recv, self.line_sent, self.line_recv = sems
        self.place = my_place()

    def peers(self):
        z, y, x, core = self.place
        turns = [(a, b, c) for a in range(2) for b in range(2) for c in range(2) if a + b + c]
        return [((y + a) % 2, (x + b) % 2, (core + c) % 2) for a, b, c in turns]

    def copy(self, origin, target):
        z = self.place[0]
        number = lambda where: where[0] * 4 + where[1] * 2 + where[2]
        return send(
            self.own, self.plane.at[number(origin)], self.sent.at[number(target)], self.recv.at[number(origin)],
            (z,) + tuple(target),
        )

    def begin(self):
        here = self.place[1:]
        self.plane[here[0] * 4 + here[1] * 2 + here[2]] = self.own[...]
        for peer in self.peers():
            self.copy(here, peer).start()

    def line_copy(self, origin, target):
        z, y, x, core = self.place
        return send(
            self.along.at[z], self.along.at[origin], self.line_sent.at[target], self.line_recv.at[origin],
            (target, y, x, core),
        )

    def others(self, act):
        z = self.place[0]
        for r in range(1, LINE):
            pl.when(z + r < LINE)(lambda r=r: act(z + r))
            pl.when(z - r >= 0)(lambda r=r: act(z - r))

    def turn(self):
        z, here = self.place[0], self.place[1:]
        for peer in self.peers():
            self.copy(peer, here).wait_recv()
        total = self.plane[0]
        for k in range(1, 8):
            total = total + self.plane[k]
        self.along[z] = total
        self.others(lambda target: self.line_copy(z, target).start())

    def finish(self):
        z, here = self.place[0], self.place[1:]
        self.others(lambda origin: self.line_copy(origin, z).wait_recv())
        total = self.along[0]
        for k in range(1, LINE):
            total = total + self.along[k]
        self.out[...] = total
        for peer in self.peers():
            self.copy(here, peer).wait_send()
        self.others(lambda target: self.line_copy(z, target).wait_send())


class Total:
    def __init__(self, own, out, held, got, sent, recv):
        self.own, self.out, self.held, self.got, self.sent, self.recv = own, out, held, got, sent, recv

    def copy(self, k):
        z, y, x, core = my_place()
        near = z + 1 - 2 * (z % 2)
        peer = [
            (z, y, x, 1 - core), (z, y, 1 - x, core), (z, 1 - y, x, core), (near, y, x, core),
            ((z + 2) % LINE, y, x, core),
        ][k]
        return send(self.own if k == 0 else self.held.at[k], self.got.at[k], self.sent.at[k], self.recv.at[k], peer)

    def begin(self):
        self.copy(0).start()

    def turn(self, k):
        self.copy(k).wait_recv()
        mine = self.own[...] if k == 0 else self.held[k]
        total = mine + self.got[k]
        if k < 4:
            self.held[k + 1] = total
            self.copy(k + 1).start()
        else:
            self.out[...] = total

    def finish(self):
        for k in range(5):
            self.copy(k).wait_send()

    def steps(self):
        return [self.begin] + [lambda k=k: self.turn(k) for k in range(5)] + [self.finish]


WIDE = 512
PIECES = ((0, 1024), (1024, 1024), (2048, UW - 2048))


def patched(values, fixed, first):
    count = values.shape[0]
    end = values[count - 16 :].astype(F32)
    own = jnp.logical_and(rows_of(end.shape) >= 8, lanes_of(end.shape) + first < CH)
    chosen = jnp.where(own, fixed, end)
    return jnp.concatenate([values[: count - 16], chosen.astype(BF16)], 0)


def final_kernel(*refs):
    (
        turned_ref, du_cols, dz_ref, du_ref, tok_ref, gain_ref, wz_any, wu_any, gate_ref, conv_ref, gsum_ref,
        small_ref, last_ref, edge_ref,
    ) = refs[:14]
    grad_ref, inw_ref, sums_ref, norm_ref = refs[14:18]
    (
        wz, wu, sems, parts_a, parts_b, parts_c, out_a, out_b, out_c, packed, normed_grad, held, got, sent, recv, gains,
        gains_plane, gains_line, gains_sent, gains_recv, gains_out, gains_in, fixed, edge_got, edge_sems, du_block,
    ) = refs[18:44]
    i = pl.program_id(0)
    steps = pl.num_programs(0) - tok_blocks(turned_ref)
    z, y, x, core = my_place()
    scr_a, scr_b, scr_c = refs[44:57], refs[57:70], refs[70:83]
    sum_a = Scatter(parts_a, out_a, *scr_a[:7], scr_a[7:])
    sum_b = Scatter(parts_b, out_b, *scr_b[:7], scr_b[7:])
    sum_c = Scatter(parts_c, out_c, *scr_c[:7], scr_c[7:])
    small = Total(packed, sums_ref, held, got, sent, recv)
    norm = Quick(gains, norm_ref, gains_plane, gains_line, (gains_sent, gains_recv, gains_out, gains_in))
    load_z = pltpu.make_async_copy(wz_any, wz, sems.at[0])
    load_u = pltpu.make_async_copy(wu_any, wu, sems.at[1])

    @pl.when(i == 0)
    def _():
        load_z.start()
        load_u.start()
        meet(plane_peers() + line_peers() + chain_peers())
        packed[...] = jnp.zeros_like(packed)
        packed[0:5, :] = conv_ref[0:5, :]
        packed[5:6, :DI] = gsum_ref[0:1, :]
        packed[5:6, DI : DI + 128] = small_ref[0:1, :]
        packed[5:6, DI + 128 :] = small_ref[1:2, :]
        packed[6:7, :DI] = gsum_ref[1:2, :]
        pos = lax.axis_index("ctx")
        back_edge = pass_on(edge_ref, edge_got, edge_sems, -1)

        @pl.when(pos > 0)
        def _():
            back_edge.start()

        gains[...] = jnp.zeros_like(gains)
        small.begin()
        inw_ref[:, :DI] = gate_ref[...]
        fixed[...] = jnp.zeros_like(fixed)
        fixed[8:16, :CH] = last_ref[...]

        @pl.when(pos < lax.axis_size("ctx") - 1)
        def _():
            back_edge.wait_recv()
            fixed[8:16, :CH] += edge_got[...]

        @pl.when(pos > 0)
        def _():
            back_edge.wait_send()

    first = [
        (8, lambda: (sum_a.begin(), small.turn(0))), (12, sum_a.corners), (16, lambda: (sum_b.begin(), small.turn(1))),
    ]
    second = [
        (20, lambda: (sum_a.sides_out(), sum_c.begin())), (22, sum_b.corners), (23, lambda: small.turn(2)),
        (24, sum_c.corners), (26, lambda: small.turn(3)), (28, sum_b.sides_out),
        (29, lambda: (sum_a.sides_in(), sum_a.line())), (30, lambda: small.turn(4)), (31, sum_c.sides_out),
    ]

    @pl.when(i < steps)
    def _():
        when_at(4 * i, first)
        at = pl.ds(pl.multiple_of(i * WIDE, WIDE), WIDE)
        result = nn(turned_ref[...], patched(du_cols[...], fixed[:, at], i * WIDE)).astype(BF16)
        rows = parts_a.shape[2]

        def keep(parts, cols, width):
            for b in range(LINE):
                for q in range(8):
                    first = (b * 8 + q) * rows
                    parts[b, q, :, cols] = result[first : first + rows, :width]

        for parts, (begin, count) in zip((parts_a, parts_b, parts_c), PIECES):
            for at in range(0, count, WIDE):
                wide = min(WIDE, count - at)

                @pl.when(i == (begin + at) // WIDE)
                def _(parts=parts, at=at, wide=wide):
                    keep(parts, slice(at, at + wide), wide)

    @pl.when(i == steps)
    def _():
        load_z.wait()
        load_u.wait()

    @pl.when(i >= steps)
    def _():
        width = tok_ref.shape[1]
        chunk = width // 4
        at_end = i == pl.num_programs(0) - 1
        du_block[:, :CH] = patched(du_ref[:, :CH], fixed[:, :CH], jnp.where(at_end, 0, CH))
        du_block[:, CH:] = du_ref[:, CH:]

        def part(n, unused):
            when_at(4 * i + n, second)
            feats = pl.ds(pl.multiple_of(n * chunk, chunk), chunk)
            normed_grad[:, feats] = nt(dz_ref[...], wz[feats, :]) + nt(du_block[...], wu[feats, :])
            return unused

        lax.fori_loop(0, 4, part, 0)
        values = tok_ref[...].astype(F32)
        scale = lax.rsqrt(jnp.sum(values * values, axis=1, keepdims=True) * (1.0 / width) + epsilon)
        hat = values * scale
        grad = normed_grad[...]
        gains[...] += jnp.sum(grad * hat, axis=0, keepdims=True)
        inner = grad * gain_ref[...]
        mean = jnp.sum(inner * hat, axis=1, keepdims=True) * (1.0 / width)
        grad_ref[...] = (scale * (inner - hat * mean)).astype(BF16)

    @pl.when(i == pl.num_programs(0) - 1)
    def _():
        norm.begin()
        sum_b.sides_in()
        sum_b.line()
        norm.turn()
        sum_c.sides_in()
        sum_c.line()
        sum_a.finish()
        norm.finish()
        sum_b.finish()
        sum_c.finish()
        small.finish()
        for out, (begin, count) in zip((out_a, out_b, out_c), PIECES):
            count = min(count, DPROJ - DI - begin)
            inw_ref[:, DI + begin : DI + begin + count] = out[:, :count]


def tok_blocks(turned_ref):
    return turned_ref.shape[1] // Q


def final(turned, du, dz, tokens, gain, w_z, w_u, gate_columns, conv_sums, gate_sums, small, last, edge, number):
    width, rows = turned.shape
    steps = -(-UW // WIDE)
    blocks = rows // Q
    dma = pltpu.SemaphoreType.DMA
    own = width // 32
    anywhere = pl.BlockSpec(memory_space=pl.ANY)
    later = lambda i: (jnp.maximum(i - steps, 0), 0)
    sums = (8, CH)
    return pl.pallas_call(
        final_kernel,
        grid=(steps + blocks,),
        in_specs=[
            whole((width, rows)),
            spec((rows, WIDE), lambda i: (0, jnp.minimum(i, steps - 1))),
            spec((Q, DI), later),
            spec((Q, UW), later),
            spec((Q, width), later),
            whole((1, width)),
            anywhere,
            anywhere,
            whole((own, DI)),
            whole(sums),
            whole((8, DI)),
            whole((8, 128)),
            whole((8, CH)),
            whole((8, CH)),
        ],
        out_specs=[spec((Q, width), later), whole((own, DPROJ)), whole(sums), whole((1, width))],
        out_shape=[
            shaped((rows, width), BF16), shaped((own, DPROJ), F32), shaped(sums, F32), shaped((1, width), F32),
        ],
        scratch_shapes=[
            pltpu.VMEM((width, DI), BF16),
            pltpu.VMEM((width, UW), BF16),
            dma((2,)),
            *[pltpu.VMEM((LINE, 8, own, count), BF16) for begin, count in PIECES],
            *[pltpu.VMEM((own, count), F32) for begin, count in PIECES],
            pltpu.VMEM(sums, F32),
            pltpu.VMEM((Q, width), F32),
            pltpu.VMEM((5,) + sums, F32),
            pltpu.VMEM((5,) + sums, F32),
            dma((5,)),
            dma((5,)),
            pltpu.VMEM((1, width), F32),
            pltpu.VMEM((8, 1, width), F32),
            pltpu.VMEM((LINE, 1, width), F32),
            dma((8,)),
            dma((8,)),
            dma((LINE,)),
            dma((LINE,)),
            pltpu.VMEM((16, -(-UW // WIDE) * WIDE), F32),
            pltpu.VMEM((8, CH), F32),
            dma((2,)),
            pltpu.VMEM((Q, UW), BF16),
        ]
        + [each for begin, count in PIECES for each in scatter_scratch(own, count)],
        compiler_params=params(number),
        cost_estimate=cost(20e9, 60e6),
        name="final",
    )(turned, du, dz, du, tokens, gain, w_z, w_u, gate_columns, conv_sums, gate_sums, small, last, edge)


def close_kernel(
    part_ref, cot_ref, inw_in, outw_in, sums_ref, norm_in, back_in,
    grad_ref, inw_ref, outw_ref, norm_ref, taps_ref, shift_ref, bias_ref, decay_ref, skip_ref, gate_ref,
):
    grad_ref[...] = cot_ref[...].astype(F32) + part_ref[...].astype(F32)

    @pl.when(pl.program_id(0) == 0)
    def _():
        inw_ref[...] = inw_in[...]
        outw_ref[...] = outw_in[...]
        norm_ref[...] = norm_in[0]
        taps_ref[...] = sums_ref[:CONVK]
        shift_ref[...] = sums_ref[CONVK]
        bias_ref[...] = sums_ref[5, DI : DI + 128]
        decay_ref[...] = sums_ref[5, DI + 128 :]
        gate_ref[...] = sums_ref[5, :DI]
        lane = lanes_of((1, 128))
        total = jnp.zeros((1, 128), F32)
        for h in range(HEADS):
            here = jnp.sum(back_in[6:7, h * P_SIZE : (h + 1) * P_SIZE], axis=1, keepdims=True)
            total = jnp.where(lane == h, here, total)
        skip_ref[...] = total[0]


def close(part, cotangent, inw, outw, sums, norm):
    rows, width = part.shape
    at = lambda i: (i, 0)
    line = lambda n: pl.BlockSpec((n,), lambda i: (0,))
    return pl.pallas_call(
        close_kernel,
        grid=(rows // Q,),
        in_specs=[
            spec((Q, width), at), spec((Q, width), at), whole(inw.shape), whole(outw.shape), whole(sums.shape),
            whole(norm.shape), whole(sums.shape),
        ],
        out_specs=[
            spec((Q, width), at), whole(inw.shape), whole(outw.shape), line(width), whole((CONVK, CH)), line(CH),
            line(128), line(128), line(128), line(DI),
        ],
        out_shape=[
            shaped((rows, width), F32), shaped(inw.shape, F32), shaped(outw.shape, F32), shaped((width,), F32),
            shaped((CONVK, CH), F32), shaped((CH,), F32), shaped((128,), F32), shaped((128,), F32),
            shaped((128,), F32), shaped((DI,), F32),
        ],
        compiler_params=params(),
        name="close",
    )(part, cotangent, inw, outw, sums, norm, sums)


def local(
    tokens,
    valid_mask,
    stretch_start,
    cotangent,
    norm_gain,
    in_weight,
    conv_weight,
    conv_bias,
    step_bias,
    decay_log,
    skip_gain,
    gate_gain,
    out_weight,
):
    axes = ("fsdp", "ctx")
    rows, width = tokens.shape
    blocks = rows // Q
    near = lax.axis_size("ctx")
    boxed = lax.axis_size("fsdp") == 8 and near == 4
    if boxed:
        own = jnp.pad(in_weight, ((0, 0), (0, UW + DI - DPROJ)))
        w_u, normed_more, turned = gathered(own, tokens, norm_gain.reshape(1, width), 1)
        later = [own, out_weight]
        later_widths = [DI, width]
    else:
        own_u = jnp.pad(in_weight[:, DI:], ((0, 0), (0, UW - (DPROJ - DI))))
        w_u, w_z, w_o = [
            lax.all_gather(a, axes, axis=0, tiled=True) for a in (own_u, in_weight[:, :DI], out_weight)
        ]
        later = []
        later_widths = []
        halo_tokens = lax.ppermute(tokens[rows - HALO :], "ctx", [(k, k + 1) for k in range(near - 1)])
        wide = jnp.concatenate([tokens, halo_tokens], 0).astype(F32)
        scale = lax.rsqrt(jnp.mean(wide * wide, axis=-1, keepdims=True) + epsilon)
        normed_more = (wide * scale * norm_gain).astype(BF16)
    extra = len(later)
    anywhere = pl.BlockSpec(memory_space=pl.ANY)

    normed = normed_more[:rows]
    valid = jnp.broadcast_to(valid_mask.astype(F32)[:, None], (rows, 128))
    keep = (1.0 - stretch_start[0].astype(F32)).reshape(1, 1)
    taps = conv_weight

    same = lambda c: (c, 0)
    same3 = lambda c: (c, 0, 0)
    one = lambda i: (jnp.minimum(i, blocks - 1), 0)
    one3 = lambda i: (jnp.minimum(i, blocks - 1), 0, 0)
    two = lambda i: (jnp.maximum(i - blocks, 0), 0)
    val, vp, conv, bc, ssd, ent, logd, step, cum, start, u, ahead, *filled = pl.pallas_call(
        lambda *refs: forward_kernel(extra, *refs),
        grid=(2 * blocks,),
        in_specs=[
            spec((Q, width), one),
            spec((HALO, width), lambda c: (rows // HALO, 0)),
            anywhere,
            spec((Q, 128), one),
            scalar(),
            whole((CONVK, CH)),
            whole((CH,)),
            whole((HEADS,)),
            whole((HEADS,)),
            scalar(),
        ]
        + [anywhere] * extra,
        out_specs=[
            spec((Q, DI), one),
            spec((Q, DI), one),
            spec((Q, CH), one),
            spec((Q, 2 * N), one),
            spec((Q, DI), two),
            spec((1, N, DI), one3),
            spec((Q, 128), one),
            spec((Q, 128), one),
            whole((blocks + 1, 8, DI)),
            whole((N, DI)),
            spec((Q, UW), one),
            whole((8, UW)),
        ]
        + [anywhere] * extra,
        out_shape=[
            shaped((rows, DI), BF16),
            shaped((rows, DI), BF16),
            shaped((rows, CH), BF16),
            shaped((rows, 2 * N), BF16),
            shaped((rows, DI), BF16),
            shaped((blocks, N, DI), BF16),
            shaped((rows, 128), F32),
            shaped((rows, 128), F32),
            shaped((blocks + 1, 8, DI), F32),
            shaped((N, DI), BF16),
            shaped((rows, UW), F32),
            shaped((8, UW), F32),
        ]
        + [shaped((32 * a.shape[0], n), a.dtype) for a, n in zip(later, later_widths)],
        scratch_shapes=[
            pltpu.VMEM((8, CH), F32),
            pltpu.VMEM((GROUPS, Q, 128), F32),
            pltpu.VMEM((128, DI), BF16),
            pltpu.VMEM((GROUPS, 8, Q), F32),
            pltpu.VMEM((Q, Q), F32),
            pltpu.VMEM((N, DI), F32),
            pltpu.VMEM((blocks, Q, DI), BF16),
            pltpu.VMEM((blocks, Q, DI), BF16),
            pltpu.VMEM((blocks, Q, 2 * N), BF16),
            pltpu.VMEM((blocks, Q, 128), F32),
            pltpu.VMEM((N, DI), BF16),
            pltpu.VMEM((N, DI), BF16),
            pltpu.SemaphoreType.DMA((2,)),
            pltpu.VMEM((w_u.shape[0], UW), BF16),
            pltpu.SemaphoreType.DMA(()),
            pltpu.VMEM((2, Q, GW), F32),
            pltpu.VMEM((2, Q, GW), F32),
            pltpu.VMEM((1, CH), F32),
            pltpu.VMEM((1, 128), F32),
            pltpu.VMEM((1, 128), F32),
            pltpu.VMEM((1, DI), F32),
        ]
        + gather_scratch() * extra,
        compiler_params=params(2),
        cost_estimate=cost(15e9, 60e6),
        name="forward",
    )(normed_more, normed_more, w_u, valid, keep, taps, conv_bias, step_bias, decay_log, skip_gain, *later)
    if later:
        w_z, w_o = filled

    z = jnp.dot(normed, w_z, preferred_element_type=F32).astype(BF16)
    back = lambda i: (blocks - 1 - i, 0)
    back3 = lambda i: (blocks - 1 - i, 0, 0)
    output, gated, branch_grad, ds, dz, entt, gnext, gout, dlp, dc, gate_sums = pl.pallas_call(
        gate_kernel,
        grid=(blocks,),
        in_specs=[
            whole((N, DI)),
            spec((Q, DI), back),
            spec((1, N, DI), back3),
            spec((Q, DI), back),
            spec((Q, DI), back),
            spec((Q, 2 * N), back),
            spec((Q, 128), back),
            whole((blocks + 1, 8, DI)),
            spec((Q, width), back),
            spec((Q, width), back),
            spec((Q, 128), back),
            anywhere,
            whole((DI,)),
        ],
        out_specs=[
            spec((Q, width), back),
            spec((Q, DI), back),
            spec((Q, width), back),
            spec((Q, DI), back),
            spec((Q, DI), back),
            spec((1, N, DI), back3),
            spec((1, N, DI), back3),
            whole((N, DI)),
            spec((Q, 128), back),
            spec((Q, N), back),
            whole((8, DI)),
        ],
        out_shape=[
            shaped((rows, width), BF16),
            shaped((rows, DI), BF16),
            shaped((rows, width), BF16),
            shaped((rows, DI), BF16),
            shaped((rows, DI), BF16),
            shaped((blocks, N, DI), BF16),
            shaped((blocks, N, DI), BF16),
            shaped((N, DI), BF16),
            shaped((rows, 128), F32),
            shaped((rows, N), F32),
            shaped((8, DI), F32),
        ],
        scratch_shapes=[
            pltpu.VMEM((N, DI), F32),
            pltpu.VMEM((N, DI), F32),
            pltpu.VMEM((128, DI), BF16),
            pltpu.VMEM((Q, DI), F32),
            pltpu.VMEM((Q, DI), F32),
            pltpu.VMEM((Q, DI), F32),
            pltpu.VMEM((Q, DI), F32),
            pltpu.VMEM((Q, DI), F32),
            pltpu.VMEM((Q, 128), F32),
            pltpu.VMEM((1, DI), F32),
            pltpu.VMEM((DI, width), BF16),
            pltpu.SemaphoreType.DMA(()),
        ],
        compiler_params=params(),
        cost_estimate=cost(15e9, 60e6),
        name="gate",
    )(
        start, ssd, ent, z, val, bc, logd, cum, tokens, cotangent, valid, w_o, gate_gain,
    )

    def columns_of(left, right):
        return lax.dot_general(
            left, right, (((0,), (0,)), ((), ())), preferred_element_type=F32
        ).astype(BF16)

    def in_blocks(a):
        return a.reshape(LINE, 8, a.shape[0] // 32, a.shape[1])

    out_weight_grad = columns_of(gated, branch_grad)
    gate_columns = columns_of(normed, dz)
    mixing_parts = [in_blocks(out_weight_grad)] if boxed else []

    dvp, dbc, dlt, gin, *summed_out = pl.pallas_call(
        lambda *refs: mixing_kernel(len(mixing_parts), *refs),
        grid=(blocks,),
        in_specs=[
            spec((Q, DI), same),
            spec((Q, DI), same),
            spec((Q, 2 * N), same),
            spec((Q, 128), same),
            scalar(),
            whole((N, DI)),
            whole((blocks + 1, 8, DI)),
        ]
        + [anywhere for a in mixing_parts],
        out_specs=[spec((Q, DI), same), spec((Q, 2 * N), same), spec((Q, 128), same), whole((N, DI))]
        + [whole((LINE,) + a.shape[-2:]) for a in mixing_parts],
        out_shape=[
            shaped((rows, DI), BF16), shaped((rows, 2 * N), F32), shaped((rows, 128), F32), shaped((N, DI), BF16),
        ]
        + [shaped((LINE,) + a.shape[-2:], BF16) for a in mixing_parts],
        scratch_shapes=[
            pltpu.VMEM((GROUPS, Q, 128), F32),
            pltpu.VMEM((GROUPS, 8, Q), F32),
            pltpu.VMEM((Q, Q), F32),
            pltpu.VMEM((Q, Q), F32),
            pltpu.VMEM((GROUPS, 8, Q), F32),
            pltpu.VMEM((128, Q), F32),
            pltpu.VMEM((GROUPS, Q, 128), F32),
            pltpu.VMEM((N, DI), BF16),
            pltpu.VMEM((N, DI), BF16),
            pltpu.SemaphoreType.DMA((2,)),
        ]
        + [each for a in mixing_parts for each in plane_scratch(*a.shape[-2:])],
        compiler_params=params(3),
        cost_estimate=cost(15e9, 60e6),
        name="mixing",
    )(ds, vp, bc, logd, keep, gout, cum, *mixing_parts)

    back_parts = summed_out + [in_blocks(gate_columns)] if boxed else []
    du, last, edge, conv_sums, small, *summed_gate = pl.pallas_call(
        lambda *refs: back_kernel(len(back_parts), *refs),
        grid=(blocks,),
        in_specs=[
            scalar(),
            whole((N, DI)),
            spec((1, N, DI), back3),
            spec((1, N, DI), back3),
            whole((blocks + 1, 8, DI)),
            spec((Q, DI), back),
            spec((Q, DI), back),
            spec((Q, DI), back),
            spec((Q, DI), back),
            spec((Q, CH), back),
            spec((Q, UW), back),
            whole((8, UW)),
            spec((Q, 2 * N), back),
            spec((Q, 128), back),
            spec((Q, 128), back),
            spec((Q, 128), back),
            spec((Q, 128), back),
            spec((Q, 128), back),
            spec((Q, 2 * N), back),
            spec((Q, N), back),
            whole((CONVK, CH)),
            whole((HEADS,)),
            whole((HEADS,)),
            scalar(),
        ]
        + [pl.BlockSpec(memory_space=pltpu.VMEM), anywhere][: len(back_parts)],
        out_specs=[
            spec((Q, UW), back),
            whole((8, CH)),
            whole((8, CH)),
            whole((8, CH)),
            whole((8, 128)),
        ]
        + [whole(a.shape[-2:]) for a in back_parts],
        out_shape=[
            shaped((rows, UW), BF16),
            shaped((8, CH), F32),
            shaped((8, CH), F32),
            shaped((8, CH), F32),
            shaped((8, 128), F32),
        ]
        + [shaped(a.shape[-2:], F32) for a in back_parts],
        scratch_shapes=[
            pltpu.VMEM((N, DI), F32),
            pltpu.VMEM((128, DI), BF16),
            pltpu.VMEM((8, CH), F32),
            pltpu.VMEM((16, CH), F32),
            pltpu.VMEM((Q, 128), F32),
            pltpu.VMEM((Q, 128), F32),
            pltpu.VMEM((16, 128), F32),
            pltpu.VMEM((1, 128), F32),
            pltpu.VMEM((1, 128), F32),
            pltpu.VMEM((1, DI), F32),
        ]
        + (
            scatter_scratch(*back_parts[1].shape[-2:])
            + line_scratch(*back_parts[0].shape[-2:])
            + [pltpu.SemaphoreType.DMA((4,))]
            if back_parts
            else []
        ),
        compiler_params=params(4 if back_parts else None),
        cost_estimate=cost(15e9, 60e6),
        name="back",
    )(
        keep, gin, gnext, entt, cum, vp, val, dvp, ds, conv, u, ahead, bc, logd, step, valid,
        dlp, dlt, dbc, dc, taps, step_bias, decay_log, skip_gain, *back_parts,
    )
    if boxed:
        out_weight_grad, gate_columns = summed_gate
        part, in_weight_grad, sums, norm_sum = final(
            turned, du, dz, tokens, norm_gain.reshape(1, width), w_z, w_u, gate_columns, conv_sums,
            gate_sums, small, last, edge, 5,
        )
        results = close(part, cotangent, in_weight_grad, out_weight_grad, sums, norm_sum)
        input_grad, in_weight_grad, out_weight_grad, norm_sum, taps_sum, shift_sum = results[:6]
        bias_sum, decay_sum, skip_sum, gate_sum = results[6:]
        return (
            output,
            input_grad,
            in_weight_grad,
            out_weight_grad,
            norm_sum,
            taps_sum,
            shift_sum,
            bias_sum[:HEADS],
            decay_sum[:HEADS],
            skip_sum[:HEADS],
            gate_sum,
        )
    edge_back = lax.ppermute(edge, "ctx", [(k + 1, k) for k in range(near - 1)])
    du = lax.dynamic_update_slice(du, (last + edge_back).astype(BF16), (rows - 8, 0))
    conv_columns = columns_of(normed, du)
    across = (((1,), (1,)), ((), ()))
    normed_grad = lax.dot_general(dz, w_z, across, preferred_element_type=F32) + lax.dot_general(
        du, w_u, across, preferred_element_type=F32
    )
    inputs = tokens.astype(F32)
    scale = lax.rsqrt(jnp.mean(inputs * inputs, axis=-1, keepdims=True) + epsilon)
    hat = inputs * scale
    inner = normed_grad * norm_gain
    input_grad = cotangent.astype(F32) + scale * (
        inner - hat * jnp.mean(inner * hat, axis=-1, keepdims=True)
    )
    norm_grad = jnp.sum(normed_grad * hat, axis=0)
    packed = jnp.concatenate(
        [
            norm_grad,
            conv_sums[:5].reshape(-1),
            gate_sums[:2].reshape(-1),
            small[:2].reshape(-1),
        ]
    )
    conv_columns, gate_columns, out_weight_grad = [
        lax.psum_scatter(a.astype(F32), axes, scatter_dimension=0, tiled=True)
        for a in (conv_columns, gate_columns, out_weight_grad)
    ]
    summed = lax.psum(packed, axes)
    in_weight_grad = jnp.concatenate([gate_columns, conv_columns[:, : DPROJ - DI]], 1)
    at = width
    conv_weight_grad = summed[at : at + CONVK * CH].reshape(CONVK, CH)
    at += CONVK * CH
    conv_bias_grad = summed[at : at + CH]
    at += CH
    gate_gain_grad = summed[at : at + DI]
    at += DI
    skip_gain_grad = jnp.sum(summed[at : at + DI].reshape(HEADS, P_SIZE), axis=1)
    at += DI
    step_bias_grad = summed[at : at + HEADS]
    decay_log_grad = summed[at + 128 : at + 128 + HEADS]
    return (
        output,
        input_grad,
        in_weight_grad,
        out_weight_grad,
        summed[:width],
        conv_weight_grad,
        conv_bias_grad,
        step_bias_grad,
        decay_log_grad,
        skip_gain_grad,
        gate_gain_grad,
    )


def solution(mesh):
    split = P(("fsdp", "ctx"), None)
    line = P(("fsdp", "ctx"))
    return jax.shard_map(
        local,
        mesh=mesh,
        in_specs=(split, line, line, split, P(), split, P(), P(), P(), P(), P(), P(), split),
        out_specs=(split, split, split, split, P(), P(), P(), P(), P(), P(), P()),
        check_vma=False,
    )
```

```python
import jax
import jax.numpy as jnp
from jax import lax
from jax.experimental import pallas as pl
from jax.experimental.pallas import tpu as pltpu
from jax.sharding import PartitionSpec as P

DI = 2048
HEADS = 32
P_SIZE = 64
N = 128
CONVK = 4
Q = 256
CH = 2304
DPROJ = 4384
UW = CH + 128
GW = 256
GROUPS = DI // GW
HALF = Q // 2
HALO = 16

F32 = jnp.float32
BF16 = jnp.bfloat16
LOG2E = 1.4426950408889634
epsilon = 1e-05


def nn(a, b):
    return lax.dot_general(a, b, (((1,), (0,)), ((), ())), preferred_element_type=F32)


def nt(a, b):
    return lax.dot_general(a, b, (((1,), (1,)), ((), ())), preferred_element_type=F32)


def sigmoid(x):
    return 0.5 * jnp.tanh(0.5 * x) + 0.5


def softplus(x):
    e = jnp.exp(-jnp.abs(x))
    w = 1.0 + e
    d = w - 1.0
    return jnp.maximum(x, 0.0) + jnp.where(d == 0.0, e, jnp.log(w) * (e / jnp.where(d == 0.0, 1.0, d)))


def rows_of(shape):
    return lax.broadcasted_iota(jnp.int32, shape, 0)


def lanes_of(shape):
    return lax.broadcasted_iota(jnp.int32, shape, 1)


def split3(x):
    a = x.astype(BF16)
    r = x - a.astype(F32)
    b = r.astype(BF16)
    return a, b, (r - b.astype(F32)).astype(BF16)


def ordered_sum(triangle, x):
    a, b, c = split3(x)
    return nn(triangle, c) + nn(triangle, b) + nn(triangle, a)


def spread(x, out):
    out[0] = x
    for g in range(1, GROUPS):
        out[g] = pltpu.roll(x, 128 - 4 * g, 1)


def delayed(before, x, by):
    if by == 0:
        return x
    return pltpu.roll(jnp.concatenate([before, x], 0), by, 0)[8:]


def advanced(x, after, by):
    if by == 0:
        return x
    count = x.shape[0]
    return pltpu.roll(jnp.concatenate([x, after], 0), count + 8 - by, 0)[:count]


def fill_picks(out):
    for g in range(GROUPS):
        shape = (128, GW)
        head = lax.shift_right_logical(lanes_of(shape), 6) + 4 * g
        at = rows_of(shape)
        own = jnp.logical_and(jnp.bitwise_and(at, HEADS - 1) == head, at < 3 * HEADS)
        out[:, g * GW : (g + 1) * GW] = jnp.where(own, 1.0, 0.0).astype(BF16)


def in_parts(x):
    lane = lanes_of(x.shape)
    a, b, c = split3(jnp.where(lane < HEADS, x, 0.0))
    wide = a.astype(F32) + pltpu.roll(b.astype(F32), HEADS, 1) + pltpu.roll(c.astype(F32), 2 * HEADS, 1)
    return wide.astype(BF16)


def spread_rows(x, out):
    for g in range(GROUPS):
        out[g, 0:4] = x[4 * g : 4 * g + 4]


def head_lanes(x, i):
    return jnp.broadcast_to(x[:, i : i + 1], (x.shape[0], 128))


def pick_heads(g):
    shape = (GW, 128)
    return jnp.where(
        lax.shift_right_logical(rows_of(shape), 6) + 4 * g == lanes_of(shape), 1.0, 0.0
    ).astype(BF16)


def when_at(now, plan):
    plan = sorted(plan, key=lambda entry: entry[0])
    if len(plan) == 1:
        place, act = plan[0]

        @pl.when(now == place)
        def _():
            act()

    elif plan:
        middle = len(plan) // 2

        def early():
            when_at(now, plan[:middle])

        def late():
            when_at(now, plan[middle:])

        lax.cond(now < plan[middle][0], early, late)


def chain_peers():
    pos = lax.axis_index("ctx")
    return [(pos > 0, {"ctx": pos - 1}), (pos < lax.axis_size("ctx") - 1, {"ctx": pos + 1})]


def pass_on(message, arrived, sems, by):
    return pltpu.make_async_remote_copy(
        src_ref=message, dst_ref=arrived, send_sem=sems.at[0], recv_sem=sems.at[1],
        device_id={"ctx": lax.axis_index("ctx") + by}, device_id_type=pl.DeviceIdType.MESH,
    )


def lay_heads(out, line):
    out[...] = jnp.zeros_like(out)
    out[0, :HEADS] = line[...]


def lay_out(out, line, picks):
    shape = (8, 128)
    heads = jnp.zeros((1, 128), F32)
    for h in range(HEADS):
        heads = jnp.where(lanes_of((1, 128)) == h, line[h], heads)
    out[...] = nn(in_parts(jnp.broadcast_to(heads, shape)), picks[...])[0:1]


def forward_kernel(count, *refs):
    (
        normed_ref, halo_ref, wu_any, valid_ref, keep_ref, cw_ref, cb_line, sb_line, dl_line, skip_line,
    ) = refs[:10]
    own = refs[10 : 10 + count]
    (
        val_ref, vp_ref, conv_ref, bc_ref, ssd_ref, ent_ref, log_ref, step_ref, cum_ref, start_ref, u_ref, ahead_ref,
    ) = refs[10 + count : 22 + count]
    outs = refs[22 + count : 22 + 2 * count]
    (
        past, logs, picks, logt, inter, state, all_vp, all_val, all_bc, all_log, message, arrived, sems, wu, load, log_wide, step_wide, cb_ref, sb_ref, dl_ref, skip_ref,
    ) = refs[22 + 2 * count : 43 + 2 * count]
    gather_sems = refs[43 + 2 * count :]
    i = pl.program_id(0)
    blocks = pl.num_programs(0) // 2
    first = i < blocks
    c = jnp.where(first, i, i - blocks)
    near = lax.axis_size("ctx")
    pos = lax.axis_index("ctx")
    plan = []
    if count:
        lists = [Gather(own[k], outs[k], (0, outs[k].shape[1], 0), *gather_sems[5 * k : 5 * k + 5]).steps() for k in range(count)]
        length = len(lists[0])
        for at in range(length + 2 * (count - 1)):
            acts = [lists[k][at - 2 * k] for k in range(count) if 0 <= at - 2 * k < length]
            plan.append((FORWARD_PLACES[at], lambda acts=acts: [act() for act in acts]))

    @pl.when(i == 0)
    def _():
        fetch = pltpu.make_async_copy(wu_any, wu, load)
        fetch.start()
        fill_picks(picks)
        cb_ref[0] = cb_line[...]
        lay_heads(sb_ref, sb_line)
        lay_heads(dl_ref, dl_line)
        lay_out(skip_ref, skip_line, picks)
        meet((box_peers() if count else []) + chain_peers())
        fetch.wait()
        before = nn(halo_ref[...], wu[...])[8:]
        ahead_ref[...] = before
        past[...] = before[:, :CH] * keep_ref[0, 0]
        state[...] = jnp.zeros_like(state)
        cum_ref[...] = jnp.zeros_like(cum_ref)

    half = lanes_of((Q, 128)) < P_SIZE
    square = (Q, Q)
    causal = rows_of(square) >= lanes_of(square)

    @pl.when(first)
    def _():
        tail = nn(normed_ref[...], wu[:, DI:])
        u_ref[:, DI:] = tail
        raw = tail[:, 2 * N :] + sb_ref[...]
        step = softplus(raw) * valid_ref[...]
        step = jnp.where(lanes_of(step.shape) < HEADS, step, 0.0)
        rate = -jnp.exp(dl_ref[...]) * LOG2E
        logd = ordered_sum(jnp.where(causal, 1.0, 0.0).astype(BF16), step * rate)
        log_ref[...] = logd
        all_log[c] = logd
        step_ref[...] = step
        log_parts = in_parts(logd)
        step_parts = in_parts(step)

        def convolved(cols, x):
            before = past[:, cols]
            past[:, cols] = x[Q - 8 :]
            total = cb_ref[:, cols] + cw_ref[CONVK - 1 : CONVK, cols] * x
            for k in range(CONVK - 1):
                total = total + cw_ref[k : k + 1, cols] * delayed(before, x, CONVK - 1 - k)
            return total

        conv_b = convolved(pl.ds(DI, N), tail[:, :N])
        conv_c = convolved(pl.ds(DI + N, N), tail[:, N : 2 * N])
        conv_ref[:, DI : DI + N] = conv_b.astype(BF16)
        conv_ref[:, DI + N :] = conv_c.astype(BF16)
        act_b = conv_b * sigmoid(conv_b)
        act_c = conv_c * sigmoid(conv_c)
        both = jnp.concatenate([act_b.astype(BF16), act_c.astype(BF16)], 1)
        bc_ref[...] = both
        all_bc[c] = both
        turned_b = act_b.T.astype(BF16)
        ent_ref[0] = state[...].astype(BF16)

        def ahead(g):
            cols = pl.ds(pl.multiple_of(g * GW, GW), GW)
            slot = g % 2
            u_ref[:, cols] = nn(normed_ref[...], wu[:, cols])
            log_wide[slot] = nn(log_parts, picks[:, cols])
            step_wide[slot] = nn(step_parts, picks[:, cols])

        ahead(0)

        def group(g, unused):
            when_at(i * GROUPS + g, plan)
            slot = g % 2
            for j in range(2):
                cols = pl.ds(pl.multiple_of(g * GW + 128 * j, 128), 128)
                cv = convolved(cols, u_ref[:, cols])
                conv_ref[:, cols] = cv.astype(BF16)
                val = cv * sigmoid(cv)
                low = val.astype(BF16)
                val_ref[:, cols] = low
                all_val[c, :, cols] = low
                lp = log_wide[slot, :, 128 * j : 128 * j + 128]
                vp = val * step_wide[slot, :, 128 * j : 128 * j + 128]
                low = vp.astype(BF16)
                vp_ref[:, cols] = low
                all_vp[c, :, cols] = low
                last = lp[Q - 1 : Q, :]
                weighted = (vp * jnp.exp2(last - lp)).astype(BF16)
                state[:, cols] = jnp.exp2(last) * state[:, cols] + nn(turned_b, weighted)
                cum_ref[c + 1, :, cols] = cum_ref[c, :, cols] + last
            ahead(lax.rem(g + 1, GROUPS))
            return unused

        lax.fori_loop(0, GROUPS, group, 0)

    def hop(k):
        @pl.when(pos == k)
        def _():
            if k:
                pass_on(message, arrived, sems, 1).wait_recv()
                entering = keep_ref[0, 0] * arrived[...].astype(F32)
                start_ref[...] = entering.astype(BF16)
            else:
                start_ref[...] = jnp.zeros_like(start_ref)
            if k < near - 1:
                if k:
                    message[...] = (jnp.exp2(cum_ref[blocks, 0:1, :]) * entering + state[...]).astype(BF16)
                else:
                    message[...] = state[...].astype(BF16)
                pass_on(message, arrived, sems, 1).start()

    hops = [(blocks * GROUPS + FORWARD_HOPS[k], lambda k=k: hop(k)) for k in range(near)]

    @pl.when(jnp.logical_not(first))
    def _():
        logd = all_log[c]
        spread(logd, logs)
        spread_rows(logd.T, logt)
        inter[...] = jnp.where(causal, nt(all_bc[c, :, N:], all_bc[c, :, :N]), 0.0)
        left = jnp.where(half[:1], 1.0, 0.0).astype(BF16)
        right = jnp.where(half[:1], 0.0, 1.0).astype(BF16)

        def group(g, unused):
            when_at(i * GROUPS + g, plan)
            when_at(i * GROUPS + g, hops)
            lg = logs[g]
            for j in range(2):
                cols = pl.ds(pl.multiple_of(g * GW + 128 * j, 128), 128)
                vp = all_vp[c, :, cols]
                v0 = vp * left
                v1 = vp * right
                top = []
                low = []
                for h in range(2):
                    row = logt[g, 2 * j + h : 2 * j + h + 1]
                    early, late = row[:, :HALF], row[:, HALF:]
                    lb = head_lanes(lg, 2 * j + h)
                    up, down = lb[:HALF], lb[HALF:]
                    top.append((inter[:HALF, :HALF] * jnp.exp2(jnp.minimum(up - early, 0.0))).astype(BF16))
                    low.append((inter[HALF:, :HALF] * jnp.exp2(jnp.minimum(down - early, 0.0))).astype(BF16))
                    low.append((inter[HALF:, HALF:] * jnp.exp2(jnp.minimum(down - late, 0.0))).astype(BF16))
                skipped = skip_ref[:, cols] * all_val[c, :, cols].astype(F32)
                above = nn(jnp.concatenate(top, 1), jnp.concatenate([v0[:HALF], v1[:HALF]], 0))
                below = nn(jnp.concatenate(low, 1), jnp.concatenate([v0, v1], 0))
                ssd_ref[:HALF, cols] = (above + skipped[:HALF]).astype(BF16)
                ssd_ref[HALF:, cols] = (below + skipped[HALF:]).astype(BF16)
            return unused

        lax.fori_loop(0, GROUPS, group, 0)

    @pl.when(jnp.logical_and(i == 2 * blocks - 1, pos < near - 1))
    def _():
        pass_on(message, arrived, sems, 1).wait_send()


def gate_kernel(
    start_ref, ssd_in, ent_ref, z_ref, val_ref, bc_ref, log_ref, cum_ref,
    tok_ref, cot_ref, valid_ref, ow_any, gain_line,
    out_ref, gated_ref, bg_ref, ds_ref, dz_ref, entt_ref, gnext_ref, gout_ref, dlp_ref, dc_ref, sums_ref,
    start, gstate, picks, ssd_s, mix_s, el_s, pe_s, gg_s, acc, gain_ref, ow_ref, load,
):
    i = pl.program_id(0)
    c = pl.num_programs(0) - 1 - i

    @pl.when(i == 0)
    def _():
        pltpu.make_async_copy(ow_any, ow_ref, load).start()
        start[...] = start_ref[...].astype(F32)
        fill_picks(picks)
        gain_ref[0] = gain_line[...]
        gstate[...] = jnp.zeros_like(gstate)
        sums_ref[...] = jnp.zeros_like(sums_ref)

    log_parts = in_parts(log_ref[...])
    low_c = bc_ref[:, N:]
    turned_c = low_c.astype(F32).T.astype(BF16)
    acc[...] = jnp.zeros_like(acc)

    def enter(g, unused):
        cols = pl.ds(pl.multiple_of(g * GW, GW), GW)
        decay = jnp.exp2(nn(log_parts, picks[:, cols]))
        entering = (
            ent_ref[0, :, cols].astype(F32) + jnp.exp2(cum_ref[c, 0:1, cols]) * start[:, cols]
        ).astype(BF16)
        entt_ref[0, :, cols] = entering
        part = nn(low_c, entering)
        for j in range(2):
            pc = pl.ds(pl.multiple_of(g * GW + 128 * j, 128), 128)
            el = decay[:, 128 * j : 128 * j + 128]
            pe = el * part[:, 128 * j : 128 * j + 128]
            el_s[:, pc] = el
            pe_s[:, pc] = pe
            ssd = ssd_in[:, pc].astype(F32) + pe
            z = z_ref[:, pc].astype(F32)
            mixed = ssd * (z * sigmoid(z))
            ssd_s[:, pc] = ssd
            mix_s[:, pc] = mixed
            acc[...] += mixed * mixed
        return unused

    lax.fori_loop(0, GROUPS, enter, 0)

    @pl.when(i == 0)
    def _():
        pltpu.make_async_copy(ow_any, ow_ref, load).wait()

    inv = lax.rsqrt(jnp.sum(acc[...], axis=1, keepdims=True) * (1.0 / DI) + epsilon)
    inv = jnp.broadcast_to(inv, (Q, 128))
    valid = valid_ref[...]
    valid8 = jnp.concatenate([valid] * (tok_ref.shape[1] // 128), 1)
    branch_grad = (cot_ref[...].astype(F32) * valid8).astype(BF16)
    bg_ref[...] = branch_grad
    acc[...] = jnp.zeros_like(acc)

    def gate(g, unused):
        cols = pl.ds(pl.multiple_of(g * GW, GW), GW)
        ggrad = nt(branch_grad, ow_ref[cols, :])
        for j in range(2):
            pc = pl.ds(pl.multiple_of(g * GW + 128 * j, 128), 128)
            hat = mix_s[:, pc] * inv
            gain = gain_ref[:, pc]
            mix_s[:, pc] = hat
            gated_ref[:, pc] = (hat * gain).astype(BF16)
            gg = ggrad[:, 128 * j : 128 * j + 128]
            both = gg * hat
            sums_ref[0:1, pc] += jnp.sum(both, axis=0, keepdims=True)
            acc[...] += both * gain
            gg_s[:, pc] = gg * gain
        return unused

    lax.fori_loop(0, GROUPS, gate, 0)
    mean = jnp.sum(acc[...], axis=1, keepdims=True) * (1.0 / DI)
    mean = jnp.broadcast_to(mean, (Q, 128))

    for n in range(tok_ref.shape[1] // 256):
        cols = slice(256 * n, 256 * n + 256)
        branch = nn(gated_ref[...], ow_ref[:, cols])
        out_ref[:, cols] = (tok_ref[:, cols].astype(F32) + valid8[:, :256] * branch).astype(BF16)

    acc[...] = jnp.zeros_like(acc)
    dc_ref[...] = jnp.zeros_like(dc_ref)

    def back(g, unused):
        cols = pl.ds(pl.multiple_of(g * GW, GW), GW)
        dparts = []
        prods = []
        for j in range(2):
            pc = pl.ds(pl.multiple_of(g * GW + 128 * j, 128), 128)
            dmixed = inv * (gg_s[:, pc] - mix_s[:, pc] * mean)
            z = z_ref[:, pc].astype(F32)
            s = sigmoid(z)
            ds = (dmixed * (z * s)).astype(BF16)
            ds_ref[:, pc] = ds
            dz_ref[:, pc] = (dmixed * ssd_s[:, pc] * (s * (1.0 + z * (1.0 - s)))).astype(BF16)
            ds = ds.astype(F32)
            sums_ref[1:2, pc] += jnp.sum(ds * val_ref[:, pc].astype(F32), axis=0, keepdims=True)
            dparts.append((ds * el_s[:, pc]).astype(BF16))
            prods.append((ds * pe_s[:, pc]).astype(BF16))
        dpart = jnp.concatenate(dparts, 1)
        acc[...] += nn(jnp.concatenate(prods, 1), pick_heads(g))
        dc_ref[...] += nt(dpart, entt_ref[0, :, cols])
        gnext_ref[0, :, cols] = gstate[:, cols].astype(BF16)
        total = cum_ref[c + 1, 0:1, cols] - cum_ref[c, 0:1, cols]
        gstate[:, cols] = nn(turned_c, dpart) + jnp.exp2(total) * gstate[:, cols]
        return unused

    lax.fori_loop(0, GROUPS, back, 0)
    dlp_ref[...] = acc[...]

    @pl.when(c == 0)
    def _():
        gout_ref[...] = gstate[...].astype(BF16)


FORWARD_PLACES = (0, 3, 7, 11, 16, 21, 26, 31, 36, 41, 47, 53, 63)
FORWARD_HOPS = (0, 8, 20, 30)
MIXING_HOPS = (0, 6, 18, 28)
MIXING_PLACES = (0, 5, 12, 31)
LINE_PLACES = (1, 12)
BACK_PLACES = (0, 3, 8, 19, 30)


def acting(places, acts):
    joined = {}
    for place, act in zip(places, acts):
        joined.setdefault(place, []).append(act)
    return [(place, lambda acts=acts: [act() for act in acts]) for place, acts in joined.items()]


def plane_scratch(rows, columns):
    dma = pltpu.SemaphoreType.DMA
    return scatter_scratch(rows, columns)[:6] + [dma((4,))] * 5


def line_scratch(rows, columns):
    dma = pltpu.SemaphoreType.DMA
    return [
        pltpu.VMEM((1, LINE, rows, columns), BF16), pltpu.VMEM((LINE, rows, columns), BF16), dma((LINE,)), dma((LINE,)),
    ]


def mixing_kernel(count, *refs):
    ds_ref, vp_ref, bc_ref, log_ref, keep_ref, gout_ref, cum_ref = refs[:7]
    parts = refs[7 : 7 + count]
    dvp_ref, dbc_ref, dlt_ref, gin_ref = refs[7 + count : 11 + count]
    outs = refs[11 + count : 11 + 2 * count]
    (
        logs, logt, inter, dinter, rowsum, turned, colsum, message, arrived, sems,
    ) = refs[11 + 2 * count : 21 + 2 * count]
    i = pl.program_id(0)
    blocks = pl.num_programs(0)
    near = lax.axis_size("ctx")
    pos = lax.axis_index("ctx")
    plan = []
    if count:
        held = refs[21 + 2 * count :]
        part = Scatter(parts[0], None, *held[:6], None, tuple(held[6:10]) + (None, None), held[10])
        acts = [part.begin, part.corners, part.sides_out, lambda: part.hand_on(outs[0])]
        plan = acting(MIXING_PLACES, acts)

    @pl.when(i == 0)
    def _():
        meet((box_peers() if count else []) + chain_peers())

    def hop(k):
        @pl.when(pos == near - 1 - k)
        def _():
            total = gout_ref[...].astype(F32)
            if k:
                pass_on(message, arrived, sems, -1).wait_recv()
                gin_ref[...] = arrived[...]
                total = total + jnp.exp2(cum_ref[blocks, 0:1, :]) * arrived[...].astype(F32)
            else:
                gin_ref[...] = jnp.zeros_like(gin_ref)
            if k < near - 1:
                message[...] = (keep_ref[0, 0] * total).astype(BF16)
                pass_on(message, arrived, sems, -1).start()

    hops = [(MIXING_HOPS[k], lambda k=k: hop(k)) for k in range(near)]

    logd = log_ref[...]
    spread(logd, logs)
    spread_rows(logd.T, logt)
    low_b = bc_ref[:, :N]
    low_c = bc_ref[:, N:]
    square = (Q, Q)
    causal = rows_of(square) <= lanes_of(square)
    inter[...] = jnp.where(causal, nt(low_b, low_c), 0.0)
    dinter[...] = jnp.zeros_like(dinter)
    half = lanes_of((Q, 128)) < P_SIZE
    lane = lanes_of((HALF, 128))

    def group(g, unused):
        when_at(i * GROUPS + g, plan)
        when_at(i * GROUPS + g, hops)
        lg = logs[g]
        first_col = jnp.zeros((HALF, 128), F32)
        second_col = jnp.zeros((HALF, 128), F32)
        for j in range(2):
            cols = pl.ds(pl.multiple_of(g * GW + 128 * j, 128), 128)
            vp = vp_ref[:, cols].astype(F32)
            ds = ds_ref[:, cols]
            wide = ds.astype(F32)
            first = []
            second = []
            outs = []
            for h in range(2):
                head = 2 * j + h
                own = half if h == 0 else jnp.logical_not(half)
                vm = jnp.where(own, vp, 0.0).astype(BF16)
                dsm = jnp.where(own, wide, 0.0).astype(BF16)
                outs.append(dsm)
                row = logt[g, head : head + 1]
                early, late = row[:, :HALF], row[:, HALF:]
                lb = head_lanes(lg, head)
                up, down = lb[:HALF], lb[HALF:]
                dup = nt(vm[:HALF], ds)
                ddown = nt(vm[HALF:], ds[HALF:])
                decay = jnp.exp2(jnp.minimum(early - up, 0.0))
                grad = dup[:, :HALF] * decay
                dinter[:HALF, :HALF] += grad
                part = inter[:HALF, :HALF]
                first.append((part * decay).astype(BF16))
                both = grad * part
                row_early = jnp.sum(both, axis=0, keepdims=True)
                col = both
                decay = jnp.exp2(jnp.minimum(late - up, 0.0))
                grad = dup[:, HALF:] * decay
                dinter[:HALF, HALF:] += grad
                part = inter[:HALF, HALF:]
                first.append((part * decay).astype(BF16))
                both = grad * part
                row_late = jnp.sum(both, axis=0, keepdims=True)
                col = jnp.sum(col + both, axis=1, keepdims=True)
                first_col = jnp.where(lane == head, col, first_col)
                decay = jnp.exp2(jnp.minimum(late - down, 0.0))
                grad = ddown * decay
                dinter[HALF:, HALF:] += grad
                part = inter[HALF:, HALF:]
                second.append((part * decay).astype(BF16))
                both = grad * part
                row_late = row_late + jnp.sum(both, axis=0, keepdims=True)
                col = jnp.sum(both, axis=1, keepdims=True)
                second_col = jnp.where(lane == head, col, second_col)
                rowsum[g, head : head + 1, :HALF] = row_early
                rowsum[g, head : head + 1, HALF:] = row_late
            dvp_ref[:HALF, cols] = nn(
                jnp.concatenate(first, 1), jnp.concatenate(outs, 0)
            ).astype(BF16)
            dvp_ref[HALF:, cols] = nn(
                jnp.concatenate(second, 1), jnp.concatenate([outs[0][HALF:], outs[1][HALF:]], 0)
            ).astype(BF16)
        colsum[g, :HALF] = first_col
        colsum[g, HALF:] = second_col
        return unused

    lax.fori_loop(0, GROUPS, group, 0)
    turned[...] = jnp.zeros_like(turned)
    for g in range(GROUPS):
        turned[4 * g : 4 * g + 4] = rowsum[g, 0:4]
    total = turned[...].T
    for g in range(GROUPS):
        total = total - (colsum[g] if g == 0 else pltpu.roll(colsum[g], 4 * g, 1))
    dlt_ref[...] = total
    masked = jnp.where(causal, dinter[...], 0.0)
    dbc_ref[:, :N] = nn(masked.astype(BF16), low_c)
    dbc_ref[:, N:] = nn(masked.T.astype(BF16), low_b)

    @pl.when(jnp.logical_and(i == blocks - 1, pos > 0))
    def _():
        pass_on(message, arrived, sems, -1).wait_send()


def back_kernel(count, *refs):
    (
        keep_ref, gin_ref, gnext_ref, entt_ref, cum_ref, vp_ref, val_ref, dvp_ref, ds_ref, conv_ref,
        u_ref, halo_ref, bc_ref, log_ref, step_ref, valid_ref, dlp_ref, dlt_ref, dbc_ref, dc_ref,
        cw_ref, sb_line, dl_line, skip_line,
    ) = refs[:24]
    parts = refs[24 : 24 + count]
    du_ref, last_ref, edge_ref, sums_ref, small_ref = refs[24 + count : 29 + count]
    outs = refs[29 + count : 29 + 2 * count]
    gin, picks, head, epad, dlw, dst, drow, sb_ref, dl_ref, skip_ref = refs[29 + 2 * count : 39 + 2 * count]
    plan = []
    if count:
        held = refs[39 + 2 * count :]
        full = Scatter(parts[1], outs[1], *held[:7], held[7:13], held[17])
        line = Scatter(None, outs[0], None, held[13], None, None, None, None, held[14], (None,) * 4 + tuple(held[15:17]))
        acts = [line.line, line.line_done]
        plan = acting(BACK_PLACES + LINE_PLACES, full.steps() + acts)
    i = pl.program_id(0)
    top = pl.num_programs(0)
    c = top - 1 - i

    @pl.when(i == 0)
    def _():
        if count:
            meet(box_peers()[:3] + line_peers())
            line.kept[0] = parts[0][...]
        gin[...] = gin_ref[...].astype(F32)
        fill_picks(picks)
        lay_heads(sb_ref, sb_line)
        lay_heads(dl_ref, dl_line)
        lay_out(skip_ref, skip_line, picks)
        head[...] = jnp.zeros_like(head)
        sums_ref[...] = jnp.zeros_like(sums_ref)
        small_ref[...] = jnp.zeros_like(small_ref)

    log_parts = in_parts(log_ref[...])
    step_parts = in_parts(step_ref[...])
    low_b = bc_ref[:, :N]
    dlw[...] = jnp.zeros_like(dlw)
    dst[...] = jnp.zeros_like(dst)
    drow[...] = jnp.zeros_like(drow)

    def conv_back(cols, dact):
        cv = conv_ref[:, cols].astype(F32)
        s = sigmoid(cv)
        dcv = dact * (s * (1.0 + cv * (1.0 - s)))
        after = head[:, cols]
        head[:, cols] = dcv[:8]
        x = u_ref[:, cols]
        sums_ref[4:5, cols] += jnp.sum(dcv, axis=0, keepdims=True)
        total = None
        for j in range(CONVK):
            k = CONVK - 1 - j
            moved = advanced(dcv, after, j)
            sums_ref[k : k + 1, cols] += jnp.sum(moved * x, axis=0, keepdims=True)
            term = cw_ref[k : k + 1, cols] * moved
            total = term if total is None else total + term
        du_ref[:, cols] = total.astype(BF16)

        @pl.when(i == 0)
        def _():
            last_ref[:, cols] = total[Q - 8 :]

    def group(g, db):
        when_at(i * GROUPS + g, plan)
        cols = pl.ds(pl.multiple_of(g * GW, GW), GW)
        log_wide = nn(log_parts, picks[:, cols])
        step_wide = nn(step_parts, picks[:, cols])
        done = cum_ref[c + 1, 0:1, cols]
        after = jnp.exp2(cum_ref[top, 0:1, cols] - done)
        grad = gnext_ref[0, :, cols].astype(F32) + after * gin[:, cols]
        low_g = grad.astype(BF16)
        decay = jnp.exp2(done - cum_ref[c, 0:1, cols])
        row = decay * jnp.sum(grad * entt_ref[0, :, cols].astype(F32), axis=0, keepdims=True)
        coarse = row.astype(BF16).astype(F32)
        r = rows_of((16, GW))
        two = jnp.where(r == 0, jnp.broadcast_to(coarse, (16, GW)), 0.0)
        two = jnp.where(r == 1, jnp.broadcast_to(row - coarse, (16, GW)), two)
        chosen = pick_heads(g)
        drow[...] += nn(two.astype(BF16), chosen)
        dweighted = nn(low_b, low_g)
        weights = []
        moves = []
        stepped = []
        dacts = []
        for j in range(2):
            pc = pl.ds(pl.multiple_of(g * GW + 128 * j, 128), 128)
            lp = log_wide[:, 128 * j : 128 * j + 128]
            sp = step_wide[:, 128 * j : 128 * j + 128]
            fade = jnp.exp2(lp[Q - 1 : Q, :] - lp)
            vp = vp_ref[:, pc].astype(F32)
            faded = dweighted[:, 128 * j : 128 * j + 128] * fade
            weights.append((vp * fade).astype(BF16))
            moves.append((faded * vp).astype(BF16))
            both = dvp_ref[:, pc].astype(F32) + faded
            stepped.append((both * val_ref[:, pc].astype(F32)).astype(BF16))
            dacts.append((pc, sp * both + skip_ref[:, pc] * ds_ref[:, pc].astype(F32)))
        dlw[...] += nn(jnp.concatenate(moves, 1), chosen)
        dst[...] += nn(jnp.concatenate(stepped, 1), chosen)
        for pc, dact in dacts:
            conv_back(pc, dact)
        return db + nt(jnp.concatenate(weights, 1), low_g)

    db = lax.fori_loop(0, GROUPS, group, dbc_ref[:, :N])
    conv_back(pl.ds(DI, N), db)
    conv_back(pl.ds(DI + N, N), dbc_ref[:, N:] + dc_ref[...])

    moved = dlw[...]
    at_last = jnp.sum(moved, axis=0, keepdims=True) + drow[0:1] + drow[1:2]
    dlog = dlp_ref[...] + dlt_ref[...] - moved
    dlog = dlog + jnp.where(rows_of(dlog.shape) == Q - 1, at_last, 0.0)
    square = (Q, Q)
    later = jnp.where(rows_of(square) <= lanes_of(square), 1.0, 0.0).astype(BF16)
    dsum = ordered_sum(later, dlog)
    rate = -jnp.exp(dl_ref[...])
    dstep = (dst[...] + dsum * rate) * valid_ref[...]
    raw = u_ref[:, CH:] + sb_ref[...]
    draw = dstep * (1.0 / (1.0 + jnp.exp(-raw)))
    draw = jnp.where(lanes_of(draw.shape) < HEADS, draw, 0.0)
    du_ref[:, CH:] = draw.astype(BF16)
    small_ref[0:1] += jnp.sum(draw, axis=0, keepdims=True)
    small_ref[1:2] += jnp.sum(dsum * step_ref[...], axis=0, keepdims=True) * rate

    @pl.when(c == 0)
    def _():
        epad[0:8, :] = jnp.zeros((8, CH), F32)
        epad[8:16, :] = head[...]
        x = halo_ref[:, :CH] * keep_ref[0, 0]
        total = jnp.zeros((8, CH), F32)
        for j in range(CONVK):
            k = CONVK - 1 - j
            moved = epad[j : j + 8, :]
            sums_ref[k : k + 1, :] += jnp.sum(moved * x, axis=0, keepdims=True)
            total = total + cw_ref[k : k + 1, :] * moved
        edge_ref[...] = total * keep_ref[0, 0]


def spec(block, index):
    return pl.BlockSpec(block, index)


def whole(shape):
    return pl.BlockSpec(shape, lambda *_: (0,) * len(shape))


def scalar():
    return pl.BlockSpec(memory_space=pltpu.SMEM)


def shaped(shape, kind):
    return jax.ShapeDtypeStruct(shape, kind)


def cost(flops, moved):
    return pl.CostEstimate(flops=int(flops), bytes_accessed=int(moved), transcendentals=0)


def params(number=None):
    return pltpu.CompilerParams(
        dimension_semantics=("arbitrary",), vmem_limit_bytes=60 * 1024 * 1024, collective_id=number,
        has_side_effects=number is not None,
    )


LINE = 4


def my_place():
    f = lax.axis_index("fsdp")
    t = lax.axis_index("ctx")
    return f // 2, f % 2, t // 2, t % 2


def device_at(z, y, x, core):
    return {"fsdp": z * 2 + y, "ctx": x * 2 + core}


def order_of(z, y, x, core):
    return (z * 2 + y) * 4 + x * 2 + core


def box_peers():
    z, y, x, core = my_place()
    return [
        (None, device_at(z, y, x, 1 - core)), (None, device_at(z, y, 1 - x, core)),
        (None, device_at(z, 1 - y, x, core)),
        (z > 0, device_at(z - 1, y, x, core)), (z < LINE - 1, device_at(z + 1, y, x, core)),
    ]


def plane_peers():
    z, y, x, core = my_place()
    turns = [(a, b, c) for a in range(2) for b in range(2) for c in range(2) if a + b + c]
    return [(None, device_at(z, (y + a) % 2, (x + b) % 2, (core + c) % 2)) for a, b, c in turns]


def line_peers():
    z, y, x, core = my_place()
    ups = [(z + r < LINE, device_at(z + r, y, x, core)) for r in range(1, LINE)]
    return ups + [(z - r >= 0, device_at(z - r, y, x, core)) for r in range(1, LINE)]


def meet(peers):
    barrier = pltpu.get_barrier_semaphore()
    count = 0
    for valid, peer in peers:

        def greet(peer=peer):
            pl.semaphore_signal(barrier, inc=1, device_id=peer, device_id_type=pl.DeviceIdType.MESH)

        if valid is None:
            greet()
            count = count + 1
        else:
            pl.when(valid)(greet)
            count = count + jnp.where(valid, 1, 0)
    pl.semaphore_wait(barrier, count)


def send(src, dst, send_sem, recv_sem, peer):
    return pltpu.make_async_remote_copy(
        src_ref=src, dst_ref=dst, send_sem=send_sem, recv_sem=recv_sem,
        device_id=device_at(*peer), device_id_type=pl.DeviceIdType.MESH,
    )


class Gather:
    def __init__(self, own, out, window, recv, halves, twin, sent, here):
        first, self.width, self.at = window
        self.own, self.out, self.rows = own.at[:, pl.ds(first, self.width)], out, own.shape[0]
        self.recv, self.halves, self.twin, self.sent, self.here = recv, halves, twin, sent, here
        self.place = my_place()

    def block(self, z, y, x, core, half=None):
        size = self.rows if half is None else self.rows // 2
        start = order_of(z, y, x, core) * self.rows + (0 if half is None else half * size)
        return self.out.at[pl.ds(pl.multiple_of(start, 16), size), pl.ds(self.at, self.width)]

    def copy(self, origin, way, half=None, own=False):
        z, y, x, core = self.place
        oz, oy, ox = origin
        o = oz * 4 + oy * 2 + ox
        dst = self.block(oz, oy, ox, core, half)
        src = self.own if own else dst
        peer = {
            "up": (z + 1, y, x, core), "down": (z - 1, y, x, core), "x": (z, y, 1 - x, core),
            "y": (z, 1 - y, x, core), "twin": (z, y, x, 1 - core),
        }[way]
        sem = self.sent.at[("up", "down", "x", "y", "twin").index(way), o]
        if way == "twin":
            arrival = self.twin.at[o]
        elif half is not None:
            arrival = self.halves.at[half, o]
        else:
            arrival = self.recv.at[o]
        return send(src, dst, sem, arrival, peer)

    def arrived(self, origin, half=None):
        self.copy(origin, "x", half).wait_recv()

    def column(self, r):
        z = self.place[0]
        if r == 0:
            return [(None, z, True, True)]
        return [(z - r >= 0, z - r, True, False), (z + r < LINE, z + r, False, True)]

    def each(self, r, act):
        for valid, oz, below, above in self.column(r):
            if valid is None:
                act(oz, below, above)
            else:
                pl.when(valid)(lambda oz=oz, below=below, above=above: act(oz, below, above))

    def begin(self):
        z, y, x, core = self.place
        pltpu.make_async_copy(self.own, self.block(z, y, x, core), self.here).start()
        self.forward(0)

    def ways(self, oz, below, above, act):
        z = self.place[0]
        if below:
            pl.when(z < LINE - 1)(lambda: act("up"))
        if above:
            pl.when(z > 0)(lambda: act("down"))
        act("x")
        act("y")
        act("twin")

    def forward(self, r):
        z, y, x, core = self.place

        def act(oz, below, above):
            origin = (oz, y, x)
            if r:
                self.arrived(origin)
            self.ways(oz, below, above, lambda way: self.copy(origin, way, own=r == 0).start())

        self.each(r, act)

    def across(self, r):
        z, y, x, core = self.place

        def act(oz, below, above):
            self.arrived((oz, y, 1 - x))
            self.copy((oz, y, 1 - x), "y", 0).start()
            self.copy((oz, y, 1 - x), "twin").start()
            self.arrived((oz, 1 - y, x))
            self.copy((oz, 1 - y, x), "x", 1).start()
            self.copy((oz, 1 - y, x), "twin").start()

        self.each(r, act)

    def corner(self, r):
        z, y, x, core = self.place

        def act(oz, below, above):
            origin = (oz, 1 - y, 1 - x)
            self.arrived(origin, 0)
            self.arrived(origin, 1)
            self.copy(origin, "twin").start()

        self.each(r, act)

    def finish(self):
        z, y, x, core = self.place
        pltpu.make_async_copy(self.own, self.block(z, y, x, core), self.here).wait()
        for r in range(LINE):

            def act(oz, below, above, r=r):
                self.ways(oz, below, above, lambda way: self.copy((oz, y, x), way, own=r == 0).wait_send())
                self.copy((oz, y, 1 - x), "y", 0).wait_send()
                self.copy((oz, 1 - y, x), "x", 1).wait_send()
                for oy, ox in ((y, 1 - x), (1 - y, x), (1 - y, 1 - x)):
                    self.copy((oz, oy, ox), "twin").wait_send()
                for oy, ox in ((y, x), (y, 1 - x), (1 - y, x), (1 - y, 1 - x)):
                    self.copy((oz, oy, ox), "twin").wait_recv()

            self.each(r, act)

    def steps(self):
        return [
            self.begin,
            lambda: self.forward(1),
            lambda: self.across(0),
            lambda: self.forward(2),
            lambda: self.across(1),
            lambda: (self.forward(3), self.corner(0)),
            lambda: self.across(2),
            lambda: self.corner(1),
            lambda: self.across(3),
            lambda: (self.corner(2), self.corner(3)),
            self.finish,
        ]


def gather_scratch():
    dma = pltpu.SemaphoreType.DMA
    return [dma((16,)), dma((2, 16)), dma((16,)), dma((5, 16)), dma(())]


U_WINDOWS = ((DI, 1280, 0), (DI + 1280, UW - 1280, 1280))


def gather_kernel(own, tok_ref, gain_ref, out, normed_ref, turned_ref, near_rows, sems, *gather_sems):
    rows, width = tok_ref.shape
    meet(box_peers() + chain_peers())
    pos = lax.axis_index("ctx")
    last = pos == lax.axis_size("ctx") - 1
    lists = [Gather(own, out, window, *gather_sems[5 * k : 5 * k + 5]).steps() for k, window in enumerate(U_WINDOWS)]
    for each in lists:
        each[0]()
    halo = pass_on(tok_ref.at[pl.ds(rows - HALO, HALO)], near_rows, sems, 1)

    @pl.when(jnp.logical_not(last))
    def _():
        halo.start()

    def normed(values):
        wide = values.astype(F32)
        scale = lax.rsqrt(jnp.sum(wide * wide, axis=1, keepdims=True) * (1.0 / width) + epsilon)
        return wide * scale * gain_ref[...]

    def block(r, unused):
        here = pl.ds(pl.multiple_of(r * 128, 128), 128)
        values = normed(tok_ref[here, :])
        normed_ref[here, :] = values.astype(BF16)
        turned_ref[:, here] = values.T.astype(BF16)
        return unused

    def hops(at):
        for k, each in enumerate(lists):
            if 1 <= at - k < len(each):
                each[at - k]()

    parts = 4
    for at in range(parts):
        lax.fori_loop(at * rows // 128 // parts, (at + 1) * rows // 128 // parts, block, 0)
        hops(at + 1)

    @pl.when(pos > 0)
    def _():
        halo.wait_recv()

    @pl.when(pos == 0)
    def _():
        near_rows[...] = jnp.zeros_like(near_rows)

    normed_ref[rows:, :] = normed(near_rows[...]).astype(BF16)

    @pl.when(jnp.logical_not(last))
    def _():
        halo.wait_send()

    for at in range(parts + 1, len(lists[0]) + len(lists) - 1):
        hops(at)


def gathered(own, tokens, gain, number):
    rows, width = tokens.shape
    anywhere = pl.BlockSpec(memory_space=pl.ANY)
    vmem = pl.BlockSpec(memory_space=pltpu.VMEM)
    return pl.pallas_call(
        gather_kernel,
        in_specs=[anywhere, vmem, vmem],
        out_specs=[anywhere, vmem, vmem],
        out_shape=[
            shaped((32 * own.shape[0], UW), BF16), shaped((rows + HALO, width), BF16), shaped((width, rows), BF16),
        ],
        scratch_shapes=[pltpu.VMEM((HALO, width), BF16), pltpu.SemaphoreType.DMA((2,))] + gather_scratch() * 2,
        compiler_params=pltpu.CompilerParams(
            collective_id=number, has_side_effects=True, vmem_limit_bytes=60 * 1024 * 1024
        ),
        name="gather",
    )(own, tokens, gain)


class Scatter:
    def __init__(self, parts, out, got, kept, mixed_y, mixed_x, from_x, from_y, along, sems, fetched=None):
        self.parts, self.out = parts, out
        self.got, self.kept = got, kept
        self.mixed = (mixed_y, mixed_x)
        self.sides = (from_x, from_y)
        self.along = along
        self.twin_sent, self.twin_recv, self.sent, self.recv, self.line_sent, self.line_recv = sems
        self.place = my_place()
        self.rows = kept.shape[-2]
        self.last = kept.shape[0] - 1
        self.fetched = fetched

    def groups(self):
        z, y, x, core = self.place
        return [(1 - y, 1 - x), (y, 1 - x), (1 - y, x), (y, x)]

    def to_twin(self, k):
        z, y, x, core = self.place
        gy, gx = self.groups()[k]
        return send(
            self.parts.at[:, gy * 4 + gx * 2 + 1 - core], self.got.at[k], self.twin_sent.at[k], self.twin_recv.at[k],
            (z, y, x, 1 - core),
        )

    def fetch(self, k):
        z, y, x, core = self.place
        gy, gx = self.groups()[k]
        return pltpu.make_async_copy(
            self.parts.at[:, gy * 4 + gx * 2 + core], self.kept.at[k], self.fetched.at[k]
        )

    def begin(self):
        for k in range(4):
            self.to_twin(k).start()
        if self.fetched is not None:
            for k in range(4):
                self.fetch(k).start()

    def add(self, k, sources, first=0, rows=None):
        rows = self.rows if rows is None else rows
        pieces = rows // 16

        def piece(n, unused):
            b = n // pieces
            at = (n - b * pieces) * 16
            here = pl.ds(pl.multiple_of(first + at, 16), 16)
            total = None
            for source in sources:
                term = source(b, pl.multiple_of(at, 16), here).astype(F32)
                total = term if total is None else total + term
            self.kept[k, b, here] = total.astype(BF16)
            return unused

        lax.fori_loop(0, LINE * pieces, piece, 0)

    def own(self, k):
        return lambda b, at, here: self.kept[k, b, here]

    def both(self, k):
        z, y, x, core = self.place
        gy, gx = self.groups()[k]
        self.to_twin(k).wait_recv()
        mine = lambda b, at, here: self.parts[b, gy * 4 + gx * 2 + core, here]
        if self.fetched is not None:
            self.fetch(k).wait()
            mine = self.own(k)
        self.add(k, [mine, lambda b, at, here: self.got[k, b, here]])

    def corner_copy(self, half):
        z, y, x, core = self.place
        size = self.rows // 2
        src = self.kept.at[0, :, pl.ds(half * size, size)]
        peer = (z, 1 - y, x, core) if half == 0 else (z, y, 1 - x, core)
        return send(src, self.mixed[half], self.sent.at[half], self.recv.at[half], peer)

    def side_copy(self, k):
        z, y, x, core = self.place
        peer = (z, y, 1 - x, core) if k == 1 else (z, 1 - y, x, core)
        return send(self.kept.at[k], self.sides[k - 1], self.sent.at[1 + k], self.recv.at[1 + k], peer)

    def corners(self):
        self.both(0)
        self.corner_copy(0).start()
        self.corner_copy(1).start()
        self.both(1)
        self.both(2)
        self.both(3)

    def sides_out(self):
        size = self.rows // 2
        for half, k in ((0, 1), (1, 2)):
            self.corner_copy(half).wait_recv()
            self.add(
                k, [self.own(k), lambda b, at, here, half=half: self.mixed[half][b, pl.ds(at, 16)]],
                half * size, size,
            )
            self.side_copy(k).start()

    def sides_in(self):
        self.side_copy(1).wait_recv()
        self.side_copy(2).wait_recv()
        self.add(
            3,
            [
                self.own(3), lambda b, at, here: self.sides[0][b, here], lambda b, at, here: self.sides[1][b, here],
            ],
        )

    def line_copy(self, origin, target):
        z, y, x, core = self.place
        return send(
            self.kept.at[self.last, target], self.along.at[origin], self.line_sent.at[target],
            self.line_recv.at[origin], (target, y, x, core),
        )

    def others(self, act):
        z = self.place[0]
        for r in range(1, LINE):
            pl.when(z + r < LINE)(lambda r=r: act(z + r))
            pl.when(z - r >= 0)(lambda r=r: act(z - r))

    def line(self):
        z = self.place[0]
        self.others(lambda target: self.line_copy(z, target).start())

    def plane_sent(self):
        for k in range(4):
            self.to_twin(k).wait_send()
        for half in range(2):
            self.corner_copy(half).wait_send()
        for k in (1, 2):
            self.side_copy(k).wait_send()

    def hand_on(self, out):
        self.sides_in()
        out[...] = self.kept[self.last]
        self.plane_sent()

    def line_done(self):
        z = self.place[0]
        self.out[...] = self.kept[self.last, z].astype(F32)

        def arrive(origin):
            self.line_copy(origin, z).wait_recv()
            self.out[...] += self.along[origin].astype(F32)

        self.others(arrive)
        self.others(lambda target: self.line_copy(z, target).wait_send())

    def finish(self):
        self.line_done()
        self.plane_sent()

    def steps(self):
        return [
            self.begin, self.corners, self.sides_out, lambda: (self.sides_in(), self.line()), self.finish,
        ]


def scatter_scratch(rows, columns):
    dma = pltpu.SemaphoreType.DMA
    half = rows // 2
    return [
        pltpu.VMEM((4, LINE, rows, columns), BF16),
        pltpu.VMEM((4, LINE, rows, columns), BF16),
        pltpu.VMEM((LINE, half, columns), BF16),
        pltpu.VMEM((LINE, half, columns), BF16),
        pltpu.VMEM((LINE, rows, columns), BF16),
        pltpu.VMEM((LINE, rows, columns), BF16),
        pltpu.VMEM((LINE, rows, columns), BF16),
        dma((4,)), dma((4,)), dma((4,)), dma((4,)), dma((LINE,)), dma((LINE,)),
    ]


class Quick:
    def __init__(self, own, out, plane, line, sems):
        self.own, self.out, self.plane, self.along = own, out, plane, line
        self.sent, self.recv, self.line_sent, self.line_recv = sems
        self.place = my_place()

    def peers(self):
        z, y, x, core = self.place
        turns = [(a, b, c) for a in range(2) for b in range(2) for c in range(2) if a + b + c]
        return [((y + a) % 2, (x + b) % 2, (core + c) % 2) for a, b, c in turns]

    def copy(self, origin, target):
        z = self.place[0]
        number = lambda where: where[0] * 4 + where[1] * 2 + where[2]
        return send(
            self.own, self.plane.at[number(origin)], self.sent.at[number(target)], self.recv.at[number(origin)],
            (z,) + tuple(target),
        )

    def begin(self):
        here = self.place[1:]
        self.plane[here[0] * 4 + here[1] * 2 + here[2]] = self.own[...]
        for peer in self.peers():
            self.copy(here, peer).start()

    def line_copy(self, origin, target):
        z, y, x, core = self.place
        return send(
            self.along.at[z], self.along.at[origin], self.line_sent.at[target], self.line_recv.at[origin],
            (target, y, x, core),
        )

    def others(self, act):
        z = self.place[0]
        for r in range(1, LINE):
            pl.when(z + r < LINE)(lambda r=r: act(z + r))
            pl.when(z - r >= 0)(lambda r=r: act(z - r))

    def turn(self):
        z, here = self.place[0], self.place[1:]
        for peer in self.peers():
            self.copy(peer, here).wait_recv()
        total = self.plane[0]
        for k in range(1, 8):
            total = total + self.plane[k]
        self.along[z] = total
        self.others(lambda target: self.line_copy(z, target).start())

    def finish(self):
        z, here = self.place[0], self.place[1:]
        self.others(lambda origin: self.line_copy(origin, z).wait_recv())
        total = self.along[0]
        for k in range(1, LINE):
            total = total + self.along[k]
        self.out[...] = total
        for peer in self.peers():
            self.copy(here, peer).wait_send()
        self.others(lambda target: self.line_copy(z, target).wait_send())


class Total:
    def __init__(self, own, out, held, got, sent, recv):
        self.own, self.out, self.held, self.got, self.sent, self.recv = own, out, held, got, sent, recv

    def copy(self, k):
        z, y, x, core = my_place()
        near = z + 1 - 2 * (z % 2)
        peer = [
            (z, y, x, 1 - core), (z, y, 1 - x, core), (z, 1 - y, x, core), (near, y, x, core),
            ((z + 2) % LINE, y, x, core),
        ][k]
        return send(self.own if k == 0 else self.held.at[k], self.got.at[k], self.sent.at[k], self.recv.at[k], peer)

    def begin(self):
        self.copy(0).start()

    def turn(self, k):
        self.copy(k).wait_recv()
        mine = self.own[...] if k == 0 else self.held[k]
        total = mine + self.got[k]
        if k < 4:
            self.held[k + 1] = total
            self.copy(k + 1).start()
        else:
            self.out[...] = total

    def finish(self):
        for k in range(5):
            self.copy(k).wait_send()

    def steps(self):
        return [self.begin] + [lambda k=k: self.turn(k) for k in range(5)] + [self.finish]


WIDE = 512
PIECES = ((0, 1024), (1024, 1024), (2048, UW - 2048))


def patched(values, fixed, first):
    count = values.shape[0]
    end = values[count - 16 :].astype(F32)
    own = jnp.logical_and(rows_of(end.shape) >= 8, lanes_of(end.shape) + first < CH)
    chosen = jnp.where(own, fixed, end)
    return jnp.concatenate([values[: count - 16], chosen.astype(BF16)], 0)


def final_kernel(*refs):
    (
        turned_ref, du_cols, dz_ref, du_ref, tok_ref, gain_ref, wz_any, wu_any, gate_ref, conv_ref, gsum_ref,
        small_ref, last_ref, edge_ref,
    ) = refs[:14]
    grad_ref, inw_ref, sums_ref, norm_ref = refs[14:18]
    (
        wz, wu, sems, parts_a, parts_b, parts_c, out_a, out_b, out_c, packed, normed_grad, held, got, sent, recv, gains,
        gains_plane, gains_line, gains_sent, gains_recv, gains_out, gains_in, fixed, edge_got, edge_sems, du_block,
    ) = refs[18:44]
    i = pl.program_id(0)
    steps = pl.num_programs(0) - tok_blocks(turned_ref)
    z, y, x, core = my_place()
    scr_a, scr_b, scr_c = refs[44:57], refs[57:70], refs[70:83]
    sum_a = Scatter(parts_a, out_a, *scr_a[:7], scr_a[7:])
    sum_b = Scatter(parts_b, out_b, *scr_b[:7], scr_b[7:])
    sum_c = Scatter(parts_c, out_c, *scr_c[:7], scr_c[7:])
    small = Total(packed, sums_ref, held, got, sent, recv)
    norm = Quick(gains, norm_ref, gains_plane, gains_line, (gains_sent, gains_recv, gains_out, gains_in))
    load_z = pltpu.make_async_copy(wz_any, wz, sems.at[0])
    load_u = pltpu.make_async_copy(wu_any, wu, sems.at[1])

    @pl.when(i == 0)
    def _():
        load_z.start()
        load_u.start()
        meet(plane_peers() + line_peers() + chain_peers())
        packed[...] = jnp.zeros_like(packed)
        packed[0:5, :] = conv_ref[0:5, :]
        packed[5:6, :DI] = gsum_ref[0:1, :]
        packed[5:6, DI : DI + 128] = small_ref[0:1, :]
        packed[5:6, DI + 128 :] = small_ref[1:2, :]
        packed[6:7, :DI] = gsum_ref[1:2, :]
        pos = lax.axis_index("ctx")
        back_edge = pass_on(edge_ref, edge_got, edge_sems, -1)

        @pl.when(pos > 0)
        def _():
            back_edge.start()

        gains[...] = jnp.zeros_like(gains)
        small.begin()
        inw_ref[:, :DI] = gate_ref[...]
        fixed[...] = jnp.zeros_like(fixed)
        fixed[8:16, :CH] = last_ref[...]

        @pl.when(pos < lax.axis_size("ctx") - 1)
        def _():
            back_edge.wait_recv()
            fixed[8:16, :CH] += edge_got[...]

        @pl.when(pos > 0)
        def _():
            back_edge.wait_send()

    first = [
        (8, lambda: (sum_a.begin(), small.turn(0))), (12, sum_a.corners), (16, lambda: (sum_b.begin(), small.turn(1))),
    ]
    second = [
        (20, lambda: (sum_a.sides_out(), sum_c.begin())), (22, sum_b.corners), (23, lambda: small.turn(2)),
        (24, sum_c.corners), (26, lambda: small.turn(3)), (28, sum_b.sides_out),
        (29, lambda: (sum_a.sides_in(), sum_a.line())), (30, lambda: small.turn(4)), (31, sum_c.sides_out),
    ]

    @pl.when(i < steps)
    def _():
        when_at(4 * i, first)
        at = pl.ds(pl.multiple_of(i * WIDE, WIDE), WIDE)
        result = nn(turned_ref[...], patched(du_cols[...], fixed[:, at], i * WIDE)).astype(BF16)
        rows = parts_a.shape[2]

        def keep(parts, cols, width):
            for b in range(LINE):
                for q in range(8):
                    first = (b * 8 + q) * rows
                    parts[b, q, :, cols] = result[first : first + rows, :width]

        for parts, (begin, count) in zip((parts_a, parts_b, parts_c), PIECES):
            for at in range(0, count, WIDE):
                wide = min(WIDE, count - at)

                @pl.when(i == (begin + at) // WIDE)
                def _(parts=parts, at=at, wide=wide):
                    keep(parts, slice(at, at + wide), wide)

    @pl.when(i == steps)
    def _():
        load_z.wait()
        load_u.wait()

    @pl.when(i >= steps)
    def _():
        width = tok_ref.shape[1]
        chunk = width // 4
        at_end = i == pl.num_programs(0) - 1
        du_block[:, :CH] = patched(du_ref[:, :CH], fixed[:, :CH], jnp.where(at_end, 0, CH))
        du_block[:, CH:] = du_ref[:, CH:]

        def part(n, unused):
            when_at(4 * i + n, second)
            feats = pl.ds(pl.multiple_of(n * chunk, chunk), chunk)
            normed_grad[:, feats] = nt(dz_ref[...], wz[feats, :]) + nt(du_block[...], wu[feats, :])
            return unused

        lax.fori_loop(0, 4, part, 0)
        values = tok_ref[...].astype(F32)
        scale = lax.rsqrt(jnp.sum(values * values, axis=1, keepdims=True) * (1.0 / width) + epsilon)
        hat = values * scale
        grad = normed_grad[...]
        gains[...] += jnp.sum(grad * hat, axis=0, keepdims=True)
        inner = grad * gain_ref[...]
        mean = jnp.sum(inner * hat, axis=1, keepdims=True) * (1.0 / width)
        grad_ref[...] = (scale * (inner - hat * mean)).astype(BF16)

    @pl.when(i == pl.num_programs(0) - 1)
    def _():
        norm.begin()
        sum_b.sides_in()
        sum_b.line()
        norm.turn()
        sum_c.sides_in()
        sum_c.line()
        sum_a.finish()
        norm.finish()
        sum_b.finish()
        sum_c.finish()
        small.finish()
        for out, (begin, count) in zip((out_a, out_b, out_c), PIECES):
            count = min(count, DPROJ - DI - begin)
            inw_ref[:, DI + begin : DI + begin + count] = out[:, :count]


def tok_blocks(turned_ref):
    return turned_ref.shape[1] // Q


def final(turned, du, dz, tokens, gain, w_z, w_u, gate_columns, conv_sums, gate_sums, small, last, edge, number):
    width, rows = turned.shape
    steps = -(-UW // WIDE)
    blocks = rows // Q
    dma = pltpu.SemaphoreType.DMA
    own = width // 32
    anywhere = pl.BlockSpec(memory_space=pl.ANY)
    later = lambda i: (jnp.maximum(i - steps, 0), 0)
    sums = (8, CH)
    return pl.pallas_call(
        final_kernel,
        grid=(steps + blocks,),
        in_specs=[
            whole((width, rows)),
            spec((rows, WIDE), lambda i: (0, jnp.minimum(i, steps - 1))),
            spec((Q, DI), later),
            spec((Q, UW), later),
            spec((Q, width), later),
            whole((1, width)),
            anywhere,
            anywhere,
            whole((own, DI)),
            whole(sums),
            whole((8, DI)),
            whole((8, 128)),
            whole((8, CH)),
            whole((8, CH)),
        ],
        out_specs=[spec((Q, width), later), whole((own, DPROJ)), whole(sums), whole((1, width))],
        out_shape=[
            shaped((rows, width), BF16), shaped((own, DPROJ), F32), shaped(sums, F32), shaped((1, width), F32),
        ],
        scratch_shapes=[
            pltpu.VMEM((width, DI), BF16),
            pltpu.VMEM((width, UW), BF16),
            dma((2,)),
            *[pltpu.VMEM((LINE, 8, own, count), BF16) for begin, count in PIECES],
            *[pltpu.VMEM((own, count), F32) for begin, count in PIECES],
            pltpu.VMEM(sums, F32),
            pltpu.VMEM((Q, width), F32),
            pltpu.VMEM((5,) + sums, F32),
            pltpu.VMEM((5,) + sums, F32),
            dma((5,)),
            dma((5,)),
            pltpu.VMEM((1, width), F32),
            pltpu.VMEM((8, 1, width), F32),
            pltpu.VMEM((LINE, 1, width), F32),
            dma((8,)),
            dma((8,)),
            dma((LINE,)),
            dma((LINE,)),
            pltpu.VMEM((16, -(-UW // WIDE) * WIDE), F32),
            pltpu.VMEM((8, CH), F32),
            dma((2,)),
            pltpu.VMEM((Q, UW), BF16),
        ]
        + [each for begin, count in PIECES for each in scatter_scratch(own, count)],
        compiler_params=params(number),
        cost_estimate=cost(20e9, 60e6),
        name="final",
    )(turned, du, dz, du, tokens, gain, w_z, w_u, gate_columns, conv_sums, gate_sums, small, last, edge)


def close_kernel(
    part_ref, cot_ref, inw_in, outw_in, sums_ref, norm_in, back_in,
    grad_ref, inw_ref, outw_ref, norm_ref, taps_ref, shift_ref, bias_ref, decay_ref, skip_ref, gate_ref,
):
    grad_ref[...] = cot_ref[...].astype(F32) + part_ref[...].astype(F32)

    @pl.when(pl.program_id(0) == 0)
    def _():
        inw_ref[...] = inw_in[...]
        outw_ref[...] = outw_in[...]
        norm_ref[...] = norm_in[0]
        taps_ref[...] = sums_ref[:CONVK]
        shift_ref[...] = sums_ref[CONVK]
        bias_ref[...] = sums_ref[5, DI : DI + 128]
        decay_ref[...] = sums_ref[5, DI + 128 :]
        gate_ref[...] = sums_ref[5, :DI]
        lane = lanes_of((1, 128))
        total = jnp.zeros((1, 128), F32)
        for h in range(HEADS):
            here = jnp.sum(back_in[6:7, h * P_SIZE : (h + 1) * P_SIZE], axis=1, keepdims=True)
            total = jnp.where(lane == h, here, total)
        skip_ref[...] = total[0]


def close(part, cotangent, inw, outw, sums, norm):
    rows, width = part.shape
    at = lambda i: (i, 0)
    line = lambda n: pl.BlockSpec((n,), lambda i: (0,))
    return pl.pallas_call(
        close_kernel,
        grid=(rows // Q,),
        in_specs=[
            spec((Q, width), at), spec((Q, width), at), whole(inw.shape), whole(outw.shape), whole(sums.shape),
            whole(norm.shape), whole(sums.shape),
        ],
        out_specs=[
            spec((Q, width), at), whole(inw.shape), whole(outw.shape), line(width), whole((CONVK, CH)), line(CH),
            line(128), line(128), line(128), line(DI),
        ],
        out_shape=[
            shaped((rows, width), F32), shaped(inw.shape, F32), shaped(outw.shape, F32), shaped((width,), F32),
            shaped((CONVK, CH), F32), shaped((CH,), F32), shaped((128,), F32), shaped((128,), F32),
            shaped((128,), F32), shaped((DI,), F32),
        ],
        compiler_params=params(),
        name="close",
    )(part, cotangent, inw, outw, sums, norm, sums)


def local(
    tokens,
    valid_mask,
    stretch_start,
    cotangent,
    norm_gain,
    in_weight,
    conv_weight,
    conv_bias,
    step_bias,
    decay_log,
    skip_gain,
    gate_gain,
    out_weight,
):
    axes = ("fsdp", "ctx")
    rows, width = tokens.shape
    blocks = rows // Q
    near = lax.axis_size("ctx")
    boxed = lax.axis_size("fsdp") == 8 and near == 4
    if boxed:
        own = jnp.pad(in_weight, ((0, 0), (0, UW + DI - DPROJ)))
        w_u, normed_more, turned = gathered(own, tokens, norm_gain.reshape(1, width), 1)
        later = [own, out_weight]
        later_widths = [DI, width]
    else:
        own_u = jnp.pad(in_weight[:, DI:], ((0, 0), (0, UW - (DPROJ - DI))))
        w_u, w_z, w_o = [
            lax.all_gather(a, axes, axis=0, tiled=True) for a in (own_u, in_weight[:, :DI], out_weight)
        ]
        later = []
        later_widths = []
        halo_tokens = lax.ppermute(tokens[rows - HALO :], "ctx", [(k, k + 1) for k in range(near - 1)])
        wide = jnp.concatenate([tokens, halo_tokens], 0).astype(F32)
        scale = lax.rsqrt(jnp.mean(wide * wide, axis=-1, keepdims=True) + epsilon)
        normed_more = (wide * scale * norm_gain).astype(BF16)
    extra = len(later)
    anywhere = pl.BlockSpec(memory_space=pl.ANY)

    normed = normed_more[:rows]
    valid = jnp.broadcast_to(valid_mask.astype(F32)[:, None], (rows, 128))
    keep = (1.0 - stretch_start[0].astype(F32)).reshape(1, 1)
    taps = conv_weight

    same = lambda c: (c, 0)
    same3 = lambda c: (c, 0, 0)
    one = lambda i: (jnp.minimum(i, blocks - 1), 0)
    one3 = lambda i: (jnp.minimum(i, blocks - 1), 0, 0)
    two = lambda i: (jnp.maximum(i - blocks, 0), 0)
    val, vp, conv, bc, ssd, ent, logd, step, cum, start, u, ahead, *filled = pl.pallas_call(
        lambda *refs: forward_kernel(extra, *refs),
        grid=(2 * blocks,),
        in_specs=[
            spec((Q, width), one),
            spec((HALO, width), lambda c: (rows // HALO, 0)),
            anywhere,
            spec((Q, 128), one),
            scalar(),
            whole((CONVK, CH)),
            whole((CH,)),
            whole((HEADS,)),
            whole((HEADS,)),
            scalar(),
        ]
        + [anywhere] * extra,
        out_specs=[
            spec((Q, DI), one),
            spec((Q, DI), one),
            spec((Q, CH), one),
            spec((Q, 2 * N), one),
            spec((Q, DI), two),
            spec((1, N, DI), one3),
            spec((Q, 128), one),
            spec((Q, 128), one),
            whole((blocks + 1, 8, DI)),
            whole((N, DI)),
            spec((Q, UW), one),
            whole((8, UW)),
        ]
        + [anywhere] * extra,
        out_shape=[
            shaped((rows, DI), BF16),
            shaped((rows, DI), BF16),
            shaped((rows, CH), BF16),
            shaped((rows, 2 * N), BF16),
            shaped((rows, DI), BF16),
            shaped((blocks, N, DI), BF16),
            shaped((rows, 128), F32),
            shaped((rows, 128), F32),
            shaped((blocks + 1, 8, DI), F32),
            shaped((N, DI), BF16),
            shaped((rows, UW), F32),
            shaped((8, UW), F32),
        ]
        + [shaped((32 * a.shape[0], n), a.dtype) for a, n in zip(later, later_widths)],
        scratch_shapes=[
            pltpu.VMEM((8, CH), F32),
            pltpu.VMEM((GROUPS, Q, 128), F32),
            pltpu.VMEM((128, DI), BF16),
            pltpu.VMEM((GROUPS, 8, Q), F32),
            pltpu.VMEM((Q, Q), F32),
            pltpu.VMEM((N, DI), F32),
            pltpu.VMEM((blocks, Q, DI), BF16),
            pltpu.VMEM((blocks, Q, DI), BF16),
            pltpu.VMEM((blocks, Q, 2 * N), BF16),
            pltpu.VMEM((blocks, Q, 128), F32),
            pltpu.VMEM((N, DI), BF16),
            pltpu.VMEM((N, DI), BF16),
            pltpu.SemaphoreType.DMA((2,)),
            pltpu.VMEM((w_u.shape[0], UW), BF16),
            pltpu.SemaphoreType.DMA(()),
            pltpu.VMEM((2, Q, GW), F32),
            pltpu.VMEM((2, Q, GW), F32),
            pltpu.VMEM((1, CH), F32),
            pltpu.VMEM((1, 128), F32),
            pltpu.VMEM((1, 128), F32),
            pltpu.VMEM((1, DI), F32),
        ]
        + gather_scratch() * extra,
        compiler_params=params(2),
        cost_estimate=cost(15e9, 60e6),
        name="forward",
    )(normed_more, normed_more, w_u, valid, keep, taps, conv_bias, step_bias, decay_log, skip_gain, *later)
    if later:
        w_z, w_o = filled

    z = jnp.dot(normed, w_z, preferred_element_type=F32).astype(BF16)
    back = lambda i: (blocks - 1 - i, 0)
    back3 = lambda i: (blocks - 1 - i, 0, 0)
    output, gated, branch_grad, ds, dz, entt, gnext, gout, dlp, dc, gate_sums = pl.pallas_call(
        gate_kernel,
        grid=(blocks,),
        in_specs=[
            whole((N, DI)),
            spec((Q, DI), back),
            spec((1, N, DI), back3),
            spec((Q, DI), back),
            spec((Q, DI), back),
            spec((Q, 2 * N), back),
            spec((Q, 128), back),
            whole((blocks + 1, 8, DI)),
            spec((Q, width), back),
            spec((Q, width), back),
            spec((Q, 128), back),
            anywhere,
            whole((DI,)),
        ],
        out_specs=[
            spec((Q, width), back),
            spec((Q, DI), back),
            spec((Q, width), back),
            spec((Q, DI), back),
            spec((Q, DI), back),
            spec((1, N, DI), back3),
            spec((1, N, DI), back3),
            whole((N, DI)),
            spec((Q, 128), back),
            spec((Q, N), back),
            whole((8, DI)),
        ],
        out_shape=[
            shaped((rows, width), BF16),
            shaped((rows, DI), BF16),
            shaped((rows, width), BF16),
            shaped((rows, DI), BF16),
            shaped((rows, DI), BF16),
            shaped((blocks, N, DI), BF16),
            shaped((blocks, N, DI), BF16),
            shaped((N, DI), BF16),
            shaped((rows, 128), F32),
            shaped((rows, N), F32),
            shaped((8, DI), F32),
        ],
        scratch_shapes=[
            pltpu.VMEM((N, DI), F32),
            pltpu.VMEM((N, DI), F32),
            pltpu.VMEM((128, DI), BF16),
            pltpu.VMEM((Q, DI), F32),
            pltpu.VMEM((Q, DI), F32),
            pltpu.VMEM((Q, DI), F32),
            pltpu.VMEM((Q, DI), F32),
            pltpu.VMEM((Q, DI), F32),
            pltpu.VMEM((Q, 128), F32),
            pltpu.VMEM((1, DI), F32),
            pltpu.VMEM((DI, width), BF16),
            pltpu.SemaphoreType.DMA(()),
        ],
        compiler_params=params(),
        cost_estimate=cost(15e9, 60e6),
        name="gate",
    )(
        start, ssd, ent, z, val, bc, logd, cum, tokens, cotangent, valid, w_o, gate_gain,
    )

    def columns_of(left, right):
        return lax.dot_general(
            left, right, (((0,), (0,)), ((), ())), preferred_element_type=F32
        ).astype(BF16)

    def in_blocks(a):
        return a.reshape(LINE, 8, a.shape[0] // 32, a.shape[1])

    out_weight_grad = columns_of(gated, branch_grad)
    gate_columns = columns_of(normed, dz)
    mixing_parts = [in_blocks(out_weight_grad)] if boxed else []

    dvp, dbc, dlt, gin, *summed_out = pl.pallas_call(
        lambda *refs: mixing_kernel(len(mixing_parts), *refs),
        grid=(blocks,),
        in_specs=[
            spec((Q, DI), same),
            spec((Q, DI), same),
            spec((Q, 2 * N), same),
            spec((Q, 128), same),
            scalar(),
            whole((N, DI)),
            whole((blocks + 1, 8, DI)),
        ]
        + [anywhere for a in mixing_parts],
        out_specs=[spec((Q, DI), same), spec((Q, 2 * N), same), spec((Q, 128), same), whole((N, DI))]
        + [whole((LINE,) + a.shape[-2:]) for a in mixing_parts],
        out_shape=[
            shaped((rows, DI), BF16), shaped((rows, 2 * N), F32), shaped((rows, 128), F32), shaped((N, DI), BF16),
        ]
        + [shaped((LINE,) + a.shape[-2:], BF16) for a in mixing_parts],
        scratch_shapes=[
            pltpu.VMEM((GROUPS, Q, 128), F32),
            pltpu.VMEM((GROUPS, 8, Q), F32),
            pltpu.VMEM((Q, Q), F32),
            pltpu.VMEM((Q, Q), F32),
            pltpu.VMEM((GROUPS, 8, Q), F32),
            pltpu.VMEM((128, Q), F32),
            pltpu.VMEM((GROUPS, Q, 128), F32),
            pltpu.VMEM((N, DI), BF16),
            pltpu.VMEM((N, DI), BF16),
            pltpu.SemaphoreType.DMA((2,)),
        ]
        + [each for a in mixing_parts for each in plane_scratch(*a.shape[-2:])],
        compiler_params=params(3),
        cost_estimate=cost(15e9, 60e6),
        name="mixing",
    )(ds, vp, bc, logd, keep, gout, cum, *mixing_parts)

    back_parts = summed_out + [in_blocks(gate_columns)] if boxed else []
    du, last, edge, conv_sums, small, *summed_gate = pl.pallas_call(
        lambda *refs: back_kernel(len(back_parts), *refs),
        grid=(blocks,),
        in_specs=[
            scalar(),
            whole((N, DI)),
            spec((1, N, DI), back3),
            spec((1, N, DI), back3),
            whole((blocks + 1, 8, DI)),
            spec((Q, DI), back),
            spec((Q, DI), back),
            spec((Q, DI), back),
            spec((Q, DI), back),
            spec((Q, CH), back),
            spec((Q, UW), back),
            whole((8, UW)),
            spec((Q, 2 * N), back),
            spec((Q, 128), back),
            spec((Q, 128), back),
            spec((Q, 128), back),
            spec((Q, 128), back),
            spec((Q, 128), back),
            spec((Q, 2 * N), back),
            spec((Q, N), back),
            whole((CONVK, CH)),
            whole((HEADS,)),
            whole((HEADS,)),
            scalar(),
        ]
        + [pl.BlockSpec(memory_space=pltpu.VMEM), anywhere][: len(back_parts)],
        out_specs=[
            spec((Q, UW), back),
            whole((8, CH)),
            whole((8, CH)),
            whole((8, CH)),
            whole((8, 128)),
        ]
        + [whole(a.shape[-2:]) for a in back_parts],
        out_shape=[
            shaped((rows, UW), BF16),
            shaped((8, CH), F32),
            shaped((8, CH), F32),
            shaped((8, CH), F32),
            shaped((8, 128), F32),
        ]
        + [shaped(a.shape[-2:], F32) for a in back_parts],
        scratch_shapes=[
            pltpu.VMEM((N, DI), F32),
            pltpu.VMEM((128, DI), BF16),
            pltpu.VMEM((8, CH), F32),
            pltpu.VMEM((16, CH), F32),
            pltpu.VMEM((Q, 128), F32),
            pltpu.VMEM((Q, 128), F32),
            pltpu.VMEM((16, 128), F32),
            pltpu.VMEM((1, 128), F32),
            pltpu.VMEM((1, 128), F32),
            pltpu.VMEM((1, DI), F32),
        ]
        + (
            scatter_scratch(*back_parts[1].shape[-2:])
            + line_scratch(*back_parts[0].shape[-2:])
            + [pltpu.SemaphoreType.DMA((4,))]
            if back_parts
            else []
        ),
        compiler_params=params(4 if back_parts else None),
        cost_estimate=cost(15e9, 60e6),
        name="back",
    )(
        keep, gin, gnext, entt, cum, vp, val, dvp, ds, conv, u, ahead, bc, logd, step, valid,
        dlp, dlt, dbc, dc, taps, step_bias, decay_log, skip_gain, *back_parts,
    )
    if boxed:
        out_weight_grad, gate_columns = summed_gate
        part, in_weight_grad, sums, norm_sum = final(
            turned, du, dz, tokens, norm_gain.reshape(1, width), w_z, w_u, gate_columns, conv_sums,
            gate_sums, small, last, edge, 5,
        )
        results = close(part, cotangent, in_weight_grad, out_weight_grad, sums, norm_sum)
        input_grad, in_weight_grad, out_weight_grad, norm_sum, taps_sum, shift_sum = results[:6]
        bias_sum, decay_sum, skip_sum, gate_sum = results[6:]
        return (
            output,
            input_grad,
            in_weight_grad,
            out_weight_grad,
            norm_sum,
            taps_sum,
            shift_sum,
            bias_sum[:HEADS],
            decay_sum[:HEADS],
            skip_sum[:HEADS],
            gate_sum,
        )
    edge_back = lax.ppermute(edge, "ctx", [(k + 1, k) for k in range(near - 1)])
    du = lax.dynamic_update_slice(du, (last + edge_back).astype(BF16), (rows - 8, 0))
    conv_columns = columns_of(normed, du)
    across = (((1,), (1,)), ((), ()))
    normed_grad = lax.dot_general(dz, w_z, across, preferred_element_type=F32) + lax.dot_general(
        du, w_u, across, preferred_element_type=F32
    )
    inputs = tokens.astype(F32)
    scale = lax.rsqrt(jnp.mean(inputs * inputs, axis=-1, keepdims=True) + epsilon)
    hat = inputs * scale
    inner = normed_grad * norm_gain
    input_grad = cotangent.astype(F32) + scale * (
        inner - hat * jnp.mean(inner * hat, axis=-1, keepdims=True)
    )
    norm_grad = jnp.sum(normed_grad * hat, axis=0)
    packed = jnp.concatenate(
        [
            norm_grad,
            conv_sums[:5].reshape(-1),
            gate_sums[:2].reshape(-1),
            small[:2].reshape(-1),
        ]
    )
    conv_columns, gate_columns, out_weight_grad = [
        lax.psum_scatter(a.astype(F32), axes, scatter_dimension=0, tiled=True)
        for a in (conv_columns, gate_columns, out_weight_grad)
    ]
    summed = lax.psum(packed, axes)
    in_weight_grad = jnp.concatenate([gate_columns, conv_columns[:, : DPROJ - DI]], 1)
    at = width
    conv_weight_grad = summed[at : at + CONVK * CH].reshape(CONVK, CH)
    at += CONVK * CH
    conv_bias_grad = summed[at : at + CH]
    at += CH
    gate_gain_grad = summed[at : at + DI]
    at += DI
    skip_gain_grad = jnp.sum(summed[at : at + DI].reshape(HEADS, P_SIZE), axis=1)
    at += DI
    step_bias_grad = summed[at : at + HEADS]
    decay_log_grad = summed[at + 128 : at + 128 + HEADS]
    return (
        output,
        input_grad,
        in_weight_grad,
        out_weight_grad,
        summed[:width],
        conv_weight_grad,
        conv_bias_grad,
        step_bias_grad,
        decay_log_grad,
        skip_gain_grad,
        gate_gain_grad,
    )


def solution(mesh):
    split = P(("fsdp", "ctx"), None)
    line = P(("fsdp", "ctx"))
    return jax.shard_map(
        local,
        mesh=mesh,
        in_specs=(split, line, line, split, P(), split, P(), P(), P(), P(), P(), P(), split),
        out_specs=(split, split, split, split, P(), P(), P(), P(), P(), P(), P()),
        check_vma=False,
    )
```
